32 devices in a mesh: fsdp: 8 (over z, core), seq: 4 (over y, x).
Axes of the slice: x: 2, y: 2, z: 4, core: 2. Of those that a mesh axis runs over, the one named last changes fastest.
Arguments:
- hidden: float32 [8, 1024, 2048], P('fsdp', 'seq'), may hold values from -6 to 6
- positions: int32 [8, 1024], P('fsdp', 'seq'), may hold values from 0 to 1023, as said below
- gains: float32 [1, 2, 2048], replicated, may hold values from 0.5 to 1.5
- w_qkv: bfloat16 [1, 2560, 2048], P(None, 'fsdp')
- w_out: bfloat16 [1, 2048, 2048], P(None, 'fsdp'), may hold values from -0.5 to 0.5
- w_gate_up: bfloat16 [1, 11264, 2048], P(None, 'fsdp'), may hold values from -0.125 to 0.125
- w_down: bfloat16 [1, 2048, 5632], P(None, 'fsdp'), may hold values from -0.078125 to 0.078125
- cotangent: float32 [8, 1024, 2048], P('fsdp', 'seq'), may hold values from -6 to 6
Outputs:
- hidden_out: float32 [8, 1024, 2048], P('fsdp', 'seq')
- grad_hidden: float32 [8, 1024, 2048], P('fsdp', 'seq')
- grad_gains: float32 [1, 2, 2048], replicated
- grad_w_qkv: float32 [1, 2560, 2048], P(None, 'fsdp')
- grad_w_out: float32 [1, 2048, 2048], P(None, 'fsdp')
- grad_w_gate_up: float32 [1, 11264, 2048], P(None, 'fsdp')
- grad_w_down: float32 [1, 2048, 5632], P(None, 'fsdp')
The draws below stay inside these ranges and needn't reach their ends.
Inputs may be any that keep to these rules, and one draw needn't show every extreme that they name: `positions`: within a sequence, a position is 0 where a document starts (always at the sequence's first token) and one more than the position before it elsewhere. Sequence 0 is a single document.
All inputs are finite; a program needn't handle non-finite values.
Results may differ from the reference program's by a relative error of at most 0.02.
Values may be sent and summed in bfloat16 or wider, within the bound.
A program may use at most 448 MiB of HBM per device.

```python
import math
import jax
import jax.numpy as jnp
from jax import lax

D = 2048
H = 32
KVH = 4
HD = 64
FF = 5632
LAYERS = 1
LEN = 1024
QKV = 2560
NSEQ = 8
N_SEQ = 4


def draw_w_qkv(key, part):
    base = jax.random.normal(key, (LAYERS, QKV, D), jnp.float32) * D ** (-0.5)
    return base.astype(jnp.bfloat16)


def draw_positions(key, part):
    marks = jax.random.randint(key, (NSEQ, LEN), 0, 96) == 0
    index = jnp.arange(LEN, dtype=jnp.int32)
    first_row = (jnp.arange(NSEQ) == 0)[:, None]
    marks = marks & jnp.logical_not(first_row) | (index == 0)[None, :]
    starts = lax.cummax(jnp.where(marks, index[None, :], 0), axis=1)
    return (index[None, :] - starts).astype(jnp.int32)


def steps_of(rng, shape, pieces, least, largest):
    level, own = 1.0, jax.random.fold_in(rng, 6)
    for position, blocks in pieces:
        steps = jnp.exp(jax.random.uniform(jax.random.fold_in(own, position), (blocks,), jnp.float32, least / len(pieces), largest / len(pieces)))
        level = level * jnp.repeat(steps, shape[position] // blocks).reshape([-1 if axis == position else 1 for axis in range(len(shape))])
    return level


def noise(stream_key, extent, spread, most, split=(), held_as=jnp.bfloat16):
    entries = spread * jax.random.normal(stream_key, extent, jnp.float32)
    if split:
        entries = entries * steps_of(stream_key, extent, split, -0.22, 0.18)
    return jnp.clip(entries, -most, most).astype(held_as)


def setup_inputs(seed: int = 0) -> dict:
    arg_keys = jax.random.split(jax.random.key(seed), 9)
    hidden = noise(arg_keys[0], (NSEQ, LEN, D), 1.0, 6.0, ((0, 8), (1, 4)), jnp.float32)
    positions = draw_positions(jax.random.fold_in(arg_keys[8], 71), 0)
    gains = jnp.clip(1.0 + 0.1 * jax.random.normal(arg_keys[2], (LAYERS, 2, D), jnp.float32), 0.5, 1.5)
    w_qkv = draw_w_qkv(jax.random.fold_in(arg_keys[8], 71), 0)
    w_out = noise(arg_keys[4], (LAYERS, D, D), (D // 16) ** -0.5, 0.5, ((1, 8),))
    w_gate_up = noise(arg_keys[5], (LAYERS, 2 * FF, D), D ** -0.5, 0.125, ((1, 8),))
    w_down = noise(arg_keys[6], (LAYERS, D, FF), FF ** -0.5, 0.078125, ((1, 8),))
    cotangent = noise(arg_keys[7], (NSEQ, LEN, D), 1.0, 6.0, ((0, 8), (1, 4)), jnp.float32)
    return dict(hidden=hidden, positions=positions, gains=gains, w_qkv=w_qkv, w_out=w_out, w_gate_up=w_gate_up, w_down=w_down, cotangent=cotangent)


EPS = 1e-05

def rope_tables(position_ids):
    halfway = HD // 2
    frequency = jnp.exp(jnp.arange(halfway, dtype=jnp.float32) * (-2.0 * math.log(10000.0) / HD))
    angles = position_ids.astype(jnp.float32)[..., None] * frequency
    cosines = jnp.cos(angles)
    sines = jnp.sin(angles)
    return (jnp.concatenate([cosines, cosines], -1)[..., None, :], jnp.concatenate([sines, sines], -1)[..., None, :])

def rotate(values, cosines, sines):
    halfway = values.shape[-1] // 2
    turned = jnp.concatenate([-values[..., halfway:], values[..., :halfway]], -1)
    return values * cosines + turned * sines

def unrotate(grads, cosines, sines):
    halfway = grads.shape[-1] // 2
    scaled = grads * sines
    return grads * cosines + jnp.concatenate([scaled[..., halfway:], -scaled[..., :halfway]], -1)

def normalize(values, gain):
    scale = lax.rsqrt(lax.optimization_barrier(jnp.mean(values * values, -1, keepdims=True)) + EPS)
    return ((values * scale * gain).astype(jnp.bfloat16), scale)

def normalize_back(grads, values, scale, gain):
    unit = values * scale
    gain_grad = lax.optimization_barrier(jnp.sum((grads * unit).reshape(-1, unit.shape[-1]), 0))
    inner = grads * gain
    return (scale * (inner - unit * lax.optimization_barrier(jnp.mean(inner * unit, -1, keepdims=True))), gain_grad)

def rounded(values):
    return lax.optimization_barrier(values.astype(jnp.bfloat16)).astype(jnp.float32)

def masked_scores(queries, keys_wide):
    scores = jnp.einsum('qhd,khd->hqk', queries.astype(jnp.float32), keys_wide.astype(jnp.float32), precision=lax.Precision.HIGHEST) * HD ** (-0.5)
    length = queries.shape[0]
    causal = jnp.arange(length)[:, None] >= jnp.arange(length)[None, :]
    return jnp.where(causal[None], scores, -1e+30)

def attend(queries, keys_in, values_in):
    share = H // KVH
    keys_wide = jnp.repeat(keys_in, share, axis=1)
    values_wide = jnp.repeat(values_in, share, axis=1)
    scores = masked_scores(queries, keys_wide)
    peak = lax.optimization_barrier(jnp.max(scores, -1, keepdims=True))
    log_total = peak[..., 0] + jnp.log(lax.optimization_barrier(jnp.sum(jnp.exp(scores - peak), -1)))
    weights = rounded(jnp.exp(scores - log_total[..., None]))
    output = jnp.einsum('hqk,khd->qhd', weights, values_wide.astype(jnp.float32), precision=lax.Precision.HIGHEST)
    return (output.astype(jnp.bfloat16), log_total)

def group_heads(per_head):
    length = per_head.shape[0]
    heads_dev = H // N_SEQ
    kv_dev = max(1, heads_dev // (H // KVH))
    repeat_count = N_SEQ * kv_dev // KVH
    partial_sums = lax.optimization_barrier(jnp.sum(per_head.reshape(length, N_SEQ * kv_dev, H // (N_SEQ * kv_dev), HD), 2))
    return lax.optimization_barrier(jnp.sum(rounded(partial_sums).reshape(length, KVH, repeat_count, HD), 2))

def attend_back(queries, keys_in, values_in, output, log_total, dattn):
    share = H // KVH
    keys_wide = jnp.repeat(keys_in, share, axis=1).astype(jnp.float32)
    values_wide = jnp.repeat(values_in, share, axis=1).astype(jnp.float32)
    scores = masked_scores(queries, keys_wide)
    probs = jnp.exp(scores - log_total[..., None])
    dattn_wide = dattn.astype(jnp.float32)
    delta = lax.optimization_barrier(jnp.sum(output.astype(jnp.float32) * dattn_wide, -1)).T
    dprob = jnp.einsum('qhd,khd->hqk', dattn_wide, values_wide, precision=lax.Precision.HIGHEST)
    dscore = rounded(probs * (dprob - delta[..., None]))
    dqueries = jnp.einsum('hqk,khd->qhd', dscore, keys_wide, precision=lax.Precision.HIGHEST) * HD ** (-0.5)
    dkeys = jnp.einsum('hqk,qhd->khd', dscore, queries.astype(jnp.float32), precision=lax.Precision.HIGHEST) * HD ** (-0.5)
    dvalues = jnp.einsum('hqk,qhd->khd', rounded(probs), dattn_wide, precision=lax.Precision.HIGHEST)
    return (rounded(dqueries), group_heads(dkeys), group_heads(dvalues))

def layer_forward(current, cosines, sines, gain, wqkv, wout, wgu, wdown):
    length = current.shape[0]
    normed, scale_one = normalize(current, gain[0])
    joint = jnp.dot(normed, wqkv.T, preferred_element_type=jnp.float32)
    queries = joint[:, :H * HD].reshape(length, H, HD)
    keys_in = joint[:, H * HD:(H + KVH) * HD].reshape(length, KVH, HD)
    values_in = joint[:, (H + KVH) * HD:].reshape(length, KVH, HD)
    q_rot = rotate(queries, cosines, sines).astype(jnp.bfloat16)
    k_rot = rotate(keys_in, cosines, sines).astype(jnp.bfloat16)
    v_kept = values_in.astype(jnp.bfloat16)
    output, log_total = attend(q_rot, k_rot, v_kept)
    attn_flat = output.reshape(length, H * HD)
    middle = current + jnp.dot(attn_flat, wout.T, preferred_element_type=jnp.float32)
    normed_two, scale_two = normalize(middle, gain[1])
    both = jnp.dot(normed_two, wgu.T, preferred_element_type=jnp.float32)
    gate_part = both[:, :FF]
    up_part = both[:, FF:]
    activated = (jax.nn.silu(gate_part) * up_part).astype(jnp.bfloat16)
    result = middle + jnp.dot(activated, wdown.T, preferred_element_type=jnp.float32)
    return (result, (normed, scale_one, q_rot, k_rot, v_kept, output, log_total, attn_flat, middle, normed_two, scale_two, gate_part, up_part, activated))

def layer_backward(flowing, saved, current, cosines, sines, gain, wqkv, wout, wgu, wdown):
    normed, scale_one, q_rot, k_rot, v_kept, output, log_total, attn_flat, middle, normed_two, scale_two, gate_part, up_part, activated = saved
    length = current.shape[0]
    dm_cast = flowing.astype(jnp.bfloat16)
    grad_down = jnp.dot(dm_cast.T, activated, preferred_element_type=jnp.float32)
    dact = jnp.dot(dm_cast, wdown, preferred_element_type=jnp.float32)
    sigma = jax.nn.sigmoid(gate_part)
    dgate = dact * up_part * sigma * (1.0 + gate_part * (1.0 - sigma))
    dup = dact * gate_part * sigma
    dgu = jnp.concatenate([dgate, dup], 1).astype(jnp.bfloat16)
    grad_gu = jnp.dot(dgu.T, normed_two, preferred_element_type=jnp.float32)
    dnormed_two = jnp.dot(dgu, wgu, preferred_element_type=jnp.float32)
    dmid_norm, gain_two = normalize_back(dnormed_two, middle, scale_two, gain[1])
    dmiddle = flowing + dmid_norm
    dy_cast = dmiddle.astype(jnp.bfloat16)
    grad_out = jnp.dot(dy_cast.T, attn_flat, preferred_element_type=jnp.float32)
    dattn = jnp.dot(dy_cast, wout, preferred_element_type=jnp.float32).astype(jnp.bfloat16).reshape(length, H, HD)
    dqueries, dkeys, dvalues = attend_back(q_rot, k_rot, v_kept, output, log_total, dattn)
    dq_pre = unrotate(dqueries, cosines, sines)
    dk_pre = unrotate(dkeys, cosines, sines)
    djoint = jnp.concatenate([dq_pre.reshape(length, -1), dk_pre.reshape(length, -1), dvalues.reshape(length, -1)], 1).astype(jnp.bfloat16)
    grad_qkv = jnp.dot(djoint.T, normed, preferred_element_type=jnp.float32)
    dnormed = jnp.dot(djoint, wqkv, preferred_element_type=jnp.float32)
    dcur_norm, gain_one = normalize_back(dnormed, current, scale_one, gain[0])
    return (dmiddle + dcur_norm, (grad_qkv, grad_out, grad_gu, grad_down), jnp.stack([gain_one, gain_two]))

def reference(hidden, positions, gains, w_qkv, w_out, w_gate_up, w_down, cotangent):

    def one_sequence(carry, inputs):
        tokens_in, position_ids, upstream = inputs
        cosines, sines = rope_tables(position_ids)
        layer_inputs = []
        kept = []
        current = tokens_in
        for layer_index in range(LAYERS):
            layer_inputs.append(current)
            current, saved = layer_forward(current, cosines, sines, gains[layer_index], w_qkv[layer_index], w_out[layer_index], w_gate_up[layer_index], w_down[layer_index])
            kept.append(saved)
        flowing = upstream
        running = list(carry)
        for layer_index in reversed(range(LAYERS)):
            flowing, weight_grads, gain_grads = layer_backward(flowing, kept[layer_index], layer_inputs[layer_index], cosines, sines, gains[layer_index], w_qkv[layer_index], w_out[layer_index], w_gate_up[layer_index], w_down[layer_index])
            for which_grad in range(4):
                running[which_grad] = running[which_grad].at[layer_index].add(weight_grads[which_grad])
            running[4] = running[4].at[layer_index].add(gain_grads)
        return (tuple(running), (current, flowing))
    start_sums = (jnp.zeros(w_qkv.shape, jnp.float32), jnp.zeros(w_out.shape, jnp.float32), jnp.zeros(w_gate_up.shape, jnp.float32), jnp.zeros(w_down.shape, jnp.float32), jnp.zeros(gains.shape, jnp.float32))
    totals, stacked = lax.scan(one_sequence, start_sums, (hidden, positions, cotangent))
    return (stacked[0], stacked[1], totals[4], totals[0], totals[1], totals[2], totals[3])
```

```python
import math

import jax
import jax.numpy as jnp
import numpy as np
from jax import lax
from jax.experimental import pallas as pl
from jax.experimental.pallas import tpu as pltpu
from jax.sharding import PartitionSpec as P


H = 32
KVH = 4
HD = 64
FF = 5632
LAYERS = 1


EPS = 1e-05


def rope_tables(position_ids):
    halfway = HD // 2
    frequency = jnp.exp(jnp.arange(halfway, dtype=jnp.float32) * (-2.0 * math.log(10000.0) / HD))
    angles = position_ids.astype(jnp.float32)[..., None] * frequency
    cosines = jnp.cos(angles)
    sines = jnp.sin(angles)
    return (
        jnp.concatenate([cosines, cosines], -1)[..., None, :],
        jnp.concatenate([sines, sines], -1)[..., None, :],
    )


def rotate(values, cosines, sines):
    halfway = values.shape[-1] // 2
    turned = jnp.concatenate([-values[..., halfway:], values[..., :halfway]], -1)
    return values * cosines + turned * sines


def unrotate(grads, cosines, sines):
    halfway = grads.shape[-1] // 2
    scaled = grads * sines
    return grads * cosines + jnp.concatenate([scaled[..., halfway:], -scaled[..., :halfway]], -1)


def normalize(values, gain):
    scale = lax.rsqrt(jnp.mean(values * values, -1, keepdims=True) + EPS)
    return ((values * scale * gain).astype(jnp.bfloat16), scale)


def normalize_back(grads, values, scale, gain):
    unit = values * scale
    gain_grad = jnp.sum((grads * unit).reshape(-1, unit.shape[-1]), 0)
    inner = grads * gain
    return (scale * (inner - unit * jnp.mean(inner * unit, -1, keepdims=True)), gain_grad)


def masked_scores(queries, keys_wide):
    scores = jnp.einsum(
        "qhd,khd->hqk", queries, keys_wide, preferred_element_type=jnp.float32
    ) * queries.shape[-1] ** (-0.5)
    length = queries.shape[0]
    causal = jnp.arange(length)[:, None] >= jnp.arange(length)[None, :]
    return jnp.where(causal[None], scores, -1e30)


def local_attend(operands):
    queries, keys_in, values_in = operands
    repeat_by = queries.shape[1] // keys_in.shape[1]
    keys_wide = jnp.repeat(keys_in, repeat_by, axis=1)
    values_wide = jnp.repeat(values_in, repeat_by, axis=1)
    scores = masked_scores(queries, keys_wide)
    peak = jnp.max(scores, -1, keepdims=True)
    log_total = peak[..., 0] + jnp.log(jnp.sum(jnp.exp(scores - peak), -1))
    weights = jnp.exp(scores - log_total[..., None]).astype(jnp.bfloat16)
    output = jnp.einsum("hqk,khd->qhd", weights, values_wide, preferred_element_type=jnp.float32)
    return (output.astype(jnp.bfloat16), log_total)


def local_attend_back(operands):
    queries, keys_in, values_in, output, log_total, dattn = operands
    length, kv_dev, head_dim = keys_in.shape
    repeat_by = queries.shape[1] // kv_dev
    keys_wide = jnp.repeat(keys_in, repeat_by, axis=1)
    values_wide = jnp.repeat(values_in, repeat_by, axis=1)
    scores = masked_scores(queries, keys_wide)
    probs = jnp.exp(scores - log_total[..., None])
    delta = jnp.sum(output.astype(jnp.float32) * dattn.astype(jnp.float32), -1).T
    dprob = jnp.einsum("qhd,khd->hqk", dattn, values_wide, preferred_element_type=jnp.float32)
    dscore = (probs * (dprob - delta[..., None])).astype(jnp.bfloat16)
    dqueries = jnp.einsum(
        "hqk,khd->qhd", dscore, keys_wide, preferred_element_type=jnp.float32
    ) * head_dim ** (-0.5)
    dkeys = jnp.einsum(
        "hqk,qhd->khd", dscore, queries, preferred_element_type=jnp.float32
    ) * head_dim ** (-0.5)
    dvalues = jnp.einsum(
        "hqk,qhd->khd", probs.astype(jnp.bfloat16), dattn, preferred_element_type=jnp.float32
    )

    def fold_heads(per_head):
        return jnp.sum(per_head.reshape(length, kv_dev, repeat_by, head_dim), 2).astype(
            jnp.bfloat16
        )

    return (dqueries.astype(jnp.bfloat16), fold_heads(dkeys), fold_heads(dvalues))


def project(inputs, weight):
    return lax.dot_general(
        inputs,
        lax.all_gather(weight, "fsdp", axis=0, tiled=True),
        (((1,), (1,)), ((), ())),
        preferred_element_type=jnp.float32,
    )


def project_back(grads, weight):
    shard_rows = lax.all_gather(weight, "fsdp", axis=0, tiled=True)
    picked = lax.slice_in_dim(grads, 0, shard_rows.shape[0], axis=1)
    return jnp.dot(picked, shard_rows, preferred_element_type=jnp.float32)


def weight_grad(grads, inputs, shard_size):
    picked = lax.slice_in_dim(grads, 0, shard_size * lax.axis_size("fsdp"), axis=1)
    summed = lax.psum_scatter(
        lax.dot_general(
            picked, inputs, (((0,), (0,)), ((), ())), preferred_element_type=jnp.float32
        ).astype(jnp.bfloat16),
        "fsdp",
        scatter_dimension=0,
        tiled=True,
    )
    return lax.psum(summed, "seq").astype(jnp.float32)


def backward_pair(grads, inputs, weight):
    wgrad = weight_grad(grads, inputs, weight.shape[0])
    return (project_back(grads, weight), wgrad)


def body(hidden, positions, gains, w_qkv, w_out, w_gate_up, w_down, cotangent):
    seq_count, part_len, model_width = hidden.shape
    row_count = seq_count * part_len
    group_count = lax.axis_size("seq")
    full_len = part_len * group_count
    heads_dev = H // group_count
    share = H // KVH
    kv_dev = max(1, heads_dev // share)
    first_kv = np.arange(group_count) * heads_dev // share
    slot_table = np.concatenate(
        [
            first_kv[:, None] + np.arange(kv_dev)[None, :],
            KVH + first_kv[:, None] + np.arange(kv_dev)[None, :],
        ],
        1,
    ).reshape(-1)
    slot_onehot = jnp.asarray(
        (slot_table[:, None] == np.arange(2 * KVH)[None, :]).astype(np.float32), jnp.bfloat16
    )
    cosines, sines = rope_tables(positions)
    layer_index = 0
    gain = gains[layer_index]
    normed, scale_one = normalize(hidden, gain[0])
    normed_flat = normed.reshape(row_count, model_width)
    joint = project(normed_flat, w_qkv[layer_index]).reshape(seq_count, part_len, -1)
    queries = joint[..., : H * HD].reshape(seq_count, part_len, H, HD)
    keys_in = joint[..., H * HD : (H + KVH) * HD].reshape(seq_count, part_len, KVH, HD)
    values_in = joint[..., (H + KVH) * HD :].reshape(seq_count, part_len, KVH, HD)
    q_rot = rotate(queries, cosines, sines).astype(jnp.bfloat16)
    kv_all = jnp.concatenate(
        [rotate(keys_in, cosines, sines).astype(jnp.bfloat16), values_in.astype(jnp.bfloat16)], 2
    )
    q_send = q_rot.reshape(seq_count, part_len, group_count, heads_dev * HD)
    kv_send = jnp.take(kv_all, slot_table, axis=2).reshape(
        seq_count, part_len, group_count, 2 * kv_dev * HD
    )
    q_heads = lax.all_to_all(q_send, "seq", split_axis=2, concat_axis=1, tiled=True)
    kv_heads = lax.all_to_all(kv_send, "seq", split_axis=2, concat_axis=1, tiled=True)
    q_heads = q_heads.reshape(seq_count, full_len, heads_dev, HD)
    kv_heads = kv_heads.reshape(seq_count, full_len, 2 * kv_dev, HD)
    k_heads = kv_heads[:, :, :kv_dev]
    v_heads = kv_heads[:, :, kv_dev:]
    o_heads, log_total = lax.map(local_attend, (q_heads, k_heads, v_heads))
    o_back = lax.all_to_all(
        o_heads.reshape(seq_count, full_len, 1, heads_dev * HD),
        "seq",
        split_axis=1,
        concat_axis=2,
        tiled=True,
    )
    attn_flat = o_back.reshape(row_count, model_width)
    middle = hidden + project(attn_flat, w_out[layer_index]).reshape(
        seq_count, part_len, model_width
    )
    normed_two, scale_two = normalize(middle, gain[1])
    normed_two_flat = normed_two.reshape(row_count, model_width)
    both = project(normed_two_flat, w_gate_up[layer_index])
    gate_part = both[:, :FF]
    up_part = both[:, FF:]
    activated = (jax.nn.silu(gate_part) * up_part).astype(jnp.bfloat16)
    result = middle + project(activated, w_down[layer_index]).reshape(
        seq_count, part_len, model_width
    )
    saved = [
        (
            hidden,
            normed_flat,
            scale_one,
            q_heads,
            k_heads,
            v_heads,
            o_heads,
            log_total,
            attn_flat,
            middle,
            normed_two_flat,
            scale_two,
            gate_part,
            up_part,
            activated,
        )
    ]
    flowing = cotangent
    grads_qkv = [None] * LAYERS
    grads_out = [None] * LAYERS
    grads_gate_up = [None] * LAYERS
    grads_down = [None] * LAYERS
    gain_terms = [None] * LAYERS
    for layer_index in reversed(range(LAYERS)):
        (
            layer_in,
            normed_flat,
            scale_one,
            q_heads,
            k_heads,
            v_heads,
            o_heads,
            log_total,
            attn_flat,
            middle,
            normed_two_flat,
            scale_two,
            gate_part,
            up_part,
            activated,
        ) = saved[layer_index]
        gain = gains[layer_index]
        dm_cast = flowing.reshape(row_count, model_width).astype(jnp.bfloat16)
        dact, grads_down[layer_index] = backward_pair(dm_cast, activated, w_down[layer_index])
        sigma = jax.nn.sigmoid(gate_part)
        dgate = dact * up_part * sigma * (1.0 + gate_part * (1.0 - sigma))
        dup = dact * gate_part * sigma
        dgu = jnp.concatenate([dgate, dup], 1).astype(jnp.bfloat16)
        dnormed_two, grads_gate_up[layer_index] = backward_pair(
            dgu, normed_two_flat, w_gate_up[layer_index]
        )
        dnormed_two = dnormed_two.reshape(seq_count, part_len, model_width)
        dmid_norm, gain_two = normalize_back(dnormed_two, middle, scale_two, gain[1])
        dmiddle = flowing + dmid_norm
        dy_cast = dmiddle.reshape(row_count, model_width).astype(jnp.bfloat16)
        dattn_wide, grads_out[layer_index] = backward_pair(dy_cast, attn_flat, w_out[layer_index])
        dattn = dattn_wide.astype(jnp.bfloat16)
        dattn_heads = lax.all_to_all(
            dattn.reshape(seq_count, part_len, group_count, heads_dev * HD),
            "seq",
            split_axis=2,
            concat_axis=1,
            tiled=True,
        )
        dattn_heads = dattn_heads.reshape(seq_count, full_len, heads_dev, HD)
        dq_heads, dk_heads, dv_heads = lax.map(
            local_attend_back, (q_heads, k_heads, v_heads, o_heads, log_total, dattn_heads)
        )
        dkv_heads = jnp.concatenate([dk_heads, dv_heads], 2).reshape(
            seq_count, full_len, 1, 2 * kv_dev * HD
        )
        dq_tok, dkv_tok = (
            lax.all_to_all(
                dq_heads.reshape(seq_count, full_len, 1, heads_dev * HD),
                "seq",
                split_axis=1,
                concat_axis=2,
                tiled=True,
            ),
            lax.all_to_all(dkv_heads, "seq", split_axis=1, concat_axis=2, tiled=True),
        )
        dqueries = dq_tok.reshape(seq_count, part_len, H, HD)
        dkv_sum = jnp.einsum(
            "stnd,nm->stmd",
            dkv_tok.reshape(seq_count, part_len, group_count * 2 * kv_dev, HD),
            slot_onehot,
            preferred_element_type=jnp.float32,
        )
        dq_pre = unrotate(dqueries, cosines, sines)
        dk_pre = unrotate(dkv_sum[:, :, :KVH], cosines, sines)
        dvalues = dkv_sum[:, :, KVH:]
        djoint = jnp.concatenate(
            [
                dq_pre.reshape(row_count, -1),
                dk_pre.reshape(row_count, -1),
                dvalues.reshape(row_count, -1),
            ],
            1,
        ).astype(jnp.bfloat16)
        dnormed, grads_qkv[layer_index] = backward_pair(djoint, normed_flat, w_qkv[layer_index])
        dnormed = dnormed.reshape(seq_count, part_len, model_width)
        dcur_norm, gain_one = normalize_back(dnormed, layer_in, scale_one, gain[0])
        gain_terms[layer_index] = jnp.stack([gain_one, gain_two])
        flowing = dmiddle + dcur_norm
    gain_total = lax.psum(jnp.stack(gain_terms), ("fsdp", "seq"))
    return (
        result,
        flowing,
        gain_total,
        jnp.stack(grads_qkv),
        jnp.stack(grads_out),
        jnp.stack(grads_gate_up),
        jnp.stack(grads_down),
    )


def neighbour(values, step):
    count = lax.axis_size("seq")
    return lax.ppermute(values, "seq", [(i, i ^ step) for i in range(count)])


def gather_tokens(block):
    half = block.shape[0] // 2
    side = neighbour(block, 1)
    below = neighbour(block, 2)
    far_top = neighbour(side[:half], 2)
    far_bottom = neighbour(below[half:], 1)
    return jnp.concatenate([block, side, below, far_top, far_bottom], 0)


def scatter_tokens(partial):
    count = lax.axis_size("seq")
    blocks = partial.reshape(count, 2, -1, partial.shape[-1])
    top, bottom = blocks[:, 0], blocks[:, 1]
    from_side = neighbour(jnp.stack([top[1], top[3]]), 1)
    from_below = neighbour(jnp.stack([bottom[2], bottom[3]]), 2)
    wide = jnp.float32
    second_top = neighbour((top[2].astype(wide) + from_side[1].astype(wide)).astype(partial.dtype), 2)
    second_bottom = neighbour((bottom[1].astype(wide) + from_below[1].astype(wide)).astype(partial.dtype), 1)
    return jnp.concatenate(
        [
            top[0].astype(wide) + from_side[0].astype(wide) + second_top.astype(wide),
            bottom[0].astype(wide) + from_below[0].astype(wide) + second_bottom.astype(wide),
        ],
        0,
    )


def gather_shards(block, axis):
    count = lax.axis_size("seq")
    index = lax.axis_index("seq")
    half = block.shape[0] // 2
    side = neighbour(block, 1)
    below = neighbour(block, 2)
    far = jnp.concatenate([neighbour(side[:half], 2), neighbour(below[half:], 1)], 0)
    shape = list(block.shape)
    shape.insert(axis, count)
    whole = jnp.zeros(shape, jnp.float32)
    for step, part in enumerate((block, side, below, far)):
        whole = lax.dynamic_update_index_in_dim(whole, part.astype(jnp.float32), index ^ step, axis)
    return whole


def matmul(left, right, left_dim, right_dim):
    return lax.dot_general(
        left, right, (((left_dim,), (right_dim,)), ((), ())), preferred_element_type=jnp.float32
    )


ROOT = HD ** (-0.5)
LIMIT = 60 * 1024 * 1024


def swap_halves(values):
    width = values.shape[1]
    half = HD // 2
    column = lax.broadcasted_iota(jnp.int32, values.shape, 1)
    return jnp.where(
        column % HD < half, pltpu.roll(values, width - half, 1), pltpu.roll(values, half, 1)
    )


def spread_tables(table, pairs, last):
    half = HD // 2
    cosines, sines = table[:, :half], table[:, half:]
    ones, zeros = jnp.ones_like(table), jnp.zeros_like(table)
    tail = [[cosines, cosines, ones], [-sines, sines, zeros]] if last else [[], []]
    if not pairs:
        return jnp.concatenate(tail[0], 1), jnp.concatenate(tail[1], 1)
    cosines = [jnp.concatenate([cosines] * 4, 1)] * pairs
    sines = [jnp.concatenate([-sines, sines] * 2, 1)] * pairs
    if last:
        cosines.append(jnp.concatenate(tail[0], 1))
        sines.append(jnp.concatenate(tail[1], 1))
    return jnp.concatenate(cosines, 1), jnp.concatenate(sines, 1)


def qkv_kernel(index_ref, normed_ref, weight_ref, table_ref, q_ref, k_ref, v_ref):
    heads = q_ref.shape[0]
    joint = matmul(normed_ref[...], weight_ref[...], 1, 1)
    cosines, sines = spread_tables(table_ref[...], heads // 2, True)
    turned = joint * cosines + swap_halves(joint) * sines
    for head in range(heads):
        q_ref[head] = (turned[:, head * HD : (head + 1) * HD].astype(jnp.bfloat16).astype(jnp.float32) * ROOT).astype(
            jnp.bfloat16
        )
    k_ref[...] = turned[:, heads * HD : (heads + 1) * HD].astype(jnp.bfloat16)
    v_ref[...] = turned[:, (heads + 1) * HD :].astype(jnp.bfloat16)


def project_qkv(index, normed, weight, table, count):
    length, width = normed.shape
    part = length // count
    heads = weight.shape[0] // HD - 2
    return pl.pallas_call(
        qkv_kernel,
        out_shape=(
            jax.ShapeDtypeStruct((heads, length, HD), jnp.bfloat16),
            jax.ShapeDtypeStruct((length, HD), jnp.bfloat16),
            jax.ShapeDtypeStruct((length, HD), jnp.bfloat16),
        ),
        grid_spec=pltpu.PrefetchScalarGridSpec(
            num_scalar_prefetch=1,
            grid=(count,),
            in_specs=[
                pl.BlockSpec((part, width), lambda i, s: (i, 0)),
                pl.BlockSpec(weight.shape, lambda i, s: (0, 0)),
                pl.BlockSpec((part, table.shape[1]), lambda i, s: (i, 0)),
            ],
            out_specs=[
                pl.BlockSpec((heads, part, HD), lambda i, s: (0, i ^ s[0], 0)),
                pl.BlockSpec((part, HD), lambda i, s: (i ^ s[0], 0)),
                pl.BlockSpec((part, HD), lambda i, s: (i ^ s[0], 0)),
            ],
        ),
        compiler_params=pltpu.CompilerParams(vmem_limit_bytes=LIMIT),
        name="project_qkv",
    )(index, normed, weight, table)


def attend_kernel(count, index_ref, q_ref, k_ref, v_ref, weight_ref, sent_ref, attn_ref, lse_ref, held_ref):
    heads, part, _ = q_ref.shape
    here = pl.program_id(0)
    row = lax.broadcasted_iota(jnp.int32, (part, part), 0)
    column = lax.broadcasted_iota(jnp.int32, (part, part), 1)
    for block in range(count):

        @pl.when(here == block)
        def _():
            before = block * part
            seen = before + part
            keys_in, values_in = k_ref[:seen], v_ref[:seen]

            def one_head(head, carry):
                scores = matmul(q_ref[head], keys_in, 1, 1)
                last = jnp.where(row >= column, scores[:, before:], -1e30)
                scores = jnp.concatenate([scores[:, :before], last], 1) if block else last
                peak = jnp.max(scores, 1, keepdims=True)
                weights = jnp.exp(scores - peak)
                total = jnp.sum(weights, 1, keepdims=True)
                output = matmul(weights.astype(jnp.bfloat16), values_in, 1, 0) / total
                held_ref[head] = output.astype(jnp.bfloat16)
                log_total = jnp.broadcast_to(peak + jnp.log(total), (part, 128))
                lse_ref[pl.ds(head, 1), :] = jnp.transpose(log_total)[:1]
                return carry

            lax.fori_loop(0, heads, one_head, 0, unroll=2)

    attn = jnp.concatenate([held_ref[head] for head in range(heads)], 1)
    attn_ref[...] = attn
    sent_ref[...] = matmul(attn, weight_ref[...], 1, 1).astype(jnp.bfloat16)


def attend(index, queries, keys_in, values_in, weight, count):
    heads, length, _ = queries.shape
    part = length // count
    width = weight.shape[0]
    return pl.pallas_call(
        lambda *refs: attend_kernel(count, *refs),
        out_shape=(
            jax.ShapeDtypeStruct((length, width), jnp.bfloat16),
            jax.ShapeDtypeStruct((length, heads * HD), jnp.bfloat16),
            jax.ShapeDtypeStruct((heads, length), jnp.float32),
        ),
        grid_spec=pltpu.PrefetchScalarGridSpec(
            num_scalar_prefetch=1,
            grid=(count,),
            in_specs=[
                pl.BlockSpec((heads, part, HD), lambda i, s: (0, i, 0)),
                pl.BlockSpec((length, HD), lambda i, s: (0, 0)),
                pl.BlockSpec((length, HD), lambda i, s: (0, 0)),
                pl.BlockSpec(weight.shape, lambda i, s: (0, 0)),
            ],
            out_specs=[
                pl.BlockSpec((part, width), lambda i, s: (i ^ s[0], 0)),
                pl.BlockSpec((part, heads * HD), lambda i, s: (i ^ s[0], 0)),
                pl.BlockSpec((heads, part), lambda i, s: (0, i)),
            ],
            scratch_shapes=[pltpu.VMEM((heads, part, HD), jnp.bfloat16)],
        ),
        compiler_params=pltpu.CompilerParams(vmem_limit_bytes=LIMIT),
        name="attend",
    )(index, queries, keys_in, values_in, weight)


def attend_back_kernel(
    count, index_ref, q_ref, k_ref, v_ref, attn_ref, lse_ref, dy_ref, weight_ref, table_ref, pick_ref,
    out_ref, turned_ref, do_ref, delta_ref, dq_ref, dk_ref, dv_ref,
):
    heads, part, _ = q_ref.shape
    wide = jnp.float32
    here = pl.program_id(0)
    index = index_ref[0]
    spot = here ^ index

    @pl.when(here == 0)
    def _():
        dk_ref[...] = jnp.zeros_like(dk_ref)
        dv_ref[...] = jnp.zeros_like(dv_ref)

    dattn = matmul(dy_ref[...], weight_ref[...], 1, 0).astype(jnp.bfloat16)
    product = dattn.astype(wide) * attn_ref[...].astype(wide)
    owner = lax.broadcasted_iota(jnp.int32, (heads, heads * HD), 1) // HD
    same = owner == lax.broadcasted_iota(jnp.int32, (heads, heads * HD), 0)
    delta_ref[...] = lax.dot_general(
        same.astype(wide), product, (((1,), (1,)), ((), ())),
        precision=lax.Precision.HIGHEST, preferred_element_type=wide,
    )
    for head in range(heads):
        do_ref[head] = dattn[:, head * HD : (head + 1) * HD]
    row = lax.broadcasted_iota(jnp.int32, (part, part), 0)
    column = lax.broadcasted_iota(jnp.int32, (part, part), 1)
    for block in range(count):

        @pl.when(here == block)
        def _():
            before = block * part
            seen = before + part
            keys_in, values_in = k_ref[:seen], v_ref[:seen]

            def one_head(head, carry):
                query, dout = q_ref[head], do_ref[head]
                scores = matmul(keys_in, query, 1, 1)
                last = jnp.where(row <= column, scores[before:], -1e30)
                scores = jnp.concatenate([scores[:before], last], 0) if block else last
                probs = jnp.exp(scores - lse_ref[pl.ds(head, 1), :])
                dprob = matmul(values_in, dout, 1, 1)
                dscore = (probs * (dprob - delta_ref[pl.ds(head, 1), :])).astype(jnp.bfloat16)
                dv_ref[:seen] += matmul(probs.astype(jnp.bfloat16), dout, 1, 0)
                dk_ref[:seen] += matmul(dscore, query, 1, 0)
                dq_ref[head] = (matmul(dscore, keys_in, 0, 0) * ROOT).astype(jnp.bfloat16)
                return carry

            lax.fori_loop(0, heads, one_head, 0, unroll=2)

    def unturn(grads, cosines, sines):
        return grads * cosines + swap_halves(grads * sines)

    rows_here = pl.ds(pl.multiple_of(spot * part, part), part)
    dq = jnp.concatenate([dq_ref[head] for head in range(heads)], 1).astype(wide)
    dq = unturn(dq, *spread_tables(table_ref[rows_here, :], heads // 2, False))
    out_ref[rows_here, : heads * HD] = dq.astype(jnp.bfloat16)

    @pl.when(here == count - 1)
    def _():
        for block in range(count):
            rows_there = pl.ds(pl.multiple_of((block ^ index) * part, part), part)
            rows_block = slice(block * part, (block + 1) * part)
            both = jnp.concatenate([dk_ref[rows_block], dv_ref[rows_block]], 1).astype(jnp.bfloat16).astype(wide)
            both = unturn(both, *spread_tables(table_ref[rows_there, :], 0, True))
            out_ref[rows_there, heads * HD :] = both.astype(jnp.bfloat16)
        chosen = matmul(pick_ref[...], out_ref[...], 1, 1).astype(jnp.bfloat16)
        size = turned_ref.shape[1]
        for block in range(count):
            turned_ref[block] = chosen[block * size : (block + 1) * size]


def attend_back(index, queries, keys_in, values_in, attn, lse, dy, weight, table, pick, count):
    heads, length, _ = queries.shape
    part = length // count
    width = weight.shape[0]
    columns = (heads + 2) * HD
    return pl.pallas_call(
        lambda *refs: attend_back_kernel(count, *refs),
        out_shape=(
            jax.ShapeDtypeStruct((length, columns), jnp.bfloat16),
            jax.ShapeDtypeStruct((count, columns // count, length), jnp.bfloat16),
        ),
        grid_spec=pltpu.PrefetchScalarGridSpec(
            num_scalar_prefetch=1,
            grid=(count,),
            in_specs=[
                pl.BlockSpec((heads, part, HD), lambda i, s: (0, i, 0)),
                pl.BlockSpec((length, HD), lambda i, s: (0, 0)),
                pl.BlockSpec((length, HD), lambda i, s: (0, 0)),
                pl.BlockSpec((part, heads * HD), lambda i, s: (i ^ s[0], 0)),
                pl.BlockSpec((heads, part), lambda i, s: (0, i)),
                pl.BlockSpec((part, width), lambda i, s: (i ^ s[0], 0)),
                pl.BlockSpec(weight.shape, lambda i, s: (0, 0)),
                pl.BlockSpec(table.shape, lambda i, s: (0, 0)),
                pl.BlockSpec(pick.shape, lambda i, s: (0, 0)),
            ],
            out_specs=[
                pl.BlockSpec((length, columns), lambda i, s: (0, 0)),
                pl.BlockSpec((count, columns // count, length), lambda i, s: (0, 0, 0)),
            ],
            scratch_shapes=[
                pltpu.VMEM((heads, part, HD), jnp.bfloat16),
                pltpu.VMEM((heads, part), jnp.float32),
                pltpu.VMEM((heads, part, HD), jnp.bfloat16),
                pltpu.VMEM((length, HD), jnp.float32),
                pltpu.VMEM((length, HD), jnp.float32),
            ],
        ),
        compiler_params=pltpu.CompilerParams(vmem_limit_bytes=LIMIT),
        name="attend_back",
    )(index, queries, keys_in, values_in, attn, lse, dy, weight, table, pick)


def fast_body(hidden, positions, gains, w_qkv, w_out, w_gate_up, w_down, cotangent):
    count = lax.axis_size("seq")
    fsdp = lax.axis_size("fsdp")
    index = lax.axis_index("seq")
    place = index.astype(jnp.int32).reshape(1)
    current = hidden[0]
    part_len, width = current.shape
    length = part_len * count
    heads = H // count
    gain = gains[0]
    after = lax.optimization_barrier

    rows = w_qkv.shape[1]
    group = math.gcd(rows, HD)
    chunk = group // count
    per_head = HD // group
    qkv_part = lax.dynamic_index_in_dim(
        w_qkv[0].reshape(rows // group, count, chunk, width), index, 1, keepdims=False
    ).reshape(rows // count, width)
    qkv_part = lax.all_gather(qkv_part, "fsdp", axis=0, tiled=True)

    def by_owner(values):
        values = values.reshape(H + 2 * KVH, per_head, chunk, width)
        return jnp.concatenate(
            [
                values[:H].reshape(count, H // count, per_head, chunk, width),
                values[H : H + KVH].reshape(count, KVH // count, per_head, chunk, width),
                values[H + KVH :].reshape(count, KVH // count, per_head, chunk, width),
            ],
            1,
        )

    qkv_rows = lax.all_to_all(by_owner(qkv_part), "seq", 0, 0, tiled=True)
    qkv_rows = jnp.transpose(qkv_rows, (1, 2, 0, 3, 4)).reshape(-1, width)
    out_cols = lax.all_gather(
        lax.dynamic_slice_in_dim(w_out[0], index * heads * HD, heads * HD, 1), "fsdp", axis=0, tiled=True
    )
    gu_rows = w_gate_up.shape[1] // count
    gate_up = lax.all_gather(
        lax.dynamic_slice_in_dim(w_gate_up[0], index * gu_rows, gu_rows, 0), "fsdp", axis=0, tiled=True
    )
    units = FF // count
    down_rows = w_down.shape[1]
    down_cols = lax.all_gather(
        lax.dynamic_index_in_dim(
            w_down[0].reshape(down_rows, fsdp // 2, count, gu_rows), index, 2, keepdims=False
        ).reshape(down_rows, units),
        "fsdp",
        axis=0,
        tiled=True,
    )

    normed, scale_one = normalize(current, gain[0])
    normed_all = gather_tokens(normed)
    spots = positions[0]
    spots = jnp.concatenate([spots] + [neighbour(spots, step) for step in range(1, count)])
    frequency = jnp.exp(jnp.arange(HD // 2, dtype=jnp.float32) * (-2.0 * math.log(10000.0) / HD))
    angles = spots.astype(jnp.float32)[:, None] * frequency
    table = jnp.concatenate([jnp.cos(angles), jnp.sin(angles)], 1)
    flowing = cotangent[0]
    normed_all, qkv_rows, dm_sent = after((normed_all, qkv_rows, flowing.astype(jnp.bfloat16)))
    dm_all = gather_tokens(dm_sent)
    queries, keys_in, values_in = project_qkv(place, normed_all, qkv_rows, table, count)
    sent, attn_flat, log_total = attend(place, queries, keys_in, values_in, out_cols, count)
    middle = current + scatter_tokens(sent)
    normed_two, scale_two = normalize(middle, gain[1])
    normed_two_all = gather_tokens(normed_two)
    both = matmul(normed_two_all, gate_up, 1, 1)
    gate_part, up_part = both[:, :units], both[:, units:]
    activated = (jax.nn.silu(gate_part) * up_part).astype(jnp.bfloat16)
    down_sent = matmul(activated, down_cols, 1, 1).astype(jnp.bfloat16)


    def owned(grad):
        return lax.psum_scatter(grad.astype(jnp.bfloat16), "fsdp", scatter_dimension=0, tiled=True)

    term_down = matmul(dm_all, activated, 0, 0).astype(jnp.bfloat16)
    dm_all, term_down = after((dm_all, term_down))
    grad_down = owned(term_down)
    dact = matmul(dm_all, down_cols, 1, 0)
    sigma = jax.nn.sigmoid(gate_part)
    dgate = dact * up_part * sigma * (1.0 + gate_part * (1.0 - sigma))
    dup = dact * gate_part * sigma
    dgu = jnp.concatenate([dgate, dup], 1).astype(jnp.bfloat16)
    term_gate_up = matmul(dgu, normed_two_all, 0, 0).astype(jnp.bfloat16)
    dnormed_two = scatter_tokens(matmul(dgu, gate_up, 1, 0).astype(jnp.bfloat16))
    dnormed_two, term_gate_up = after((dnormed_two, term_gate_up))
    grad_gate_up = owned(term_gate_up)
    dmid_norm, gain_two = normalize_back(dnormed_two, middle, scale_two, gain[1])
    dmiddle = flowing + dmid_norm
    dy_all = gather_tokens(dmiddle.astype(jnp.bfloat16))
    dy_all, down_sent, grad_down = after((dy_all, down_sent, grad_down))
    result = middle + scatter_tokens(down_sent)
    grad_out = owned(matmul(dy_all, attn_flat, 0, 0))
    share = KVH // count
    pieces = heads + 2 * share
    picked = np.arange(pieces * HD).reshape(pieces * per_head, count, chunk).transpose(1, 0, 2).reshape(-1)
    pick = jnp.asarray(picked[:, None] == np.arange(pieces * HD)[None, :], jnp.bfloat16)
    djoint, djoint_turned = attend_back(
        place, queries, keys_in, values_in, attn_flat, log_total, dy_all, out_cols, table, pick, count
    )
    dnormed = scatter_tokens(matmul(djoint, qkv_rows, 1, 0).astype(jnp.bfloat16))

    whole = jnp.zeros((count,) + djoint_turned.shape[1:], jnp.bfloat16)
    for step in range(count):
        part = lax.dynamic_index_in_dim(djoint_turned, index ^ step, 0, keepdims=False)
        if step:
            part = neighbour(part, step).reshape(-1, count, part_len)
            part = jnp.concatenate([part[:, step ^ block] for block in range(count)], 1)
        whole = lax.dynamic_update_index_in_dim(whole, part, index ^ step, 0)
    whole = whole.reshape(count, pieces, per_head, chunk, length)
    whole = jnp.concatenate(
        [
            whole[:, :heads].reshape(-1, length),
            whole[:, heads : heads + share].reshape(-1, length),
            whole[:, heads + share :].reshape(-1, length),
        ],
        0,
    )
    term_qkv = matmul(whole, normed_all, 1, 0)
    grad_qkv = owned(term_qkv)
    gain_one = jnp.sum(term_qkv * qkv_part.astype(jnp.float32), 0) / gain[0]
    gain_total = jnp.stack([gain_one, gain_two])[None]
    for axis in ("seq", "fsdp"):
        step = 1
        while step < lax.axis_size(axis):
            pairs = [(i, i ^ step) for i in range(lax.axis_size(axis))]
            gain_total = gain_total + lax.ppermute(gain_total, axis, pairs)
            step *= 2
    unit = current * scale_one
    inner = dnormed * gain[0]
    dcur_norm = scale_one * (inner - unit * jnp.mean(inner * unit, -1, keepdims=True))
    qkv_shard = gather_shards(grad_qkv.reshape(rows // group, chunk, width), 1)
    down_shard = gather_shards(grad_down.reshape(down_rows, fsdp // 2, gu_rows), 2)
    return (
        result[None],
        (dmiddle + dcur_norm)[None],
        gain_total,
        qkv_shard.reshape(1, rows, width),
        gather_shards(grad_out, 1).reshape(1, down_rows, width),
        gather_shards(grad_gate_up, 0).reshape(1, -1, width),
        down_shard.reshape(1, down_rows, FF),
    )


def fits(mesh):
    count, fsdp = mesh.shape["seq"], mesh.shape["fsdp"]
    return count == KVH == 4 and fsdp % 2 == 0 and fsdp & (fsdp - 1) == 0


def solution(mesh):
    placed = (
        P("fsdp", "seq", None),
        P("fsdp", "seq"),
        P(),
        P(None, "fsdp", None),
        P(None, "fsdp", None),
        P(None, "fsdp", None),
        P(None, "fsdp", None),
        P("fsdp", "seq", None),
    )
    fast = fits(mesh)
    return jax.shard_map(
        fast_body if fast else body,
        mesh=mesh,
        in_specs=placed,
        out_specs=(
            P("fsdp", "seq", None),
            P("fsdp", "seq", None),
            P(),
            P(None, "fsdp", None),
            P(None, "fsdp", None),
            P(None, "fsdp", None),
            P(None, "fsdp", None),
        ),
        check_vma=False,
    )
```

```python
import math

import jax
import jax.numpy as jnp
import numpy as np
from jax import lax
from jax.experimental import pallas as pl
from jax.experimental.pallas import tpu as pltpu
from jax.sharding import PartitionSpec as P


H = 32
KVH = 4
HD = 64
FF = 5632
LAYERS = 1


EPS = 1e-05


def rope_tables(position_ids):
    halfway = HD // 2
    frequency = jnp.exp(jnp.arange(halfway, dtype=jnp.float32) * (-2.0 * math.log(10000.0) / HD))
    angles = position_ids.astype(jnp.float32)[..., None] * frequency
    cosines = jnp.cos(angles)
    sines = jnp.sin(angles)
    return (
        jnp.concatenate([cosines, cosines], -1)[..., None, :],
        jnp.concatenate([sines, sines], -1)[..., None, :],
    )


def rotate(values, cosines, sines):
    halfway = values.shape[-1] // 2
    turned = jnp.concatenate([-values[..., halfway:], values[..., :halfway]], -1)
    return values * cosines + turned * sines


def unrotate(grads, cosines, sines):
    halfway = grads.shape[-1] // 2
    scaled = grads * sines
    return grads * cosines + jnp.concatenate([scaled[..., halfway:], -scaled[..., :halfway]], -1)


def normalize(values, gain):
    scale = lax.rsqrt(jnp.mean(values * values, -1, keepdims=True) + EPS)
    return ((values * scale * gain).astype(jnp.bfloat16), scale)


def normalize_back(grads, values, scale, gain):
    unit = values * scale
    gain_grad = jnp.sum((grads * unit).reshape(-1, unit.shape[-1]), 0)
    inner = grads * gain
    return (scale * (inner - unit * jnp.mean(inner * unit, -1, keepdims=True)), gain_grad)


def masked_scores(queries, keys_wide):
    scores = jnp.einsum(
        "qhd,khd->hqk", queries, keys_wide, preferred_element_type=jnp.float32
    ) * queries.shape[-1] ** (-0.5)
    length = queries.shape[0]
    causal = jnp.arange(length)[:, None] >= jnp.arange(length)[None, :]
    return jnp.where(causal[None], scores, -1e30)


def local_attend(operands):
    queries, keys_in, values_in = operands
    repeat_by = queries.shape[1] // keys_in.shape[1]
    keys_wide = jnp.repeat(keys_in, repeat_by, axis=1)
    values_wide = jnp.repeat(values_in, repeat_by, axis=1)
    scores = masked_scores(queries, keys_wide)
    peak = jnp.max(scores, -1, keepdims=True)
    log_total = peak[..., 0] + jnp.log(jnp.sum(jnp.exp(scores - peak), -1))
    weights = jnp.exp(scores - log_total[..., None]).astype(jnp.bfloat16)
    output = jnp.einsum("hqk,khd->qhd", weights, values_wide, preferred_element_type=jnp.float32)
    return (output.astype(jnp.bfloat16), log_total)


def local_attend_back(operands):
    queries, keys_in, values_in, output, log_total, dattn = operands
    length, kv_dev, head_dim = keys_in.shape
    repeat_by = queries.shape[1] // kv_dev
    keys_wide = jnp.repeat(keys_in, repeat_by, axis=1)
    values_wide = jnp.repeat(values_in, repeat_by, axis=1)
    scores = masked_scores(queries, keys_wide)
    probs = jnp.exp(scores - log_total[..., None])
    delta = jnp.sum(output.astype(jnp.float32) * dattn.astype(jnp.float32), -1).T
    dprob = jnp.einsum("qhd,khd->hqk", dattn, values_wide, preferred_element_type=jnp.float32)
    dscore = (probs * (dprob - delta[..., None])).astype(jnp.bfloat16)
    dqueries = jnp.einsum(
        "hqk,khd->qhd", dscore, keys_wide, preferred_element_type=jnp.float32
    ) * head_dim ** (-0.5)
    dkeys = jnp.einsum(
        "hqk,qhd->khd", dscore, queries, preferred_element_type=jnp.float32
    ) * head_dim ** (-0.5)
    dvalues = jnp.einsum(
        "hqk,qhd->khd", probs.astype(jnp.bfloat16), dattn, preferred_element_type=jnp.float32
    )

    def fold_heads(per_head):
        return jnp.sum(per_head.reshape(length, kv_dev, repeat_by, head_dim), 2).astype(
            jnp.bfloat16
        )

    return (dqueries.astype(jnp.bfloat16), fold_heads(dkeys), fold_heads(dvalues))


def project(inputs, weight):
    return lax.dot_general(
        inputs,
        lax.all_gather(weight, "fsdp", axis=0, tiled=True),
        (((1,), (1,)), ((), ())),
        preferred_element_type=jnp.float32,
    )


def project_back(grads, weight):
    shard_rows = lax.all_gather(weight, "fsdp", axis=0, tiled=True)
    picked = lax.slice_in_dim(grads, 0, shard_rows.shape[0], axis=1)
    return jnp.dot(picked, shard_rows, preferred_element_type=jnp.float32)


def weight_grad(grads, inputs, shard_size):
    picked = lax.slice_in_dim(grads, 0, shard_size * lax.axis_size("fsdp"), axis=1)
    summed = lax.psum_scatter(
        lax.dot_general(
            picked, inputs, (((0,), (0,)), ((), ())), preferred_element_type=jnp.float32
        ).astype(jnp.bfloat16),
        "fsdp",
        scatter_dimension=0,
        tiled=True,
    )
    return lax.psum(summed, "seq").astype(jnp.float32)


def backward_pair(grads, inputs, weight):
    wgrad = weight_grad(grads, inputs, weight.shape[0])
    return (project_back(grads, weight), wgrad)


def body(hidden, positions, gains, w_qkv, w_out, w_gate_up, w_down, cotangent):
    seq_count, part_len, model_width = hidden.shape
    row_count = seq_count * part_len
    group_count = lax.axis_size("seq")
    full_len = part_len * group_count
    heads_dev = H // group_count
    share = H // KVH
    kv_dev = max(1, heads_dev // share)
    first_kv = np.arange(group_count) * heads_dev // share
    slot_table = np.concatenate(
        [
            first_kv[:, None] + np.arange(kv_dev)[None, :],
            KVH + first_kv[:, None] + np.arange(kv_dev)[None, :],
        ],
        1,
    ).reshape(-1)
    slot_onehot = jnp.asarray(
        (slot_table[:, None] == np.arange(2 * KVH)[None, :]).astype(np.float32), jnp.bfloat16
    )
    cosines, sines = rope_tables(positions)
    layer_index = 0
    gain = gains[layer_index]
    normed, scale_one = normalize(hidden, gain[0])
    normed_flat = normed.reshape(row_count, model_width)
    joint = project(normed_flat, w_qkv[layer_index]).reshape(seq_count, part_len, -1)
    queries = joint[..., : H * HD].reshape(seq_count, part_len, H, HD)
    keys_in = joint[..., H * HD : (H + KVH) * HD].reshape(seq_count, part_len, KVH, HD)
    values_in = joint[..., (H + KVH) * HD :].reshape(seq_count, part_len, KVH, HD)
    q_rot = rotate(queries, cosines, sines).astype(jnp.bfloat16)
    kv_all = jnp.concatenate(
        [rotate(keys_in, cosines, sines).astype(jnp.bfloat16), values_in.astype(jnp.bfloat16)], 2
    )
    q_send = q_rot.reshape(seq_count, part_len, group_count, heads_dev * HD)
    kv_send = jnp.take(kv_all, slot_table, axis=2).reshape(
        seq_count, part_len, group_count, 2 * kv_dev * HD
    )
    q_heads = lax.all_to_all(q_send, "seq", split_axis=2, concat_axis=1, tiled=True)
    kv_heads = lax.all_to_all(kv_send, "seq", split_axis=2, concat_axis=1, tiled=True)
    q_heads = q_heads.reshape(seq_count, full_len, heads_dev, HD)
    kv_heads = kv_heads.reshape(seq_count, full_len, 2 * kv_dev, HD)
    k_heads = kv_heads[:, :, :kv_dev]
    v_heads = kv_heads[:, :, kv_dev:]
    o_heads, log_total = lax.map(local_attend, (q_heads, k_heads, v_heads))
    o_back = lax.all_to_all(
        o_heads.reshape(seq_count, full_len, 1, heads_dev * HD),
        "seq",
        split_axis=1,
        concat_axis=2,
        tiled=True,
    )
    attn_flat = o_back.reshape(row_count, model_width)
    middle = hidden + project(attn_flat, w_out[layer_index]).reshape(
        seq_count, part_len, model_width
    )
    normed_two, scale_two = normalize(middle, gain[1])
    normed_two_flat = normed_two.reshape(row_count, model_width)
    both = project(normed_two_flat, w_gate_up[layer_index])
    gate_part = both[:, :FF]
    up_part = both[:, FF:]
    activated = (jax.nn.silu(gate_part) * up_part).astype(jnp.bfloat16)
    result = middle + project(activated, w_down[layer_index]).reshape(
        seq_count, part_len, model_width
    )
    saved = [
        (
            hidden,
            normed_flat,
            scale_one,
            q_heads,
            k_heads,
            v_heads,
            o_heads,
            log_total,
            attn_flat,
            middle,
            normed_two_flat,
            scale_two,
            gate_part,
            up_part,
            activated,
        )
    ]
    flowing = cotangent
    grads_qkv = [None] * LAYERS
    grads_out = [None] * LAYERS
    grads_gate_up = [None] * LAYERS
    grads_down = [None] * LAYERS
    gain_terms = [None] * LAYERS
    for layer_index in reversed(range(LAYERS)):
        (
            layer_in,
            normed_flat,
            scale_one,
            q_heads,
            k_heads,
            v_heads,
            o_heads,
            log_total,
            attn_flat,
            middle,
            normed_two_flat,
            scale_two,
            gate_part,
            up_part,
            activated,
        ) = saved[layer_index]
        gain = gains[layer_index]
        dm_cast = flowing.reshape(row_count, model_width).astype(jnp.bfloat16)
        dact, grads_down[layer_index] = backward_pair(dm_cast, activated, w_down[layer_index])
        sigma = jax.nn.sigmoid(gate_part)
        dgate = dact * up_part * sigma * (1.0 + gate_part * (1.0 - sigma))
        dup = dact * gate_part * sigma
        dgu = jnp.concatenate([dgate, dup], 1).astype(jnp.bfloat16)
        dnormed_two, grads_gate_up[layer_index] = backward_pair(
            dgu, normed_two_flat, w_gate_up[layer_index]
        )
        dnormed_two = dnormed_two.reshape(seq_count, part_len, model_width)
        dmid_norm, gain_two = normalize_back(dnormed_two, middle, scale_two, gain[1])
        dmiddle = flowing + dmid_norm
        dy_cast = dmiddle.reshape(row_count, model_width).astype(jnp.bfloat16)
        dattn_wide, grads_out[layer_index] = backward_pair(dy_cast, attn_flat, w_out[layer_index])
        dattn = dattn_wide.astype(jnp.bfloat16)
        dattn_heads = lax.all_to_all(
            dattn.reshape(seq_count, part_len, group_count, heads_dev * HD),
            "seq",
            split_axis=2,
            concat_axis=1,
            tiled=True,
        )
        dattn_heads = dattn_heads.reshape(seq_count, full_len, heads_dev, HD)
        dq_heads, dk_heads, dv_heads = lax.map(
            local_attend_back, (q_heads, k_heads, v_heads, o_heads, log_total, dattn_heads)
        )
        dkv_heads = jnp.concatenate([dk_heads, dv_heads], 2).reshape(
            seq_count, full_len, 1, 2 * kv_dev * HD
        )
        dq_tok, dkv_tok = (
            lax.all_to_all(
                dq_heads.reshape(seq_count, full_len, 1, heads_dev * HD),
                "seq",
                split_axis=1,
                concat_axis=2,
                tiled=True,
            ),
            lax.all_to_all(dkv_heads, "seq", split_axis=1, concat_axis=2, tiled=True),
        )
        dqueries = dq_tok.reshape(seq_count, part_len, H, HD)
        dkv_sum = jnp.einsum(
            "stnd,nm->stmd",
            dkv_tok.reshape(seq_count, part_len, group_count * 2 * kv_dev, HD),
            slot_onehot,
            preferred_element_type=jnp.float32,
        )
        dq_pre = unrotate(dqueries, cosines, sines)
        dk_pre = unrotate(dkv_sum[:, :, :KVH], cosines, sines)
        dvalues = dkv_sum[:, :, KVH:]
        djoint = jnp.concatenate(
            [
                dq_pre.reshape(row_count, -1),
                dk_pre.reshape(row_count, -1),
                dvalues.reshape(row_count, -1),
            ],
            1,
        ).astype(jnp.bfloat16)
        dnormed, grads_qkv[layer_index] = backward_pair(djoint, normed_flat, w_qkv[layer_index])
        dnormed = dnormed.reshape(seq_count, part_len, model_width)
        dcur_norm, gain_one = normalize_back(dnormed, layer_in, scale_one, gain[0])
        gain_terms[layer_index] = jnp.stack([gain_one, gain_two])
        flowing = dmiddle + dcur_norm
    gain_total = lax.psum(jnp.stack(gain_terms), ("fsdp", "seq"))
    return (
        result,
        flowing,
        gain_total,
        jnp.stack(grads_qkv),
        jnp.stack(grads_out),
        jnp.stack(grads_gate_up),
        jnp.stack(grads_down),
    )


def neighbour(values, step):
    count = lax.axis_size("seq")
    return lax.ppermute(values, "seq", [(i, i ^ step) for i in range(count)])


def matmul(left, right, left_dim, right_dim):
    return lax.dot_general(
        left, right, (((left_dim,), (right_dim,)), ((), ())), preferred_element_type=jnp.float32
    )


ROOT = HD ** (-0.5)
LIMIT = 60 * 1024 * 1024


def swap_halves(values):
    width = values.shape[1]
    half = HD // 2
    column = lax.broadcasted_iota(jnp.int32, values.shape, 1)
    return jnp.where(
        column % HD < half, pltpu.roll(values, width - half, 1), pltpu.roll(values, half, 1)
    )


def spread_tables(table, pairs, last):
    half = HD // 2
    cosines, sines = table[:, :half], table[:, half:]
    ones, zeros = jnp.ones_like(table), jnp.zeros_like(table)
    tail = [[cosines, cosines, ones], [-sines, sines, zeros]] if last else [[], []]
    if not pairs:
        return jnp.concatenate(tail[0], 1), jnp.concatenate(tail[1], 1)
    cosines = [jnp.concatenate([cosines] * 4, 1)] * pairs
    sines = [jnp.concatenate([-sines, sines] * 2, 1)] * pairs
    if last:
        cosines.append(jnp.concatenate(tail[0], 1))
        sines.append(jnp.concatenate(tail[1], 1))
    return jnp.concatenate(cosines, 1), jnp.concatenate(sines, 1)


MESH = pl.DeviceIdType.MESH


def seq_peer(step):
    return {"seq": lax.axis_index("seq") ^ step}


def fsdp_peer(place):
    return {"fsdp": place}


def remote(source, target, sems, slot, peer):
    return pltpu.make_async_remote_copy(
        src_ref=source,
        dst_ref=target,
        send_sem=sems[0].at[slot],
        recv_sem=sems[1].at[slot],
        device_id=peer,
        device_id_type=MESH,
    )


def gather_copies(own, slots, half, sems, base=0):
    top, bottom = pl.ds(0, half), pl.ds(half, own.shape[0] - half)

    def slot(step, rows):
        return slots.at[step].at[rows]

    return [
        remote(own.at[top], slot(1, top), sems, base, seq_peer(1)),
        remote(own.at[bottom], slot(2, bottom), sems, base + 1, seq_peer(2)),
        remote(own.at[bottom], slot(1, bottom), sems, base + 2, seq_peer(1)),
        remote(own.at[top], slot(2, top), sems, base + 3, seq_peer(2)),
        remote(slot(1, top), slot(3, top), sems, base + 4, seq_peer(2)),
        remote(slot(2, bottom), slot(3, bottom), sems, base + 5, seq_peer(1)),
    ]


def greet(peers):
    barrier = pltpu.get_barrier_semaphore()
    for peer in peers:
        pl.semaphore_signal(barrier, inc=1, device_id=peer, device_id_type=MESH)
    pl.semaphore_wait(barrier, len(peers))


def sum_copies(sent, side, below, far, half, sems, passed=None):
    top, bottom = pl.ds(0, half), pl.ds(half, half)
    return [
        remote(sent.at[3].at[top], side.at[1], sems, 0, seq_peer(1)),
        remote(sent.at[3].at[bottom], below.at[1], sems, 1, seq_peer(2)),
        remote(sent.at[2].at[bottom], below.at[0], sems, 2, seq_peer(2)),
        remote(sent.at[1].at[top], side.at[0], sems, 3, seq_peer(1)),
        remote(passed.at[0] if passed is not None else sent.at[2].at[top], far.at[0], sems, 4, seq_peer(2)),
        remote(passed.at[1] if passed is not None else sent.at[1].at[bottom], far.at[1], sems, 5, seq_peer(1)),
    ]


def pass_sums(turn, step, partial, sums, sent_ref, side_ref, below_ref, own_ref, half):
    wide, narrow = jnp.float32, jnp.bfloat16
    last = len(sums) // 2

    @pl.when(turn == last)
    def _():
        own_ref[...] = partial

    @pl.when(turn < last)
    def _():
        sent_ref[step] = partial.astype(narrow)

    @pl.when(turn == 0)
    def _():
        sums[0].start()
        sums[1].start()

    @pl.when(turn == 1)
    def _():
        sums[2].start()

    @pl.when(turn == 2)
    def _():
        sums[3].start()
        sums[0].wait_recv()
        sent_ref[2, :half] = (sent_ref[2, :half].astype(wide) + side_ref[1].astype(wide)).astype(narrow)
        sums[4].start()
        sums[1].wait_recv()
        sent_ref[1, half:] = (sent_ref[1, half:].astype(wide) + below_ref[1].astype(wide)).astype(narrow)
        sums[5].start()


def end_sums(sums, side_ref, below_ref, far_ref, own_ref, half):
    wide = jnp.float32
    sums[2].wait_recv()
    sums[3].wait_recv()
    own_ref[:half] += side_ref[0].astype(wide)
    own_ref[half:] += below_ref[0].astype(wide)
    sums[4].wait_recv()
    own_ref[:half] += far_ref[0].astype(wide)
    sums[5].wait_recv()
    own_ref[half:] += far_ref[1].astype(wide)


def share_own(all_ref, half, sems, before):
    copies = gather_copies(all_ref.at[0], all_ref, half, sems, len(before))
    for copy in copies[:4]:
        copy.start()
    copies[0].wait_recv()
    copies[4].start()
    copies[1].wait_recv()
    copies[5].start()
    for copy in copies[2:]:
        copy.wait_recv()
    for copy in before + copies:
        copy.wait_send()


def enter_kernel(
    count, normed_ref, spots_ref, shard_ref, out_shard_ref,
    all_ref, rows_ref, out_ref, table_ref,
    held_ref, send_sems, recv_sems, spot_send, spot_recv, item_up, item_down, item_side, item_recv, local_sem,
):
    part, _ = normed_ref.shape
    heads = H // count
    pieces = heads + 2
    items = pieces + lax.axis_size("fsdp")
    per_shard = shard_ref.shape[0] // HD
    out_rows, columns = out_shard_ref.shape[0], heads * HD
    chips = lax.axis_size("fsdp") // 2
    index = lax.axis_index("seq")
    place = lax.axis_index("fsdp")
    chip, core = place // 2, place % 2
    sems = (send_sems, recv_sems)

    barrier = pltpu.get_barrier_semaphore()
    for peer in [seq_peer(step) for step in range(1, count)] + [fsdp_peer(place ^ 1)]:
        pl.semaphore_signal(barrier, inc=1, device_id=peer, device_id_type=MESH)

    @pl.when(chip > 0)
    def _():
        pl.semaphore_signal(barrier, inc=1, device_id=fsdp_peer(place - 2), device_id_type=MESH)

    @pl.when(chip < chips - 1)
    def _():
        pl.semaphore_signal(barrier, inc=1, device_id=fsdp_peer(place + 2), device_id_type=MESH)

    greetings = count + (chip > 0).astype(jnp.int32) + (chip < chips - 1).astype(jnp.int32)
    pl.semaphore_wait(barrier, greetings)

    copies = gather_copies(normed_ref, all_ref, part // 2, sems)
    for copy in copies[:4]:
        copy.start()
    held_ref[0] = spots_ref[...]
    spot_copies = [
        remote(spots_ref, held_ref.at[step], (spot_send, spot_recv), step - 1, seq_peer(step))
        for step in range(1, count)
    ]
    for copy in spot_copies:
        copy.start()
    own = pltpu.make_async_copy(normed_ref, all_ref.at[0], local_sem.at[items])
    own.start()

    def qkv_item(item):
        block = jnp.where(
            item < heads, index * heads + item, jnp.where(item == heads, H + index, H + KVH + index)
        )
        source = shard_ref.at[pl.ds(pl.multiple_of(block % per_shard * HD, HD), HD)]
        return block // per_shard, source, rows_ref.at[pl.ds(pl.multiple_of(item * HD, HD), HD)], item

    def out_item(item):
        source = out_shard_ref.at[:, pl.ds(pl.multiple_of(index * columns, columns), columns)]
        target = out_ref.at[pl.ds(pl.multiple_of(item * out_rows, out_rows), out_rows)]
        return item, source, target, item + pieces

    kinds = ((qkv_item, pieces), (out_item, items - pieces))

    def item_copy(source, target, slot, sem, peer):
        return pltpu.make_async_remote_copy(
            src_ref=source,
            dst_ref=target,
            send_sem=sem.at[slot],
            recv_sem=item_recv.at[slot],
            device_id=fsdp_peer(peer),
            device_id_type=MESH,
        )

    def pass_on(source, target, slot, owner_chip, act):
        @pl.when((chip >= owner_chip) & (chip < chips - 1))
        def _():
            act(item_copy(source, target, slot, item_up, place + 2))

        @pl.when((chip <= owner_chip) & (chip > 0))
        def _():
            act(item_copy(source, target, slot, item_down, place - 2))

        act(item_copy(source, target, slot, item_side, place ^ 1))

    def send_own(item_of):
        def body(item, carry):
            owner, source, target, slot = item_of(item)

            @pl.when(place == owner)
            def _():
                pass_on(source, target, slot, owner // 2, lambda copy: copy.start())
                pltpu.make_async_copy(source, target, local_sem.at[slot]).start()

            return carry

        return body

    def pass_far(item_of, distance):
        def body(item, carry):
            owner, _, target, slot = item_of(item)
            owner_chip = owner // 2
            apart = jnp.where(chip > owner_chip, chip - owner_chip, owner_chip - chip)

            @pl.when((apart == distance) & (core == owner % 2))
            def _():
                item_copy(target, target, slot, item_side, place ^ 1).wait_recv()
                pass_on(target, target, slot, owner_chip, lambda copy: copy.start())

            return carry

        return body

    for item_of, number in kinds:
        lax.fori_loop(0, number, send_own(item_of), 0)
    for distance in range(1, chips):
        for item_of, number in kinds:
            lax.fori_loop(0, number, pass_far(item_of, distance), 0)
            if distance == 1 and item_of is qkv_item:
                copies[0].wait_recv()
                copies[4].start()
                copies[1].wait_recv()
                copies[5].start()

    for copy in spot_copies:
        copy.wait()
    half = HD // 2
    for step in range(count):
        spots = held_ref[step][:1]
        frequency = jnp.exp(
            lax.broadcasted_iota(jnp.int32, (half, 1), 0).astype(jnp.float32) * (-2.0 * math.log(10000.0) / HD)
        )
        angles = frequency * spots
        turned = jnp.concatenate([jnp.cos(angles), jnp.sin(angles)], 0)
        table_ref[pl.ds(step * part, part), :] = jnp.transpose(turned)

    def finish(item_of):
        def body(item, carry):
            owner, source, target, slot = item_of(item)

            @pl.when(core != owner % 2)
            def _():
                item_copy(target, target, slot, item_side, place ^ 1).wait_recv()

            @pl.when(place == owner)
            def _():
                pltpu.make_async_copy(source, target, local_sem.at[slot]).wait()

            @pl.when(core == owner % 2)
            def _():
                pass_on(target, target, slot, owner // 2, lambda copy: copy.wait_send())

            return carry

        return body

    for item_of, number in kinds:
        lax.fori_loop(0, number, finish(item_of), 0)
    own.wait()
    for copy in copies[2:]:
        copy.wait_recv()
    for copy in copies:
        copy.wait_send()


def enter(normed, spots, shard, out_shard, count):
    part, width = normed.shape
    length = part * count
    heads = H // count
    pieces = heads + 2
    items = pieces + lax.axis_size("fsdp")
    vmem = pl.BlockSpec(memory_space=pltpu.VMEM)
    spots = jnp.broadcast_to(spots.astype(jnp.float32)[None], (8, part))
    gathered, rows, out_cols, table = pl.pallas_call(
        lambda *refs: enter_kernel(count, *refs),
        out_shape=(
            jax.ShapeDtypeStruct((count, part, width), jnp.bfloat16),
            jax.ShapeDtypeStruct((pieces * HD, width), jnp.bfloat16),
            jax.ShapeDtypeStruct((out_shard.shape[0] * (items - pieces), heads * HD), jnp.bfloat16),
            jax.ShapeDtypeStruct((length, HD), jnp.float32),
        ),
        in_specs=[vmem] * 4,
        out_specs=[vmem] * 4,
        scratch_shapes=[
            pltpu.VMEM((count, 8, part), jnp.float32),
            pltpu.SemaphoreType.DMA((6,)),
            pltpu.SemaphoreType.DMA((6,)),
            pltpu.SemaphoreType.DMA((count - 1,)),
            pltpu.SemaphoreType.DMA((count - 1,)),
            pltpu.SemaphoreType.DMA((items,)),
            pltpu.SemaphoreType.DMA((items,)),
            pltpu.SemaphoreType.DMA((items,)),
            pltpu.SemaphoreType.DMA((items,)),
            pltpu.SemaphoreType.DMA((items + 1,)),
        ],
        compiler_params=pltpu.CompilerParams(collective_id=1, has_side_effects=True, vmem_limit_bytes=LIMIT),
        name="enter",
    )(normed, spots, shard, out_shard)
    return gathered.reshape(length, width), rows, out_cols, table


def qkv_kernel(index_ref, normed_ref, weight_ref, table_ref, q_ref, k_ref, v_ref):
    heads = q_ref.shape[0]
    joint = matmul(normed_ref[...], weight_ref[...], 1, 1)
    cosines, sines = spread_tables(table_ref[...], heads // 2, True)
    turned = joint * cosines + swap_halves(joint) * sines
    for head in range(heads):
        rounded = turned[:, head * HD : (head + 1) * HD].astype(jnp.bfloat16).astype(jnp.float32)
        q_ref[head] = (rounded * ROOT).astype(jnp.bfloat16)
    k_ref[...] = turned[:, heads * HD : (heads + 1) * HD].astype(jnp.bfloat16)
    v_ref[...] = turned[:, (heads + 1) * HD :].astype(jnp.bfloat16)


def project_qkv(index, normed, weight, table, count):
    length, width = normed.shape
    part = length // count
    heads = weight.shape[0] // HD - 2
    return pl.pallas_call(
        qkv_kernel,
        out_shape=(
            jax.ShapeDtypeStruct((heads, length, HD), jnp.bfloat16),
            jax.ShapeDtypeStruct((length, HD), jnp.bfloat16),
            jax.ShapeDtypeStruct((length, HD), jnp.bfloat16),
        ),
        grid_spec=pltpu.PrefetchScalarGridSpec(
            num_scalar_prefetch=1,
            grid=(count,),
            in_specs=[
                pl.BlockSpec((part, width), lambda i, s: (i, 0)),
                pl.BlockSpec(weight.shape, lambda i, s: (0, 0)),
                pl.BlockSpec((part, table.shape[1]), lambda i, s: (i, 0)),
            ],
            out_specs=[
                pl.BlockSpec((heads, part, HD), lambda i, s: (0, i ^ s[0], 0)),
                pl.BlockSpec((part, HD), lambda i, s: (i ^ s[0], 0)),
                pl.BlockSpec((part, HD), lambda i, s: (i ^ s[0], 0)),
            ],
        ),
        compiler_params=pltpu.CompilerParams(vmem_limit_bytes=LIMIT),
        name="project_qkv",
    )(index, normed, weight, table)


def attend_kernel(
    count, q_ref, k_ref, v_ref, weight_ref, current_ref, gain_ref,
    attn_ref, lse_ref, middle_ref, scale_ref, all_ref,
    held_ref, sent_ref, side_ref, below_ref, far_ref, send_sems, recv_sems,
):
    heads, _, _ = q_ref.shape
    part, _ = current_ref.shape
    half = part // 2
    index = lax.axis_index("seq")
    top, bottom = pl.ds(0, half), pl.ds(half, half)
    sems = (send_sems, recv_sems)
    greet([seq_peer(1), seq_peer(2)])
    sums = sum_copies(sent_ref, side_ref, below_ref, far_ref, half, sems)
    row = lax.broadcasted_iota(jnp.int32, (part, part), 0)
    column = lax.broadcasted_iota(jnp.int32, (part, part), 1)

    def one_part(turn, carry):
        step = count - 1 - turn
        here = step ^ index
        rows_here = pl.ds(pl.multiple_of(here * part, part), part)
        rows_step = pl.ds(pl.multiple_of(step * part, part), part)
        for block in range(count):

            @pl.when(here == block)
            def _():
                before = block * part
                seen = before + part
                keys_in, values_in = k_ref[:seen], v_ref[:seen]

                def one_head(head, carry):
                    scores = matmul(q_ref[head, before:seen, :], keys_in, 1, 1)
                    last = jnp.where(row >= column, scores[:, before:], -1e30)
                    scores = jnp.concatenate([scores[:, :before], last], 1) if block else last
                    peak = jnp.max(scores, 1, keepdims=True)
                    weights = jnp.exp(scores - peak)
                    total = jnp.sum(weights, 1, keepdims=True)
                    output = matmul(weights.astype(jnp.bfloat16), values_in, 1, 0) / total
                    held_ref[head] = output.astype(jnp.bfloat16)
                    log_total = jnp.broadcast_to(peak + jnp.log(total), (part, 128))
                    lse_ref[pl.ds(head, 1), before:seen] = jnp.transpose(log_total)[:1]
                    return carry

                lax.fori_loop(0, heads, one_head, 0, unroll=2)

        attn = jnp.concatenate([held_ref[head] for head in range(heads)], 1)
        attn_ref[rows_step, :] = attn
        partial = matmul(attn, weight_ref[...], 1, 1)

        pass_sums(turn, step, partial, sums, sent_ref, side_ref, below_ref, middle_ref, half)
        return carry

    lax.fori_loop(0, count, one_part, 0)
    end_sums(sums, side_ref, below_ref, far_ref, middle_ref, half)
    middle_ref[...] += current_ref[...]
    middle = middle_ref[...]
    scale = lax.rsqrt(jnp.mean(middle * middle, 1, keepdims=True) + EPS)
    scale_ref[...] = jnp.broadcast_to(scale, scale_ref.shape)
    all_ref[0] = (middle * scale * gain_ref[...]).astype(jnp.bfloat16)
    share_own(all_ref, half, sems, sums)


def attend(queries, keys_in, values_in, weight, current, gain, count):
    heads, length, _ = queries.shape
    part, width = current.shape
    vmem = pl.BlockSpec(memory_space=pltpu.VMEM)
    attn, lse, middle, scale, gathered = pl.pallas_call(
        lambda *refs: attend_kernel(count, *refs),
        out_shape=(
            jax.ShapeDtypeStruct((length, heads * HD), jnp.bfloat16),
            jax.ShapeDtypeStruct((heads, length), jnp.float32),
            jax.ShapeDtypeStruct((part, width), jnp.float32),
            jax.ShapeDtypeStruct((part, 128), jnp.float32),
            jax.ShapeDtypeStruct((count, part, width), jnp.bfloat16),
        ),
        in_specs=[vmem] * 6,
        out_specs=[vmem] * 5,
        scratch_shapes=[
            pltpu.VMEM((heads, part, HD), jnp.bfloat16),
            pltpu.VMEM((count, part, width), jnp.bfloat16),
            pltpu.VMEM((2, part // 2, width), jnp.bfloat16),
            pltpu.VMEM((2, part // 2, width), jnp.bfloat16),
            pltpu.VMEM((2, part // 2, width), jnp.bfloat16),
            pltpu.SemaphoreType.DMA((12,)),
            pltpu.SemaphoreType.DMA((12,)),
        ],
        compiler_params=pltpu.CompilerParams(collective_id=2, has_side_effects=True, vmem_limit_bytes=LIMIT),
        name="attend",
    )(queries, keys_in, values_in, weight, current, gain)
    return attn, lse, middle, scale, gathered.reshape(length, width)


def share_start(copies):
    for group in copies:
        group[0].start()
        group[1].start()
    for group in copies:
        group[2].start()
        group[3].start()


def share_on(group):
    group[0].wait_recv()
    group[4].start()
    group[1].wait_recv()
    group[5].start()


def share_end(copies):
    for group in copies:
        for copy in group[2:]:
            copy.wait_recv()
    for group in copies:
        for copy in group:
            copy.wait_send()


def upper_half(rows):
    return -(-(rows // 2) // 16) * 16


def attend_back_kernel(
    count, q_ref, k_ref, v_ref, attn_ref, lse_ref, dy_ref, weight_ref, table_ref, pick_ref, down_ref, middle_ref,
    out_ref, turned_ref, term_ref, result_ref,
    do_ref, delta_ref, dq_ref, dk_ref, dv_ref, side_ref, below_ref, far_ref, passed_ref, send_sems, recv_sems,
):
    heads, length, _ = q_ref.shape
    part = length // count
    wide = jnp.float32
    index = lax.axis_index("seq")
    greet([seq_peer(1), seq_peer(2)])
    half = part // 2
    sums = sum_copies(down_ref, side_ref, below_ref, far_ref, half, (send_sems, recv_sems), passed_ref)
    for copy in sums[:4]:
        copy.start()
    result_ref[...] = middle_ref[...] + down_ref[0].astype(wide)
    dk_ref[...] = jnp.zeros_like(dk_ref)
    dv_ref[...] = jnp.zeros_like(dv_ref)
    owner = lax.broadcasted_iota(jnp.int32, (heads, heads * HD), 1) // HD
    same = (owner == lax.broadcasted_iota(jnp.int32, (heads, heads * HD), 0)).astype(wide)
    row = lax.broadcasted_iota(jnp.int32, (part, part), 0)
    column = lax.broadcasted_iota(jnp.int32, (part, part), 1)

    def unturn(grads, cosines, sines):
        return grads * cosines + swap_halves(grads * sines)

    def one_part(here, carry):
        spot = here ^ index
        rows_here = pl.ds(pl.multiple_of(spot * part, part), part)
        dattn = matmul(dy_ref[rows_here, :], weight_ref[...], 1, 0).astype(jnp.bfloat16)
        product = dattn.astype(wide) * attn_ref[rows_here, :].astype(wide)
        delta_ref[...] = lax.dot_general(
            same, product, (((1,), (1,)), ((), ())), precision=lax.Precision.HIGHEST, preferred_element_type=wide
        )
        for head in range(heads):
            do_ref[head] = dattn[:, head * HD : (head + 1) * HD]
        for block in range(count):

            @pl.when(here == block)
            def _():
                before = block * part
                seen = before + part
                keys_in, values_in = k_ref[:seen], v_ref[:seen]

                def one_head(head, carry):
                    query, dout = q_ref[head, before:seen, :], do_ref[head]
                    scores = matmul(keys_in, query, 1, 1)
                    last = jnp.where(row <= column, scores[before:], -1e30)
                    scores = jnp.concatenate([scores[:before], last], 0) if block else last
                    probs = jnp.exp(scores - lse_ref[pl.ds(head, 1), before:seen])
                    dprob = matmul(values_in, dout, 1, 1)
                    dscore = (probs * (dprob - delta_ref[pl.ds(head, 1), :])).astype(jnp.bfloat16)
                    dv_ref[:seen] += matmul(probs.astype(jnp.bfloat16), dout, 1, 0)
                    dk_ref[:seen] += matmul(dscore, query, 1, 0)
                    dq_ref[head] = (matmul(dscore, keys_in, 0, 0) * ROOT).astype(jnp.bfloat16)
                    return carry

                lax.fori_loop(0, heads, one_head, 0, unroll=2)

        dq = jnp.concatenate([dq_ref[head] for head in range(heads)], 1).astype(wide)
        dq = unturn(dq, *spread_tables(table_ref[rows_here, :], heads // 2, False))
        out_ref[rows_here, : heads * HD] = dq.astype(jnp.bfloat16)

        @pl.when(here == 1)
        def _():
            sums[0].wait_recv()
            passed_ref[0] = (down_ref[2, :half].astype(wide) + side_ref[1].astype(wide)).astype(jnp.bfloat16)
            sums[4].start()
            sums[1].wait_recv()
            passed_ref[1] = (down_ref[1, half:].astype(wide) + below_ref[1].astype(wide)).astype(jnp.bfloat16)
            sums[5].start()

        return carry

    lax.fori_loop(0, count, one_part, 0)
    for block in range(count):
        rows_there = pl.ds(pl.multiple_of((block ^ index) * part, part), part)
        rows_block = slice(block * part, (block + 1) * part)
        both = jnp.concatenate([dk_ref[rows_block], dv_ref[rows_block]], 1).astype(jnp.bfloat16).astype(wide)
        both = unturn(both, *spread_tables(table_ref[rows_there, :], 0, True))
        out_ref[rows_there, heads * HD :] = both.astype(jnp.bfloat16)
    chosen = matmul(pick_ref[...], out_ref[...], 1, 1).astype(jnp.bfloat16)
    size = turned_ref.shape[1]
    for block in range(count):
        turned_ref[block] = chosen[block * size : (block + 1) * size]
    tile = 2 * 128

    def one_tile(number, carry):
        columns = pl.ds(pl.multiple_of(number * tile, tile), tile)
        term_ref[columns, :] = matmul(dy_ref[:, columns], attn_ref[...], 0, 0).astype(jnp.bfloat16)
        return carry

    lax.fori_loop(0, dy_ref.shape[1] // tile, one_tile, 0)
    end_sums(sums, side_ref, below_ref, far_ref, result_ref, half)
    for copy in sums:
        copy.wait_send()


def attend_back(queries, keys_in, values_in, attn, lse, dy, weight, table, pick, down, middle, count):
    heads, length, _ = queries.shape
    part, width = middle.shape
    columns = (heads + 2) * HD
    vmem = pl.BlockSpec(memory_space=pltpu.VMEM)
    return pl.pallas_call(
        lambda *refs: attend_back_kernel(count, *refs),
        out_shape=[
            jax.ShapeDtypeStruct((length, columns), jnp.bfloat16),
            jax.ShapeDtypeStruct((count, columns // count, length), jnp.bfloat16),
            jax.ShapeDtypeStruct((width, heads * HD), jnp.bfloat16),
            jax.ShapeDtypeStruct((part, width), jnp.float32),
        ],
        in_specs=[vmem] * 11,
        out_specs=[vmem] * 4,
        scratch_shapes=[
            pltpu.VMEM((heads, part, HD), jnp.bfloat16),
            pltpu.VMEM((heads, part), jnp.float32),
            pltpu.VMEM((heads, part, HD), jnp.bfloat16),
            pltpu.VMEM((length, HD), jnp.float32),
            pltpu.VMEM((length, HD), jnp.float32),
        ]
        + [pltpu.VMEM((2, part // 2, width), jnp.bfloat16)] * 4
        + [pltpu.SemaphoreType.DMA((6,)), pltpu.SemaphoreType.DMA((6,))],
        compiler_params=pltpu.CompilerParams(collective_id=4, has_side_effects=True, vmem_limit_bytes=LIMIT),
        name="attend_back",
    )(queries, keys_in, values_in, attn, lse, dy, weight, table, pick, down, middle)


def leave_kernel(
    count, grads_ref, weight_ref, flowing_ref, first_ref, scale_ref, gain_ref, turned_ref, normed_ref,
    own_ref, gain_out_ref, term_ref,
    sent_ref, side_ref, below_ref, far_ref, slot_ref, whole_ref, send_sems, recv_sems, swap_send, swap_recv,
):
    part, _ = flowing_ref.shape
    half = part // 2
    size = turned_ref.shape[1]
    heads = H // count
    chunk = size // (heads + 2)
    index = lax.axis_index("seq")
    greet([seq_peer(step) for step in range(1, count)])
    swaps = [
        remote(turned_ref.at[index ^ step], slot_ref.at[step], (swap_send, swap_recv), step - 1, seq_peer(step))
        for step in range(1, count)
    ]
    for copy in swaps:
        copy.start()
    slot_ref[0] = turned_ref[index]
    sums = sum_copies(sent_ref, side_ref, below_ref, far_ref, half, (send_sems, recv_sems))

    def one_part(turn, carry):
        step = count - 1 - turn
        rows_step = pl.ds(pl.multiple_of(step * part, part), part)
        partial = matmul(grads_ref[rows_step, :], weight_ref[...], 1, 0)
        pass_sums(turn, step, partial, sums, sent_ref, side_ref, below_ref, own_ref, half)
        return carry

    lax.fori_loop(0, count, one_part, 0)
    for step in range(count):
        if step:
            swaps[step - 1].wait_recv()
        peer = index ^ step
        for block in range(count):
            piece = slot_ref[step, :, (step ^ block) * part : ((step ^ block) + 1) * part]
            tokens = slice(block * part, (block + 1) * part)
            for start, rows in ((0, heads * chunk), (H * chunk, chunk), ((H + KVH) * chunk, chunk)):
                begin = 0 if start == 0 else heads * chunk + (0 if start == H * chunk else chunk)
                spot = pl.multiple_of(start + peer * rows, chunk)
                whole_ref[pl.ds(spot, rows), tokens] = piece[begin : begin + rows]
    term_ref[...] = matmul(whole_ref[...], normed_ref[...], 1, 0).astype(jnp.bfloat16)
    end_sums(sums, side_ref, below_ref, far_ref, own_ref, half)
    unit = first_ref[...] * scale_ref[:, :1]
    grads = own_ref[...]
    gain_out_ref[...] = jnp.sum(grads * unit, 0, keepdims=True)
    inner = grads * gain_ref[...]
    own_ref[...] = flowing_ref[...] + scale_ref[:, :1] * (inner - unit * jnp.mean(inner * unit, 1, keepdims=True))
    for copy in sums + swaps:
        copy.wait_send()


def leave(grads, weight, flowing, first, scale, gain, turned, normed, count):
    part, width = flowing.shape
    vmem = pl.BlockSpec(memory_space=pltpu.VMEM)
    size, length = turned.shape[1:]
    own, gain_term, term = pl.pallas_call(
        lambda *refs: leave_kernel(count, *refs),
        out_shape=(
            jax.ShapeDtypeStruct((part, width), jnp.float32),
            jax.ShapeDtypeStruct((1, width), jnp.float32),
            jax.ShapeDtypeStruct((size * count, width), jnp.bfloat16),
        ),
        in_specs=[vmem] * 8,
        out_specs=[vmem] * 3,
        scratch_shapes=[
            pltpu.VMEM((count, part, width), jnp.bfloat16),
            pltpu.VMEM((2, part // 2, width), jnp.bfloat16),
            pltpu.VMEM((2, part // 2, width), jnp.bfloat16),
            pltpu.VMEM((2, part // 2, width), jnp.bfloat16),
            pltpu.VMEM((count, size, length), jnp.bfloat16),
            pltpu.VMEM((count * size, length), jnp.bfloat16),
            pltpu.SemaphoreType.DMA((6,)),
            pltpu.SemaphoreType.DMA((6,)),
            pltpu.SemaphoreType.DMA((count - 1,)),
            pltpu.SemaphoreType.DMA((count - 1,)),
        ],
        compiler_params=pltpu.CompilerParams(collective_id=5, has_side_effects=True, vmem_limit_bytes=LIMIT),
        name="leave",
    )(grads, weight, flowing, first, scale, gain, turned, normed)
    return own, gain_term[0], term


def share_kernel(number, fsdp, *refs):
    extra = 1 if fsdp else 0
    shards, slots = refs[:number], refs[number + extra : 2 * number + extra]
    send_sems, recv_sems = refs[2 * number + 2 * extra : 2 * number + 2 * extra + 2]
    peers = [seq_peer(1), seq_peer(2)]
    steps = []
    if fsdp:
        term_ref, total_ref = refs[number], refs[2 * number + 1]
        heard_ref, told_ref, sum_send, sum_recv = refs[2 * number + 4 :]
        place = lax.axis_index("fsdp")
        steps = [seq_peer(1), seq_peer(2)] + [fsdp_peer(place ^ (1 << bit)) for bit in range(fsdp.bit_length() - 1)]
        peers += steps[2:]
    greet(peers)
    copies = [
        gather_copies(shard, slot, upper_half(shard.shape[0]), (send_sems, recv_sems), 6 * spot)
        for spot, (shard, slot) in enumerate(zip(shards, slots))
    ]
    share_start(copies)
    if fsdp:
        total_ref[...] = term_ref[...]
    tells = []
    for step, peer in enumerate(steps):
        told_ref[step] = total_ref[...]
        tell = remote(told_ref.at[step], heard_ref.at[step], (sum_send, sum_recv), step, peer)
        tell.start()
        tell.wait_recv()
        total_ref[...] += heard_ref[step]
        tells.append(tell)
    for shard, slot in zip(shards, slots):
        slot[0] = shard[...]
    for group in copies:
        share_on(group)
    share_end(copies)
    for tell in tells:
        tell.wait_send()


def share(name, shards, count, term=None):
    vmem = pl.BlockSpec(memory_space=pltpu.VMEM)
    fsdp = lax.axis_size("fsdp") if term is not None else 0
    extra = [] if term is None else [term]
    scratch = [pltpu.SemaphoreType.DMA((6 * len(shards),)) for _ in range(2)]
    if fsdp:
        steps = fsdp.bit_length() + 1
        scratch += [pltpu.VMEM((steps,) + term.shape, term.dtype) for _ in range(2)]
        scratch += [pltpu.SemaphoreType.DMA((steps,)) for _ in range(2)]
    return pl.pallas_call(
        lambda *refs: share_kernel(len(shards), fsdp, *refs),
        out_shape=[jax.ShapeDtypeStruct((count,) + shard.shape, shard.dtype) for shard in shards]
        + [jax.ShapeDtypeStruct(value.shape, value.dtype) for value in extra],
        in_specs=[vmem] * (len(shards) + len(extra)),
        out_specs=[vmem] * (len(shards) + len(extra)),
        scratch_shapes=scratch,
        compiler_params=pltpu.CompilerParams(
            collective_id=name, has_side_effects=True, vmem_limit_bytes=LIMIT
        ),
        name="share",
    )(*shards, *extra)


def join_rows_kernel(index_ref, *refs):
    out_ref = refs[-1]
    out_ref[...] = jnp.concatenate([ref[0] for ref in refs[:-1]], 1).astype(jnp.float32)


def join_rows(index, slots, count):
    rows = slots[0].shape[1]
    width = sum(slot.shape[2] for slot in slots)
    return pl.pallas_call(
        join_rows_kernel,
        out_shape=jax.ShapeDtypeStruct((rows * count, width), jnp.float32),
        grid_spec=pltpu.PrefetchScalarGridSpec(
            num_scalar_prefetch=1,
            grid=(count,),
            in_specs=[pl.BlockSpec((1,) + slot.shape[1:], lambda i, s: (i ^ s[0], 0, 0)) for slot in slots],
            out_specs=pl.BlockSpec((rows, width), lambda i, s: (i, 0)),
        ),
        compiler_params=pltpu.CompilerParams(vmem_limit_bytes=LIMIT),
        name="join_rows",
    )(index, *slots)


def join_pieces_kernel(count, row_piece, column_piece, index_ref, slot_ref, out_ref):
    index = index_ref[0]
    _, rows, columns = slot_ref.shape
    for device in range(count):
        values = slot_ref[device ^ index].astype(jnp.float32)
        for top in range(0, rows, row_piece):
            for left in range(0, columns, column_piece):
                down = top * count + device * row_piece if row_piece < rows else top
                across = left * count + device * column_piece if row_piece == rows else left
                out_ref[down : down + row_piece, across : across + column_piece] = values[
                    top : top + row_piece, left : left + column_piece
                ]


def join_pieces(index, slots, row_piece, column_piece):
    count, rows, columns = slots.shape
    shape = (rows * count, columns) if row_piece < rows else (rows, columns * count)
    return pl.pallas_call(
        lambda *refs: join_pieces_kernel(count, row_piece, column_piece, *refs),
        out_shape=jax.ShapeDtypeStruct(shape, jnp.float32),
        grid_spec=pltpu.PrefetchScalarGridSpec(
            num_scalar_prefetch=1,
            grid=(1,),
            in_specs=[pl.BlockSpec(slots.shape, lambda i, s: (0, 0, 0))],
            out_specs=pl.BlockSpec(shape, lambda i, s: (0, 0)),
        ),
        compiler_params=pltpu.CompilerParams(vmem_limit_bytes=LIMIT),
        name="join_pieces",
    )(index, slots)


def norm_back_kernel(
    count, grads_ref, weight_ref, flowing_ref, middle_ref, scale_ref, gain_ref, inputs_ref,
    own_ref, gain_out_ref, dy_ref, left_ref, right_ref,
    sent_ref, side_ref, below_ref, far_ref, stage_ref, send_sems, recv_sems, store_sems,
):
    part, width = flowing_ref.shape
    half = part // 2
    sems = (send_sems, recv_sems)
    greet([seq_peer(1), seq_peer(2)])
    sums = sum_copies(sent_ref, side_ref, below_ref, far_ref, half, sems)

    def one_part(turn, carry):
        step = count - 1 - turn
        rows_step = pl.ds(pl.multiple_of(step * part, part), part)
        partial = matmul(grads_ref[rows_step, :], weight_ref[...], 1, 0)
        pass_sums(turn, step, partial, sums, sent_ref, side_ref, below_ref, own_ref, half)
        return carry

    lax.fori_loop(0, count, one_part, 0)

    tile = stage_ref.shape[1]
    tiles = grads_ref.shape[1] // tile

    def stores(number):
        slot = number % 2
        rows = pl.ds(pl.multiple_of(number * tile, tile), tile)
        return [
            pltpu.make_async_copy(
                stage_ref.at[slot, :, pl.ds(place * (width // 2), width // 2)],
                target.at[rows],
                store_sems.at[place, slot],
            )
            for place, target in enumerate((left_ref, right_ref))
        ]

    def one_tile(number, carry):
        @pl.when(number >= 2)
        def _():
            for store in stores(number - 2):
                store.wait()

        columns = pl.ds(pl.multiple_of(number * tile, tile), tile)
        stage_ref[number % 2] = matmul(grads_ref[:, columns], inputs_ref[...], 0, 0).astype(jnp.bfloat16)
        for store in stores(number):
            store.start()
        return carry

    lax.fori_loop(0, tiles, one_tile, 0)
    end_sums(sums, side_ref, below_ref, far_ref, own_ref, half)
    scale = scale_ref[:, :1]
    unit = middle_ref[...] * scale
    grads = own_ref[...]
    gain_out_ref[...] = jnp.sum(grads * unit, 0, keepdims=True)
    inner = grads * gain_ref[...]
    own_ref[...] = flowing_ref[...] + scale * (inner - unit * jnp.mean(inner * unit, 1, keepdims=True))
    dy_ref[...] = own_ref[...].astype(jnp.bfloat16)
    for number in range(tiles - 2, tiles):
        for store in stores(number):
            store.wait()
    for copy in sums:
        copy.wait_send()


def norm_back(grads, weight, flowing, middle, scale, gain, inputs, count):
    part, width = flowing.shape
    units = grads.shape[1]
    tile = 2 * 128
    vmem = pl.BlockSpec(memory_space=pltpu.VMEM)
    own, gain_term, dy, left, right = pl.pallas_call(
        lambda *refs: norm_back_kernel(count, *refs),
        out_shape=(
            jax.ShapeDtypeStruct((part, width), jnp.float32),
            jax.ShapeDtypeStruct((1, width), jnp.float32),
            jax.ShapeDtypeStruct((part, width), jnp.bfloat16),
            jax.ShapeDtypeStruct((units, width // 2), jnp.bfloat16),
            jax.ShapeDtypeStruct((units, width // 2), jnp.bfloat16),
        ),
        in_specs=[vmem] * 7,
        out_specs=[vmem] * 3 + [pl.BlockSpec(memory_space=pl.ANY)] * 2,
        scratch_shapes=[
            pltpu.VMEM((count, part, width), jnp.bfloat16),
            pltpu.VMEM((2, part // 2, width), jnp.bfloat16),
            pltpu.VMEM((2, part // 2, width), jnp.bfloat16),
            pltpu.VMEM((2, part // 2, width), jnp.bfloat16),
            pltpu.VMEM((2, tile, width), jnp.bfloat16),
            pltpu.SemaphoreType.DMA((6,)),
            pltpu.SemaphoreType.DMA((6,)),
            pltpu.SemaphoreType.DMA((2, 2)),
        ],
        compiler_params=pltpu.CompilerParams(collective_id=3, has_side_effects=True, vmem_limit_bytes=LIMIT),
        name="norm_back",
    )(grads, weight, flowing, middle, scale, gain, inputs)
    return own, gain_term[0], dy, left, right


def share_dy_kernel(count, dy_ref, act_ref, weight_ref, all_ref, down_ref, send_sems, recv_sems):
    part = dy_ref.shape[0]
    greet([seq_peer(1), seq_peer(2)])
    group = gather_copies(dy_ref, all_ref, part // 2, (send_sems, recv_sems))
    share_start([group])
    all_ref[0] = dy_ref[...]

    def one_part(step, carry):
        rows = pl.ds(pl.multiple_of(step * part, part), part)
        down_ref[step] = matmul(act_ref[rows, :], weight_ref[...], 1, 1).astype(jnp.bfloat16)
        return carry

    lax.fori_loop(0, count, one_part, 0)
    share_on(group)
    share_end([group])


def share_dy(dy, act, weight, count):
    part, width = dy.shape
    vmem = pl.BlockSpec(memory_space=pltpu.VMEM)
    gathered, down = pl.pallas_call(
        lambda *refs: share_dy_kernel(count, *refs),
        out_shape=[jax.ShapeDtypeStruct((count, part, width), jnp.bfloat16)] * 2,
        in_specs=[vmem] * 3,
        out_specs=[vmem] * 2,
        scratch_shapes=[pltpu.SemaphoreType.DMA((6,)), pltpu.SemaphoreType.DMA((6,))],
        compiler_params=pltpu.CompilerParams(collective_id=8, has_side_effects=True, vmem_limit_bytes=LIMIT),
        name="share_dy",
    )(dy, act, weight)
    return gathered.reshape(part * count, width), down


def fast_body(hidden, positions, gains, w_qkv, w_out, w_gate_up, w_down, cotangent):
    count = lax.axis_size("seq")
    fsdp = lax.axis_size("fsdp")
    index = lax.axis_index("seq")
    place = index.astype(jnp.int32).reshape(1)
    current = hidden[0]
    part_len, width = current.shape
    heads = H // count
    gain = gains[0]
    after = lax.optimization_barrier

    rows = w_qkv.shape[1]
    group = math.gcd(rows, HD)
    chunk = group // count
    per_head = HD // group
    normed, scale_one = normalize(current, gain[0])
    scale_one = jnp.broadcast_to(scale_one, (part_len, 128))
    normed_all, qkv_rows, out_cols, table = enter(normed, positions[0], w_qkv[0], w_out[0], count)
    normed_all, gate_up_shard = after((normed_all, w_gate_up[0]))
    gu_rows = w_gate_up.shape[1] // count
    gate_up = lax.all_gather(
        lax.dynamic_slice_in_dim(gate_up_shard, index * gu_rows, gu_rows, 0), "fsdp", axis=0, tiled=True
    )
    units = FF // count
    down_rows = w_down.shape[1]
    down_cols = lax.all_gather(
        lax.dynamic_index_in_dim(
            w_down[0].reshape(down_rows, fsdp // 2, count, gu_rows), index, 2, keepdims=False
        ).reshape(down_rows, units),
        "fsdp",
        axis=0,
        tiled=True,
    )

    queries, keys_in, values_in = project_qkv(place, normed_all, qkv_rows, table, count)
    attn_flat, log_total, middle, scale_two, normed_two_all = attend(
        queries, keys_in, values_in, out_cols, current, gain[1:], count
    )
    flowing = cotangent[0]
    normed_two_all, dm_sent = after((normed_two_all, flowing.astype(jnp.bfloat16)))
    dm_all = jnp.concatenate([dm_sent] + [neighbour(dm_sent, step) for step in range(1, count)], 0)
    both = matmul(normed_two_all, gate_up, 1, 1)
    gate_part, up_part = both[:, :units], both[:, units:]
    activated = (jax.nn.silu(gate_part) * up_part).astype(jnp.bfloat16)

    def owned(grad):
        return lax.psum_scatter(grad.astype(jnp.bfloat16), "fsdp", scatter_dimension=0, tiled=True)

    term_down = matmul(dm_all, activated, 0, 0).astype(jnp.bfloat16)
    dm_all, term_down = after((dm_all, term_down))
    grad_down = owned(term_down)
    dact = matmul(dm_all, down_cols, 1, 0)
    sigma = jax.nn.sigmoid(gate_part)
    dgate = dact * up_part * sigma * (1.0 + gate_part * (1.0 - sigma))
    dup = dact * gate_part * sigma
    dgu = jnp.concatenate([dgate, dup], 1).astype(jnp.bfloat16)
    dmiddle, gain_two, dy, *terms_gate_up = norm_back(
        dgu, gate_up, flowing, middle, scale_two, gain[1:], normed_two_all, count
    )
    grads_gate_up = [owned(terms_gate_up[0]), owned(terms_gate_up[1])]
    dy_all, down_sent = share_dy(dy, activated, down_cols, count)
    pieces = heads + 2
    picked = np.arange(pieces * HD).reshape(pieces * per_head, count, chunk).transpose(1, 0, 2).reshape(-1)
    pick = jnp.asarray(picked[:, None] == np.arange(pieces * HD)[None, :], jnp.bfloat16)
    djoint, djoint_turned, term_out, result = attend_back(
        queries, keys_in, values_in, attn_flat, log_total, dy_all, out_cols, table, pick, down_sent, middle, count
    )
    grad_out = owned(term_out)
    grad_hidden, gain_one, term_qkv = leave(
        djoint, qkv_rows, dmiddle, current, scale_one, gain[:1], djoint_turned, normed_all, count
    )
    grad_qkv = owned(term_qkv)
    down_slots, gate_up_slots, gain_total = share(
        6, (grad_down, grads_gate_up[0]), count, jnp.stack([gain_one, gain_two])
    )
    grad_gate_up_b, gate_up_slots = after((grads_gate_up[1], gate_up_slots))
    gate_up_slots_b, out_slots = share(7, (grad_gate_up_b, grad_out), count)
    gate_up_slots_b, grad_qkv = after((gate_up_slots_b, grad_qkv))
    (qkv_slots,) = share(9, (grad_qkv,), count)
    gain_total = gain_total[None]
    down_shard = join_pieces(place, down_slots, down_rows, gu_rows)
    gate_up_shard = join_rows(place, (gate_up_slots, gate_up_slots_b), count)
    out_shard = join_pieces(place, out_slots, down_rows, heads * HD)
    qkv_shard = join_pieces(place, qkv_slots, chunk, width)
    return (
        result[None],
        grad_hidden[None],
        gain_total,
        qkv_shard[None],
        out_shard[None],
        gate_up_shard[None],
        down_shard[None],
    )


def fits(mesh):
    count, fsdp = mesh.shape["seq"], mesh.shape["fsdp"]
    rows = (H + 2 * KVH) * HD // fsdp
    return count == KVH == 4 and fsdp % 2 == 0 and fsdp & (fsdp - 1) == 0 and rows % HD == 0


def solution(mesh):
    placed = (
        P("fsdp", "seq", None),
        P("fsdp", "seq"),
        P(),
        P(None, "fsdp", None),
        P(None, "fsdp", None),
        P(None, "fsdp", None),
        P(None, "fsdp", None),
        P("fsdp", "seq", None),
    )
    fast = fits(mesh)
    return jax.shard_map(
        fast_body if fast else body,
        mesh=mesh,
        in_specs=placed,
        out_specs=(
            P("fsdp", "seq", None),
            P("fsdp", "seq", None),
            P(),
            P(None, "fsdp", None),
            P(None, "fsdp", None),
            P(None, "fsdp", None),
            P(None, "fsdp", None),
        ),
        check_vma=False,
    )
```

```python
import math

import jax
import jax.numpy as jnp
import numpy as np
from jax import lax
from jax.experimental import pallas as pl
from jax.experimental.pallas import tpu as pltpu
from jax.sharding import PartitionSpec as P


H = 32
KVH = 4
HD = 64
FF = 5632
LAYERS = 1


EPS = 1e-05


def rope_tables(position_ids):
    halfway = HD // 2
    frequency = jnp.exp(jnp.arange(halfway, dtype=jnp.float32) * (-2.0 * math.log(10000.0) / HD))
    angles = position_ids.astype(jnp.float32)[..., None] * frequency
    cosines = jnp.cos(angles)
    sines = jnp.sin(angles)
    return (
        jnp.concatenate([cosines, cosines], -1)[..., None, :],
        jnp.concatenate([sines, sines], -1)[..., None, :],
    )


def rotate(values, cosines, sines):
    halfway = values.shape[-1] // 2
    turned = jnp.concatenate([-values[..., halfway:], values[..., :halfway]], -1)
    return values * cosines + turned * sines


def unrotate(grads, cosines, sines):
    halfway = grads.shape[-1] // 2
    scaled = grads * sines
    return grads * cosines + jnp.concatenate([scaled[..., halfway:], -scaled[..., :halfway]], -1)


def normalize(values, gain):
    scale = lax.rsqrt(jnp.mean(values * values, -1, keepdims=True) + EPS)
    return ((values * scale * gain).astype(jnp.bfloat16), scale)


def normalize_back(grads, values, scale, gain):
    unit = values * scale
    gain_grad = jnp.sum((grads * unit).reshape(-1, unit.shape[-1]), 0)
    inner = grads * gain
    return (scale * (inner - unit * jnp.mean(inner * unit, -1, keepdims=True)), gain_grad)


def masked_scores(queries, keys_wide):
    scores = jnp.einsum(
        "qhd,khd->hqk", queries, keys_wide, preferred_element_type=jnp.float32
    ) * queries.shape[-1] ** (-0.5)
    length = queries.shape[0]
    causal = jnp.arange(length)[:, None] >= jnp.arange(length)[None, :]
    return jnp.where(causal[None], scores, -1e30)


def local_attend(operands):
    queries, keys_in, values_in = operands
    repeat_by = queries.shape[1] // keys_in.shape[1]
    keys_wide = jnp.repeat(keys_in, repeat_by, axis=1)
    values_wide = jnp.repeat(values_in, repeat_by, axis=1)
    scores = masked_scores(queries, keys_wide)
    peak = jnp.max(scores, -1, keepdims=True)
    log_total = peak[..., 0] + jnp.log(jnp.sum(jnp.exp(scores - peak), -1))
    weights = jnp.exp(scores - log_total[..., None]).astype(jnp.bfloat16)
    output = jnp.einsum("hqk,khd->qhd", weights, values_wide, preferred_element_type=jnp.float32)
    return (output.astype(jnp.bfloat16), log_total)


def local_attend_back(operands):
    queries, keys_in, values_in, output, log_total, dattn = operands
    length, kv_dev, head_dim = keys_in.shape
    repeat_by = queries.shape[1] // kv_dev
    keys_wide = jnp.repeat(keys_in, repeat_by, axis=1)
    values_wide = jnp.repeat(values_in, repeat_by, axis=1)
    scores = masked_scores(queries, keys_wide)
    probs = jnp.exp(scores - log_total[..., None])
    delta = jnp.sum(output.astype(jnp.float32) * dattn.astype(jnp.float32), -1).T
    dprob = jnp.einsum("qhd,khd->hqk", dattn, values_wide, preferred_element_type=jnp.float32)
    dscore = (probs * (dprob - delta[..., None])).astype(jnp.bfloat16)
    dqueries = jnp.einsum(
        "hqk,khd->qhd", dscore, keys_wide, preferred_element_type=jnp.float32
    ) * head_dim ** (-0.5)
    dkeys = jnp.einsum(
        "hqk,qhd->khd", dscore, queries, preferred_element_type=jnp.float32
    ) * head_dim ** (-0.5)
    dvalues = jnp.einsum(
        "hqk,qhd->khd", probs.astype(jnp.bfloat16), dattn, preferred_element_type=jnp.float32
    )

    def fold_heads(per_head):
        return jnp.sum(per_head.reshape(length, kv_dev, repeat_by, head_dim), 2).astype(
            jnp.bfloat16
        )

    return (dqueries.astype(jnp.bfloat16), fold_heads(dkeys), fold_heads(dvalues))


def project(inputs, weight):
    return lax.dot_general(
        inputs,
        lax.all_gather(weight, "fsdp", axis=0, tiled=True),
        (((1,), (1,)), ((), ())),
        preferred_element_type=jnp.float32,
    )


def project_back(grads, weight):
    shard_rows = lax.all_gather(weight, "fsdp", axis=0, tiled=True)
    picked = lax.slice_in_dim(grads, 0, shard_rows.shape[0], axis=1)
    return jnp.dot(picked, shard_rows, preferred_element_type=jnp.float32)


def weight_grad(grads, inputs, shard_size):
    picked = lax.slice_in_dim(grads, 0, shard_size * lax.axis_size("fsdp"), axis=1)
    summed = lax.psum_scatter(
        lax.dot_general(
            picked, inputs, (((0,), (0,)), ((), ())), preferred_element_type=jnp.float32
        ).astype(jnp.bfloat16),
        "fsdp",
        scatter_dimension=0,
        tiled=True,
    )
    return lax.psum(summed, "seq").astype(jnp.float32)


def backward_pair(grads, inputs, weight):
    wgrad = weight_grad(grads, inputs, weight.shape[0])
    return (project_back(grads, weight), wgrad)


def body(hidden, positions, gains, w_qkv, w_out, w_gate_up, w_down, cotangent):
    seq_count, part_len, model_width = hidden.shape
    row_count = seq_count * part_len
    group_count = lax.axis_size("seq")
    full_len = part_len * group_count
    heads_dev = H // group_count
    share = H // KVH
    kv_dev = max(1, heads_dev // share)
    first_kv = np.arange(group_count) * heads_dev // share
    slot_table = np.concatenate(
        [
            first_kv[:, None] + np.arange(kv_dev)[None, :],
            KVH + first_kv[:, None] + np.arange(kv_dev)[None, :],
        ],
        1,
    ).reshape(-1)
    slot_onehot = jnp.asarray(
        (slot_table[:, None] == np.arange(2 * KVH)[None, :]).astype(np.float32), jnp.bfloat16
    )
    cosines, sines = rope_tables(positions)
    layer_index = 0
    gain = gains[layer_index]
    normed, scale_one = normalize(hidden, gain[0])
    normed_flat = normed.reshape(row_count, model_width)
    joint = project(normed_flat, w_qkv[layer_index]).reshape(seq_count, part_len, -1)
    queries = joint[..., : H * HD].reshape(seq_count, part_len, H, HD)
    keys_in = joint[..., H * HD : (H + KVH) * HD].reshape(seq_count, part_len, KVH, HD)
    values_in = joint[..., (H + KVH) * HD :].reshape(seq_count, part_len, KVH, HD)
    q_rot = rotate(queries, cosines, sines).astype(jnp.bfloat16)
    kv_all = jnp.concatenate(
        [rotate(keys_in, cosines, sines).astype(jnp.bfloat16), values_in.astype(jnp.bfloat16)], 2
    )
    q_send = q_rot.reshape(seq_count, part_len, group_count, heads_dev * HD)
    kv_send = jnp.take(kv_all, slot_table, axis=2).reshape(
        seq_count, part_len, group_count, 2 * kv_dev * HD
    )
    q_heads = lax.all_to_all(q_send, "seq", split_axis=2, concat_axis=1, tiled=True)
    kv_heads = lax.all_to_all(kv_send, "seq", split_axis=2, concat_axis=1, tiled=True)
    q_heads = q_heads.reshape(seq_count, full_len, heads_dev, HD)
    kv_heads = kv_heads.reshape(seq_count, full_len, 2 * kv_dev, HD)
    k_heads = kv_heads[:, :, :kv_dev]
    v_heads = kv_heads[:, :, kv_dev:]
    o_heads, log_total = lax.map(local_attend, (q_heads, k_heads, v_heads))
    o_back = lax.all_to_all(
        o_heads.reshape(seq_count, full_len, 1, heads_dev * HD),
        "seq",
        split_axis=1,
        concat_axis=2,
        tiled=True,
    )
    attn_flat = o_back.reshape(row_count, model_width)
    middle = hidden + project(attn_flat, w_out[layer_index]).reshape(
        seq_count, part_len, model_width
    )
    normed_two, scale_two = normalize(middle, gain[1])
    normed_two_flat = normed_two.reshape(row_count, model_width)
    both = project(normed_two_flat, w_gate_up[layer_index])
    gate_part = both[:, :FF]
    up_part = both[:, FF:]
    activated = (jax.nn.silu(gate_part) * up_part).astype(jnp.bfloat16)
    result = middle + project(activated, w_down[layer_index]).reshape(
        seq_count, part_len, model_width
    )
    saved = [
        (
            hidden,
            normed_flat,
            scale_one,
            q_heads,
            k_heads,
            v_heads,
            o_heads,
            log_total,
            attn_flat,
            middle,
            normed_two_flat,
            scale_two,
            gate_part,
            up_part,
            activated,
        )
    ]
    flowing = cotangent
    grads_qkv = [None] * LAYERS
    grads_out = [None] * LAYERS
    grads_gate_up = [None] * LAYERS
    grads_down = [None] * LAYERS
    gain_terms = [None] * LAYERS
    for layer_index in reversed(range(LAYERS)):
        (
            layer_in,
            normed_flat,
            scale_one,
            q_heads,
            k_heads,
            v_heads,
            o_heads,
            log_total,
            attn_flat,
            middle,
            normed_two_flat,
            scale_two,
            gate_part,
            up_part,
            activated,
        ) = saved[layer_index]
        gain = gains[layer_index]
        dm_cast = flowing.reshape(row_count, model_width).astype(jnp.bfloat16)
        dact, grads_down[layer_index] = backward_pair(dm_cast, activated, w_down[layer_index])
        sigma = jax.nn.sigmoid(gate_part)
        dgate = dact * up_part * sigma * (1.0 + gate_part * (1.0 - sigma))
        dup = dact * gate_part * sigma
        dgu = jnp.concatenate([dgate, dup], 1).astype(jnp.bfloat16)
        dnormed_two, grads_gate_up[layer_index] = backward_pair(
            dgu, normed_two_flat, w_gate_up[layer_index]
        )
        dnormed_two = dnormed_two.reshape(seq_count, part_len, model_width)
        dmid_norm, gain_two = normalize_back(dnormed_two, middle, scale_two, gain[1])
        dmiddle = flowing + dmid_norm
        dy_cast = dmiddle.reshape(row_count, model_width).astype(jnp.bfloat16)
        dattn_wide, grads_out[layer_index] = backward_pair(dy_cast, attn_flat, w_out[layer_index])
        dattn = dattn_wide.astype(jnp.bfloat16)
        dattn_heads = lax.all_to_all(
            dattn.reshape(seq_count, part_len, group_count, heads_dev * HD),
            "seq",
            split_axis=2,
            concat_axis=1,
            tiled=True,
        )
        dattn_heads = dattn_heads.reshape(seq_count, full_len, heads_dev, HD)
        dq_heads, dk_heads, dv_heads = lax.map(
            local_attend_back, (q_heads, k_heads, v_heads, o_heads, log_total, dattn_heads)
        )
        dkv_heads = jnp.concatenate([dk_heads, dv_heads], 2).reshape(
            seq_count, full_len, 1, 2 * kv_dev * HD
        )
        dq_tok, dkv_tok = (
            lax.all_to_all(
                dq_heads.reshape(seq_count, full_len, 1, heads_dev * HD),
                "seq",
                split_axis=1,
                concat_axis=2,
                tiled=True,
            ),
            lax.all_to_all(dkv_heads, "seq", split_axis=1, concat_axis=2, tiled=True),
        )
        dqueries = dq_tok.reshape(seq_count, part_len, H, HD)
        dkv_sum = jnp.einsum(
            "stnd,nm->stmd",
            dkv_tok.reshape(seq_count, part_len, group_count * 2 * kv_dev, HD),
            slot_onehot,
            preferred_element_type=jnp.float32,
        )
        dq_pre = unrotate(dqueries, cosines, sines)
        dk_pre = unrotate(dkv_sum[:, :, :KVH], cosines, sines)
        dvalues = dkv_sum[:, :, KVH:]
        djoint = jnp.concatenate(
            [
                dq_pre.reshape(row_count, -1),
                dk_pre.reshape(row_count, -1),
                dvalues.reshape(row_count, -1),
            ],
            1,
        ).astype(jnp.bfloat16)
        dnormed, grads_qkv[layer_index] = backward_pair(djoint, normed_flat, w_qkv[layer_index])
        dnormed = dnormed.reshape(seq_count, part_len, model_width)
        dcur_norm, gain_one = normalize_back(dnormed, layer_in, scale_one, gain[0])
        gain_terms[layer_index] = jnp.stack([gain_one, gain_two])
        flowing = dmiddle + dcur_norm
    gain_total = lax.psum(jnp.stack(gain_terms), ("fsdp", "seq"))
    return (
        result,
        flowing,
        gain_total,
        jnp.stack(grads_qkv),
        jnp.stack(grads_out),
        jnp.stack(grads_gate_up),
        jnp.stack(grads_down),
    )


def neighbour(values, step):
    count = lax.axis_size("seq")
    return lax.ppermute(values, "seq", [(i, i ^ step) for i in range(count)])


def matmul(left, right, left_dim, right_dim):
    return lax.dot_general(
        left, right, (((left_dim,), (right_dim,)), ((), ())), preferred_element_type=jnp.float32
    )


ROOT = HD ** (-0.5)
LIMIT = 60 * 1024 * 1024


def swap_halves(values):
    width = values.shape[1]
    half = HD // 2
    column = lax.broadcasted_iota(jnp.int32, values.shape, 1)
    return jnp.where(
        column % HD < half, pltpu.roll(values, width - half, 1), pltpu.roll(values, half, 1)
    )


def spread_tables(table, pairs, last):
    half = HD // 2
    cosines, sines = table[:, :half], table[:, half:]
    ones, zeros = jnp.ones_like(table), jnp.zeros_like(table)
    tail = [[cosines, cosines, ones], [-sines, sines, zeros]] if last else [[], []]
    if not pairs:
        return jnp.concatenate(tail[0], 1), jnp.concatenate(tail[1], 1)
    cosines = [jnp.concatenate([cosines] * 4, 1)] * pairs
    sines = [jnp.concatenate([-sines, sines] * 2, 1)] * pairs
    if last:
        cosines.append(jnp.concatenate(tail[0], 1))
        sines.append(jnp.concatenate(tail[1], 1))
    return jnp.concatenate(cosines, 1), jnp.concatenate(sines, 1)


MESH = pl.DeviceIdType.MESH


def seq_peer(step):
    return {"seq": lax.axis_index("seq") ^ step}


def fsdp_peer(place):
    return {"fsdp": place}


def remote(source, target, sems, slot, peer):
    return pltpu.make_async_remote_copy(
        src_ref=source,
        dst_ref=target,
        send_sem=sems[0].at[slot],
        recv_sem=sems[1].at[slot],
        device_id=peer,
        device_id_type=MESH,
    )


def gather_copies(own, slots, half, sems, base=0):
    top, bottom = pl.ds(0, half), pl.ds(half, own.shape[0] - half)

    def slot(step, rows):
        return slots.at[step].at[rows]

    return [
        remote(own.at[top], slot(1, top), sems, base, seq_peer(1)),
        remote(own.at[bottom], slot(2, bottom), sems, base + 1, seq_peer(2)),
        remote(own.at[bottom], slot(1, bottom), sems, base + 2, seq_peer(1)),
        remote(own.at[top], slot(2, top), sems, base + 3, seq_peer(2)),
        remote(slot(1, top), slot(3, top), sems, base + 4, seq_peer(2)),
        remote(slot(2, bottom), slot(3, bottom), sems, base + 5, seq_peer(1)),
    ]


def greet(peers):
    barrier = pltpu.get_barrier_semaphore()
    for peer in peers:
        pl.semaphore_signal(barrier, inc=1, device_id=peer, device_id_type=MESH)
    pl.semaphore_wait(barrier, len(peers))


def sum_copies(sent, side, below, far, half, sems, passed=None):
    top, bottom = pl.ds(0, half), pl.ds(half, half)
    return [
        remote(sent.at[3].at[top], side.at[1], sems, 0, seq_peer(1)),
        remote(sent.at[3].at[bottom], below.at[1], sems, 1, seq_peer(2)),
        remote(sent.at[2].at[bottom], below.at[0], sems, 2, seq_peer(2)),
        remote(sent.at[1].at[top], side.at[0], sems, 3, seq_peer(1)),
        remote(passed.at[0] if passed is not None else sent.at[2].at[top], far.at[0], sems, 4, seq_peer(2)),
        remote(passed.at[1] if passed is not None else sent.at[1].at[bottom], far.at[1], sems, 5, seq_peer(1)),
    ]


def pass_sums(turn, step, partial, sums, sent_ref, side_ref, below_ref, own_ref, half):
    wide, narrow = jnp.float32, jnp.bfloat16
    last = len(sums) // 2

    @pl.when(turn == last)
    def _():
        own_ref[...] = partial

    @pl.when(turn < last)
    def _():
        sent_ref[step] = partial.astype(narrow)

    @pl.when(turn == 0)
    def _():
        sums[0].start()
        sums[1].start()

    @pl.when(turn == 1)
    def _():
        sums[2].start()

    @pl.when(turn == 2)
    def _():
        sums[3].start()
        sums[0].wait_recv()
        sent_ref[2, :half] = (sent_ref[2, :half].astype(wide) + side_ref[1].astype(wide)).astype(narrow)
        sums[4].start()
        sums[1].wait_recv()
        sent_ref[1, half:] = (sent_ref[1, half:].astype(wide) + below_ref[1].astype(wide)).astype(narrow)
        sums[5].start()


def end_sums(sums, side_ref, below_ref, far_ref, own_ref, half):
    wide = jnp.float32
    sums[2].wait_recv()
    sums[3].wait_recv()
    own_ref[:half] += side_ref[0].astype(wide)
    own_ref[half:] += below_ref[0].astype(wide)
    sums[4].wait_recv()
    own_ref[:half] += far_ref[0].astype(wide)
    sums[5].wait_recv()
    own_ref[half:] += far_ref[1].astype(wide)


def share_own(own_ref, all_ref, half, sems, before):
    copies = gather_copies(own_ref, all_ref, half, sems, len(before))
    for copy in copies[:4]:
        copy.start()
    copies[0].wait_recv()
    copies[4].start()
    copies[1].wait_recv()
    copies[5].start()
    for copy in copies[2:]:
        copy.wait_recv()
    for copy in before + copies:
        copy.wait_send()


def enter_kernel(
    count, current_ref, gain_ref, spots_ref, shard_ref, out_shard_ref, gate_up_ref, down_ref,
    all_ref, rows_ref, out_ref, table_ref, gate_up_part_ref, down_part_ref, scale_ref,
    normed_ref, held_ref, part_ref, held_down,
    send_sems, recv_sems, spot_send, spot_recv, item_up, item_down, item_side, item_recv, local_sem,
):
    part, _ = current_ref.shape
    heads = H // count
    pieces = heads + 2
    items = pieces + lax.axis_size("fsdp")
    per_shard = shard_ref.shape[0] // HD
    out_rows, columns = out_shard_ref.shape[0], heads * HD
    chips = lax.axis_size("fsdp") // 2
    index = lax.axis_index("seq")
    place = lax.axis_index("fsdp")
    chip, core = place // 2, place % 2
    sems = (send_sems, recv_sems)

    barrier = pltpu.get_barrier_semaphore()
    for peer in [seq_peer(step) for step in range(1, count)] + [fsdp_peer(place ^ 1)]:
        pl.semaphore_signal(barrier, inc=1, device_id=peer, device_id_type=MESH)

    @pl.when(chip > 0)
    def _():
        pl.semaphore_signal(barrier, inc=1, device_id=fsdp_peer(place - 2), device_id_type=MESH)

    @pl.when(chip < chips - 1)
    def _():
        pl.semaphore_signal(barrier, inc=1, device_id=fsdp_peer(place + 2), device_id_type=MESH)

    greetings = count + (chip > 0).astype(jnp.int32) + (chip < chips - 1).astype(jnp.int32)
    pl.semaphore_wait(barrier, greetings)

    part_rows = part_ref.shape[0]
    take = pltpu.make_async_copy(
        gate_up_ref.at[pl.ds(pl.multiple_of(index * part_rows, part_rows), part_rows)], part_ref, local_sem.at[items + 1]
    )
    take.start()
    take_down = pltpu.make_async_copy(down_ref, held_down, local_sem.at[items + 3])
    take_down.start()

    def qkv_item(item):
        block = jnp.where(
            item < heads, index * heads + item, jnp.where(item == heads, H + index, H + KVH + index)
        )
        source = shard_ref.at[pl.ds(pl.multiple_of(block % per_shard * HD, HD), HD)]
        return block // per_shard, source, rows_ref.at[pl.ds(pl.multiple_of(item * HD, HD), HD)], item

    def out_item(item):
        source = out_shard_ref.at[:, pl.ds(pl.multiple_of(index * columns, columns), columns)]
        target = out_ref.at[pl.ds(pl.multiple_of(item * out_rows, out_rows), out_rows)]
        return item, source, target, item + pieces

    kinds = ((qkv_item, pieces), (out_item, items - pieces))

    def item_copy(source, target, slot, sem, peer):
        return pltpu.make_async_remote_copy(
            src_ref=source,
            dst_ref=target,
            send_sem=sem.at[slot],
            recv_sem=item_recv.at[slot],
            device_id=fsdp_peer(peer),
            device_id_type=MESH,
        )

    def pass_on(source, target, slot, owner_chip, act):
        @pl.when((chip >= owner_chip) & (chip < chips - 1))
        def _():
            act(item_copy(source, target, slot, item_up, place + 2))

        @pl.when((chip <= owner_chip) & (chip > 0))
        def _():
            act(item_copy(source, target, slot, item_down, place - 2))

        act(item_copy(source, target, slot, item_side, place ^ 1))

    def send_own(item_of):
        def body(item, carry):
            owner, source, target, slot = item_of(item)

            @pl.when(place == owner)
            def _():
                pass_on(source, target, slot, owner // 2, lambda copy: copy.start())
                pltpu.make_async_copy(source, target, local_sem.at[slot]).start()

            return carry

        return body

    def pass_far(item_of, distance):
        def body(item, carry):
            owner, _, target, slot = item_of(item)
            owner_chip = owner // 2
            apart = jnp.where(chip > owner_chip, chip - owner_chip, owner_chip - chip)

            @pl.when((apart == distance) & (core == owner % 2))
            def _():
                item_copy(target, target, slot, item_side, place ^ 1).wait_recv()
                pass_on(target, target, slot, owner_chip, lambda copy: copy.start())

            return carry

        return body

    for item_of, number in kinds:
        lax.fori_loop(0, number, send_own(item_of), 0)
    current = current_ref[...]
    scale = lax.rsqrt(jnp.mean(current * current, 1, keepdims=True) + EPS)
    scale_ref[...] = jnp.broadcast_to(scale, scale_ref.shape)
    normed_ref[...] = (current * scale * gain_ref[...]).astype(jnp.bfloat16)
    copies = gather_copies(normed_ref, all_ref, part // 2, sems)
    for copy in copies[:4]:
        copy.start()
    held_ref[0] = spots_ref[...]
    spot_copies = [
        remote(spots_ref, held_ref.at[step], (spot_send, spot_recv), step - 1, seq_peer(step))
        for step in range(1, count)
    ]
    for copy in spot_copies:
        copy.start()
    own = pltpu.make_async_copy(normed_ref, all_ref.at[0], local_sem.at[items])
    own.start()
    for distance in range(1, chips):
        for item_of, number in kinds:
            lax.fori_loop(0, number, pass_far(item_of, distance), 0)
            if distance == 1 and item_of is qkv_item:
                copies[0].wait_recv()
                copies[4].start()
                copies[1].wait_recv()
                copies[5].start()

    take.wait()
    put = pltpu.make_async_copy(part_ref, gate_up_part_ref, local_sem.at[items + 2])
    put.start()
    take_down.wait()
    columns_here = part_rows
    for device in range(count):

        @pl.when(index == device)
        def _():
            down_part_ref[...] = jnp.concatenate(
                [
                    held_down[:, start + device * columns_here : start + (device + 1) * columns_here]
                    for start in range(0, held_down.shape[1], count * columns_here)
                ],
                1,
            )

    for copy in spot_copies:
        copy.wait()
    half = HD // 2
    for step in range(count):
        spots = held_ref[step][:1]
        frequency = jnp.exp(
            lax.broadcasted_iota(jnp.int32, (half, 1), 0).astype(jnp.float32) * (-2.0 * math.log(10000.0) / HD)
        )
        angles = frequency * spots
        turned = jnp.concatenate([jnp.cos(angles), jnp.sin(angles)], 0)
        table_ref[pl.ds(step * part, part), :] = jnp.transpose(turned)

    def finish(item_of):
        def body(item, carry):
            owner, source, target, slot = item_of(item)

            @pl.when(core != owner % 2)
            def _():
                item_copy(target, target, slot, item_side, place ^ 1).wait_recv()

            @pl.when(place == owner)
            def _():
                pltpu.make_async_copy(source, target, local_sem.at[slot]).wait()

            @pl.when(core == owner % 2)
            def _():
                pass_on(target, target, slot, owner // 2, lambda copy: copy.wait_send())

            return carry

        return body

    for item_of, number in kinds:
        lax.fori_loop(0, number, finish(item_of), 0)
    own.wait()
    put.wait()
    for copy in copies[2:]:
        copy.wait_recv()
    for copy in copies:
        copy.wait_send()


def enter(current, gain, spots, shard, out_shard, gate_up, down, count):
    part, width = current.shape
    length = part * count
    heads = H // count
    pieces = heads + 2
    items = pieces + lax.axis_size("fsdp")
    vmem = pl.BlockSpec(memory_space=pltpu.VMEM)
    spots = jnp.broadcast_to(spots.astype(jnp.float32)[None], (8, part))
    whole = pl.BlockSpec(memory_space=pl.ANY)
    part_shape = (gate_up.shape[0] // count, width)
    gathered, rows, out_cols, table, gate_up_part, down_part, scale = pl.pallas_call(
        lambda *refs: enter_kernel(count, *refs),
        out_shape=(
            jax.ShapeDtypeStruct((count, part, width), jnp.bfloat16),
            jax.ShapeDtypeStruct((pieces * HD, width), jnp.bfloat16),
            jax.ShapeDtypeStruct((out_shard.shape[0] * (items - pieces), heads * HD), jnp.bfloat16),
            jax.ShapeDtypeStruct((length, HD), jnp.float32),
            jax.ShapeDtypeStruct(part_shape, gate_up.dtype),
            jax.ShapeDtypeStruct((down.shape[0], down.shape[1] // count), down.dtype),
            jax.ShapeDtypeStruct((part, 128), jnp.float32),
        ),
        in_specs=[vmem] * 5 + [whole] * 2,
        out_specs=[whole] + [vmem] * 3 + [whole] + [vmem] * 2,
        scratch_shapes=[
            pltpu.VMEM((part, width), jnp.bfloat16),
            pltpu.VMEM((count, 8, part), jnp.float32),
            pltpu.VMEM(part_shape, gate_up.dtype),
            pltpu.VMEM(down.shape, down.dtype),
            pltpu.SemaphoreType.DMA((6,)),
            pltpu.SemaphoreType.DMA((6,)),
            pltpu.SemaphoreType.DMA((count - 1,)),
            pltpu.SemaphoreType.DMA((count - 1,)),
            pltpu.SemaphoreType.DMA((items,)),
            pltpu.SemaphoreType.DMA((items,)),
            pltpu.SemaphoreType.DMA((items,)),
            pltpu.SemaphoreType.DMA((items,)),
            pltpu.SemaphoreType.DMA((items + 4,)),
        ],
        compiler_params=pltpu.CompilerParams(collective_id=1, has_side_effects=True, vmem_limit_bytes=LIMIT),
        name="enter",
    )(current, gain, spots, shard, out_shard, gate_up, down)
    return gathered.reshape(length, width), rows, out_cols, table, gate_up_part, down_part, scale


def qkv_kernel(index_ref, normed_ref, weight_ref, table_ref, q_ref, k_ref, v_ref):
    heads = q_ref.shape[0]
    joint = matmul(normed_ref[...], weight_ref[...], 1, 1)
    cosines, sines = spread_tables(table_ref[...], heads // 2, True)
    turned = joint * cosines + swap_halves(joint) * sines
    for head in range(heads):
        rounded = turned[:, head * HD : (head + 1) * HD].astype(jnp.bfloat16).astype(jnp.float32)
        q_ref[head] = (rounded * ROOT).astype(jnp.bfloat16)
    k_ref[...] = turned[:, heads * HD : (heads + 1) * HD].astype(jnp.bfloat16)
    v_ref[...] = turned[:, (heads + 1) * HD :].astype(jnp.bfloat16)


def project_qkv(index, normed, weight, table, count):
    length, width = normed.shape
    part = length // count
    heads = weight.shape[0] // HD - 2
    return pl.pallas_call(
        qkv_kernel,
        out_shape=(
            jax.ShapeDtypeStruct((heads, length, HD), jnp.bfloat16),
            jax.ShapeDtypeStruct((length, HD), jnp.bfloat16),
            jax.ShapeDtypeStruct((length, HD), jnp.bfloat16),
        ),
        grid_spec=pltpu.PrefetchScalarGridSpec(
            num_scalar_prefetch=1,
            grid=(count,),
            in_specs=[
                pl.BlockSpec((part, width), lambda i, s: (i, 0)),
                pl.BlockSpec(weight.shape, lambda i, s: (0, 0)),
                pl.BlockSpec((part, table.shape[1]), lambda i, s: (i, 0)),
            ],
            out_specs=[
                pl.BlockSpec((heads, part, HD), lambda i, s: (0, i ^ s[0], 0)),
                pl.BlockSpec((part, HD), lambda i, s: (i ^ s[0], 0)),
                pl.BlockSpec((part, HD), lambda i, s: (i ^ s[0], 0)),
            ],
        ),
        compiler_params=pltpu.CompilerParams(vmem_limit_bytes=LIMIT),
        name="project_qkv",
    )(index, normed, weight, table)


def attend_kernel(
    count, q_ref, k_ref, v_ref, weight_ref, current_ref, gain_ref,
    attn_ref, lse_ref, middle_ref, scale_ref, all_ref,
    held_ref, sent_ref, side_ref, below_ref, far_ref, two_ref, send_sems, recv_sems, own_sem,
):
    heads, _, _ = q_ref.shape
    part, _ = current_ref.shape
    half = part // 2
    index = lax.axis_index("seq")
    top, bottom = pl.ds(0, half), pl.ds(half, half)
    sems = (send_sems, recv_sems)
    greet([seq_peer(1), seq_peer(2)])
    sums = sum_copies(sent_ref, side_ref, below_ref, far_ref, half, sems)
    row = lax.broadcasted_iota(jnp.int32, (part, part), 0)
    column = lax.broadcasted_iota(jnp.int32, (part, part), 1)

    def one_part(turn, carry):
        step = count - 1 - turn
        here = step ^ index
        rows_here = pl.ds(pl.multiple_of(here * part, part), part)
        rows_step = pl.ds(pl.multiple_of(step * part, part), part)
        for block in range(count):

            @pl.when(here == block)
            def _():
                before = block * part
                seen = before + part
                keys_in, values_in = k_ref[:seen], v_ref[:seen]

                def one_head(head, carry):
                    scores = matmul(q_ref[head, before:seen, :], keys_in, 1, 1)
                    last = jnp.where(row >= column, scores[:, before:], -1e30)
                    scores = jnp.concatenate([scores[:, :before], last], 1) if block else last
                    peak = jnp.max(scores, 1, keepdims=True)
                    weights = jnp.exp(scores - peak)
                    total = jnp.sum(weights, 1, keepdims=True)
                    output = matmul(weights.astype(jnp.bfloat16), values_in, 1, 0) / total
                    held_ref[head] = output.astype(jnp.bfloat16)
                    log_total = jnp.broadcast_to(peak + jnp.log(total), (part, 128))
                    lse_ref[pl.ds(head, 1), before:seen] = jnp.transpose(log_total)[:1]
                    return carry

                lax.fori_loop(0, heads, one_head, 0, unroll=2)

        attn = jnp.concatenate([held_ref[head] for head in range(heads)], 1)
        attn_ref[rows_step, :] = attn
        partial = matmul(attn, weight_ref[...], 1, 1)

        pass_sums(turn, step, partial, sums, sent_ref, side_ref, below_ref, middle_ref, half)
        return carry

    lax.fori_loop(0, count, one_part, 0)
    end_sums(sums, side_ref, below_ref, far_ref, middle_ref, half)
    middle_ref[...] += current_ref[...]
    middle = middle_ref[...]
    scale = lax.rsqrt(jnp.mean(middle * middle, 1, keepdims=True) + EPS)
    scale_ref[...] = jnp.broadcast_to(scale, scale_ref.shape)
    two_ref[...] = (middle * scale * gain_ref[...]).astype(jnp.bfloat16)
    own = pltpu.make_async_copy(two_ref, all_ref.at[0], own_sem)
    share_own(two_ref, all_ref, half, sems, sums)
    own.start()
    own.wait()


def attend(queries, keys_in, values_in, weight, current, gain, count):
    heads, length, _ = queries.shape
    part, width = current.shape
    vmem = pl.BlockSpec(memory_space=pltpu.VMEM)
    attn, lse, middle, scale, gathered = pl.pallas_call(
        lambda *refs: attend_kernel(count, *refs),
        out_shape=(
            jax.ShapeDtypeStruct((length, heads * HD), jnp.bfloat16),
            jax.ShapeDtypeStruct((heads, length), jnp.float32),
            jax.ShapeDtypeStruct((part, width), jnp.float32),
            jax.ShapeDtypeStruct((part, 128), jnp.float32),
            jax.ShapeDtypeStruct((count, part, width), jnp.bfloat16),
        ),
        in_specs=[vmem] * 6,
        out_specs=[vmem] * 4 + [pl.BlockSpec(memory_space=pl.ANY)],
        scratch_shapes=[
            pltpu.VMEM((heads, part, HD), jnp.bfloat16),
            pltpu.VMEM((count, part, width), jnp.bfloat16),
            pltpu.VMEM((2, part // 2, width), jnp.bfloat16),
            pltpu.VMEM((2, part // 2, width), jnp.bfloat16),
            pltpu.VMEM((2, part // 2, width), jnp.bfloat16),
            pltpu.VMEM((part, width), jnp.bfloat16),
            pltpu.SemaphoreType.DMA((12,)),
            pltpu.SemaphoreType.DMA((12,)),
            pltpu.SemaphoreType.DMA,
        ],
        compiler_params=pltpu.CompilerParams(collective_id=2, has_side_effects=True, vmem_limit_bytes=LIMIT),
        name="attend",
    )(queries, keys_in, values_in, weight, current, gain)
    return attn, lse, middle, scale, gathered.reshape(length, width)


def share_start(copies):
    for group in copies:
        group[0].start()
        group[1].start()
    for group in copies:
        group[2].start()
        group[3].start()


def share_on(group):
    group[0].wait_recv()
    group[4].start()
    group[1].wait_recv()
    group[5].start()


def share_end(copies):
    for group in copies:
        for copy in group[2:]:
            copy.wait_recv()
    for group in copies:
        for copy in group:
            copy.wait_send()


def upper_half(rows):
    return -(-(rows // 2) // 16) * 16


def attend_back_kernel(
    count, q_ref, k_ref, v_ref, attn_ref, lse_ref, dy_ref, weight_ref, table_ref, pick_ref, passed_ref, base_ref, shard_ref,
    out_ref, turned_ref, term_ref, result_ref, slot_ref,
    do_ref, delta_ref, dq_ref, dk_ref, dv_ref, far_ref, held_dy, held_base, held_pick,
    send_sems, recv_sems, load_sems,
):
    heads, length, _ = q_ref.shape
    part = length // count
    wide = jnp.float32
    index = lax.axis_index("seq")
    greet([seq_peer(1), seq_peer(2)])
    half = part // 2
    sems = (send_sems, recv_sems)
    sums = [
        remote(passed_ref.at[0], far_ref.at[0], sems, 6, seq_peer(2)),
        remote(passed_ref.at[1], far_ref.at[1], sems, 7, seq_peer(1)),
    ]
    group = gather_copies(shard_ref, slot_ref, upper_half(shard_ref.shape[0]), sems)
    share_start([group])
    for copy in sums:
        copy.start()

    def load_dy(step):
        rows = pl.ds(pl.multiple_of(step * part, part), part)
        return pltpu.make_async_copy(dy_ref.at[rows], held_dy.at[rows], load_sems.at[step])

    loads = [
        pltpu.make_async_copy(base_ref, held_base, load_sems.at[count]),
        pltpu.make_async_copy(pick_ref, held_pick, load_sems.at[count + 1]),
    ]
    for here in range(count):
        load_dy(here ^ index).start()
    for load in loads:
        load.start()
    dk_ref[...] = jnp.zeros_like(dk_ref)
    dv_ref[...] = jnp.zeros_like(dv_ref)
    owner = lax.broadcasted_iota(jnp.int32, (heads, heads * HD), 1) // HD
    same = (owner == lax.broadcasted_iota(jnp.int32, (heads, heads * HD), 0)).astype(wide)
    row = lax.broadcasted_iota(jnp.int32, (part, part), 0)
    column = lax.broadcasted_iota(jnp.int32, (part, part), 1)

    def unturn(grads, cosines, sines):
        return grads * cosines + swap_halves(grads * sines)

    def one_part(here, carry):
        spot = here ^ index
        rows_here = pl.ds(pl.multiple_of(spot * part, part), part)
        load_dy(spot).wait()
        dattn = matmul(held_dy[rows_here, :], weight_ref[...], 1, 0).astype(jnp.bfloat16)
        product = dattn.astype(wide) * attn_ref[rows_here, :].astype(wide)
        delta_ref[...] = lax.dot_general(
            same, product, (((1,), (1,)), ((), ())), precision=lax.Precision.HIGHEST, preferred_element_type=wide
        )
        for head in range(heads):
            do_ref[head] = dattn[:, head * HD : (head + 1) * HD]
        for block in range(count):

            @pl.when(here == block)
            def _():
                before = block * part
                seen = before + part
                keys_in, values_in = k_ref[:seen], v_ref[:seen]

                def one_head(head, carry):
                    query, dout = q_ref[head, before:seen, :], do_ref[head]
                    scores = matmul(keys_in, query, 1, 1)
                    last = jnp.where(row <= column, scores[before:], -1e30)
                    scores = jnp.concatenate([scores[:before], last], 0) if block else last
                    probs = jnp.exp(scores - lse_ref[pl.ds(head, 1), before:seen])
                    dprob = matmul(values_in, dout, 1, 1)
                    dscore = (probs * (dprob - delta_ref[pl.ds(head, 1), :])).astype(jnp.bfloat16)
                    dv_ref[:seen] += matmul(probs.astype(jnp.bfloat16), dout, 1, 0)
                    dk_ref[:seen] += matmul(dscore, query, 1, 0)
                    dq_ref[head] = (matmul(dscore, keys_in, 0, 0) * ROOT).astype(jnp.bfloat16)
                    return carry

                lax.fori_loop(0, heads, one_head, 0, unroll=2)

        dq = jnp.concatenate([dq_ref[head] for head in range(heads)], 1).astype(wide)
        dq = unturn(dq, *spread_tables(table_ref[rows_here, :], heads // 2, False))
        out_ref[rows_here, : heads * HD] = dq.astype(jnp.bfloat16)

        @pl.when(here == 1)
        def _():
            share_on(group)

        return carry

    lax.fori_loop(0, count, one_part, 0)
    for block in range(count):
        rows_there = pl.ds(pl.multiple_of((block ^ index) * part, part), part)
        rows_block = slice(block * part, (block + 1) * part)
        both = jnp.concatenate([dk_ref[rows_block], dv_ref[rows_block]], 1).astype(jnp.bfloat16).astype(wide)
        both = unturn(both, *spread_tables(table_ref[rows_there, :], 0, True))
        out_ref[rows_there, heads * HD :] = both.astype(jnp.bfloat16)
    for load in loads:
        load.wait()
    chosen = matmul(held_pick[...], out_ref[...], 1, 1).astype(jnp.bfloat16)
    size = turned_ref.shape[1]
    for block in range(count):
        turned_ref[block] = chosen[block * size : (block + 1) * size]
    tile = 2 * 128

    def one_tile(number, carry):
        columns = pl.ds(pl.multiple_of(number * tile, tile), tile)
        term_ref[columns, :] = matmul(held_dy[:, columns], attn_ref[...], 0, 0).astype(jnp.bfloat16)
        return carry

    lax.fori_loop(0, held_dy.shape[1] // tile, one_tile, 0)
    for copy in sums:
        copy.wait_recv()
    result_ref[:half] = held_base[:half] + far_ref[0].astype(wide)
    result_ref[half:] = held_base[half:] + far_ref[1].astype(wide)
    share_end([group])
    for copy in sums:
        copy.wait_send()


def attend_back(queries, keys_in, values_in, attn, lse, dy, weight, table, pick, passed, base, shard, count):
    heads, length, _ = queries.shape
    part, width = base.shape
    columns = (heads + 2) * HD
    vmem, whole = pl.BlockSpec(memory_space=pltpu.VMEM), pl.BlockSpec(memory_space=pl.ANY)
    return pl.pallas_call(
        lambda *refs: attend_back_kernel(count, *refs),
        out_shape=[
            jax.ShapeDtypeStruct((length, columns), jnp.bfloat16),
            jax.ShapeDtypeStruct((count, columns // count, length), jnp.bfloat16),
            jax.ShapeDtypeStruct((width, heads * HD), jnp.bfloat16),
            jax.ShapeDtypeStruct((part, width), jnp.float32),
            jax.ShapeDtypeStruct((count,) + shard.shape, shard.dtype),
        ],
        in_specs=[vmem] * 5 + [whole] + [vmem] * 2 + [whole] * 4,
        out_specs=[vmem] * 4 + [whole],
        scratch_shapes=[
            pltpu.VMEM((heads, part, HD), jnp.bfloat16),
            pltpu.VMEM((heads, part), jnp.float32),
            pltpu.VMEM((heads, part, HD), jnp.bfloat16),
            pltpu.VMEM((length, HD), jnp.float32),
            pltpu.VMEM((length, HD), jnp.float32),
        ]
        + [pltpu.VMEM((2, part // 2, width), jnp.bfloat16)]
        + [pltpu.VMEM(dy.shape, dy.dtype), pltpu.VMEM(base.shape, base.dtype), pltpu.VMEM(pick.shape, pick.dtype)]
        + [pltpu.SemaphoreType.DMA((8,)), pltpu.SemaphoreType.DMA((8,)), pltpu.SemaphoreType.DMA((count + 2,))],
        compiler_params=pltpu.CompilerParams(collective_id=4, has_side_effects=True, vmem_limit_bytes=LIMIT),
        name="attend_back",
    )(queries, keys_in, values_in, attn, lse, dy, weight, table, pick, passed, base, shard)


def leave_kernel(
    count, grads_ref, weight_ref, flowing_in, first_in, scale_ref, gain_ref, turned_ref, normed_in,
    own_ref, gain_out_ref, term_ref,
    sent_ref, side_ref, below_ref, far_ref, slot_ref, whole_ref, normed_ref, flowing_ref, first_ref,
    send_sems, recv_sems, swap_send, swap_recv, load_sems,
):
    part, _ = flowing_ref.shape
    half = part // 2
    size = turned_ref.shape[1]
    heads = H // count
    chunk = size // (heads + 2)
    index = lax.axis_index("seq")
    greet([seq_peer(step) for step in range(1, count)])
    swaps = [
        remote(turned_ref.at[index ^ step], slot_ref.at[step], (swap_send, swap_recv), step - 1, seq_peer(step))
        for step in range(1, count)
    ]
    for copy in swaps:
        copy.start()
    loads = [
        pltpu.make_async_copy(source, target, load_sems.at[number])
        for number, (source, target) in enumerate(
            (
                (turned_ref.at[index], slot_ref.at[0]),
                (normed_in, normed_ref),
                (flowing_in, flowing_ref),
                (first_in, first_ref),
            )
        )
    ]
    for load in loads:
        load.start()
    sums = sum_copies(sent_ref, side_ref, below_ref, far_ref, half, (send_sems, recv_sems))

    def one_part(turn, carry):
        step = count - 1 - turn
        rows_step = pl.ds(pl.multiple_of(step * part, part), part)
        partial = matmul(grads_ref[rows_step, :], weight_ref[...], 1, 0)
        pass_sums(turn, step, partial, sums, sent_ref, side_ref, below_ref, own_ref, half)
        return carry

    lax.fori_loop(0, count, one_part, 0)
    for load in loads:
        load.wait()
    for step in range(count):
        if step:
            swaps[step - 1].wait_recv()
        peer = index ^ step
        for block in range(count):
            piece = slot_ref[step, :, (step ^ block) * part : ((step ^ block) + 1) * part]
            tokens = slice(block * part, (block + 1) * part)
            for start, rows in ((0, heads * chunk), (H * chunk, chunk), ((H + KVH) * chunk, chunk)):
                begin = 0 if start == 0 else heads * chunk + (0 if start == H * chunk else chunk)
                spot = pl.multiple_of(start + peer * rows, chunk)
                whole_ref[pl.ds(spot, rows), tokens] = piece[begin : begin + rows]
    term_ref[...] = matmul(whole_ref[...], normed_ref[...], 1, 0).astype(jnp.bfloat16)
    end_sums(sums, side_ref, below_ref, far_ref, own_ref, half)
    unit = first_ref[...] * scale_ref[:, :1]
    grads = own_ref[...]
    gain_out_ref[...] = jnp.sum(grads * unit, 0, keepdims=True)
    inner = grads * gain_ref[...]
    own_ref[...] = flowing_ref[...] + scale_ref[:, :1] * (inner - unit * jnp.mean(inner * unit, 1, keepdims=True))
    for copy in sums + swaps:
        copy.wait_send()


def leave(grads, weight, flowing, first, scale, gain, turned, normed, count):
    part, width = flowing.shape
    vmem, whole = pl.BlockSpec(memory_space=pltpu.VMEM), pl.BlockSpec(memory_space=pl.ANY)
    size, length = turned.shape[1:]
    own, gain_term, term = pl.pallas_call(
        lambda *refs: leave_kernel(count, *refs),
        out_shape=(
            jax.ShapeDtypeStruct((part, width), jnp.float32),
            jax.ShapeDtypeStruct((1, width), jnp.float32),
            jax.ShapeDtypeStruct((size * count, width), jnp.bfloat16),
        ),
        in_specs=[vmem] * 2 + [whole] * 2 + [vmem] * 2 + [whole] * 2,
        out_specs=[vmem] * 3,
        scratch_shapes=[
            pltpu.VMEM((count, part, width), jnp.bfloat16),
            pltpu.VMEM((2, part // 2, width), jnp.bfloat16),
            pltpu.VMEM((2, part // 2, width), jnp.bfloat16),
            pltpu.VMEM((2, part // 2, width), jnp.bfloat16),
            pltpu.VMEM((count, size, length), jnp.bfloat16),
            pltpu.VMEM((count * size, length), jnp.bfloat16),
            pltpu.VMEM(normed.shape, jnp.bfloat16),
            pltpu.VMEM((part, width), jnp.float32),
            pltpu.VMEM((part, width), jnp.float32),
            pltpu.SemaphoreType.DMA((6,)),
            pltpu.SemaphoreType.DMA((6,)),
            pltpu.SemaphoreType.DMA((count - 1,)),
            pltpu.SemaphoreType.DMA((count - 1,)),
            pltpu.SemaphoreType.DMA((4,)),
        ],
        compiler_params=pltpu.CompilerParams(collective_id=5, has_side_effects=True, vmem_limit_bytes=LIMIT),
        name="leave",
    )(grads, weight, flowing, first, scale, gain, turned, normed)
    return own, gain_term[0], term


def share_kernel(number, fsdp, *refs):
    extra = 1 if fsdp else 0
    shards, slots = refs[:number], refs[number + extra : 2 * number + extra]
    send_sems, recv_sems = refs[2 * number + 2 * extra : 2 * number + 2 * extra + 2]
    peers = [seq_peer(1), seq_peer(2)]
    steps = []
    if fsdp:
        term_ref, total_ref = refs[number], refs[2 * number + 1]
        heard_ref, told_ref, sum_send, sum_recv = refs[2 * number + 4 :]
        place = lax.axis_index("fsdp")
        steps = [seq_peer(1), seq_peer(2)] + [fsdp_peer(place ^ (1 << bit)) for bit in range(fsdp.bit_length() - 1)]
        peers += steps[2:]
    greet(peers)
    copies = [
        gather_copies(shard, slot, upper_half(shard.shape[0]), (send_sems, recv_sems), 6 * spot)
        for spot, (shard, slot) in enumerate(zip(shards, slots))
    ]
    if fsdp:
        total_ref[...] = term_ref[...]
    tells = []
    for step, peer in enumerate(steps):
        if step == 2:
            share_start(copies)
        told_ref[step] = total_ref[...]
        tell = remote(told_ref.at[step], heard_ref.at[step], (sum_send, sum_recv), step, peer)
        tell.start()
        tell.wait_recv()
        total_ref[...] += heard_ref[step]
        tells.append(tell)
    if not fsdp:
        share_start(copies)
    for group in copies:
        share_on(group)
    share_end(copies)
    for tell in tells:
        tell.wait_send()


def share(name, shards, count, term=None):
    vmem = pl.BlockSpec(memory_space=pltpu.VMEM)
    fsdp = lax.axis_size("fsdp") if term is not None else 0
    extra = [] if term is None else [term]
    scratch = [pltpu.SemaphoreType.DMA((6 * len(shards),)) for _ in range(2)]
    if fsdp:
        steps = fsdp.bit_length() + 1
        scratch += [pltpu.VMEM((steps,) + term.shape, term.dtype) for _ in range(2)]
        scratch += [pltpu.SemaphoreType.DMA((steps,)) for _ in range(2)]
    return pl.pallas_call(
        lambda *refs: share_kernel(len(shards), fsdp, *refs),
        out_shape=[jax.ShapeDtypeStruct((count,) + shard.shape, shard.dtype) for shard in shards]
        + [jax.ShapeDtypeStruct(value.shape, value.dtype) for value in extra],
        in_specs=[pl.BlockSpec(memory_space=pl.ANY)] * len(shards) + [vmem] * len(extra),
        out_specs=[pl.BlockSpec(memory_space=pl.ANY)] * len(shards) + [vmem] * len(extra),
        scratch_shapes=scratch,
        compiler_params=pltpu.CompilerParams(
            collective_id=name, has_side_effects=True, vmem_limit_bytes=LIMIT
        ),
        name="share",
    )(*shards, *extra)


def join_rows_kernel(number, index_ref, *refs):
    owns, slots, out_ref = refs[:number], refs[number : 2 * number], refs[-1]
    mine = pl.program_id(0) == index_ref[0]

    @pl.when(mine)
    def _():
        out_ref[...] = jnp.concatenate([ref[...] for ref in owns], 1).astype(jnp.float32)

    @pl.when(jnp.logical_not(mine))
    def _():
        out_ref[...] = jnp.concatenate([ref[0] for ref in slots], 1).astype(jnp.float32)


def join_rows(index, owns, slots, count):
    rows = slots[0].shape[1]
    width = sum(slot.shape[2] for slot in slots)
    return pl.pallas_call(
        lambda *refs: join_rows_kernel(len(owns), *refs),
        out_shape=jax.ShapeDtypeStruct((rows * count, width), jnp.float32),
        grid_spec=pltpu.PrefetchScalarGridSpec(
            num_scalar_prefetch=1,
            grid=(count,),
            in_specs=[pl.BlockSpec(own.shape, lambda i, s: (0, 0)) for own in owns]
            + [pl.BlockSpec((1,) + slot.shape[1:], lambda i, s: (i ^ s[0], 0, 0)) for slot in slots],
            out_specs=pl.BlockSpec((rows, width), lambda i, s: (i, 0)),
        ),
        compiler_params=pltpu.CompilerParams(vmem_limit_bytes=LIMIT),
        name="join_rows",
    )(index, *owns, *slots)


def join_pieces_kernel(count, row_piece, column_piece, index_ref, own_ref, *refs):
    slot_refs, out_ref = refs[:-1], refs[-1]
    index = index_ref[0]
    rows, columns = own_ref.shape

    for device in range(count):

        def place_pieces(values):
            values = values.astype(jnp.float32)
            for top in range(0, rows, row_piece):
                for left in range(0, columns, column_piece):
                    down = top * count + device * row_piece if row_piece < rows else top
                    across = left * count + device * column_piece if row_piece == rows else left
                    out_ref[down : down + row_piece, across : across + column_piece] = values[
                        top : top + row_piece, left : left + column_piece
                    ]

        if len(slot_refs) == 1:
            values = slot_refs[0][device ^ index]
        else:
            values = own_ref[...]
            for step, ref in enumerate(slot_refs):
                values = jnp.where(device ^ index == step + 1, ref[...], values)
        place_pieces(jnp.where(device == index, own_ref[...], values))


def join_pieces(index, own, slots, count, row_piece, column_piece):
    rows, columns = own.shape
    shape = (rows * count, columns) if row_piece < rows else (rows, columns * count)
    return pl.pallas_call(
        lambda *refs: join_pieces_kernel(count, row_piece, column_piece, *refs),
        out_shape=jax.ShapeDtypeStruct(shape, jnp.float32),
        grid_spec=pltpu.PrefetchScalarGridSpec(
            num_scalar_prefetch=1,
            grid=(1,),
            in_specs=[pl.BlockSpec(own.shape, lambda i, s: (0, 0))]
            + [pl.BlockSpec(slot.shape, lambda i, s, n=slot.ndim: (0,) * n) for slot in slots],
            out_specs=pl.BlockSpec(shape, lambda i, s: (0, 0)),
        ),
        compiler_params=pltpu.CompilerParams(vmem_limit_bytes=LIMIT),
        name="join_pieces",
    )(index, own, *slots)


def norm_back_kernel(
    count, grads_ref, weight_ref, flowing_in, middle_in, scale_ref, gain_ref, inputs_ref,
    own_ref, gain_out_ref, dy_ref, term_ref,
    sent_ref, side_ref, below_ref, far_ref, stage_ref, held_grads, held_weight, held_inputs, flowing_ref, middle_ref,
    send_sems, recv_sems, store_sems, load_sems,
):
    part, width = flowing_ref.shape
    half = part // 2
    sems = (send_sems, recv_sems)
    units = grads_ref.shape[1]
    tile = stage_ref.shape[1]
    tiles = units // tile
    cuts = [tiles * number // 4 * tile for number in range(5)]
    last = pl.ds((count - 1) * part, part)
    rest = pl.ds(0, (count - 1) * part)
    load_last = pltpu.make_async_copy(grads_ref.at[last], held_grads.at[last], load_sems.at[0])
    load_last.start()
    load_weight = []
    for number in range(4):
        rows = pl.ds(cuts[number], cuts[number + 1] - cuts[number])
        load = pltpu.make_async_copy(weight_ref.at[rows], held_weight.at[rows], load_sems.at[1 + number])
        load.start()
        load_weight.append(load)
    load_rest = pltpu.make_async_copy(grads_ref.at[rest], held_grads.at[rest], load_sems.at[5])
    load_rest.start()
    load_inputs = pltpu.make_async_copy(inputs_ref, held_inputs, load_sems.at[6])
    load_inputs.start()
    load_ends = [
        pltpu.make_async_copy(flowing_in, flowing_ref, load_sems.at[7]),
        pltpu.make_async_copy(middle_in, middle_ref, load_sems.at[8]),
    ]
    for load in load_ends:
        load.start()
    grads_ref, weight_ref, inputs_ref = held_grads, held_weight, held_inputs
    load_last.wait()
    partial = jnp.zeros((part, width), jnp.float32)
    for number in range(4):
        load_weight[number].wait()
        rows = slice(cuts[number], cuts[number + 1])
        partial += matmul(grads_ref[last, rows], weight_ref[rows, :], 1, 0)
    sent_ref[count - 1] = partial.astype(jnp.bfloat16)
    greet([seq_peer(1), seq_peer(2)])
    sums = sum_copies(sent_ref, side_ref, below_ref, far_ref, half, sems)
    sums[0].start()
    sums[1].start()
    load_rest.wait()

    def one_part(turn, carry):
        step = count - 1 - turn
        rows_step = pl.ds(pl.multiple_of(step * part, part), part)
        partial = matmul(grads_ref[rows_step, :], weight_ref[...], 1, 0)
        pass_sums(turn, step, partial, sums, sent_ref, side_ref, below_ref, own_ref, half)
        return carry

    lax.fori_loop(1, count, one_part, 0)
    load_inputs.wait()
    for load in load_ends:
        load.wait()

    def store(number):
        rows = pl.ds(pl.multiple_of(number * tile, tile), tile)
        return pltpu.make_async_copy(stage_ref.at[number % 2], term_ref.at[rows], store_sems.at[number % 2])

    def one_tile(number, carry):
        @pl.when(number >= 2)
        def _():
            store(number - 2).wait()

        columns = pl.ds(pl.multiple_of(number * tile, tile), tile)
        stage_ref[number % 2] = matmul(grads_ref[:, columns], inputs_ref[...], 0, 0).astype(jnp.bfloat16)
        store(number).start()
        return carry

    lax.fori_loop(0, tiles, one_tile, 0)
    end_sums(sums, side_ref, below_ref, far_ref, own_ref, half)
    scale = scale_ref[:, :1]
    unit = middle_ref[...] * scale
    grads = own_ref[...]
    gain_out_ref[...] = jnp.sum(grads * unit, 0, keepdims=True)
    inner = grads * gain_ref[...]
    own_ref[...] = flowing_ref[...] + scale * (inner - unit * jnp.mean(inner * unit, 1, keepdims=True))
    dy_ref[...] = own_ref[...].astype(jnp.bfloat16)
    for number in range(tiles - 2, tiles):
        store(number).wait()
    for copy in sums:
        copy.wait_send()


def norm_back(grads, weight, flowing, middle, scale, gain, inputs, count):
    part, width = flowing.shape
    units = grads.shape[1]
    tile = 2 * 128
    vmem = pl.BlockSpec(memory_space=pltpu.VMEM)
    own, gain_term, dy, term = pl.pallas_call(
        lambda *refs: norm_back_kernel(count, *refs),
        out_shape=(
            jax.ShapeDtypeStruct((part, width), jnp.float32),
            jax.ShapeDtypeStruct((1, width), jnp.float32),
            jax.ShapeDtypeStruct((part, width), jnp.bfloat16),
            jax.ShapeDtypeStruct((units, width), jnp.bfloat16),
        ),
        in_specs=[pl.BlockSpec(memory_space=pl.ANY)] * 4 + [vmem] * 2 + [pl.BlockSpec(memory_space=pl.ANY)],
        out_specs=[vmem] * 3 + [pl.BlockSpec(memory_space=pl.ANY)],
        scratch_shapes=[
            pltpu.VMEM((count, part, width), jnp.bfloat16),
            pltpu.VMEM((2, part // 2, width), jnp.bfloat16),
            pltpu.VMEM((2, part // 2, width), jnp.bfloat16),
            pltpu.VMEM((2, part // 2, width), jnp.bfloat16),
            pltpu.VMEM((2, tile, width), jnp.bfloat16),
            pltpu.VMEM(grads.shape, jnp.bfloat16),
            pltpu.VMEM(weight.shape, jnp.bfloat16),
            pltpu.VMEM(inputs.shape, jnp.bfloat16),
            pltpu.VMEM((part, width), jnp.float32),
            pltpu.VMEM((part, width), jnp.float32),
            pltpu.SemaphoreType.DMA((6,)),
            pltpu.SemaphoreType.DMA((6,)),
            pltpu.SemaphoreType.DMA((2,)),
            pltpu.SemaphoreType.DMA((9,)),
        ],
        compiler_params=pltpu.CompilerParams(collective_id=3, has_side_effects=True, vmem_limit_bytes=LIMIT),
        name="norm_back",
    )(grads, weight, flowing, middle, scale, gain, inputs)
    return own, gain_term[0], dy, term


def share_dy_kernel(
    dy_ref, down_ref, side_ref, below_ref, middle_ref, all_ref, base_ref, passed_ref,
    piece_ref, send_sems, recv_sems, load_sems,
):
    part = dy_ref.shape[0]
    half = part // 2
    wide = jnp.float32
    top, bottom = pl.ds(0, half), pl.ds(half, half)
    loads = [
        pltpu.make_async_copy(down_ref.at[0], piece_ref.at[0], load_sems.at[0]),
        pltpu.make_async_copy(down_ref.at[2].at[top], piece_ref.at[1].at[top], load_sems.at[1]),
        pltpu.make_async_copy(down_ref.at[1].at[bottom], piece_ref.at[1].at[bottom], load_sems.at[2]),
        pltpu.make_async_copy(dy_ref, all_ref.at[0], load_sems.at[3]),
    ]
    greet([seq_peer(1), seq_peer(2)])
    group = gather_copies(dy_ref, all_ref, half, (send_sems, recv_sems))
    share_start([group])
    for load in loads:
        load.start()
    for load in loads:
        load.wait()
    base_ref[...] = middle_ref[...] + piece_ref[0].astype(wide)
    base_ref[:half] += side_ref[0].astype(wide)
    base_ref[half:] += below_ref[0].astype(wide)
    passed_ref[0] = (piece_ref[1, :half].astype(wide) + side_ref[1].astype(wide)).astype(jnp.bfloat16)
    passed_ref[1] = (piece_ref[1, half:].astype(wide) + below_ref[1].astype(wide)).astype(jnp.bfloat16)
    share_on(group)
    share_end([group])


def share_dy(dy, down, side, below, middle, count):
    part, width = dy.shape
    vmem, whole = pl.BlockSpec(memory_space=pltpu.VMEM), pl.BlockSpec(memory_space=pl.ANY)
    gathered, base, passed = pl.pallas_call(
        lambda *refs: share_dy_kernel(*refs),
        out_shape=[
            jax.ShapeDtypeStruct((count, part, width), jnp.bfloat16),
            jax.ShapeDtypeStruct((part, width), jnp.float32),
            jax.ShapeDtypeStruct((2, part // 2, width), jnp.bfloat16),
        ],
        in_specs=[vmem, whole, vmem, vmem, vmem],
        out_specs=[whole, vmem, vmem],
        scratch_shapes=[
            pltpu.VMEM((2, part, width), jnp.bfloat16),
            pltpu.SemaphoreType.DMA((6,)),
            pltpu.SemaphoreType.DMA((6,)),
            pltpu.SemaphoreType.DMA((4,)),
        ],
        compiler_params=pltpu.CompilerParams(collective_id=8, has_side_effects=True, vmem_limit_bytes=LIMIT),
        name="share_dy",
    )(dy, down, side, below, middle)
    return gathered.reshape(part * count, width), base, passed


def fast_body(hidden, positions, gains, w_qkv, w_out, w_gate_up, w_down, cotangent):
    count = lax.axis_size("seq")
    index = lax.axis_index("seq")
    place = index.astype(jnp.int32).reshape(1)
    current = hidden[0]
    part_len, width = current.shape
    heads = H // count
    gain = gains[0]
    after = lax.optimization_barrier

    rows = w_qkv.shape[1]
    group = math.gcd(rows, HD)
    chunk = group // count
    per_head = HD // group
    normed_all, qkv_rows, out_cols, table, gate_up_part, down_part, scale_one = enter(
        current, gain[:1], positions[0], w_qkv[0], w_out[0], w_gate_up[0], w_down[0], count
    )
    gu_rows = w_gate_up.shape[1] // count
    gate_up = lax.all_gather(gate_up_part, "fsdp", axis=0, tiled=True)
    units = FF // count
    down_rows = w_down.shape[1]

    queries, keys_in, values_in = project_qkv(place, normed_all, qkv_rows, table, count)
    attn_flat, log_total, middle, scale_two, normed_two_all = attend(
        queries, keys_in, values_in, out_cols, current, gain[1:], count
    )
    flowing = cotangent[0]
    normed_two_all, dm_sent, down_part = after((normed_two_all, flowing.astype(jnp.bfloat16), down_part))
    down_cols = lax.all_gather(down_part, "fsdp", axis=0, tiled=True)
    dm_all = jnp.concatenate([dm_sent] + [neighbour(dm_sent, step) for step in range(1, count)], 0)
    both = matmul(normed_two_all, gate_up, 1, 1)
    gate_part, up_part = both[:, :units], both[:, units:]
    activated = (jax.nn.silu(gate_part) * up_part).astype(jnp.bfloat16)

    def owned(grad):
        return lax.psum_scatter(grad.astype(jnp.bfloat16), "fsdp", scatter_dimension=0, tiled=True)

    term_down = matmul(dm_all, activated, 0, 0).astype(jnp.bfloat16)
    dm_all, activated, term_down = after((dm_all, activated, term_down))
    grad_down = owned(term_down)
    down_sent = matmul(activated, down_cols, 1, 1).astype(jnp.bfloat16)
    down_sent = down_sent.reshape(count, part_len, width)
    dm_all, down_sent = after((dm_all, down_sent))
    half = part_len // 2
    from_side = neighbour(jnp.stack([down_sent[1, :half], down_sent[3, :half]]), 1)
    from_below = neighbour(jnp.stack([down_sent[2, half:], down_sent[3, half:]]), 2)
    dact = matmul(dm_all, down_cols, 1, 0)
    sigma = jax.nn.sigmoid(gate_part)
    dgate = dact * up_part * sigma * (1.0 + gate_part * (1.0 - sigma))
    dup = dact * gate_part * sigma
    dgu = jnp.concatenate([dgate, dup], 1).astype(jnp.bfloat16)
    dmiddle, gain_two, dy, term_gate_up = norm_back(
        dgu, gate_up, flowing, middle, scale_two, gain[1:], normed_two_all, count
    )
    grad_gate_up = owned(term_gate_up)
    dy_all, base, passed = share_dy(dy, down_sent, from_side, from_below, middle, count)
    pieces = heads + 2
    picked = np.arange(pieces * HD).reshape(pieces * per_head, count, chunk).transpose(1, 0, 2).reshape(-1)
    pick = jnp.asarray(picked[:, None] == np.arange(pieces * HD)[None, :], jnp.bfloat16)
    djoint, djoint_turned, term_out, result, down_slots = attend_back(
        queries, keys_in, values_in, attn_flat, log_total, dy_all, out_cols, table, pick, passed, base, grad_down,
        count,
    )
    grad_out = owned(term_out)
    grad_hidden, gain_one, term_qkv = leave(
        djoint, qkv_rows, dmiddle, current, scale_one, gain[:1], djoint_turned, normed_all, count
    )
    grad_qkv = owned(term_qkv)
    gate_up_slots, gain_total = share(6, (grad_gate_up,), count, jnp.stack([gain_one, gain_two]))
    grad_out, gate_up_slots = after((grad_out, gate_up_slots))
    (out_slots,) = share(7, (grad_out,), count)
    gate_up_slots, grad_qkv, down_slots, out_slots = after((gate_up_slots, grad_qkv, down_slots, out_slots))
    qkv_slots = [neighbour(grad_qkv, step) for step in range(1, count)]
    gain_total = gain_total[None]
    down_shard = join_pieces(place, grad_down, (down_slots,), count, down_rows, gu_rows)
    gate_up_shard = join_rows(place, (grad_gate_up,), (gate_up_slots,), count)
    out_shard = join_pieces(place, grad_out, (out_slots,), count, down_rows, heads * HD)
    qkv_shard = join_pieces(place, grad_qkv, qkv_slots, count, chunk, width)
    return (
        result[None],
        grad_hidden[None],
        gain_total,
        qkv_shard[None],
        out_shard[None],
        gate_up_shard[None],
        down_shard[None],
    )


def fits(mesh):
    count, fsdp = mesh.shape["seq"], mesh.shape["fsdp"]
    rows = (H + 2 * KVH) * HD // fsdp
    return count == KVH == 4 and fsdp % 2 == 0 and fsdp & (fsdp - 1) == 0 and rows % HD == 0


def solution(mesh):
    placed = (
        P("fsdp", "seq", None),
        P("fsdp", "seq"),
        P(),
        P(None, "fsdp", None),
        P(None, "fsdp", None),
        P(None, "fsdp", None),
        P(None, "fsdp", None),
        P("fsdp", "seq", None),
    )
    fast = fits(mesh)
    return jax.shard_map(
        fast_body if fast else body,
        mesh=mesh,
        in_specs=placed,
        out_specs=(
            P("fsdp", "seq", None),
            P("fsdp", "seq", None),
            P(),
            P(None, "fsdp", None),
            P(None, "fsdp", None),
            P(None, "fsdp", None),
            P(None, "fsdp", None),
        ),
        check_vma=False,
    )
```

```python
import math

import jax
import jax.numpy as jnp
import numpy as np
from jax import lax
from jax.experimental import pallas as pl
from jax.experimental.pallas import tpu as pltpu
from jax.sharding import PartitionSpec as P


H = 32
KVH = 4
HD = 64
FF = 5632
LAYERS = 1


EPS = 1e-05


def rope_tables(position_ids):
    halfway = HD // 2
    frequency = jnp.exp(jnp.arange(halfway, dtype=jnp.float32) * (-2.0 * math.log(10000.0) / HD))
    angles = position_ids.astype(jnp.float32)[..., None] * frequency
    cosines = jnp.cos(angles)
    sines = jnp.sin(angles)
    return (
        jnp.concatenate([cosines, cosines], -1)[..., None, :],
        jnp.concatenate([sines, sines], -1)[..., None, :],
    )


def rotate(values, cosines, sines):
    halfway = values.shape[-1] // 2
    turned = jnp.concatenate([-values[..., halfway:], values[..., :halfway]], -1)
    return values * cosines + turned * sines


def unrotate(grads, cosines, sines):
    halfway = grads.shape[-1] // 2
    scaled = grads * sines
    return grads * cosines + jnp.concatenate([scaled[..., halfway:], -scaled[..., :halfway]], -1)


def normalize(values, gain):
    scale = lax.rsqrt(jnp.mean(values * values, -1, keepdims=True) + EPS)
    return ((values * scale * gain).astype(jnp.bfloat16), scale)


def normalize_back(grads, values, scale, gain):
    unit = values * scale
    gain_grad = jnp.sum((grads * unit).reshape(-1, unit.shape[-1]), 0)
    inner = grads * gain
    return (scale * (inner - unit * jnp.mean(inner * unit, -1, keepdims=True)), gain_grad)


def masked_scores(queries, keys_wide):
    scores = jnp.einsum(
        "qhd,khd->hqk", queries, keys_wide, preferred_element_type=jnp.float32
    ) * queries.shape[-1] ** (-0.5)
    length = queries.shape[0]
    causal = jnp.arange(length)[:, None] >= jnp.arange(length)[None, :]
    return jnp.where(causal[None], scores, -1e30)


def local_attend(operands):
    queries, keys_in, values_in = operands
    repeat_by = queries.shape[1] // keys_in.shape[1]
    keys_wide = jnp.repeat(keys_in, repeat_by, axis=1)
    values_wide = jnp.repeat(values_in, repeat_by, axis=1)
    scores = masked_scores(queries, keys_wide)
    peak = jnp.max(scores, -1, keepdims=True)
    log_total = peak[..., 0] + jnp.log(jnp.sum(jnp.exp(scores - peak), -1))
    weights = jnp.exp(scores - log_total[..., None]).astype(jnp.bfloat16)
    output = jnp.einsum("hqk,khd->qhd", weights, values_wide, preferred_element_type=jnp.float32)
    return (output.astype(jnp.bfloat16), log_total)


def local_attend_back(operands):
    queries, keys_in, values_in, output, log_total, dattn = operands
    length, kv_dev, head_dim = keys_in.shape
    repeat_by = queries.shape[1] // kv_dev
    keys_wide = jnp.repeat(keys_in, repeat_by, axis=1)
    values_wide = jnp.repeat(values_in, repeat_by, axis=1)
    scores = masked_scores(queries, keys_wide)
    probs = jnp.exp(scores - log_total[..., None])
    delta = jnp.sum(output.astype(jnp.float32) * dattn.astype(jnp.float32), -1).T
    dprob = jnp.einsum("qhd,khd->hqk", dattn, values_wide, preferred_element_type=jnp.float32)
    dscore = (probs * (dprob - delta[..., None])).astype(jnp.bfloat16)
    dqueries = jnp.einsum(
        "hqk,khd->qhd", dscore, keys_wide, preferred_element_type=jnp.float32
    ) * head_dim ** (-0.5)
    dkeys = jnp.einsum(
        "hqk,qhd->khd", dscore, queries, preferred_element_type=jnp.float32
    ) * head_dim ** (-0.5)
    dvalues = jnp.einsum(
        "hqk,qhd->khd", probs.astype(jnp.bfloat16), dattn, preferred_element_type=jnp.float32
    )

    def fold_heads(per_head):
        return jnp.sum(per_head.reshape(length, kv_dev, repeat_by, head_dim), 2).astype(
            jnp.bfloat16
        )

    return (dqueries.astype(jnp.bfloat16), fold_heads(dkeys), fold_heads(dvalues))


def project(inputs, weight):
    return lax.dot_general(
        inputs,
        lax.all_gather(weight, "fsdp", axis=0, tiled=True),
        (((1,), (1,)), ((), ())),
        preferred_element_type=jnp.float32,
    )


def project_back(grads, weight):
    shard_rows = lax.all_gather(weight, "fsdp", axis=0, tiled=True)
    picked = lax.slice_in_dim(grads, 0, shard_rows.shape[0], axis=1)
    return jnp.dot(picked, shard_rows, preferred_element_type=jnp.float32)


def weight_grad(grads, inputs, shard_size):
    picked = lax.slice_in_dim(grads, 0, shard_size * lax.axis_size("fsdp"), axis=1)
    summed = lax.psum_scatter(
        lax.dot_general(
            picked, inputs, (((0,), (0,)), ((), ())), preferred_element_type=jnp.float32
        ).astype(jnp.bfloat16),
        "fsdp",
        scatter_dimension=0,
        tiled=True,
    )
    return lax.psum(summed, "seq").astype(jnp.float32)


def backward_pair(grads, inputs, weight):
    wgrad = weight_grad(grads, inputs, weight.shape[0])
    return (project_back(grads, weight), wgrad)


def body(hidden, positions, gains, w_qkv, w_out, w_gate_up, w_down, cotangent):
    seq_count, part_len, model_width = hidden.shape
    row_count = seq_count * part_len
    group_count = lax.axis_size("seq")
    full_len = part_len * group_count
    heads_dev = H // group_count
    share = H // KVH
    kv_dev = max(1, heads_dev // share)
    first_kv = np.arange(group_count) * heads_dev // share
    slot_table = np.concatenate(
        [
            first_kv[:, None] + np.arange(kv_dev)[None, :],
            KVH + first_kv[:, None] + np.arange(kv_dev)[None, :],
        ],
        1,
    ).reshape(-1)
    slot_onehot = jnp.asarray(
        (slot_table[:, None] == np.arange(2 * KVH)[None, :]).astype(np.float32), jnp.bfloat16
    )
    cosines, sines = rope_tables(positions)
    layer_index = 0
    gain = gains[layer_index]
    normed, scale_one = normalize(hidden, gain[0])
    normed_flat = normed.reshape(row_count, model_width)
    joint = project(normed_flat, w_qkv[layer_index]).reshape(seq_count, part_len, -1)
    queries = joint[..., : H * HD].reshape(seq_count, part_len, H, HD)
    keys_in = joint[..., H * HD : (H + KVH) * HD].reshape(seq_count, part_len, KVH, HD)
    values_in = joint[..., (H + KVH) * HD :].reshape(seq_count, part_len, KVH, HD)
    q_rot = rotate(queries, cosines, sines).astype(jnp.bfloat16)
    kv_all = jnp.concatenate(
        [rotate(keys_in, cosines, sines).astype(jnp.bfloat16), values_in.astype(jnp.bfloat16)], 2
    )
    q_send = q_rot.reshape(seq_count, part_len, group_count, heads_dev * HD)
    kv_send = jnp.take(kv_all, slot_table, axis=2).reshape(
        seq_count, part_len, group_count, 2 * kv_dev * HD
    )
    q_heads = lax.all_to_all(q_send, "seq", split_axis=2, concat_axis=1, tiled=True)
    kv_heads = lax.all_to_all(kv_send, "seq", split_axis=2, concat_axis=1, tiled=True)
    q_heads = q_heads.reshape(seq_count, full_len, heads_dev, HD)
    kv_heads = kv_heads.reshape(seq_count, full_len, 2 * kv_dev, HD)
    k_heads = kv_heads[:, :, :kv_dev]
    v_heads = kv_heads[:, :, kv_dev:]
    o_heads, log_total = lax.map(local_attend, (q_heads, k_heads, v_heads))
    o_back = lax.all_to_all(
        o_heads.reshape(seq_count, full_len, 1, heads_dev * HD),
        "seq",
        split_axis=1,
        concat_axis=2,
        tiled=True,
    )
    attn_flat = o_back.reshape(row_count, model_width)
    middle = hidden + project(attn_flat, w_out[layer_index]).reshape(
        seq_count, part_len, model_width
    )
    normed_two, scale_two = normalize(middle, gain[1])
    normed_two_flat = normed_two.reshape(row_count, model_width)
    both = project(normed_two_flat, w_gate_up[layer_index])
    gate_part = both[:, :FF]
    up_part = both[:, FF:]
    activated = (jax.nn.silu(gate_part) * up_part).astype(jnp.bfloat16)
    result = middle + project(activated, w_down[layer_index]).reshape(
        seq_count, part_len, model_width
    )
    saved = [
        (
            hidden,
            normed_flat,
            scale_one,
            q_heads,
            k_heads,
            v_heads,
            o_heads,
            log_total,
            attn_flat,
            middle,
            normed_two_flat,
            scale_two,
            gate_part,
            up_part,
            activated,
        )
    ]
    flowing = cotangent
    grads_qkv = [None] * LAYERS
    grads_out = [None] * LAYERS
    grads_gate_up = [None] * LAYERS
    grads_down = [None] * LAYERS
    gain_terms = [None] * LAYERS
    for layer_index in reversed(range(LAYERS)):
        (
            layer_in,
            normed_flat,
            scale_one,
            q_heads,
            k_heads,
            v_heads,
            o_heads,
            log_total,
            attn_flat,
            middle,
            normed_two_flat,
            scale_two,
            gate_part,
            up_part,
            activated,
        ) = saved[layer_index]
        gain = gains[layer_index]
        dm_cast = flowing.reshape(row_count, model_width).astype(jnp.bfloat16)
        dact, grads_down[layer_index] = backward_pair(dm_cast, activated, w_down[layer_index])
        sigma = jax.nn.sigmoid(gate_part)
        dgate = dact * up_part * sigma * (1.0 + gate_part * (1.0 - sigma))
        dup = dact * gate_part * sigma
        dgu = jnp.concatenate([dgate, dup], 1).astype(jnp.bfloat16)
        dnormed_two, grads_gate_up[layer_index] = backward_pair(
            dgu, normed_two_flat, w_gate_up[layer_index]
        )
        dnormed_two = dnormed_two.reshape(seq_count, part_len, model_width)
        dmid_norm, gain_two = normalize_back(dnormed_two, middle, scale_two, gain[1])
        dmiddle = flowing + dmid_norm
        dy_cast = dmiddle.reshape(row_count, model_width).astype(jnp.bfloat16)
        dattn_wide, grads_out[layer_index] = backward_pair(dy_cast, attn_flat, w_out[layer_index])
        dattn = dattn_wide.astype(jnp.bfloat16)
        dattn_heads = lax.all_to_all(
            dattn.reshape(seq_count, part_len, group_count, heads_dev * HD),
            "seq",
            split_axis=2,
            concat_axis=1,
            tiled=True,
        )
        dattn_heads = dattn_heads.reshape(seq_count, full_len, heads_dev, HD)
        dq_heads, dk_heads, dv_heads = lax.map(
            local_attend_back, (q_heads, k_heads, v_heads, o_heads, log_total, dattn_heads)
        )
        dkv_heads = jnp.concatenate([dk_heads, dv_heads], 2).reshape(
            seq_count, full_len, 1, 2 * kv_dev * HD
        )
        dq_tok, dkv_tok = (
            lax.all_to_all(
                dq_heads.reshape(seq_count, full_len, 1, heads_dev * HD),
                "seq",
                split_axis=1,
                concat_axis=2,
                tiled=True,
            ),
            lax.all_to_all(dkv_heads, "seq", split_axis=1, concat_axis=2, tiled=True),
        )
        dqueries = dq_tok.reshape(seq_count, part_len, H, HD)
        dkv_sum = jnp.einsum(
            "stnd,nm->stmd",
            dkv_tok.reshape(seq_count, part_len, group_count * 2 * kv_dev, HD),
            slot_onehot,
            preferred_element_type=jnp.float32,
        )
        dq_pre = unrotate(dqueries, cosines, sines)
        dk_pre = unrotate(dkv_sum[:, :, :KVH], cosines, sines)
        dvalues = dkv_sum[:, :, KVH:]
        djoint = jnp.concatenate(
            [
                dq_pre.reshape(row_count, -1),
                dk_pre.reshape(row_count, -1),
                dvalues.reshape(row_count, -1),
            ],
            1,
        ).astype(jnp.bfloat16)
        dnormed, grads_qkv[layer_index] = backward_pair(djoint, normed_flat, w_qkv[layer_index])
        dnormed = dnormed.reshape(seq_count, part_len, model_width)
        dcur_norm, gain_one = normalize_back(dnormed, layer_in, scale_one, gain[0])
        gain_terms[layer_index] = jnp.stack([gain_one, gain_two])
        flowing = dmiddle + dcur_norm
    gain_total = lax.psum(jnp.stack(gain_terms), ("fsdp", "seq"))
    return (
        result,
        flowing,
        gain_total,
        jnp.stack(grads_qkv),
        jnp.stack(grads_out),
        jnp.stack(grads_gate_up),
        jnp.stack(grads_down),
    )


def neighbour(values, step):
    count = lax.axis_size("seq")
    return lax.ppermute(values, "seq", [(i, i ^ step) for i in range(count)])


def matmul(left, right, left_dim, right_dim):
    return lax.dot_general(
        left, right, (((left_dim,), (right_dim,)), ((), ())), preferred_element_type=jnp.float32
    )


ROOT = HD ** (-0.5)
LIMIT = 60 * 1024 * 1024


def swap_halves(values):
    width = values.shape[1]
    half = HD // 2
    column = lax.broadcasted_iota(jnp.int32, values.shape, 1)
    return jnp.where(
        column % HD < half, pltpu.roll(values, width - half, 1), pltpu.roll(values, half, 1)
    )


def spread_tables(table, pairs, last):
    half = HD // 2
    cosines, sines = table[:, :half], table[:, half:]
    ones, zeros = jnp.ones_like(table), jnp.zeros_like(table)
    tail = [[cosines, cosines, ones], [-sines, sines, zeros]] if last else [[], []]
    if not pairs:
        return jnp.concatenate(tail[0], 1), jnp.concatenate(tail[1], 1)
    cosines = [jnp.concatenate([cosines] * 4, 1)] * pairs
    sines = [jnp.concatenate([-sines, sines] * 2, 1)] * pairs
    if last:
        cosines.append(jnp.concatenate(tail[0], 1))
        sines.append(jnp.concatenate(tail[1], 1))
    return jnp.concatenate(cosines, 1), jnp.concatenate(sines, 1)


MESH = pl.DeviceIdType.MESH


def seq_peer(step):
    return {"seq": lax.axis_index("seq") ^ step}


def fsdp_peer(place):
    return {"fsdp": place}


def remote(source, target, sems, slot, peer):
    return pltpu.make_async_remote_copy(
        src_ref=source,
        dst_ref=target,
        send_sem=sems[0].at[slot],
        recv_sem=sems[1].at[slot],
        device_id=peer,
        device_id_type=MESH,
    )


def gather_copies(own, slots, half, sems, base=0):
    top, bottom = pl.ds(0, half), pl.ds(half, own.shape[0] - half)

    def slot(step, rows):
        return slots.at[step].at[rows]

    return [
        remote(own.at[top], slot(1, top), sems, base, seq_peer(1)),
        remote(own.at[bottom], slot(2, bottom), sems, base + 1, seq_peer(2)),
        remote(own.at[bottom], slot(1, bottom), sems, base + 2, seq_peer(1)),
        remote(own.at[top], slot(2, top), sems, base + 3, seq_peer(2)),
        remote(slot(1, top), slot(3, top), sems, base + 4, seq_peer(2)),
        remote(slot(2, bottom), slot(3, bottom), sems, base + 5, seq_peer(1)),
    ]


def greet(peers):
    barrier = pltpu.get_barrier_semaphore()
    for peer in peers:
        pl.semaphore_signal(barrier, inc=1, device_id=peer, device_id_type=MESH)
    pl.semaphore_wait(barrier, len(peers))


def sum_copies(sent, side, below, far, half, sems, passed=None):
    top, bottom = pl.ds(0, half), pl.ds(half, half)
    return [
        remote(sent.at[3].at[top], side.at[1], sems, 0, seq_peer(1)),
        remote(sent.at[3].at[bottom], below.at[1], sems, 1, seq_peer(2)),
        remote(sent.at[2].at[bottom], below.at[0], sems, 2, seq_peer(2)),
        remote(sent.at[1].at[top], side.at[0], sems, 3, seq_peer(1)),
        remote(passed.at[0] if passed is not None else sent.at[2].at[top], far.at[0], sems, 4, seq_peer(2)),
        remote(passed.at[1] if passed is not None else sent.at[1].at[bottom], far.at[1], sems, 5, seq_peer(1)),
    ]


def pass_sums(turn, step, partial, sums, sent_ref, side_ref, below_ref, own_ref, half):
    wide, narrow = jnp.float32, jnp.bfloat16
    last = len(sums) // 2

    @pl.when(turn == last)
    def _():
        own_ref[...] = partial

    @pl.when(turn < last)
    def _():
        sent_ref[step] = partial.astype(narrow)

    @pl.when(turn == 0)
    def _():
        sums[0].start()
        sums[1].start()

    @pl.when(turn == 1)
    def _():
        sums[2].start()

    @pl.when(turn == 2)
    def _():
        sums[3].start()
        sums[0].wait_recv()
        sent_ref[2, :half] = (sent_ref[2, :half].astype(wide) + side_ref[1].astype(wide)).astype(narrow)
        sums[4].start()
        sums[1].wait_recv()
        sent_ref[1, half:] = (sent_ref[1, half:].astype(wide) + below_ref[1].astype(wide)).astype(narrow)
        sums[5].start()


def end_sums(sums, side_ref, below_ref, far_ref, own_ref, half):
    wide = jnp.float32
    sums[2].wait_recv()
    sums[3].wait_recv()
    own_ref[:half] += side_ref[0].astype(wide)
    own_ref[half:] += below_ref[0].astype(wide)
    sums[4].wait_recv()
    own_ref[:half] += far_ref[0].astype(wide)
    sums[5].wait_recv()
    own_ref[half:] += far_ref[1].astype(wide)


def share_own(own_ref, all_ref, half, sems, before):
    copies = gather_copies(own_ref, all_ref, half, sems, len(before))
    for copy in copies[:4]:
        copy.start()
    copies[0].wait_recv()
    copies[4].start()
    copies[1].wait_recv()
    copies[5].start()
    for copy in copies[2:]:
        copy.wait_recv()
    for copy in before + copies:
        copy.wait_send()


def enter_kernel(
    count, current_ref, gain_ref, spots_ref, shard_ref, out_shard_ref, gate_up_ref, down_ref,
    all_ref, rows_ref, out_ref, table_ref, gate_up_part_ref, down_part_ref, scale_ref,
    normed_ref, held_ref, part_ref, held_down,
    send_sems, recv_sems, spot_send, spot_recv, item_up, item_down, item_side, item_recv, local_sem,
):
    part, _ = current_ref.shape
    heads = H // count
    pieces = heads + 2
    items = pieces + lax.axis_size("fsdp")
    per_shard = shard_ref.shape[0] // HD
    out_rows, columns = out_shard_ref.shape[0], heads * HD
    chips = lax.axis_size("fsdp") // 2
    index = lax.axis_index("seq")
    place = lax.axis_index("fsdp")
    chip, core = place // 2, place % 2
    sems = (send_sems, recv_sems)

    barrier = pltpu.get_barrier_semaphore()
    for peer in [seq_peer(step) for step in range(1, count)] + [fsdp_peer(place ^ 1)]:
        pl.semaphore_signal(barrier, inc=1, device_id=peer, device_id_type=MESH)

    @pl.when(chip > 0)
    def _():
        pl.semaphore_signal(barrier, inc=1, device_id=fsdp_peer(place - 2), device_id_type=MESH)

    @pl.when(chip < chips - 1)
    def _():
        pl.semaphore_signal(barrier, inc=1, device_id=fsdp_peer(place + 2), device_id_type=MESH)

    greetings = count + (chip > 0).astype(jnp.int32) + (chip < chips - 1).astype(jnp.int32)
    pl.semaphore_wait(barrier, greetings)

    part_rows = part_ref.shape[0]
    take = pltpu.make_async_copy(
        gate_up_ref.at[pl.ds(pl.multiple_of(index * part_rows, part_rows), part_rows)], part_ref, local_sem.at[items + 1]
    )
    take.start()
    take_down = pltpu.make_async_copy(down_ref, held_down, local_sem.at[items + 3])
    take_down.start()

    def qkv_item(item):
        block = jnp.where(
            item < heads, index * heads + item, jnp.where(item == heads, H + index, H + KVH + index)
        )
        source = shard_ref.at[pl.ds(pl.multiple_of(block % per_shard * HD, HD), HD)]
        return block // per_shard, source, rows_ref.at[pl.ds(pl.multiple_of(item * HD, HD), HD)], item

    def out_item(item):
        source = out_shard_ref.at[:, pl.ds(pl.multiple_of(index * columns, columns), columns)]
        target = out_ref.at[pl.ds(pl.multiple_of(item * out_rows, out_rows), out_rows)]
        return item, source, target, item + pieces

    kinds = ((qkv_item, pieces), (out_item, items - pieces))

    def item_copy(source, target, slot, sem, peer):
        return pltpu.make_async_remote_copy(
            src_ref=source,
            dst_ref=target,
            send_sem=sem.at[slot],
            recv_sem=item_recv.at[slot],
            device_id=fsdp_peer(peer),
            device_id_type=MESH,
        )

    def pass_on(source, target, slot, owner_chip, act):
        @pl.when((chip >= owner_chip) & (chip < chips - 1))
        def _():
            act(item_copy(source, target, slot, item_up, place + 2))

        @pl.when((chip <= owner_chip) & (chip > 0))
        def _():
            act(item_copy(source, target, slot, item_down, place - 2))

        act(item_copy(source, target, slot, item_side, place ^ 1))

    def send_own(item_of):
        def body(item, carry):
            owner, source, target, slot = item_of(item)

            @pl.when(place == owner)
            def _():
                pass_on(source, target, slot, owner // 2, lambda copy: copy.start())
                pltpu.make_async_copy(source, target, local_sem.at[slot]).start()

            return carry

        return body

    def pass_far(item_of, distance):
        def body(item, carry):
            owner, _, target, slot = item_of(item)
            owner_chip = owner // 2
            apart = jnp.where(chip > owner_chip, chip - owner_chip, owner_chip - chip)

            @pl.when((apart == distance) & (core == owner % 2))
            def _():
                item_copy(target, target, slot, item_side, place ^ 1).wait_recv()
                pass_on(target, target, slot, owner_chip, lambda copy: copy.start())

            return carry

        return body

    for item_of, number in kinds:
        lax.fori_loop(0, number, send_own(item_of), 0)
    current = current_ref[...]
    scale = lax.rsqrt(jnp.mean(current * current, 1, keepdims=True) + EPS)
    scale_ref[...] = jnp.broadcast_to(scale, scale_ref.shape)
    normed_ref[...] = (current * scale * gain_ref[...]).astype(jnp.bfloat16)
    copies = gather_copies(normed_ref, all_ref, part // 2, sems)
    for copy in copies[:4]:
        copy.start()
    held_ref[0] = spots_ref[...]
    spot_copies = [
        remote(spots_ref, held_ref.at[step], (spot_send, spot_recv), step - 1, seq_peer(step))
        for step in range(1, count)
    ]
    for copy in spot_copies:
        copy.start()
    own = pltpu.make_async_copy(normed_ref, all_ref.at[0], local_sem.at[items])
    own.start()
    for distance in range(1, chips):
        for item_of, number in kinds:
            lax.fori_loop(0, number, pass_far(item_of, distance), 0)
            if distance == 1 and item_of is qkv_item:
                copies[0].wait_recv()
                copies[4].start()
                copies[1].wait_recv()
                copies[5].start()

    take.wait()
    put = pltpu.make_async_copy(part_ref, gate_up_part_ref, local_sem.at[items + 2])
    put.start()
    take_down.wait()
    columns_here = part_rows
    for device in range(count):

        @pl.when(index == device)
        def _():
            down_part_ref[...] = jnp.concatenate(
                [
                    held_down[:, start + device * columns_here : start + (device + 1) * columns_here]
                    for start in range(0, held_down.shape[1], count * columns_here)
                ],
                1,
            )

    for copy in spot_copies:
        copy.wait()
    half = HD // 2
    for step in range(count):
        spots = held_ref[step][:1]
        frequency = jnp.exp(
            lax.broadcasted_iota(jnp.int32, (half, 1), 0).astype(jnp.float32) * (-2.0 * math.log(10000.0) / HD)
        )
        angles = frequency * spots
        turned = jnp.concatenate([jnp.cos(angles), jnp.sin(angles)], 0)
        table_ref[pl.ds(step * part, part), :] = jnp.transpose(turned)

    def finish(item_of):
        def body(item, carry):
            owner, source, target, slot = item_of(item)

            @pl.when(core != owner % 2)
            def _():
                item_copy(target, target, slot, item_side, place ^ 1).wait_recv()

            @pl.when(place == owner)
            def _():
                pltpu.make_async_copy(source, target, local_sem.at[slot]).wait()

            @pl.when(core == owner % 2)
            def _():
                pass_on(target, target, slot, owner // 2, lambda copy: copy.wait_send())

            return carry

        return body

    for item_of, number in kinds:
        lax.fori_loop(0, number, finish(item_of), 0)
    own.wait()
    put.wait()
    for copy in copies[2:]:
        copy.wait_recv()
    for copy in copies:
        copy.wait_send()


def enter(current, gain, spots, shard, out_shard, gate_up, down, count):
    part, width = current.shape
    length = part * count
    heads = H // count
    pieces = heads + 2
    items = pieces + lax.axis_size("fsdp")
    vmem = pl.BlockSpec(memory_space=pltpu.VMEM)
    spots = jnp.broadcast_to(spots.astype(jnp.float32)[None], (8, part))
    whole = pl.BlockSpec(memory_space=pl.ANY)
    part_shape = (gate_up.shape[0] // count, width)
    gathered, rows, out_cols, table, gate_up_part, down_part, scale = pl.pallas_call(
        lambda *refs: enter_kernel(count, *refs),
        out_shape=(
            jax.ShapeDtypeStruct((count, part, width), jnp.bfloat16),
            jax.ShapeDtypeStruct((pieces * HD, width), jnp.bfloat16),
            jax.ShapeDtypeStruct((out_shard.shape[0] * (items - pieces), heads * HD), jnp.bfloat16),
            jax.ShapeDtypeStruct((length, HD), jnp.float32),
            jax.ShapeDtypeStruct(part_shape, gate_up.dtype),
            jax.ShapeDtypeStruct((down.shape[0], down.shape[1] // count), down.dtype),
            jax.ShapeDtypeStruct((part, 128), jnp.float32),
        ),
        in_specs=[vmem] * 5 + [whole] * 2,
        out_specs=[whole] + [vmem] * 3 + [whole] + [vmem] * 2,
        scratch_shapes=[
            pltpu.VMEM((part, width), jnp.bfloat16),
            pltpu.VMEM((count, 8, part), jnp.float32),
            pltpu.VMEM(part_shape, gate_up.dtype),
            pltpu.VMEM(down.shape, down.dtype),
            pltpu.SemaphoreType.DMA((6,)),
            pltpu.SemaphoreType.DMA((6,)),
            pltpu.SemaphoreType.DMA((count - 1,)),
            pltpu.SemaphoreType.DMA((count - 1,)),
            pltpu.SemaphoreType.DMA((items,)),
            pltpu.SemaphoreType.DMA((items,)),
            pltpu.SemaphoreType.DMA((items,)),
            pltpu.SemaphoreType.DMA((items,)),
            pltpu.SemaphoreType.DMA((items + 4,)),
        ],
        compiler_params=pltpu.CompilerParams(collective_id=1, has_side_effects=True, vmem_limit_bytes=LIMIT),
        name="enter",
    )(current, gain, spots, shard, out_shard, gate_up, down)
    return gathered.reshape(length, width), rows, out_cols, table, gate_up_part, down_part, scale


def qkv_kernel(index_ref, normed_ref, weight_ref, table_ref, q_ref, k_ref, v_ref):
    heads = q_ref.shape[0]
    joint = matmul(normed_ref[...], weight_ref[...], 1, 1)
    cosines, sines = spread_tables(table_ref[...], heads // 2, True)
    turned = joint * cosines + swap_halves(joint) * sines
    for head in range(heads):
        rounded = turned[:, head * HD : (head + 1) * HD].astype(jnp.bfloat16).astype(jnp.float32)
        q_ref[head] = (rounded * ROOT).astype(jnp.bfloat16)
    k_ref[...] = turned[:, heads * HD : (heads + 1) * HD].astype(jnp.bfloat16)
    v_ref[...] = turned[:, (heads + 1) * HD :].astype(jnp.bfloat16)


def project_qkv(index, normed, weight, table, count):
    length, width = normed.shape
    part = length // count
    heads = weight.shape[0] // HD - 2
    return pl.pallas_call(
        qkv_kernel,
        out_shape=(
            jax.ShapeDtypeStruct((heads, length, HD), jnp.bfloat16),
            jax.ShapeDtypeStruct((length, HD), jnp.bfloat16),
            jax.ShapeDtypeStruct((length, HD), jnp.bfloat16),
        ),
        grid_spec=pltpu.PrefetchScalarGridSpec(
            num_scalar_prefetch=1,
            grid=(count,),
            in_specs=[
                pl.BlockSpec((part, width), lambda i, s: (i, 0)),
                pl.BlockSpec(weight.shape, lambda i, s: (0, 0)),
                pl.BlockSpec((part, table.shape[1]), lambda i, s: (i, 0)),
            ],
            out_specs=[
                pl.BlockSpec((heads, part, HD), lambda i, s: (0, i ^ s[0], 0)),
                pl.BlockSpec((part, HD), lambda i, s: (i ^ s[0], 0)),
                pl.BlockSpec((part, HD), lambda i, s: (i ^ s[0], 0)),
            ],
        ),
        compiler_params=pltpu.CompilerParams(vmem_limit_bytes=LIMIT),
        name="project_qkv",
    )(index, normed, weight, table)


def attend_kernel(
    count, q_ref, k_ref, v_ref, weight_ref, current_ref, gain_ref,
    attn_ref, lse_ref, middle_ref, scale_ref, all_ref,
    held_ref, sent_ref, side_ref, below_ref, far_ref, two_ref, send_sems, recv_sems, own_sem,
):
    heads, _, _ = q_ref.shape
    part, _ = current_ref.shape
    half = part // 2
    index = lax.axis_index("seq")
    top, bottom = pl.ds(0, half), pl.ds(half, half)
    sems = (send_sems, recv_sems)
    greet([seq_peer(1), seq_peer(2)])
    sums = sum_copies(sent_ref, side_ref, below_ref, far_ref, half, sems)
    row = lax.broadcasted_iota(jnp.int32, (part, part), 0)
    column = lax.broadcasted_iota(jnp.int32, (part, part), 1)

    def one_part(turn, carry):
        step = count - 1 - turn
        here = step ^ index
        rows_here = pl.ds(pl.multiple_of(here * part, part), part)
        rows_step = pl.ds(pl.multiple_of(step * part, part), part)
        for block in range(count):

            @pl.when(here == block)
            def _():
                before = block * part
                seen = before + part
                keys_in, values_in = k_ref[:seen], v_ref[:seen]

                def one_head(head, carry):
                    scores = matmul(q_ref[head, before:seen, :], keys_in, 1, 1)
                    last = jnp.where(row >= column, scores[:, before:], -1e30)
                    scores = jnp.concatenate([scores[:, :before], last], 1) if block else last
                    peak = jnp.max(scores, 1, keepdims=True)
                    weights = jnp.exp(scores - peak)
                    total = jnp.sum(weights, 1, keepdims=True)
                    output = matmul(weights.astype(jnp.bfloat16), values_in, 1, 0) / total
                    held_ref[head] = output.astype(jnp.bfloat16)
                    log_total = jnp.broadcast_to(peak + jnp.log(total), (part, 128))
                    lse_ref[pl.ds(head, 1), before:seen] = jnp.transpose(log_total)[:1]
                    return carry

                lax.fori_loop(0, heads, one_head, 0, unroll=2)

        attn = jnp.concatenate([held_ref[head] for head in range(heads)], 1)
        attn_ref[rows_step, :] = attn
        partial = matmul(attn, weight_ref[...], 1, 1)

        pass_sums(turn, step, partial, sums, sent_ref, side_ref, below_ref, middle_ref, half)
        return carry

    lax.fori_loop(0, count, one_part, 0)
    end_sums(sums, side_ref, below_ref, far_ref, middle_ref, half)
    middle_ref[...] += current_ref[...]
    middle = middle_ref[...]
    scale = lax.rsqrt(jnp.mean(middle * middle, 1, keepdims=True) + EPS)
    scale_ref[...] = jnp.broadcast_to(scale, scale_ref.shape)
    two_ref[...] = (middle * scale * gain_ref[...]).astype(jnp.bfloat16)
    own = pltpu.make_async_copy(two_ref, all_ref.at[0], own_sem)
    share_own(two_ref, all_ref, half, sems, sums)
    own.start()
    own.wait()


def attend(queries, keys_in, values_in, weight, current, gain, count):
    heads, length, _ = queries.shape
    part, width = current.shape
    vmem = pl.BlockSpec(memory_space=pltpu.VMEM)
    attn, lse, middle, scale, gathered = pl.pallas_call(
        lambda *refs: attend_kernel(count, *refs),
        out_shape=(
            jax.ShapeDtypeStruct((length, heads * HD), jnp.bfloat16),
            jax.ShapeDtypeStruct((heads, length), jnp.float32),
            jax.ShapeDtypeStruct((part, width), jnp.float32),
            jax.ShapeDtypeStruct((part, 128), jnp.float32),
            jax.ShapeDtypeStruct((count, part, width), jnp.bfloat16),
        ),
        in_specs=[vmem] * 6,
        out_specs=[vmem] * 4 + [pl.BlockSpec(memory_space=pl.ANY)],
        scratch_shapes=[
            pltpu.VMEM((heads, part, HD), jnp.bfloat16),
            pltpu.VMEM((count, part, width), jnp.bfloat16),
            pltpu.VMEM((2, part // 2, width), jnp.bfloat16),
            pltpu.VMEM((2, part // 2, width), jnp.bfloat16),
            pltpu.VMEM((2, part // 2, width), jnp.bfloat16),
            pltpu.VMEM((part, width), jnp.bfloat16),
            pltpu.SemaphoreType.DMA((12,)),
            pltpu.SemaphoreType.DMA((12,)),
            pltpu.SemaphoreType.DMA,
        ],
        compiler_params=pltpu.CompilerParams(collective_id=2, has_side_effects=True, vmem_limit_bytes=LIMIT),
        name="attend",
    )(queries, keys_in, values_in, weight, current, gain)
    return attn, lse, middle, scale, gathered.reshape(length, width)


def share_start(copies):
    for group in copies:
        group[0].start()
        group[1].start()
    for group in copies:
        group[2].start()
        group[3].start()


def share_on(group):
    group[0].wait_recv()
    group[4].start()
    group[1].wait_recv()
    group[5].start()


def share_end(copies):
    for group in copies:
        for copy in group[2:]:
            copy.wait_recv()
    for group in copies:
        for copy in group:
            copy.wait_send()


def upper_half(rows):
    return -(-(rows // 2) // 16) * 16


def attend_back_kernel(
    count, q_ref, k_ref, v_ref, attn_ref, lse_ref, dy_ref, weight_ref, table_ref, pick_ref, passed_ref, shard_ref,
    out_ref, turned_ref, term_ref, far_ref, slot_ref,
    do_ref, delta_ref, dq_ref, dk_ref, dv_ref, held_dy, held_pick,
    send_sems, recv_sems, load_sems,
):
    heads, length, _ = q_ref.shape
    part = length // count
    wide = jnp.float32
    index = lax.axis_index("seq")
    greet([seq_peer(1), seq_peer(2)])
    sems = (send_sems, recv_sems)
    sums = [
        remote(passed_ref.at[0], far_ref.at[0], sems, 6, seq_peer(2)),
        remote(passed_ref.at[1], far_ref.at[1], sems, 7, seq_peer(1)),
    ]
    group = gather_copies(shard_ref, slot_ref, upper_half(shard_ref.shape[0]), sems)
    share_start([group])
    for copy in sums:
        copy.start()

    def load_dy(step):
        rows = pl.ds(pl.multiple_of(step * part, part), part)
        return pltpu.make_async_copy(dy_ref.at[rows], held_dy.at[rows], load_sems.at[step])

    load = pltpu.make_async_copy(pick_ref, held_pick, load_sems.at[count])
    for here in range(count):
        load_dy(here ^ index).start()
    load.start()
    dk_ref[...] = jnp.zeros_like(dk_ref)
    dv_ref[...] = jnp.zeros_like(dv_ref)
    owner = lax.broadcasted_iota(jnp.int32, (heads, heads * HD), 1) // HD
    same = (owner == lax.broadcasted_iota(jnp.int32, (heads, heads * HD), 0)).astype(wide)
    row = lax.broadcasted_iota(jnp.int32, (part, part), 0)
    column = lax.broadcasted_iota(jnp.int32, (part, part), 1)

    def unturn(grads, cosines, sines):
        return grads * cosines + swap_halves(grads * sines)

    def one_part(here, carry):
        spot = here ^ index
        rows_here = pl.ds(pl.multiple_of(spot * part, part), part)
        load_dy(spot).wait()
        dattn = matmul(held_dy[rows_here, :], weight_ref[...], 1, 0).astype(jnp.bfloat16)
        product = dattn.astype(wide) * attn_ref[rows_here, :].astype(wide)
        delta_ref[...] = lax.dot_general(
            same, product, (((1,), (1,)), ((), ())), precision=lax.Precision.HIGHEST, preferred_element_type=wide
        )
        for head in range(heads):
            do_ref[head] = dattn[:, head * HD : (head + 1) * HD]
        for block in range(count):

            @pl.when(here == block)
            def _():
                before = block * part
                seen = before + part
                keys_in, values_in = k_ref[:seen], v_ref[:seen]

                def one_head(head, carry):
                    query, dout = q_ref[head, before:seen, :], do_ref[head]
                    scores = matmul(keys_in, query, 1, 1)
                    last = jnp.where(row <= column, scores[before:], -1e30)
                    scores = jnp.concatenate([scores[:before], last], 0) if block else last
                    probs = jnp.exp(scores - lse_ref[pl.ds(head, 1), before:seen])
                    dprob = matmul(values_in, dout, 1, 1)
                    dscore = (probs * (dprob - delta_ref[pl.ds(head, 1), :])).astype(jnp.bfloat16)
                    dv_ref[:seen] += matmul(probs.astype(jnp.bfloat16), dout, 1, 0)
                    dk_ref[:seen] += matmul(dscore, query, 1, 0)
                    dq_ref[head] = (matmul(dscore, keys_in, 0, 0) * ROOT).astype(jnp.bfloat16)
                    return carry

                lax.fori_loop(0, heads, one_head, 0, unroll=2)

        dq = jnp.concatenate([dq_ref[head] for head in range(heads)], 1).astype(wide)
        dq = unturn(dq, *spread_tables(table_ref[rows_here, :], heads // 2, False))
        out_ref[rows_here, : heads * HD] = dq.astype(jnp.bfloat16)

        @pl.when(here == 1)
        def _():
            share_on(group)

        return carry

    lax.fori_loop(0, count, one_part, 0)
    for block in range(count):
        rows_there = pl.ds(pl.multiple_of((block ^ index) * part, part), part)
        rows_block = slice(block * part, (block + 1) * part)
        both = jnp.concatenate([dk_ref[rows_block], dv_ref[rows_block]], 1).astype(jnp.bfloat16).astype(wide)
        both = unturn(both, *spread_tables(table_ref[rows_there, :], 0, True))
        out_ref[rows_there, heads * HD :] = both.astype(jnp.bfloat16)
    load.wait()
    chosen = matmul(held_pick[...], out_ref[...], 1, 1).astype(jnp.bfloat16)
    size = turned_ref.shape[1]
    for block in range(count):
        turned_ref[block] = chosen[block * size : (block + 1) * size]
    tile = 2 * 128

    def one_tile(number, carry):
        columns = pl.ds(pl.multiple_of(number * tile, tile), tile)
        term_ref[columns, :] = matmul(held_dy[:, columns], attn_ref[...], 0, 0).astype(jnp.bfloat16)
        return carry

    lax.fori_loop(0, held_dy.shape[1] // tile, one_tile, 0)
    for copy in sums:
        copy.wait_recv()
    share_end([group])
    for copy in sums:
        copy.wait_send()


def attend_back(queries, keys_in, values_in, attn, lse, dy, weight, table, pick, passed, shard, count):
    heads, length, _ = queries.shape
    part, width = length // count, dy.shape[1]
    columns = (heads + 2) * HD
    vmem, whole = pl.BlockSpec(memory_space=pltpu.VMEM), pl.BlockSpec(memory_space=pl.ANY)
    return pl.pallas_call(
        lambda *refs: attend_back_kernel(count, *refs),
        out_shape=[
            jax.ShapeDtypeStruct((length, columns), jnp.bfloat16),
            jax.ShapeDtypeStruct((count, columns // count, length), jnp.bfloat16),
            jax.ShapeDtypeStruct((width, heads * HD), jnp.bfloat16),
            jax.ShapeDtypeStruct((2, part // 2, width), jnp.bfloat16),
            jax.ShapeDtypeStruct((count,) + shard.shape, shard.dtype),
        ],
        in_specs=[vmem] * 5 + [whole] + [vmem] * 2 + [whole] * 3,
        out_specs=[vmem] * 3 + [whole] * 2,
        scratch_shapes=[
            pltpu.VMEM((heads, part, HD), jnp.bfloat16),
            pltpu.VMEM((heads, part), jnp.float32),
            pltpu.VMEM((heads, part, HD), jnp.bfloat16),
            pltpu.VMEM((length, HD), jnp.float32),
            pltpu.VMEM((length, HD), jnp.float32),
        ]
        + [pltpu.VMEM(dy.shape, dy.dtype), pltpu.VMEM(pick.shape, pick.dtype)]
        + [pltpu.SemaphoreType.DMA((8,)), pltpu.SemaphoreType.DMA((8,)), pltpu.SemaphoreType.DMA((count + 1,))],
        compiler_params=pltpu.CompilerParams(collective_id=4, has_side_effects=True, vmem_limit_bytes=LIMIT),
        name="attend_back",
    )(queries, keys_in, values_in, attn, lse, dy, weight, table, pick, passed, shard)


def leave_kernel(
    count, grads_ref, weight_ref, first_in, scale_ref, gain_ref, other_ref, turned_ref, normed_in,
    own_ref, total_ref, term_ref,
    sent_ref, side_ref, below_ref, far_ref, slot_ref, whole_ref, normed_ref, first_ref,
    told_ref, heard_ref, send_sems, recv_sems, swap_send, swap_recv, load_sems, sum_send, sum_recv,
):
    part, _ = first_ref.shape
    half = part // 2
    size = turned_ref.shape[1]
    heads = H // count
    chunk = size // (heads + 2)
    index = lax.axis_index("seq")
    place = lax.axis_index("fsdp")
    peers = [seq_peer(step) for step in range(1, count)]
    fsdp_peers = [fsdp_peer(place ^ (1 << bit)) for bit in range(lax.axis_size("fsdp").bit_length() - 1)]
    greet(peers + fsdp_peers)
    swaps = [
        remote(turned_ref.at[index ^ step], slot_ref.at[step], (swap_send, swap_recv), step - 1, seq_peer(step))
        for step in range(1, count)
    ]
    for copy in swaps:
        copy.start()
    loads = [
        pltpu.make_async_copy(source, target, load_sems.at[number])
        for number, (source, target) in enumerate(
            (
                (turned_ref.at[index], slot_ref.at[0]),
                (normed_in, normed_ref),
                (first_in, first_ref),
            )
        )
    ]
    for load in loads:
        load.start()
    total_ref[0:1] = jnp.zeros_like(other_ref)
    total_ref[1:2] = other_ref[...]
    loads[1].wait()
    sums = sum_copies(sent_ref, side_ref, below_ref, far_ref, half, (send_sems, recv_sems))

    def one_part(turn, carry):
        step = count - 1 - turn
        rows_step = pl.ds(pl.multiple_of(step * part, part), part)
        partial = matmul(grads_ref[rows_step, :], weight_ref[...], 1, 0)
        total_ref[0:1] += jnp.sum(partial * normed_ref[rows_step, :].astype(jnp.float32), 0, keepdims=True)
        pass_sums(turn, step, partial, sums, sent_ref, side_ref, below_ref, own_ref, half)
        return carry

    lax.fori_loop(0, count, one_part, 0)
    loads[0].wait()
    loads[2].wait()
    total_ref[0:1] = total_ref[0:1] / gain_ref[...]
    tells = []
    for step, peer in enumerate(fsdp_peers):
        told_ref[step] = total_ref[...]
        tell = remote(told_ref.at[step], heard_ref.at[step], (sum_send, sum_recv), step, peer)
        tell.start()
        tell.wait_recv()
        total_ref[...] += heard_ref[step]
        tells.append(tell)
    first = len(tells)
    told_ref[first] = total_ref[...]
    for step, peer in enumerate(peers):
        tells.append(
            remote(told_ref.at[first], heard_ref.at[first + step], (sum_send, sum_recv), first + step, peer)
        )
        tells[-1].start()
    for step in range(count):
        if step:
            swaps[step - 1].wait_recv()
        peer = index ^ step
        for block in range(count):
            piece = slot_ref[step, :, (step ^ block) * part : ((step ^ block) + 1) * part]
            tokens = slice(block * part, (block + 1) * part)
            for start, rows in ((0, heads * chunk), (H * chunk, chunk), ((H + KVH) * chunk, chunk)):
                begin = 0 if start == 0 else heads * chunk + (0 if start == H * chunk else chunk)
                spot = pl.multiple_of(start + peer * rows, chunk)
                whole_ref[pl.ds(spot, rows), tokens] = piece[begin : begin + rows]
    term_ref[...] = matmul(whole_ref[...], normed_ref[...], 1, 0).astype(jnp.bfloat16)
    end_sums(sums, side_ref, below_ref, far_ref, own_ref, half)
    unit = first_ref[...] * scale_ref[:, :1]
    grads = own_ref[...]
    inner = grads * gain_ref[...]
    own_ref[...] = scale_ref[:, :1] * (inner - unit * jnp.mean(inner * unit, 1, keepdims=True))
    for step in range(len(peers)):
        tells[first + step].wait_recv()
        total_ref[...] += heard_ref[first + step]
    for copy in sums + swaps + tells:
        copy.wait_send()


def leave(grads, weight, first, scale, gain, other, turned, normed, count):
    part, width = first.shape
    vmem, whole = pl.BlockSpec(memory_space=pltpu.VMEM), pl.BlockSpec(memory_space=pl.ANY)
    size, length = turned.shape[1:]
    steps = lax.axis_size("fsdp").bit_length() - 1 + count - 1
    own, total, term = pl.pallas_call(
        lambda *refs: leave_kernel(count, *refs),
        out_shape=(
            jax.ShapeDtypeStruct((part, width), jnp.float32),
            jax.ShapeDtypeStruct((2, width), jnp.float32),
            jax.ShapeDtypeStruct((size * count, width), jnp.bfloat16),
        ),
        in_specs=[vmem] * 2 + [whole] + [vmem] * 3 + [whole] * 2,
        out_specs=[vmem] * 3,
        scratch_shapes=[
            pltpu.VMEM((count, part, width), jnp.bfloat16),
            pltpu.VMEM((2, part // 2, width), jnp.bfloat16),
            pltpu.VMEM((2, part // 2, width), jnp.bfloat16),
            pltpu.VMEM((2, part // 2, width), jnp.bfloat16),
            pltpu.VMEM((count, size, length), jnp.bfloat16),
            pltpu.VMEM((count * size, length), jnp.bfloat16),
            pltpu.VMEM(normed.shape, jnp.bfloat16),
            pltpu.VMEM((part, width), jnp.float32),
            pltpu.VMEM((steps, 2, width), jnp.float32),
            pltpu.VMEM((steps, 2, width), jnp.float32),
            pltpu.SemaphoreType.DMA((6,)),
            pltpu.SemaphoreType.DMA((6,)),
            pltpu.SemaphoreType.DMA((count - 1,)),
            pltpu.SemaphoreType.DMA((count - 1,)),
            pltpu.SemaphoreType.DMA((3,)),
            pltpu.SemaphoreType.DMA((steps,)),
            pltpu.SemaphoreType.DMA((steps,)),
        ],
        compiler_params=pltpu.CompilerParams(collective_id=5, has_side_effects=True, vmem_limit_bytes=LIMIT),
        name="leave",
    )(grads, weight, first, scale, gain, other, turned, normed)
    return own, total, term


def join_rows_kernel(index_ref, own_ref, side_ref, below_ref, top_ref, bottom_ref, out_ref):
    step = pl.program_id(0) ^ index_ref[0]
    half = top_ref.shape[0]
    for number, ref in enumerate((own_ref, side_ref, below_ref)):

        @pl.when(step == number)
        def _():
            out_ref[...] = ref[...].astype(jnp.float32)

    @pl.when(step == 3)
    def _():
        out_ref[:half] = top_ref[...].astype(jnp.float32)
        out_ref[half:] = bottom_ref[...].astype(jnp.float32)


def join_rows(index, own, side, below, top, bottom, count):
    rows, width = own.shape
    parts = (own, side, below, top, bottom)
    return pl.pallas_call(
        join_rows_kernel,
        out_shape=jax.ShapeDtypeStruct((rows * count, width), jnp.float32),
        grid_spec=pltpu.PrefetchScalarGridSpec(
            num_scalar_prefetch=1,
            grid=(count,),
            in_specs=[pl.BlockSpec(part.shape, lambda i, s: (0, 0)) for part in parts],
            out_specs=pl.BlockSpec((rows, width), lambda i, s: (i, 0)),
        ),
        compiler_params=pltpu.CompilerParams(vmem_limit_bytes=LIMIT),
        name="join_rows",
    )(index, *parts)


def join_pieces_kernel(count, row_piece, column_piece, index_ref, own_ref, *refs):
    slot_refs, out_ref = refs[:-1], refs[-1]
    index = index_ref[0]
    rows, columns = own_ref.shape
    for device in range(count):
        if len(slot_refs) == 1:
            values = slot_refs[0][device ^ index]
        else:
            values = own_ref[...]
            for step, ref in enumerate(slot_refs):
                values = jnp.where(device ^ index == step + 1, ref[...], values)
        values = jnp.where(device == index, own_ref[...], values).astype(jnp.float32)
        for top in range(0, rows, row_piece):
            for left in range(0, columns, column_piece):
                down = top * count + device * row_piece if row_piece < rows else top
                across = left * count + device * column_piece if row_piece == rows else left
                out_ref[down : down + row_piece, across : across + column_piece] = values[
                    top : top + row_piece, left : left + column_piece
                ]


def join_pieces(index, own, slots, count, row_piece, column_piece):
    rows, columns = own.shape
    shape = (rows * count, columns) if row_piece < rows else (rows, columns * count)
    return pl.pallas_call(
        lambda *refs: join_pieces_kernel(count, row_piece, column_piece, *refs),
        out_shape=jax.ShapeDtypeStruct(shape, jnp.float32),
        grid_spec=pltpu.PrefetchScalarGridSpec(
            num_scalar_prefetch=1,
            grid=(1,),
            in_specs=[pl.BlockSpec(own.shape, lambda i, s: (0, 0))]
            + [pl.BlockSpec(slot.shape, lambda i, s, n=slot.ndim: (0,) * n) for slot in slots],
            out_specs=pl.BlockSpec(shape, lambda i, s: (0, 0)),
        ),
        compiler_params=pltpu.CompilerParams(vmem_limit_bytes=LIMIT),
        name="join_pieces",
    )(index, own, *slots)


def last_sums_kernel(base_ref, passed_ref, flowing_ref, piece_ref, result_ref, grad_ref):
    result_ref[...] = base_ref[...] + passed_ref[...].astype(jnp.float32)
    grad_ref[...] = flowing_ref[...] + piece_ref[...]


def last_sums(base, passed, flowing, piece):
    rows, width = base.shape
    tile = rows // 4
    block = pl.BlockSpec((tile, width), lambda i: (i, 0))
    return pl.pallas_call(
        last_sums_kernel,
        out_shape=[jax.ShapeDtypeStruct((rows, width), jnp.float32)] * 2,
        grid=(4,),
        in_specs=[block] * 4,
        out_specs=[block] * 2,
        compiler_params=pltpu.CompilerParams(vmem_limit_bytes=LIMIT),
        name="last_sums",
    )(base, passed, flowing, piece)


def norm_back_kernel(
    count, left_in, right_in, weight_ref, flowing_in, middle_in, scale_ref, gain_ref, inputs_ref,
    own_ref, gain_out_ref, dy_ref, term_ref,
    sent_ref, side_ref, below_ref, far_ref, stage_ref, held_grads, held_weight, held_inputs, flowing_ref, middle_ref,
    send_sems, recv_sems, store_sems, load_sems,
):
    part, width = flowing_ref.shape
    half = part // 2
    sems = (send_sems, recv_sems)
    units = held_grads.shape[1]
    tile = stage_ref.shape[1]
    tiles = units // tile
    cuts = [tiles * number // 4 * tile for number in range(5)]
    last = pl.ds((count - 1) * part, part)
    rest = pl.ds(0, (count - 1) * part)

    def load_grads(rows, number):
        return [
            pltpu.make_async_copy(
                source.at[rows],
                held_grads.at[rows, pl.ds(place * (units // 2), units // 2)],
                load_sems.at[number + place],
            )
            for place, source in enumerate((left_in, right_in))
        ]

    load_last, load_rest = load_grads(last, 9), load_grads(rest, 11)
    for load in load_last:
        load.start()
    load_weight = []
    for number in range(4):
        rows = pl.ds(cuts[number], cuts[number + 1] - cuts[number])
        load = pltpu.make_async_copy(weight_ref.at[rows], held_weight.at[rows], load_sems.at[number])
        load.start()
        load_weight.append(load)
    for load in load_rest:
        load.start()
    load_inputs = pltpu.make_async_copy(inputs_ref, held_inputs, load_sems.at[6])
    load_inputs.start()
    load_ends = [
        pltpu.make_async_copy(flowing_in, flowing_ref, load_sems.at[7]),
        pltpu.make_async_copy(middle_in, middle_ref, load_sems.at[8]),
    ]
    for load in load_ends:
        load.start()
    grads_ref, weight_ref, inputs_ref = held_grads, held_weight, held_inputs
    for load in load_last:
        load.wait()
    partial = jnp.zeros((part, width), jnp.float32)
    for number in range(4):
        load_weight[number].wait()
        rows = slice(cuts[number], cuts[number + 1])
        partial += matmul(grads_ref[last, rows], weight_ref[rows, :], 1, 0)
    sent_ref[count - 1] = partial.astype(jnp.bfloat16)
    greet([seq_peer(1), seq_peer(2)])
    sums = sum_copies(sent_ref, side_ref, below_ref, far_ref, half, sems)
    sums[0].start()
    sums[1].start()
    for load in load_rest:
        load.wait()

    def one_part(turn, carry):
        step = count - 1 - turn
        rows_step = pl.ds(pl.multiple_of(step * part, part), part)
        partial = matmul(grads_ref[rows_step, :], weight_ref[...], 1, 0)
        pass_sums(turn, step, partial, sums, sent_ref, side_ref, below_ref, own_ref, half)
        return carry

    lax.fori_loop(1, count, one_part, 0)
    load_inputs.wait()
    for load in load_ends:
        load.wait()

    def store(number):
        rows = pl.ds(pl.multiple_of(number * tile, tile), tile)
        return pltpu.make_async_copy(stage_ref.at[number % 2], term_ref.at[rows], store_sems.at[number % 2])

    def one_tile(number, carry):
        @pl.when(number >= 2)
        def _():
            store(number - 2).wait()

        columns = pl.ds(pl.multiple_of(number * tile, tile), tile)
        stage_ref[number % 2] = matmul(grads_ref[:, columns], inputs_ref[...], 0, 0).astype(jnp.bfloat16)
        store(number).start()
        return carry

    lax.fori_loop(0, tiles, one_tile, 0)
    end_sums(sums, side_ref, below_ref, far_ref, own_ref, half)
    scale = scale_ref[:, :1]
    unit = middle_ref[...] * scale
    grads = own_ref[...]
    gain_out_ref[...] = jnp.sum(grads * unit, 0, keepdims=True)
    inner = grads * gain_ref[...]
    own_ref[...] = flowing_ref[...] + scale * (inner - unit * jnp.mean(inner * unit, 1, keepdims=True))
    dy_ref[...] = own_ref[...].astype(jnp.bfloat16)
    for number in range(tiles - 2, tiles):
        store(number).wait()
    for copy in sums:
        copy.wait_send()


def norm_back(left, right, weight, flowing, middle, scale, gain, inputs, count):
    part, width = flowing.shape
    units = left.shape[1] + right.shape[1]
    tile = 2 * 128
    vmem = pl.BlockSpec(memory_space=pltpu.VMEM)
    own, gain_term, dy, term = pl.pallas_call(
        lambda *refs: norm_back_kernel(count, *refs),
        out_shape=(
            jax.ShapeDtypeStruct((part, width), jnp.float32),
            jax.ShapeDtypeStruct((1, width), jnp.float32),
            jax.ShapeDtypeStruct((part, width), jnp.bfloat16),
            jax.ShapeDtypeStruct((units, width), jnp.bfloat16),
        ),
        in_specs=[pl.BlockSpec(memory_space=pl.ANY)] * 5 + [vmem] * 2 + [pl.BlockSpec(memory_space=pl.ANY)],
        out_specs=[vmem] * 3 + [pl.BlockSpec(memory_space=pl.ANY)],
        scratch_shapes=[
            pltpu.VMEM((count, part, width), jnp.bfloat16),
            pltpu.VMEM((2, part // 2, width), jnp.bfloat16),
            pltpu.VMEM((2, part // 2, width), jnp.bfloat16),
            pltpu.VMEM((2, part // 2, width), jnp.bfloat16),
            pltpu.VMEM((2, tile, width), jnp.bfloat16),
            pltpu.VMEM((part * count, units), jnp.bfloat16),
            pltpu.VMEM(weight.shape, jnp.bfloat16),
            pltpu.VMEM(inputs.shape, jnp.bfloat16),
            pltpu.VMEM((part, width), jnp.float32),
            pltpu.VMEM((part, width), jnp.float32),
            pltpu.SemaphoreType.DMA((6,)),
            pltpu.SemaphoreType.DMA((6,)),
            pltpu.SemaphoreType.DMA((2,)),
            pltpu.SemaphoreType.DMA((13,)),
        ],
        compiler_params=pltpu.CompilerParams(collective_id=3, has_side_effects=True, vmem_limit_bytes=LIMIT),
        name="norm_back",
    )(left, right, weight, flowing, middle, scale, gain, inputs)
    return own, gain_term[0], dy, term


def share_dy_kernel(
    dy_ref, down_ref, side_ref, below_ref, middle_ref, all_ref, base_ref, passed_ref,
    piece_ref, send_sems, recv_sems, load_sems,
):
    part = dy_ref.shape[0]
    half = part // 2
    wide = jnp.float32
    top, bottom = pl.ds(0, half), pl.ds(half, half)
    loads = [
        pltpu.make_async_copy(down_ref.at[0], piece_ref.at[0], load_sems.at[0]),
        pltpu.make_async_copy(down_ref.at[2].at[top], piece_ref.at[1].at[top], load_sems.at[1]),
        pltpu.make_async_copy(down_ref.at[1].at[bottom], piece_ref.at[1].at[bottom], load_sems.at[2]),
        pltpu.make_async_copy(dy_ref, all_ref.at[0], load_sems.at[3]),
    ]
    greet([seq_peer(1), seq_peer(2)])
    group = gather_copies(dy_ref, all_ref, half, (send_sems, recv_sems))
    share_start([group])
    for load in loads:
        load.start()
    for load in loads:
        load.wait()
    base_ref[...] = middle_ref[...] + piece_ref[0].astype(wide)
    base_ref[:half] += side_ref[0].astype(wide)
    base_ref[half:] += below_ref[0].astype(wide)
    passed_ref[0] = (piece_ref[1, :half].astype(wide) + side_ref[1].astype(wide)).astype(jnp.bfloat16)
    passed_ref[1] = (piece_ref[1, half:].astype(wide) + below_ref[1].astype(wide)).astype(jnp.bfloat16)
    share_on(group)
    share_end([group])


def share_dy(dy, down, side, below, middle, count):
    part, width = dy.shape
    vmem, whole = pl.BlockSpec(memory_space=pltpu.VMEM), pl.BlockSpec(memory_space=pl.ANY)
    gathered, base, passed = pl.pallas_call(
        lambda *refs: share_dy_kernel(*refs),
        out_shape=[
            jax.ShapeDtypeStruct((count, part, width), jnp.bfloat16),
            jax.ShapeDtypeStruct((part, width), jnp.float32),
            jax.ShapeDtypeStruct((2, part // 2, width), jnp.bfloat16),
        ],
        in_specs=[vmem, whole, vmem, vmem, vmem],
        out_specs=[whole, vmem, vmem],
        scratch_shapes=[
            pltpu.VMEM((2, part, width), jnp.bfloat16),
            pltpu.SemaphoreType.DMA((6,)),
            pltpu.SemaphoreType.DMA((6,)),
            pltpu.SemaphoreType.DMA((4,)),
        ],
        compiler_params=pltpu.CompilerParams(collective_id=8, has_side_effects=True, vmem_limit_bytes=LIMIT),
        name="share_dy",
    )(dy, down, side, below, middle)
    return gathered.reshape(part * count, width), base, passed


def fast_body(hidden, positions, gains, w_qkv, w_out, w_gate_up, w_down, cotangent):
    count = lax.axis_size("seq")
    index = lax.axis_index("seq")
    place = index.astype(jnp.int32).reshape(1)
    current = hidden[0]
    part_len, width = current.shape
    heads = H // count
    gain = gains[0]
    after = lax.optimization_barrier

    rows = w_qkv.shape[1]
    group = math.gcd(rows, HD)
    chunk = group // count
    per_head = HD // group
    normed_all, qkv_rows, out_cols, table, gate_up_part, down_part, scale_one = enter(
        current, gain[:1], positions[0], w_qkv[0], w_out[0], w_gate_up[0], w_down[0], count
    )
    gu_rows = w_gate_up.shape[1] // count
    gate_up = lax.all_gather(gate_up_part, "fsdp", axis=0, tiled=True)
    units = FF // count
    down_rows = w_down.shape[1]

    queries, keys_in, values_in = project_qkv(place, normed_all, qkv_rows, table, count)
    attn_flat, log_total, middle, scale_two, normed_two_all = attend(
        queries, keys_in, values_in, out_cols, current, gain[1:], count
    )
    flowing = cotangent[0]
    normed_two_all, dm_sent, down_part = after((normed_two_all, flowing.astype(jnp.bfloat16), down_part))
    down_cols = lax.all_gather(down_part, "fsdp", axis=0, tiled=True)
    dm_all = jnp.concatenate([dm_sent] + [neighbour(dm_sent, step) for step in range(1, count)], 0)
    both = matmul(normed_two_all, gate_up, 1, 1)
    gate_part, up_part = both[:, :units], both[:, units:]
    activated = (jax.nn.silu(gate_part) * up_part).astype(jnp.bfloat16)

    def owned(grad):
        return lax.psum_scatter(grad.astype(jnp.bfloat16), "fsdp", scatter_dimension=0, tiled=True)

    term_down = matmul(dm_all, activated, 0, 0).astype(jnp.bfloat16)
    dm_all, activated, term_down = after((dm_all, activated, term_down))
    grad_down = owned(term_down)
    down_sent = matmul(activated, down_cols, 1, 1).astype(jnp.bfloat16)
    down_sent = down_sent.reshape(count, part_len, width)
    dm_all, down_sent = after((dm_all, down_sent))
    half = part_len // 2
    from_side = neighbour(jnp.stack([down_sent[1, :half], down_sent[3, :half]]), 1)
    from_below = neighbour(jnp.stack([down_sent[2, half:], down_sent[3, half:]]), 2)
    dact = matmul(dm_all, down_cols, 1, 0)
    sigma = jax.nn.sigmoid(gate_part)
    dgate = dact * up_part * sigma * (1.0 + gate_part * (1.0 - sigma))
    dup = dact * gate_part * sigma
    dgate, dup = dgate.astype(jnp.bfloat16), dup.astype(jnp.bfloat16)
    dmiddle, gain_two, dy, term_gate_up = norm_back(
        dgate, dup, gate_up, flowing, middle, scale_two, gain[1:], normed_two_all, count
    )
    grad_gate_up = owned(term_gate_up)
    dy_all, base, passed = share_dy(dy, down_sent, from_side, from_below, middle, count)
    pieces = heads + 2
    picked = np.arange(pieces * HD).reshape(pieces * per_head, count, chunk).transpose(1, 0, 2).reshape(-1)
    pick = jnp.asarray(picked[:, None] == np.arange(pieces * HD)[None, :], jnp.bfloat16)
    djoint, djoint_turned, term_out, passed_on, down_slots = attend_back(
        queries, keys_in, values_in, attn_flat, log_total, dy_all, out_cols, table, pick, passed, grad_down, count
    )
    grad_out = owned(term_out)
    grad_piece, gain_total, term_qkv = leave(
        djoint, qkv_rows, current, scale_one, gain[:1], gain_two[None], djoint_turned, normed_all, count
    )
    grad_qkv = owned(term_qkv)
    grad_gate_up, grad_piece = after((grad_gate_up, grad_piece))
    half = upper_half(gu_rows)
    side = neighbour(grad_gate_up, 1)
    below = neighbour(grad_gate_up, 2)
    far_top = neighbour(side[:half], 2)
    far_bottom = neighbour(below[half:], 1)
    down_shard = join_pieces(place, grad_down, (down_slots,), count, down_rows, gu_rows)
    result, grad_hidden = last_sums(base, passed_on.reshape(part_len, width), dmiddle, grad_piece)
    out_slots = [neighbour(grad_out, step) for step in range(1, count)]
    grad_qkv, out_slots = after((grad_qkv, out_slots))
    qkv_slots = [neighbour(grad_qkv, step) for step in range(1, count)]
    gate_up_shard = join_rows(place, grad_gate_up, side, below, far_top, far_bottom, count)
    out_shard = join_pieces(place, grad_out, out_slots, count, down_rows, heads * HD)
    qkv_shard = join_pieces(place, grad_qkv, qkv_slots, count, chunk, width)
    gain_total = gain_total[None]
    return (
        result[None],
        grad_hidden[None],
        gain_total,
        qkv_shard[None],
        out_shard[None],
        gate_up_shard[None],
        down_shard[None],
    )


def fits(mesh):
    count, fsdp = mesh.shape["seq"], mesh.shape["fsdp"]
    rows = (H + 2 * KVH) * HD // fsdp
    return count == KVH == 4 and fsdp % 2 == 0 and fsdp & (fsdp - 1) == 0 and rows % HD == 0


def solution(mesh):
    placed = (
        P("fsdp", "seq", None),
        P("fsdp", "seq"),
        P(),
        P(None, "fsdp", None),
        P(None, "fsdp", None),
        P(None, "fsdp", None),
        P(None, "fsdp", None),
        P("fsdp", "seq", None),
    )
    fast = fits(mesh)
    return jax.shard_map(
        fast_body if fast else body,
        mesh=mesh,
        in_specs=placed,
        out_specs=(
            P("fsdp", "seq", None),
            P("fsdp", "seq", None),
            P(),
            P(None, "fsdp", None),
            P(None, "fsdp", None),
            P(None, "fsdp", None),
            P(None, "fsdp", None),
        ),
        check_vma=False,
    )
```

```python
import math

import jax
import jax.numpy as jnp
import numpy as np
from jax import lax
from jax.experimental import pallas as pl
from jax.experimental.pallas import tpu as pltpu
from jax.sharding import PartitionSpec as P


H = 32
KVH = 4
HD = 64
FF = 5632
LAYERS = 1


EPS = 1e-05


def rope_tables(position_ids):
    halfway = HD // 2
    frequency = jnp.exp(jnp.arange(halfway, dtype=jnp.float32) * (-2.0 * math.log(10000.0) / HD))
    angles = position_ids.astype(jnp.float32)[..., None] * frequency
    cosines = jnp.cos(angles)
    sines = jnp.sin(angles)
    return (
        jnp.concatenate([cosines, cosines], -1)[..., None, :],
        jnp.concatenate([sines, sines], -1)[..., None, :],
    )


def rotate(values, cosines, sines):
    halfway = values.shape[-1] // 2
    turned = jnp.concatenate([-values[..., halfway:], values[..., :halfway]], -1)
    return values * cosines + turned * sines


def unrotate(grads, cosines, sines):
    halfway = grads.shape[-1] // 2
    scaled = grads * sines
    return grads * cosines + jnp.concatenate([scaled[..., halfway:], -scaled[..., :halfway]], -1)


def normalize(values, gain):
    scale = lax.rsqrt(jnp.mean(values * values, -1, keepdims=True) + EPS)
    return ((values * scale * gain).astype(jnp.bfloat16), scale)


def normalize_back(grads, values, scale, gain):
    unit = values * scale
    gain_grad = jnp.sum((grads * unit).reshape(-1, unit.shape[-1]), 0)
    inner = grads * gain
    return (scale * (inner - unit * jnp.mean(inner * unit, -1, keepdims=True)), gain_grad)


def masked_scores(queries, keys_wide):
    scores = jnp.einsum(
        "qhd,khd->hqk", queries, keys_wide, preferred_element_type=jnp.float32
    ) * queries.shape[-1] ** (-0.5)
    length = queries.shape[0]
    causal = jnp.arange(length)[:, None] >= jnp.arange(length)[None, :]
    return jnp.where(causal[None], scores, -1e30)


def local_attend(operands):
    queries, keys_in, values_in = operands
    repeat_by = queries.shape[1] // keys_in.shape[1]
    keys_wide = jnp.repeat(keys_in, repeat_by, axis=1)
    values_wide = jnp.repeat(values_in, repeat_by, axis=1)
    scores = masked_scores(queries, keys_wide)
    peak = jnp.max(scores, -1, keepdims=True)
    log_total = peak[..., 0] + jnp.log(jnp.sum(jnp.exp(scores - peak), -1))
    weights = jnp.exp(scores - log_total[..., None]).astype(jnp.bfloat16)
    output = jnp.einsum("hqk,khd->qhd", weights, values_wide, preferred_element_type=jnp.float32)
    return (output.astype(jnp.bfloat16), log_total)


def local_attend_back(operands):
    queries, keys_in, values_in, output, log_total, dattn = operands
    length, kv_dev, head_dim = keys_in.shape
    repeat_by = queries.shape[1] // kv_dev
    keys_wide = jnp.repeat(keys_in, repeat_by, axis=1)
    values_wide = jnp.repeat(values_in, repeat_by, axis=1)
    scores = masked_scores(queries, keys_wide)
    probs = jnp.exp(scores - log_total[..., None])
    delta = jnp.sum(output.astype(jnp.float32) * dattn.astype(jnp.float32), -1).T
    dprob = jnp.einsum("qhd,khd->hqk", dattn, values_wide, preferred_element_type=jnp.float32)
    dscore = (probs * (dprob - delta[..., None])).astype(jnp.bfloat16)
    dqueries = jnp.einsum(
        "hqk,khd->qhd", dscore, keys_wide, preferred_element_type=jnp.float32
    ) * head_dim ** (-0.5)
    dkeys = jnp.einsum(
        "hqk,qhd->khd", dscore, queries, preferred_element_type=jnp.float32
    ) * head_dim ** (-0.5)
    dvalues = jnp.einsum(
        "hqk,qhd->khd", probs.astype(jnp.bfloat16), dattn, preferred_element_type=jnp.float32
    )

    def fold_heads(per_head):
        return jnp.sum(per_head.reshape(length, kv_dev, repeat_by, head_dim), 2).astype(
            jnp.bfloat16
        )

    return (dqueries.astype(jnp.bfloat16), fold_heads(dkeys), fold_heads(dvalues))


def project(inputs, weight):
    return lax.dot_general(
        inputs,
        lax.all_gather(weight, "fsdp", axis=0, tiled=True),
        (((1,), (1,)), ((), ())),
        preferred_element_type=jnp.float32,
    )


def project_back(grads, weight):
    shard_rows = lax.all_gather(weight, "fsdp", axis=0, tiled=True)
    picked = lax.slice_in_dim(grads, 0, shard_rows.shape[0], axis=1)
    return jnp.dot(picked, shard_rows, preferred_element_type=jnp.float32)


def weight_grad(grads, inputs, shard_size):
    picked = lax.slice_in_dim(grads, 0, shard_size * lax.axis_size("fsdp"), axis=1)
    summed = lax.psum_scatter(
        lax.dot_general(
            picked, inputs, (((0,), (0,)), ((), ())), preferred_element_type=jnp.float32
        ).astype(jnp.bfloat16),
        "fsdp",
        scatter_dimension=0,
        tiled=True,
    )
    return lax.psum(summed, "seq").astype(jnp.float32)


def backward_pair(grads, inputs, weight):
    wgrad = weight_grad(grads, inputs, weight.shape[0])
    return (project_back(grads, weight), wgrad)


def body(hidden, positions, gains, w_qkv, w_out, w_gate_up, w_down, cotangent):
    seq_count, part_len, model_width = hidden.shape
    row_count = seq_count * part_len
    group_count = lax.axis_size("seq")
    full_len = part_len * group_count
    heads_dev = H // group_count
    share = H // KVH
    kv_dev = max(1, heads_dev // share)
    first_kv = np.arange(group_count) * heads_dev // share
    slot_table = np.concatenate(
        [
            first_kv[:, None] + np.arange(kv_dev)[None, :],
            KVH + first_kv[:, None] + np.arange(kv_dev)[None, :],
        ],
        1,
    ).reshape(-1)
    slot_onehot = jnp.asarray(
        (slot_table[:, None] == np.arange(2 * KVH)[None, :]).astype(np.float32), jnp.bfloat16
    )
    cosines, sines = rope_tables(positions)
    layer_index = 0
    gain = gains[layer_index]
    normed, scale_one = normalize(hidden, gain[0])
    normed_flat = normed.reshape(row_count, model_width)
    joint = project(normed_flat, w_qkv[layer_index]).reshape(seq_count, part_len, -1)
    queries = joint[..., : H * HD].reshape(seq_count, part_len, H, HD)
    keys_in = joint[..., H * HD : (H + KVH) * HD].reshape(seq_count, part_len, KVH, HD)
    values_in = joint[..., (H + KVH) * HD :].reshape(seq_count, part_len, KVH, HD)
    q_rot = rotate(queries, cosines, sines).astype(jnp.bfloat16)
    kv_all = jnp.concatenate(
        [rotate(keys_in, cosines, sines).astype(jnp.bfloat16), values_in.astype(jnp.bfloat16)], 2
    )
    q_send = q_rot.reshape(seq_count, part_len, group_count, heads_dev * HD)
    kv_send = jnp.take(kv_all, slot_table, axis=2).reshape(
        seq_count, part_len, group_count, 2 * kv_dev * HD
    )
    q_heads = lax.all_to_all(q_send, "seq", split_axis=2, concat_axis=1, tiled=True)
    kv_heads = lax.all_to_all(kv_send, "seq", split_axis=2, concat_axis=1, tiled=True)
    q_heads = q_heads.reshape(seq_count, full_len, heads_dev, HD)
    kv_heads = kv_heads.reshape(seq_count, full_len, 2 * kv_dev, HD)
    k_heads = kv_heads[:, :, :kv_dev]
    v_heads = kv_heads[:, :, kv_dev:]
    o_heads, log_total = lax.map(local_attend, (q_heads, k_heads, v_heads))
    o_back = lax.all_to_all(
        o_heads.reshape(seq_count, full_len, 1, heads_dev * HD),
        "seq",
        split_axis=1,
        concat_axis=2,
        tiled=True,
    )
    attn_flat = o_back.reshape(row_count, model_width)
    middle = hidden + project(attn_flat, w_out[layer_index]).reshape(
        seq_count, part_len, model_width
    )
    normed_two, scale_two = normalize(middle, gain[1])
    normed_two_flat = normed_two.reshape(row_count, model_width)
    both = project(normed_two_flat, w_gate_up[layer_index])
    gate_part = both[:, :FF]
    up_part = both[:, FF:]
    activated = (jax.nn.silu(gate_part) * up_part).astype(jnp.bfloat16)
    result = middle + project(activated, w_down[layer_index]).reshape(
        seq_count, part_len, model_width
    )
    saved = [
        (
            hidden,
            normed_flat,
            scale_one,
            q_heads,
            k_heads,
            v_heads,
            o_heads,
            log_total,
            attn_flat,
            middle,
            normed_two_flat,
            scale_two,
            gate_part,
            up_part,
            activated,
        )
    ]
    flowing = cotangent
    grads_qkv = [None] * LAYERS
    grads_out = [None] * LAYERS
    grads_gate_up = [None] * LAYERS
    grads_down = [None] * LAYERS
    gain_terms = [None] * LAYERS
    for layer_index in reversed(range(LAYERS)):
        (
            layer_in,
            normed_flat,
            scale_one,
            q_heads,
            k_heads,
            v_heads,
            o_heads,
            log_total,
            attn_flat,
            middle,
            normed_two_flat,
            scale_two,
            gate_part,
            up_part,
            activated,
        ) = saved[layer_index]
        gain = gains[layer_index]
        dm_cast = flowing.reshape(row_count, model_width).astype(jnp.bfloat16)
        dact, grads_down[layer_index] = backward_pair(dm_cast, activated, w_down[layer_index])
        sigma = jax.nn.sigmoid(gate_part)
        dgate = dact * up_part * sigma * (1.0 + gate_part * (1.0 - sigma))
        dup = dact * gate_part * sigma
        dgu = jnp.concatenate([dgate, dup], 1).astype(jnp.bfloat16)
        dnormed_two, grads_gate_up[layer_index] = backward_pair(
            dgu, normed_two_flat, w_gate_up[layer_index]
        )
        dnormed_two = dnormed_two.reshape(seq_count, part_len, model_width)
        dmid_norm, gain_two = normalize_back(dnormed_two, middle, scale_two, gain[1])
        dmiddle = flowing + dmid_norm
        dy_cast = dmiddle.reshape(row_count, model_width).astype(jnp.bfloat16)
        dattn_wide, grads_out[layer_index] = backward_pair(dy_cast, attn_flat, w_out[layer_index])
        dattn = dattn_wide.astype(jnp.bfloat16)
        dattn_heads = lax.all_to_all(
            dattn.reshape(seq_count, part_len, group_count, heads_dev * HD),
            "seq",
            split_axis=2,
            concat_axis=1,
            tiled=True,
        )
        dattn_heads = dattn_heads.reshape(seq_count, full_len, heads_dev, HD)
        dq_heads, dk_heads, dv_heads = lax.map(
            local_attend_back, (q_heads, k_heads, v_heads, o_heads, log_total, dattn_heads)
        )
        dkv_heads = jnp.concatenate([dk_heads, dv_heads], 2).reshape(
            seq_count, full_len, 1, 2 * kv_dev * HD
        )
        dq_tok, dkv_tok = (
            lax.all_to_all(
                dq_heads.reshape(seq_count, full_len, 1, heads_dev * HD),
                "seq",
                split_axis=1,
                concat_axis=2,
                tiled=True,
            ),
            lax.all_to_all(dkv_heads, "seq", split_axis=1, concat_axis=2, tiled=True),
        )
        dqueries = dq_tok.reshape(seq_count, part_len, H, HD)
        dkv_sum = jnp.einsum(
            "stnd,nm->stmd",
            dkv_tok.reshape(seq_count, part_len, group_count * 2 * kv_dev, HD),
            slot_onehot,
            preferred_element_type=jnp.float32,
        )
        dq_pre = unrotate(dqueries, cosines, sines)
        dk_pre = unrotate(dkv_sum[:, :, :KVH], cosines, sines)
        dvalues = dkv_sum[:, :, KVH:]
        djoint = jnp.concatenate(
            [
                dq_pre.reshape(row_count, -1),
                dk_pre.reshape(row_count, -1),
                dvalues.reshape(row_count, -1),
            ],
            1,
        ).astype(jnp.bfloat16)
        dnormed, grads_qkv[layer_index] = backward_pair(djoint, normed_flat, w_qkv[layer_index])
        dnormed = dnormed.reshape(seq_count, part_len, model_width)
        dcur_norm, gain_one = normalize_back(dnormed, layer_in, scale_one, gain[0])
        gain_terms[layer_index] = jnp.stack([gain_one, gain_two])
        flowing = dmiddle + dcur_norm
    gain_total = lax.psum(jnp.stack(gain_terms), ("fsdp", "seq"))
    return (
        result,
        flowing,
        gain_total,
        jnp.stack(grads_qkv),
        jnp.stack(grads_out),
        jnp.stack(grads_gate_up),
        jnp.stack(grads_down),
    )


def neighbour(values, step):
    count = lax.axis_size("seq")
    return lax.ppermute(values, "seq", [(i, i ^ step) for i in range(count)])


def matmul(left, right, left_dim, right_dim):
    return lax.dot_general(
        left, right, (((left_dim,), (right_dim,)), ((), ())), preferred_element_type=jnp.float32
    )


ROOT = HD ** (-0.5)
LIMIT = 60 * 1024 * 1024


def swap_halves(values):
    width = values.shape[1]
    half = HD // 2
    column = lax.broadcasted_iota(jnp.int32, values.shape, 1)
    return jnp.where(
        column % HD < half, pltpu.roll(values, width - half, 1), pltpu.roll(values, half, 1)
    )


def spread_tables(table, pairs, last):
    half = HD // 2
    cosines, sines = table[:, :half], table[:, half:]
    ones, zeros = jnp.ones_like(table), jnp.zeros_like(table)
    tail = [[cosines, cosines, ones], [-sines, sines, zeros]] if last else [[], []]
    if not pairs:
        return jnp.concatenate(tail[0], 1), jnp.concatenate(tail[1], 1)
    cosines = [jnp.concatenate([cosines] * 4, 1)] * pairs
    sines = [jnp.concatenate([-sines, sines] * 2, 1)] * pairs
    if last:
        cosines.append(jnp.concatenate(tail[0], 1))
        sines.append(jnp.concatenate(tail[1], 1))
    return jnp.concatenate(cosines, 1), jnp.concatenate(sines, 1)


MESH = pl.DeviceIdType.MESH


def seq_peer(step):
    return {"seq": lax.axis_index("seq") ^ step}


def fsdp_peer(place):
    return {"fsdp": place}


def remote(source, target, sems, slot, peer):
    return pltpu.make_async_remote_copy(
        src_ref=source,
        dst_ref=target,
        send_sem=sems[0].at[slot],
        recv_sem=sems[1].at[slot],
        device_id=peer,
        device_id_type=MESH,
    )


def gather_copies(own, slots, half, sems, base=0):
    top, bottom = pl.ds(0, half), pl.ds(half, own.shape[0] - half)

    def slot(step, rows):
        return slots.at[step].at[rows]

    return [
        remote(own.at[top], slot(1, top), sems, base, seq_peer(1)),
        remote(own.at[bottom], slot(2, bottom), sems, base + 1, seq_peer(2)),
        remote(own.at[bottom], slot(1, bottom), sems, base + 2, seq_peer(1)),
        remote(own.at[top], slot(2, top), sems, base + 3, seq_peer(2)),
        remote(slot(1, top), slot(3, top), sems, base + 4, seq_peer(2)),
        remote(slot(2, bottom), slot(3, bottom), sems, base + 5, seq_peer(1)),
    ]


def greet(peers):
    barrier = pltpu.get_barrier_semaphore()
    for peer in peers:
        pl.semaphore_signal(barrier, inc=1, device_id=peer, device_id_type=MESH)
    pl.semaphore_wait(barrier, len(peers))


def sum_copies(sent, side, below, far, half, sems, passed=None):
    top, bottom = pl.ds(0, half), pl.ds(half, half)
    return [
        remote(sent.at[3].at[top], side.at[1], sems, 0, seq_peer(1)),
        remote(sent.at[3].at[bottom], below.at[1], sems, 1, seq_peer(2)),
        remote(sent.at[2].at[bottom], below.at[0], sems, 2, seq_peer(2)),
        remote(sent.at[1].at[top], side.at[0], sems, 3, seq_peer(1)),
        remote(passed.at[0] if passed is not None else sent.at[2].at[top], far.at[0], sems, 4, seq_peer(2)),
        remote(passed.at[1] if passed is not None else sent.at[1].at[bottom], far.at[1], sems, 5, seq_peer(1)),
    ]


def pass_sums(turn, step, partial, sums, sent_ref, side_ref, below_ref, own_ref, half):
    wide, narrow = jnp.float32, jnp.bfloat16
    last = len(sums) // 2

    @pl.when(turn == last)
    def _():
        own_ref[...] = partial

    @pl.when(turn < last)
    def _():
        sent_ref[step] = partial.astype(narrow)

    @pl.when(turn == 0)
    def _():
        sums[0].start()
        sums[1].start()

    @pl.when(turn == 1)
    def _():
        sums[2].start()

    @pl.when(turn == 2)
    def _():
        sums[3].start()
        sums[0].wait_recv()
        sent_ref[2, :half] = (sent_ref[2, :half].astype(wide) + side_ref[1].astype(wide)).astype(narrow)
        sums[4].start()
        sums[1].wait_recv()
        sent_ref[1, half:] = (sent_ref[1, half:].astype(wide) + below_ref[1].astype(wide)).astype(narrow)
        sums[5].start()


def end_sums(sums, side_ref, below_ref, far_ref, own_ref, half):
    wide = jnp.float32
    sums[2].wait_recv()
    sums[3].wait_recv()
    own_ref[:half] += side_ref[0].astype(wide)
    own_ref[half:] += below_ref[0].astype(wide)
    sums[4].wait_recv()
    own_ref[:half] += far_ref[0].astype(wide)
    sums[5].wait_recv()
    own_ref[half:] += far_ref[1].astype(wide)


def share_own(own_ref, all_ref, half, sems, before):
    copies = gather_copies(own_ref, all_ref, half, sems, len(before))
    for copy in copies[:4]:
        copy.start()
    copies[0].wait_recv()
    copies[4].start()
    copies[1].wait_recv()
    copies[5].start()
    for copy in copies[2:]:
        copy.wait_recv()
    for copy in before + copies:
        copy.wait_send()


def enter_kernel(
    count, current_ref, gain_ref, spots_ref, shard_ref, out_shard_ref, gate_up_ref, down_ref,
    all_ref, rows_ref, out_ref, table_ref, gate_up_part_ref, down_part_ref, scale_ref,
    normed_ref, held_ref, part_ref, held_down,
    send_sems, recv_sems, spot_send, spot_recv, item_up, item_down, item_side, item_recv, local_sem,
):
    part, _ = current_ref.shape
    heads = H // count
    pieces = heads + 2
    items = pieces + lax.axis_size("fsdp")
    per_shard = shard_ref.shape[0] // HD
    out_rows, columns = out_shard_ref.shape[0], heads * HD
    chips = lax.axis_size("fsdp") // 2
    index = lax.axis_index("seq")
    place = lax.axis_index("fsdp")
    chip, core = place // 2, place % 2
    sems = (send_sems, recv_sems)

    barrier = pltpu.get_barrier_semaphore()
    for peer in [seq_peer(step) for step in range(1, count)] + [fsdp_peer(place ^ 1)]:
        pl.semaphore_signal(barrier, inc=1, device_id=peer, device_id_type=MESH)

    @pl.when(chip > 0)
    def _():
        pl.semaphore_signal(barrier, inc=1, device_id=fsdp_peer(place - 2), device_id_type=MESH)

    @pl.when(chip < chips - 1)
    def _():
        pl.semaphore_signal(barrier, inc=1, device_id=fsdp_peer(place + 2), device_id_type=MESH)

    greetings = count + (chip > 0).astype(jnp.int32) + (chip < chips - 1).astype(jnp.int32)
    pl.semaphore_wait(barrier, greetings)

    part_rows = part_ref.shape[0]
    take = pltpu.make_async_copy(
        gate_up_ref.at[pl.ds(pl.multiple_of(index * part_rows, part_rows), part_rows)], part_ref, local_sem.at[items + 1]
    )
    take.start()
    take_down = pltpu.make_async_copy(down_ref, held_down, local_sem.at[items + 3])
    take_down.start()

    def qkv_item(item):
        block = jnp.where(
            item < heads, index * heads + item, jnp.where(item == heads, H + index, H + KVH + index)
        )
        source = shard_ref.at[pl.ds(pl.multiple_of(block % per_shard * HD, HD), HD)]
        return block // per_shard, source, rows_ref.at[pl.ds(pl.multiple_of(item * HD, HD), HD)], item

    def out_item(item):
        source = out_shard_ref.at[:, pl.ds(pl.multiple_of(index * columns, columns), columns)]
        target = out_ref.at[pl.ds(pl.multiple_of(item * out_rows, out_rows), out_rows)]
        return item, source, target, item + pieces

    kinds = ((qkv_item, pieces), (out_item, items - pieces))

    def item_copy(source, target, slot, sem, peer):
        return pltpu.make_async_remote_copy(
            src_ref=source,
            dst_ref=target,
            send_sem=sem.at[slot],
            recv_sem=item_recv.at[slot],
            device_id=fsdp_peer(peer),
            device_id_type=MESH,
        )

    def pass_on(source, target, slot, owner_chip, act):
        @pl.when((chip >= owner_chip) & (chip < chips - 1))
        def _():
            act(item_copy(source, target, slot, item_up, place + 2))

        @pl.when((chip <= owner_chip) & (chip > 0))
        def _():
            act(item_copy(source, target, slot, item_down, place - 2))

        act(item_copy(source, target, slot, item_side, place ^ 1))

    def send_own(item_of):
        def body(item, carry):
            owner, source, target, slot = item_of(item)

            @pl.when(place == owner)
            def _():
                pass_on(source, target, slot, owner // 2, lambda copy: copy.start())
                pltpu.make_async_copy(source, target, local_sem.at[slot]).start()

            return carry

        return body

    def pass_far(item_of, distance):
        def body(item, carry):
            owner, _, target, slot = item_of(item)
            owner_chip = owner // 2
            apart = jnp.where(chip > owner_chip, chip - owner_chip, owner_chip - chip)

            @pl.when((apart == distance) & (core == owner % 2))
            def _():
                item_copy(target, target, slot, item_side, place ^ 1).wait_recv()
                pass_on(target, target, slot, owner_chip, lambda copy: copy.start())

            return carry

        return body

    for item_of, number in kinds:
        lax.fori_loop(0, number, send_own(item_of), 0)
    current = current_ref[...]
    scale = lax.rsqrt(jnp.mean(current * current, 1, keepdims=True) + EPS)
    scale_ref[...] = jnp.broadcast_to(scale, scale_ref.shape)
    normed_ref[...] = (current * scale * gain_ref[...]).astype(jnp.bfloat16)
    copies = gather_copies(normed_ref, all_ref, part // 2, sems)
    for copy in copies[:4]:
        copy.start()
    held_ref[0] = spots_ref[...]
    spot_copies = [
        remote(spots_ref, held_ref.at[step], (spot_send, spot_recv), step - 1, seq_peer(step))
        for step in range(1, count)
    ]
    for copy in spot_copies:
        copy.start()
    own = pltpu.make_async_copy(normed_ref, all_ref.at[0], local_sem.at[items])
    own.start()
    for distance in range(1, chips):
        for item_of, number in kinds:
            lax.fori_loop(0, number, pass_far(item_of, distance), 0)
            if distance == 1 and item_of is qkv_item:
                copies[0].wait_recv()
                copies[4].start()
                copies[1].wait_recv()
                copies[5].start()

    take.wait()
    put = pltpu.make_async_copy(part_ref, gate_up_part_ref, local_sem.at[items + 2])
    put.start()
    take_down.wait()
    columns_here = part_rows
    for device in range(count):

        @pl.when(index == device)
        def _():
            down_part_ref[...] = jnp.concatenate(
                [
                    held_down[:, start + device * columns_here : start + (device + 1) * columns_here]
                    for start in range(0, held_down.shape[1], count * columns_here)
                ],
                1,
            )

    for copy in spot_copies:
        copy.wait()
    half = HD // 2
    for step in range(count):
        spots = held_ref[step][:1]
        frequency = jnp.exp(
            lax.broadcasted_iota(jnp.int32, (half, 1), 0).astype(jnp.float32) * (-2.0 * math.log(10000.0) / HD)
        )
        angles = frequency * spots
        turned = jnp.concatenate([jnp.cos(angles), jnp.sin(angles)], 0)
        table_ref[pl.ds(step * part, part), :] = jnp.transpose(turned)

    def finish(item_of):
        def body(item, carry):
            owner, source, target, slot = item_of(item)

            @pl.when(core != owner % 2)
            def _():
                item_copy(target, target, slot, item_side, place ^ 1).wait_recv()

            @pl.when(place == owner)
            def _():
                pltpu.make_async_copy(source, target, local_sem.at[slot]).wait()

            @pl.when(core == owner % 2)
            def _():
                pass_on(target, target, slot, owner // 2, lambda copy: copy.wait_send())

            return carry

        return body

    for item_of, number in kinds:
        lax.fori_loop(0, number, finish(item_of), 0)
    own.wait()
    put.wait()
    for copy in copies[2:]:
        copy.wait_recv()
    for copy in copies:
        copy.wait_send()


def enter(current, gain, spots, shard, out_shard, gate_up, down, count):
    part, width = current.shape
    length = part * count
    heads = H // count
    pieces = heads + 2
    items = pieces + lax.axis_size("fsdp")
    vmem = pl.BlockSpec(memory_space=pltpu.VMEM)
    spots = jnp.broadcast_to(spots.astype(jnp.float32)[None], (8, part))
    whole = pl.BlockSpec(memory_space=pl.ANY)
    part_shape = (gate_up.shape[0] // count, width)
    gathered, rows, out_cols, table, gate_up_part, down_part, scale = pl.pallas_call(
        lambda *refs: enter_kernel(count, *refs),
        out_shape=(
            jax.ShapeDtypeStruct((count, part, width), jnp.bfloat16),
            jax.ShapeDtypeStruct((pieces * HD, width), jnp.bfloat16),
            jax.ShapeDtypeStruct((out_shard.shape[0] * (items - pieces), heads * HD), jnp.bfloat16),
            jax.ShapeDtypeStruct((length, HD), jnp.float32),
            jax.ShapeDtypeStruct(part_shape, gate_up.dtype),
            jax.ShapeDtypeStruct((down.shape[0], down.shape[1] // count), down.dtype),
            jax.ShapeDtypeStruct((part, 128), jnp.float32),
        ),
        in_specs=[vmem] * 5 + [whole] * 2,
        out_specs=[whole] + [vmem] * 3 + [whole] + [vmem] * 2,
        scratch_shapes=[
            pltpu.VMEM((part, width), jnp.bfloat16),
            pltpu.VMEM((count, 8, part), jnp.float32),
            pltpu.VMEM(part_shape, gate_up.dtype),
            pltpu.VMEM(down.shape, down.dtype),
            pltpu.SemaphoreType.DMA((6,)),
            pltpu.SemaphoreType.DMA((6,)),
            pltpu.SemaphoreType.DMA((count - 1,)),
            pltpu.SemaphoreType.DMA((count - 1,)),
            pltpu.SemaphoreType.DMA((items,)),
            pltpu.SemaphoreType.DMA((items,)),
            pltpu.SemaphoreType.DMA((items,)),
            pltpu.SemaphoreType.DMA((items,)),
            pltpu.SemaphoreType.DMA((items + 4,)),
        ],
        compiler_params=pltpu.CompilerParams(collective_id=1, has_side_effects=True, vmem_limit_bytes=LIMIT),
        name="enter",
    )(current, gain, spots, shard, out_shard, gate_up, down)
    return gathered.reshape(length, width), rows, out_cols, table, gate_up_part, down_part, scale


def qkv_kernel(index_ref, normed_ref, weight_ref, table_ref, q_ref, k_ref, v_ref):
    heads = q_ref.shape[0]
    joint = matmul(normed_ref[...], weight_ref[...], 1, 1)
    cosines, sines = spread_tables(table_ref[...], heads // 2, True)
    turned = joint * cosines + swap_halves(joint) * sines
    for head in range(heads):
        rounded = turned[:, head * HD : (head + 1) * HD].astype(jnp.bfloat16).astype(jnp.float32)
        q_ref[head] = (rounded * ROOT).astype(jnp.bfloat16)
    k_ref[...] = turned[:, heads * HD : (heads + 1) * HD].astype(jnp.bfloat16)
    v_ref[...] = turned[:, (heads + 1) * HD :].astype(jnp.bfloat16)


def project_qkv(index, normed, weight, table, count):
    length, width = normed.shape
    part = length // count
    heads = weight.shape[0] // HD - 2
    return pl.pallas_call(
        qkv_kernel,
        out_shape=(
            jax.ShapeDtypeStruct((heads, length, HD), jnp.bfloat16),
            jax.ShapeDtypeStruct((length, HD), jnp.bfloat16),
            jax.ShapeDtypeStruct((length, HD), jnp.bfloat16),
        ),
        grid_spec=pltpu.PrefetchScalarGridSpec(
            num_scalar_prefetch=1,
            grid=(count,),
            in_specs=[
                pl.BlockSpec((part, width), lambda i, s: (i, 0)),
                pl.BlockSpec(weight.shape, lambda i, s: (0, 0)),
                pl.BlockSpec((part, table.shape[1]), lambda i, s: (i, 0)),
            ],
            out_specs=[
                pl.BlockSpec((heads, part, HD), lambda i, s: (0, i ^ s[0], 0)),
                pl.BlockSpec((part, HD), lambda i, s: (i ^ s[0], 0)),
                pl.BlockSpec((part, HD), lambda i, s: (i ^ s[0], 0)),
            ],
        ),
        compiler_params=pltpu.CompilerParams(vmem_limit_bytes=LIMIT),
        name="project_qkv",
    )(index, normed, weight, table)


def attend_kernel(
    count, q_ref, k_ref, v_ref, weight_ref, current_ref, gain_ref,
    attn_ref, lse_ref, middle_ref, scale_ref, all_ref,
    held_ref, sent_ref, side_ref, below_ref, far_ref, two_ref, send_sems, recv_sems, own_sem,
):
    heads, _, _ = q_ref.shape
    part, _ = current_ref.shape
    half = part // 2
    index = lax.axis_index("seq")
    top, bottom = pl.ds(0, half), pl.ds(half, half)
    sems = (send_sems, recv_sems)
    greet([seq_peer(1), seq_peer(2)])
    sums = sum_copies(sent_ref, side_ref, below_ref, far_ref, half, sems)
    row = lax.broadcasted_iota(jnp.int32, (part, part), 0)
    column = lax.broadcasted_iota(jnp.int32, (part, part), 1)

    def one_part(turn, carry):
        step = count - 1 - turn
        here = step ^ index
        rows_here = pl.ds(pl.multiple_of(here * part, part), part)
        rows_step = pl.ds(pl.multiple_of(step * part, part), part)
        for block in range(count):

            @pl.when(here == block)
            def _():
                before = block * part
                seen = before + part
                keys_in, values_in = k_ref[:seen], v_ref[:seen]

                def one_head(head, carry):
                    scores = matmul(q_ref[head, before:seen, :], keys_in, 1, 1)
                    last = jnp.where(row >= column, scores[:, before:], -1e30)
                    scores = jnp.concatenate([scores[:, :before], last], 1) if block else last
                    peak = jnp.max(scores, 1, keepdims=True)
                    weights = jnp.exp(scores - peak)
                    total = jnp.sum(weights, 1, keepdims=True)
                    output = matmul(weights.astype(jnp.bfloat16), values_in, 1, 0) / total
                    held_ref[head] = output.astype(jnp.bfloat16)
                    log_total = jnp.broadcast_to(peak + jnp.log(total), (part, 128))
                    lse_ref[pl.ds(head, 1), before:seen] = jnp.transpose(log_total)[:1]
                    return carry

                lax.fori_loop(0, heads, one_head, 0, unroll=2)

        attn = jnp.concatenate([held_ref[head] for head in range(heads)], 1)
        attn_ref[rows_step, :] = attn
        partial = matmul(attn, weight_ref[...], 1, 1)

        pass_sums(turn, step, partial, sums, sent_ref, side_ref, below_ref, middle_ref, half)
        return carry

    lax.fori_loop(0, count, one_part, 0)
    end_sums(sums, side_ref, below_ref, far_ref, middle_ref, half)
    middle_ref[...] += current_ref[...]
    middle = middle_ref[...]
    scale = lax.rsqrt(jnp.mean(middle * middle, 1, keepdims=True) + EPS)
    scale_ref[...] = jnp.broadcast_to(scale, scale_ref.shape)
    two_ref[...] = (middle * scale * gain_ref[...]).astype(jnp.bfloat16)
    own = pltpu.make_async_copy(two_ref, all_ref.at[0], own_sem)
    share_own(two_ref, all_ref, half, sems, sums)
    own.start()
    own.wait()


def attend(queries, keys_in, values_in, weight, current, gain, count):
    heads, length, _ = queries.shape
    part, width = current.shape
    vmem = pl.BlockSpec(memory_space=pltpu.VMEM)
    attn, lse, middle, scale, gathered = pl.pallas_call(
        lambda *refs: attend_kernel(count, *refs),
        out_shape=(
            jax.ShapeDtypeStruct((length, heads * HD), jnp.bfloat16),
            jax.ShapeDtypeStruct((heads, length), jnp.float32),
            jax.ShapeDtypeStruct((part, width), jnp.float32),
            jax.ShapeDtypeStruct((part, 128), jnp.float32),
            jax.ShapeDtypeStruct((count, part, width), jnp.bfloat16),
        ),
        in_specs=[vmem] * 6,
        out_specs=[vmem] * 4 + [pl.BlockSpec(memory_space=pl.ANY)],
        scratch_shapes=[
            pltpu.VMEM((heads, part, HD), jnp.bfloat16),
            pltpu.VMEM((count, part, width), jnp.bfloat16),
            pltpu.VMEM((2, part // 2, width), jnp.bfloat16),
            pltpu.VMEM((2, part // 2, width), jnp.bfloat16),
            pltpu.VMEM((2, part // 2, width), jnp.bfloat16),
            pltpu.VMEM((part, width), jnp.bfloat16),
            pltpu.SemaphoreType.DMA((12,)),
            pltpu.SemaphoreType.DMA((12,)),
            pltpu.SemaphoreType.DMA,
        ],
        compiler_params=pltpu.CompilerParams(collective_id=2, has_side_effects=True, vmem_limit_bytes=LIMIT),
        name="attend",
    )(queries, keys_in, values_in, weight, current, gain)
    return attn, lse, middle, scale, gathered.reshape(length, width)


def share_start(copies):
    for group in copies:
        group[0].start()
        group[1].start()
    for group in copies:
        group[2].start()
        group[3].start()


def share_on(group):
    group[0].wait_recv()
    group[4].start()
    group[1].wait_recv()
    group[5].start()


def share_end(copies):
    for group in copies:
        for copy in group[2:]:
            copy.wait_recv()
    for group in copies:
        for copy in group:
            copy.wait_send()


def upper_half(rows):
    return -(-(rows // 2) // 16) * 16


def attend_back_kernel(
    count, q_ref, k_ref, v_ref, attn_ref, lse_ref, dy_ref, weight_ref, table_ref, pick_ref, passed_ref, shard_ref,
    out_ref, turned_ref, term_ref, far_ref, slot_ref,
    do_ref, delta_ref, dq_ref, dk_ref, dv_ref, held_dy, held_pick,
    send_sems, recv_sems, load_sems,
):
    heads, length, _ = q_ref.shape
    part = length // count
    wide = jnp.float32
    index = lax.axis_index("seq")
    greet([seq_peer(1), seq_peer(2)])
    sems = (send_sems, recv_sems)
    sums = [
        remote(passed_ref.at[0], far_ref.at[0], sems, 6, seq_peer(2)),
        remote(passed_ref.at[1], far_ref.at[1], sems, 7, seq_peer(1)),
    ]
    group = gather_copies(shard_ref, slot_ref, upper_half(shard_ref.shape[0]), sems)
    share_start([group])
    for copy in sums:
        copy.start()

    def load_dy(step):
        rows = pl.ds(pl.multiple_of(step * part, part), part)
        return pltpu.make_async_copy(dy_ref.at[rows], held_dy.at[rows], load_sems.at[step])

    load = pltpu.make_async_copy(pick_ref, held_pick, load_sems.at[count])
    for here in range(count):
        load_dy(here ^ index).start()
    load.start()
    dk_ref[...] = jnp.zeros_like(dk_ref)
    dv_ref[...] = jnp.zeros_like(dv_ref)
    owner = lax.broadcasted_iota(jnp.int32, (heads, heads * HD), 1) // HD
    same = (owner == lax.broadcasted_iota(jnp.int32, (heads, heads * HD), 0)).astype(wide)
    row = lax.broadcasted_iota(jnp.int32, (part, part), 0)
    column = lax.broadcasted_iota(jnp.int32, (part, part), 1)

    def unturn(grads, cosines, sines):
        return grads * cosines + swap_halves(grads * sines)

    def one_part(here, carry):
        spot = here ^ index
        rows_here = pl.ds(pl.multiple_of(spot * part, part), part)
        load_dy(spot).wait()
        dattn = matmul(held_dy[rows_here, :], weight_ref[...], 1, 0).astype(jnp.bfloat16)
        product = dattn.astype(wide) * attn_ref[rows_here, :].astype(wide)
        delta_ref[...] = lax.dot_general(
            same, product, (((1,), (1,)), ((), ())), precision=lax.Precision.HIGHEST, preferred_element_type=wide
        )
        for head in range(heads):
            do_ref[head] = dattn[:, head * HD : (head + 1) * HD]
        for block in range(count):

            @pl.when(here == block)
            def _():
                before = block * part
                seen = before + part
                keys_in, values_in = k_ref[:seen], v_ref[:seen]

                def one_head(head, carry):
                    query, dout = q_ref[head, before:seen, :], do_ref[head]
                    scores = matmul(keys_in, query, 1, 1)
                    last = jnp.where(row <= column, scores[before:], -1e30)
                    scores = jnp.concatenate([scores[:before], last], 0) if block else last
                    probs = jnp.exp(scores - lse_ref[pl.ds(head, 1), before:seen])
                    dprob = matmul(values_in, dout, 1, 1)
                    dscore = (probs * (dprob - delta_ref[pl.ds(head, 1), :])).astype(jnp.bfloat16)
                    dv_ref[:seen] += matmul(probs.astype(jnp.bfloat16), dout, 1, 0)
                    dk_ref[:seen] += matmul(dscore, query, 1, 0)
                    dq_ref[head] = (matmul(dscore, keys_in, 0, 0) * ROOT).astype(jnp.bfloat16)
                    return carry

                lax.fori_loop(0, heads, one_head, 0, unroll=2)

        dq = jnp.concatenate([dq_ref[head] for head in range(heads)], 1).astype(wide)
        dq = unturn(dq, *spread_tables(table_ref[rows_here, :], heads // 2, False))
        out_ref[rows_here, : heads * HD] = dq.astype(jnp.bfloat16)

        @pl.when(here == 1)
        def _():
            share_on(group)

        return carry

    lax.fori_loop(0, count, one_part, 0)
    for block in range(count):
        rows_there = pl.ds(pl.multiple_of((block ^ index) * part, part), part)
        rows_block = slice(block * part, (block + 1) * part)
        both = jnp.concatenate([dk_ref[rows_block], dv_ref[rows_block]], 1).astype(jnp.bfloat16).astype(wide)
        both = unturn(both, *spread_tables(table_ref[rows_there, :], 0, True))
        out_ref[rows_there, heads * HD :] = both.astype(jnp.bfloat16)
    load.wait()
    chosen = matmul(held_pick[...], out_ref[...], 1, 1).astype(jnp.bfloat16)
    size = turned_ref.shape[1]
    for block in range(count):
        turned_ref[block] = chosen[block * size : (block + 1) * size]
    tile = 2 * 128

    def one_tile(number, carry):
        columns = pl.ds(pl.multiple_of(number * tile, tile), tile)
        term_ref[columns, :] = matmul(held_dy[:, columns], attn_ref[...], 0, 0).astype(jnp.bfloat16)
        return carry

    lax.fori_loop(0, held_dy.shape[1] // tile, one_tile, 0)
    for copy in sums:
        copy.wait_recv()
    share_end([group])
    for copy in sums:
        copy.wait_send()


def attend_back(queries, keys_in, values_in, attn, lse, dy, weight, table, pick, passed, shard, count):
    heads, length, _ = queries.shape
    part, width = length // count, dy.shape[1]
    columns = (heads + 2) * HD
    vmem, whole = pl.BlockSpec(memory_space=pltpu.VMEM), pl.BlockSpec(memory_space=pl.ANY)
    return pl.pallas_call(
        lambda *refs: attend_back_kernel(count, *refs),
        out_shape=[
            jax.ShapeDtypeStruct((length, columns), jnp.bfloat16),
            jax.ShapeDtypeStruct((count, columns // count, length), jnp.bfloat16),
            jax.ShapeDtypeStruct((width, heads * HD), jnp.bfloat16),
            jax.ShapeDtypeStruct((2, part // 2, width), jnp.bfloat16),
            jax.ShapeDtypeStruct((count,) + shard.shape, shard.dtype),
        ],
        in_specs=[vmem] * 5 + [whole] + [vmem] * 2 + [whole] * 3,
        out_specs=[vmem] * 3 + [whole] * 2,
        scratch_shapes=[
            pltpu.VMEM((heads, part, HD), jnp.bfloat16),
            pltpu.VMEM((heads, part), jnp.float32),
            pltpu.VMEM((heads, part, HD), jnp.bfloat16),
            pltpu.VMEM((length, HD), jnp.float32),
            pltpu.VMEM((length, HD), jnp.float32),
        ]
        + [pltpu.VMEM(dy.shape, dy.dtype), pltpu.VMEM(pick.shape, pick.dtype)]
        + [pltpu.SemaphoreType.DMA((8,)), pltpu.SemaphoreType.DMA((8,)), pltpu.SemaphoreType.DMA((count + 1,))],
        compiler_params=pltpu.CompilerParams(collective_id=4, has_side_effects=True, vmem_limit_bytes=LIMIT),
        name="attend_back",
    )(queries, keys_in, values_in, attn, lse, dy, weight, table, pick, passed, shard)


def leave_kernel(
    count, grads_ref, weight_ref, first_in, scale_ref, gain_ref, other_ref, turned_ref, normed_in,
    own_ref, total_ref, term_ref,
    sent_ref, side_ref, below_ref, far_ref, slot_ref, whole_ref, normed_ref, first_ref,
    told_ref, heard_ref, send_sems, recv_sems, swap_send, swap_recv, load_sems, sum_send, sum_recv,
):
    part, _ = first_ref.shape
    half = part // 2
    size = turned_ref.shape[1]
    heads = H // count
    chunk = size // (heads + 2)
    index = lax.axis_index("seq")
    place = lax.axis_index("fsdp")
    peers = [seq_peer(step) for step in range(1, count)]
    fsdp_peers = [fsdp_peer(place ^ (1 << bit)) for bit in range(lax.axis_size("fsdp").bit_length() - 1)]
    greet(peers + fsdp_peers)
    swaps = [
        remote(turned_ref.at[index ^ step], slot_ref.at[step], (swap_send, swap_recv), step - 1, seq_peer(step))
        for step in range(1, count)
    ]
    for copy in swaps:
        copy.start()
    loads = [
        pltpu.make_async_copy(source, target, load_sems.at[number])
        for number, (source, target) in enumerate(
            (
                (turned_ref.at[index], slot_ref.at[0]),
                (normed_in, normed_ref),
                (first_in, first_ref),
            )
        )
    ]
    for load in loads:
        load.start()
    total_ref[0:1] = jnp.zeros_like(other_ref)
    total_ref[1:2] = other_ref[...]
    loads[1].wait()
    sums = sum_copies(sent_ref, side_ref, below_ref, far_ref, half, (send_sems, recv_sems))

    def one_part(turn, carry):
        step = count - 1 - turn
        rows_step = pl.ds(pl.multiple_of(step * part, part), part)
        partial = matmul(grads_ref[rows_step, :], weight_ref[...], 1, 0)
        total_ref[0:1] += jnp.sum(partial * normed_ref[rows_step, :].astype(jnp.float32), 0, keepdims=True)
        pass_sums(turn, step, partial, sums, sent_ref, side_ref, below_ref, own_ref, half)
        return carry

    lax.fori_loop(0, count, one_part, 0)
    loads[0].wait()
    loads[2].wait()
    total_ref[0:1] = total_ref[0:1] / gain_ref[...]
    tells = []
    for step, peer in enumerate(fsdp_peers):
        told_ref[step] = total_ref[...]
        tell = remote(told_ref.at[step], heard_ref.at[step], (sum_send, sum_recv), step, peer)
        tell.start()
        tell.wait_recv()
        total_ref[...] += heard_ref[step]
        tells.append(tell)
    first = len(tells)
    told_ref[first] = total_ref[...]
    for step, peer in enumerate(peers):
        tells.append(
            remote(told_ref.at[first], heard_ref.at[first + step], (sum_send, sum_recv), first + step, peer)
        )
        tells[-1].start()
    for step in range(count):
        if step:
            swaps[step - 1].wait_recv()
        peer = index ^ step
        for block in range(count):
            piece = slot_ref[step, :, (step ^ block) * part : ((step ^ block) + 1) * part]
            tokens = slice(block * part, (block + 1) * part)
            for start, rows in ((0, heads * chunk), (H * chunk, chunk), ((H + KVH) * chunk, chunk)):
                begin = 0 if start == 0 else heads * chunk + (0 if start == H * chunk else chunk)
                spot = pl.multiple_of(start + peer * rows, chunk)
                whole_ref[pl.ds(spot, rows), tokens] = piece[begin : begin + rows]
    term_ref[...] = matmul(whole_ref[...], normed_ref[...], 1, 0).astype(jnp.bfloat16)
    end_sums(sums, side_ref, below_ref, far_ref, own_ref, half)
    unit = first_ref[...] * scale_ref[:, :1]
    grads = own_ref[...]
    inner = grads * gain_ref[...]
    own_ref[...] = scale_ref[:, :1] * (inner - unit * jnp.mean(inner * unit, 1, keepdims=True))
    for step in range(len(peers)):
        tells[first + step].wait_recv()
        total_ref[...] += heard_ref[first + step]
    for copy in sums + swaps + tells:
        copy.wait_send()


def leave(grads, weight, first, scale, gain, other, turned, normed, count):
    part, width = first.shape
    vmem, whole = pl.BlockSpec(memory_space=pltpu.VMEM), pl.BlockSpec(memory_space=pl.ANY)
    size, length = turned.shape[1:]
    steps = lax.axis_size("fsdp").bit_length() - 1 + count - 1
    own, total, term = pl.pallas_call(
        lambda *refs: leave_kernel(count, *refs),
        out_shape=(
            jax.ShapeDtypeStruct((part, width), jnp.float32),
            jax.ShapeDtypeStruct((2, width), jnp.float32),
            jax.ShapeDtypeStruct((size * count, width), jnp.bfloat16),
        ),
        in_specs=[vmem] * 2 + [whole] + [vmem] * 3 + [whole] * 2,
        out_specs=[vmem] * 3,
        scratch_shapes=[
            pltpu.VMEM((count, part, width), jnp.bfloat16),
            pltpu.VMEM((2, part // 2, width), jnp.bfloat16),
            pltpu.VMEM((2, part // 2, width), jnp.bfloat16),
            pltpu.VMEM((2, part // 2, width), jnp.bfloat16),
            pltpu.VMEM((count, size, length), jnp.bfloat16),
            pltpu.VMEM((count * size, length), jnp.bfloat16),
            pltpu.VMEM(normed.shape, jnp.bfloat16),
            pltpu.VMEM((part, width), jnp.float32),
            pltpu.VMEM((steps, 2, width), jnp.float32),
            pltpu.VMEM((steps, 2, width), jnp.float32),
            pltpu.SemaphoreType.DMA((6,)),
            pltpu.SemaphoreType.DMA((6,)),
            pltpu.SemaphoreType.DMA((count - 1,)),
            pltpu.SemaphoreType.DMA((count - 1,)),
            pltpu.SemaphoreType.DMA((3,)),
            pltpu.SemaphoreType.DMA((steps,)),
            pltpu.SemaphoreType.DMA((steps,)),
        ],
        compiler_params=pltpu.CompilerParams(collective_id=5, has_side_effects=True, vmem_limit_bytes=LIMIT),
        name="leave",
    )(grads, weight, first, scale, gain, other, turned, normed)
    return own, total, term


def join_rows_kernel(index_ref, own_ref, side_ref, below_ref, top_ref, bottom_ref, out_ref):
    step = pl.program_id(0) ^ index_ref[0]
    half = top_ref.shape[0]
    for number, ref in enumerate((own_ref, side_ref, below_ref)):

        @pl.when(step == number)
        def _():
            out_ref[...] = ref[...].astype(jnp.float32)

    @pl.when(step == 3)
    def _():
        out_ref[:half] = top_ref[...].astype(jnp.float32)
        out_ref[half:] = bottom_ref[...].astype(jnp.float32)


def join_rows(index, own, side, below, top, bottom, count):
    rows, width = own.shape
    parts = (own, side, below, top, bottom)
    return pl.pallas_call(
        join_rows_kernel,
        out_shape=jax.ShapeDtypeStruct((rows * count, width), jnp.float32),
        grid_spec=pltpu.PrefetchScalarGridSpec(
            num_scalar_prefetch=1,
            grid=(count,),
            in_specs=[pl.BlockSpec(part.shape, lambda i, s: (0, 0)) for part in parts],
            out_specs=pl.BlockSpec((rows, width), lambda i, s: (i, 0)),
        ),
        compiler_params=pltpu.CompilerParams(vmem_limit_bytes=LIMIT),
        name="join_rows",
    )(index, *parts)


def join_pieces_kernel(count, row_piece, column_piece, index_ref, own_ref, *refs):
    slot_refs, out_ref = refs[:-1], refs[-1]
    index = index_ref[0]
    rows, columns = own_ref.shape
    for device in range(count):
        if len(slot_refs) == 1:
            values = slot_refs[0][device ^ index]
        else:
            values = own_ref[...]
            for step, ref in enumerate(slot_refs):
                values = jnp.where(device ^ index == step + 1, ref[...], values)
        values = jnp.where(device == index, own_ref[...], values).astype(jnp.float32)
        for top in range(0, rows, row_piece):
            for left in range(0, columns, column_piece):
                down = top * count + device * row_piece if row_piece < rows else top
                across = left * count + device * column_piece if row_piece == rows else left
                out_ref[down : down + row_piece, across : across + column_piece] = values[
                    top : top + row_piece, left : left + column_piece
                ]


def join_pieces(index, own, slots, count, row_piece, column_piece):
    rows, columns = own.shape
    shape = (rows * count, columns) if row_piece < rows else (rows, columns * count)
    return pl.pallas_call(
        lambda *refs: join_pieces_kernel(count, row_piece, column_piece, *refs),
        out_shape=jax.ShapeDtypeStruct(shape, jnp.float32),
        grid_spec=pltpu.PrefetchScalarGridSpec(
            num_scalar_prefetch=1,
            grid=(1,),
            in_specs=[pl.BlockSpec(own.shape, lambda i, s: (0, 0))]
            + [pl.BlockSpec(slot.shape, lambda i, s, n=slot.ndim: (0,) * n) for slot in slots],
            out_specs=pl.BlockSpec(shape, lambda i, s: (0, 0)),
        ),
        compiler_params=pltpu.CompilerParams(vmem_limit_bytes=LIMIT),
        name="join_pieces",
    )(index, own, *slots)


def last_sums_kernel(base_ref, passed_ref, flowing_ref, piece_ref, result_ref, grad_ref):
    result_ref[...] = base_ref[...] + passed_ref[...].astype(jnp.float32)
    grad_ref[...] = flowing_ref[...] + piece_ref[...]


def last_sums(base, passed, flowing, piece):
    rows, width = base.shape
    tile = rows // 4
    block = pl.BlockSpec((tile, width), lambda i: (i, 0))
    return pl.pallas_call(
        last_sums_kernel,
        out_shape=[jax.ShapeDtypeStruct((rows, width), jnp.float32)] * 2,
        grid=(4,),
        in_specs=[block] * 4,
        out_specs=[block] * 2,
        compiler_params=pltpu.CompilerParams(vmem_limit_bytes=LIMIT),
        name="last_sums",
    )(base, passed, flowing, piece)


def norm_back_kernel(
    count, act_in, down_in, dm_in, gates_in, weight_in, flowing_in, middle_in, inputs_in, scale_ref, gain_ref,
    own_ref, gain_out_ref, dy_ref, term_ref, product_ref, from_side_ref, from_below_ref,
    act_ref, down_ref, dm_ref, gates_ref, grads_ref, weight_ref, flowing_ref, middle_ref, inputs_ref,
    held_ref, sent_ref, side_ref, below_ref, far_ref, stage_ref,
    send_sems, recv_sems, load_sems, part_sems, store_sems, product_sems,
):
    part, _ = flowing_in.shape
    half = part // 2
    wide, narrow = jnp.float32, jnp.bfloat16
    units = down_ref.shape[1]
    sems = (send_sems, recv_sems)

    def load(source, target, number):
        copy = pltpu.make_async_copy(source, target, load_sems.at[number])
        copy.start()
        return copy

    def load_parts(turn):
        rows = pl.ds(pl.multiple_of((count - 1 - turn) * part, part), part)
        slot = turn % 2
        return [
            pltpu.make_async_copy(dm_in.at[rows], dm_ref.at[slot], part_sems.at[0, slot]),
            pltpu.make_async_copy(gates_in.at[rows], gates_ref.at[slot], part_sems.at[1, slot]),
        ]

    firsts = [load(act_in, act_ref, 0), load(down_in, down_ref, 1)]
    for copy in load_parts(0):
        copy.start()
    load_weight = load(weight_in, weight_ref, 2)
    for copy in load_parts(1):
        copy.start()
    lasts = [load(inputs_in, inputs_ref, 3), load(flowing_in, flowing_ref, 4), load(middle_in, middle_ref, 5)]
    greet([seq_peer(1), seq_peer(2)])
    top, bottom = pl.ds(0, half), pl.ds(half, half)
    firsts_sums = [
        remote(held_ref.at[3].at[top], from_side_ref.at[1], sems, 6, seq_peer(1)),
        remote(held_ref.at[3].at[bottom], from_below_ref.at[1], sems, 7, seq_peer(2)),
        remote(held_ref.at[2].at[bottom], from_below_ref.at[0], sems, 8, seq_peer(2)),
        remote(held_ref.at[1].at[top], from_side_ref.at[0], sems, 9, seq_peer(1)),
    ]
    sums = sum_copies(sent_ref, side_ref, below_ref, far_ref, half, sems)
    for copy in firsts:
        copy.wait()

    def down_part(turn, carry):
        step = count - 1 - turn
        rows = pl.ds(pl.multiple_of(step * part, part), part)
        held_ref[step] = matmul(act_ref[rows, :], down_ref[...], 1, 1).astype(narrow)

        @pl.when(turn == 0)
        def _():
            firsts_sums[0].start()
            firsts_sums[1].start()

        @pl.when(turn == 1)
        def _():
            firsts_sums[2].start()

        @pl.when(turn == 2)
        def _():
            firsts_sums[3].start()

        return carry

    lax.fori_loop(0, count, down_part, 0)
    product = pltpu.make_async_copy(held_ref, product_ref, product_sems.at[0])
    product.start()
    load_weight.wait()

    def one_part(turn, carry):
        step = count - 1 - turn
        slot = turn % 2
        rows = pl.ds(pl.multiple_of(step * part, part), part)
        for copy in load_parts(turn):
            copy.wait()
        dact = matmul(dm_ref[slot], down_ref[...], 1, 0)
        gate = gates_ref[slot, :, :units].astype(wide)
        up = gates_ref[slot, :, units:].astype(wide)
        sigma = jax.nn.sigmoid(gate)
        grads_ref[rows, :units] = (dact * up * sigma * (1.0 + gate * (1.0 - sigma))).astype(narrow)
        grads_ref[rows, units:] = (dact * gate * sigma).astype(narrow)

        @pl.when(turn < count - 2)
        def _():
            for copy in load_parts(turn + 2):
                copy.start()

        partial = matmul(grads_ref[rows, :], weight_ref[...], 1, 0)

        @pl.when(turn == count - 1)
        def _():
            own_ref[...] = partial

        @pl.when(turn < count - 1)
        def _():
            sent_ref[step] = partial.astype(narrow)

        @pl.when(turn == 0)
        def _():
            sums[0].start()
            sums[1].start()

        @pl.when(turn == 1)
        def _():
            sums[2].start()

        @pl.when(turn == 2)
        def _():
            sums[3].start()

        return carry

    lax.fori_loop(0, count, one_part, 0)
    sums[0].wait_recv()
    sent_ref[2, :half] = (sent_ref[2, :half].astype(wide) + side_ref[1].astype(wide)).astype(narrow)
    sums[4].start()
    sums[1].wait_recv()
    sent_ref[1, half:] = (sent_ref[1, half:].astype(wide) + below_ref[1].astype(wide)).astype(narrow)
    sums[5].start()
    for copy in lasts:
        copy.wait()
    tile = stage_ref.shape[1]
    tiles = grads_ref.shape[1] // tile

    def store(number):
        rows = pl.ds(pl.multiple_of(number * tile, tile), tile)
        return pltpu.make_async_copy(stage_ref.at[number % 2], term_ref.at[rows], store_sems.at[number % 2])

    def one_tile(number, carry):
        @pl.when(number >= 2)
        def _():
            store(number - 2).wait()

        columns = pl.ds(pl.multiple_of(number * tile, tile), tile)
        stage_ref[number % 2] = matmul(grads_ref[:, columns], inputs_ref[...], 0, 0).astype(narrow)
        store(number).start()
        return carry

    lax.fori_loop(0, tiles, one_tile, 0)
    end_sums(sums, side_ref, below_ref, far_ref, own_ref, half)
    scale = scale_ref[:, :1]
    unit = middle_ref[...] * scale
    grads = own_ref[...]
    gain_out_ref[...] = jnp.sum(grads * unit, 0, keepdims=True)
    inner = grads * gain_ref[...]
    own_ref[...] = flowing_ref[...] + scale * (inner - unit * jnp.mean(inner * unit, 1, keepdims=True))
    dy_ref[...] = own_ref[...].astype(narrow)
    for number in range(tiles - 2, tiles):
        store(number).wait()
    product.wait()
    for copy in firsts_sums:
        copy.wait_recv()
    for copy in sums + firsts_sums:
        copy.wait_send()


def norm_back(act, down, dm, gates, weight, flowing, middle, inputs, scale, gain, count):
    part, width = flowing.shape
    units = gates.shape[1]
    tile = 2 * 128
    vmem, whole = pl.BlockSpec(memory_space=pltpu.VMEM), pl.BlockSpec(memory_space=pl.ANY)
    narrow, wide = jnp.bfloat16, jnp.float32
    pair = (2, part // 2, width)
    own, gain_term, dy, term, product, from_side, from_below = pl.pallas_call(
        lambda *refs: norm_back_kernel(count, *refs),
        out_shape=(
            jax.ShapeDtypeStruct((part, width), wide),
            jax.ShapeDtypeStruct((1, width), wide),
            jax.ShapeDtypeStruct((part, width), narrow),
            jax.ShapeDtypeStruct((units, width), narrow),
            jax.ShapeDtypeStruct((count, part, width), narrow),
            jax.ShapeDtypeStruct(pair, narrow),
            jax.ShapeDtypeStruct(pair, narrow),
        ),
        in_specs=[whole] * 8 + [vmem] * 2,
        out_specs=[vmem] * 3 + [whole] * 4,
        scratch_shapes=[
            pltpu.VMEM(act.shape, narrow),
            pltpu.VMEM(down.shape, narrow),
            pltpu.VMEM((2, part, width), narrow),
            pltpu.VMEM((2, part, units), narrow),
            pltpu.VMEM((part * count, units), narrow),
            pltpu.VMEM(weight.shape, narrow),
            pltpu.VMEM((part, width), wide),
            pltpu.VMEM((part, width), wide),
            pltpu.VMEM(inputs.shape, narrow),
            pltpu.VMEM((count, part, width), narrow),
            pltpu.VMEM((count, part, width), narrow),
            pltpu.VMEM(pair, narrow),
            pltpu.VMEM(pair, narrow),
            pltpu.VMEM(pair, narrow),
            pltpu.VMEM((2, tile, width), narrow),
            pltpu.SemaphoreType.DMA((10,)),
            pltpu.SemaphoreType.DMA((10,)),
            pltpu.SemaphoreType.DMA((6,)),
            pltpu.SemaphoreType.DMA((2, 2)),
            pltpu.SemaphoreType.DMA((2,)),
            pltpu.SemaphoreType.DMA((1,)),
        ],
        compiler_params=pltpu.CompilerParams(collective_id=3, has_side_effects=True, vmem_limit_bytes=67043328),
        name="norm_back",
    )(act, down, dm, gates, weight, flowing, middle, inputs, scale, gain)
    return own, gain_term[0], dy, term, product, from_side, from_below


def share_dy_kernel(
    dy_ref, down_ref, side_ref, below_ref, middle_ref, all_ref, base_ref, passed_ref,
    piece_ref, send_sems, recv_sems, load_sems,
):
    part = dy_ref.shape[0]
    half = part // 2
    wide = jnp.float32
    top, bottom = pl.ds(0, half), pl.ds(half, half)
    loads = [
        pltpu.make_async_copy(down_ref.at[0], piece_ref.at[0], load_sems.at[0]),
        pltpu.make_async_copy(down_ref.at[2].at[top], piece_ref.at[1].at[top], load_sems.at[1]),
        pltpu.make_async_copy(down_ref.at[1].at[bottom], piece_ref.at[1].at[bottom], load_sems.at[2]),
        pltpu.make_async_copy(dy_ref, all_ref.at[0], load_sems.at[3]),
    ]
    greet([seq_peer(1), seq_peer(2)])
    group = gather_copies(dy_ref, all_ref, half, (send_sems, recv_sems))
    share_start([group])
    for load in loads:
        load.start()
    for load in loads:
        load.wait()
    base_ref[...] = middle_ref[...] + piece_ref[0].astype(wide)
    base_ref[:half] += side_ref[0].astype(wide)
    base_ref[half:] += below_ref[0].astype(wide)
    passed_ref[0] = (piece_ref[1, :half].astype(wide) + side_ref[1].astype(wide)).astype(jnp.bfloat16)
    passed_ref[1] = (piece_ref[1, half:].astype(wide) + below_ref[1].astype(wide)).astype(jnp.bfloat16)
    share_on(group)
    share_end([group])


def share_dy(dy, down, side, below, middle, count):
    part, width = dy.shape
    vmem, whole = pl.BlockSpec(memory_space=pltpu.VMEM), pl.BlockSpec(memory_space=pl.ANY)
    gathered, base, passed = pl.pallas_call(
        lambda *refs: share_dy_kernel(*refs),
        out_shape=[
            jax.ShapeDtypeStruct((count, part, width), jnp.bfloat16),
            jax.ShapeDtypeStruct((part, width), jnp.float32),
            jax.ShapeDtypeStruct((2, part // 2, width), jnp.bfloat16),
        ],
        in_specs=[vmem, whole, vmem, vmem, vmem],
        out_specs=[whole, vmem, vmem],
        scratch_shapes=[
            pltpu.VMEM((2, part, width), jnp.bfloat16),
            pltpu.SemaphoreType.DMA((6,)),
            pltpu.SemaphoreType.DMA((6,)),
            pltpu.SemaphoreType.DMA((4,)),
        ],
        compiler_params=pltpu.CompilerParams(collective_id=8, has_side_effects=True, vmem_limit_bytes=LIMIT),
        name="share_dy",
    )(dy, down, side, below, middle)
    return gathered.reshape(part * count, width), base, passed


def fast_body(hidden, positions, gains, w_qkv, w_out, w_gate_up, w_down, cotangent):
    count = lax.axis_size("seq")
    index = lax.axis_index("seq")
    place = index.astype(jnp.int32).reshape(1)
    current = hidden[0]
    part_len, width = current.shape
    heads = H // count
    gain = gains[0]
    after = lax.optimization_barrier

    rows = w_qkv.shape[1]
    group = math.gcd(rows, HD)
    chunk = group // count
    per_head = HD // group
    normed_all, qkv_rows, out_cols, table, gate_up_part, down_part, scale_one = enter(
        current, gain[:1], positions[0], w_qkv[0], w_out[0], w_gate_up[0], w_down[0], count
    )
    gu_rows = w_gate_up.shape[1] // count
    gate_up = lax.all_gather(gate_up_part, "fsdp", axis=0, tiled=True)
    units = FF // count
    down_rows = w_down.shape[1]

    queries, keys_in, values_in = project_qkv(place, normed_all, qkv_rows, table, count)
    attn_flat, log_total, middle, scale_two, normed_two_all = attend(
        queries, keys_in, values_in, out_cols, current, gain[1:], count
    )
    flowing = cotangent[0]
    normed_two_all, dm_sent, down_part = after((normed_two_all, flowing.astype(jnp.bfloat16), down_part))
    down_cols = lax.all_gather(down_part, "fsdp", axis=0, tiled=True)
    dm_all = jnp.concatenate([dm_sent] + [neighbour(dm_sent, step) for step in range(1, count)], 0)
    both = matmul(normed_two_all, gate_up, 1, 1)
    gates = both.astype(jnp.bfloat16)
    activated = (jax.nn.silu(both[:, :units]) * both[:, units:]).astype(jnp.bfloat16)

    def owned(grad):
        return lax.psum_scatter(grad.astype(jnp.bfloat16), "fsdp", scatter_dimension=0, tiled=True)

    term_down = matmul(dm_all, activated, 0, 0).astype(jnp.bfloat16)
    dm_all, activated, term_down = after((dm_all, activated, term_down))
    grad_down = owned(term_down)
    dmiddle, gain_two, dy, term_gate_up, down_sent, from_side, from_below = norm_back(
        activated, down_cols, dm_all, gates, gate_up, flowing, middle, normed_two_all, scale_two, gain[1:], count
    )
    grad_gate_up = owned(term_gate_up)
    dy_all, base, passed = share_dy(dy, down_sent, from_side, from_below, middle, count)
    pieces = heads + 2
    picked = np.arange(pieces * HD).reshape(pieces * per_head, count, chunk).transpose(1, 0, 2).reshape(-1)
    pick = jnp.asarray(picked[:, None] == np.arange(pieces * HD)[None, :], jnp.bfloat16)
    djoint, djoint_turned, term_out, passed_on, down_slots = attend_back(
        queries, keys_in, values_in, attn_flat, log_total, dy_all, out_cols, table, pick, passed, grad_down, count
    )
    grad_out = owned(term_out)
    grad_piece, gain_total, term_qkv = leave(
        djoint, qkv_rows, current, scale_one, gain[:1], gain_two[None], djoint_turned, normed_all, count
    )
    grad_qkv = owned(term_qkv)
    grad_gate_up, grad_piece = after((grad_gate_up, grad_piece))
    half = upper_half(gu_rows)
    side = neighbour(grad_gate_up, 1)
    below = neighbour(grad_gate_up, 2)
    far_top = neighbour(side[:half], 2)
    far_bottom = neighbour(below[half:], 1)
    down_shard = join_pieces(place, grad_down, (down_slots,), count, down_rows, gu_rows)
    result, grad_hidden = last_sums(base, passed_on.reshape(part_len, width), dmiddle, grad_piece)
    out_slots = [neighbour(grad_out, step) for step in range(1, count)]
    grad_qkv, out_slots = after((grad_qkv, out_slots))
    qkv_slots = [neighbour(grad_qkv, step) for step in range(1, count)]
    gate_up_shard = join_rows(place, grad_gate_up, side, below, far_top, far_bottom, count)
    out_shard = join_pieces(place, grad_out, out_slots, count, down_rows, heads * HD)
    qkv_shard = join_pieces(place, grad_qkv, qkv_slots, count, chunk, width)
    gain_total = gain_total[None]
    return (
        result[None],
        grad_hidden[None],
        gain_total,
        qkv_shard[None],
        out_shard[None],
        gate_up_shard[None],
        down_shard[None],
    )


def fits(mesh):
    count, fsdp = mesh.shape["seq"], mesh.shape["fsdp"]
    rows = (H + 2 * KVH) * HD // fsdp
    return count == KVH == 4 and fsdp % 2 == 0 and fsdp & (fsdp - 1) == 0 and rows % HD == 0


def solution(mesh):
    placed = (
        P("fsdp", "seq", None),
        P("fsdp", "seq"),
        P(),
        P(None, "fsdp", None),
        P(None, "fsdp", None),
        P(None, "fsdp", None),
        P(None, "fsdp", None),
        P("fsdp", "seq", None),
    )
    fast = fits(mesh)
    return jax.shard_map(
        fast_body if fast else body,
        mesh=mesh,
        in_specs=placed,
        out_specs=(
            P("fsdp", "seq", None),
            P("fsdp", "seq", None),
            P(),
            P(None, "fsdp", None),
            P(None, "fsdp", None),
            P(None, "fsdp", None),
            P(None, "fsdp", None),
        ),
        check_vma=False,
    )
```

```python
import math

import jax
import jax.numpy as jnp
import numpy as np
from jax import lax
from jax.experimental import pallas as pl
from jax.experimental.pallas import tpu as pltpu
from jax.sharding import PartitionSpec as P


H = 32
KVH = 4
HD = 64
FF = 5632
LAYERS = 1


EPS = 1e-05


def rope_tables(position_ids):
    halfway = HD // 2
    frequency = jnp.exp(jnp.arange(halfway, dtype=jnp.float32) * (-2.0 * math.log(10000.0) / HD))
    angles = position_ids.astype(jnp.float32)[..., None] * frequency
    cosines = jnp.cos(angles)
    sines = jnp.sin(angles)
    return (
        jnp.concatenate([cosines, cosines], -1)[..., None, :],
        jnp.concatenate([sines, sines], -1)[..., None, :],
    )


def rotate(values, cosines, sines):
    halfway = values.shape[-1] // 2
    turned = jnp.concatenate([-values[..., halfway:], values[..., :halfway]], -1)
    return values * cosines + turned * sines


def unrotate(grads, cosines, sines):
    halfway = grads.shape[-1] // 2
    scaled = grads * sines
    return grads * cosines + jnp.concatenate([scaled[..., halfway:], -scaled[..., :halfway]], -1)


def normalize(values, gain):
    scale = lax.rsqrt(jnp.mean(values * values, -1, keepdims=True) + EPS)
    return ((values * scale * gain).astype(jnp.bfloat16), scale)


def normalize_back(grads, values, scale, gain):
    unit = values * scale
    gain_grad = jnp.sum((grads * unit).reshape(-1, unit.shape[-1]), 0)
    inner = grads * gain
    return (scale * (inner - unit * jnp.mean(inner * unit, -1, keepdims=True)), gain_grad)


def masked_scores(queries, keys_wide):
    scores = jnp.einsum(
        "qhd,khd->hqk", queries, keys_wide, preferred_element_type=jnp.float32
    ) * queries.shape[-1] ** (-0.5)
    length = queries.shape[0]
    causal = jnp.arange(length)[:, None] >= jnp.arange(length)[None, :]
    return jnp.where(causal[None], scores, -1e30)


def local_attend(operands):
    queries, keys_in, values_in = operands
    repeat_by = queries.shape[1] // keys_in.shape[1]
    keys_wide = jnp.repeat(keys_in, repeat_by, axis=1)
    values_wide = jnp.repeat(values_in, repeat_by, axis=1)
    scores = masked_scores(queries, keys_wide)
    peak = jnp.max(scores, -1, keepdims=True)
    log_total = peak[..., 0] + jnp.log(jnp.sum(jnp.exp(scores - peak), -1))
    weights = jnp.exp(scores - log_total[..., None]).astype(jnp.bfloat16)
    output = jnp.einsum("hqk,khd->qhd", weights, values_wide, preferred_element_type=jnp.float32)
    return (output.astype(jnp.bfloat16), log_total)


def local_attend_back(operands):
    queries, keys_in, values_in, output, log_total, dattn = operands
    length, kv_dev, head_dim = keys_in.shape
    repeat_by = queries.shape[1] // kv_dev
    keys_wide = jnp.repeat(keys_in, repeat_by, axis=1)
    values_wide = jnp.repeat(values_in, repeat_by, axis=1)
    scores = masked_scores(queries, keys_wide)
    probs = jnp.exp(scores - log_total[..., None])
    delta = jnp.sum(output.astype(jnp.float32) * dattn.astype(jnp.float32), -1).T
    dprob = jnp.einsum("qhd,khd->hqk", dattn, values_wide, preferred_element_type=jnp.float32)
    dscore = (probs * (dprob - delta[..., None])).astype(jnp.bfloat16)
    dqueries = jnp.einsum(
        "hqk,khd->qhd", dscore, keys_wide, preferred_element_type=jnp.float32
    ) * head_dim ** (-0.5)
    dkeys = jnp.einsum(
        "hqk,qhd->khd", dscore, queries, preferred_element_type=jnp.float32
    ) * head_dim ** (-0.5)
    dvalues = jnp.einsum(
        "hqk,qhd->khd", probs.astype(jnp.bfloat16), dattn, preferred_element_type=jnp.float32
    )

    def fold_heads(per_head):
        return jnp.sum(per_head.reshape(length, kv_dev, repeat_by, head_dim), 2).astype(
            jnp.bfloat16
        )

    return (dqueries.astype(jnp.bfloat16), fold_heads(dkeys), fold_heads(dvalues))


def project(inputs, weight):
    return lax.dot_general(
        inputs,
        lax.all_gather(weight, "fsdp", axis=0, tiled=True),
        (((1,), (1,)), ((), ())),
        preferred_element_type=jnp.float32,
    )


def project_back(grads, weight):
    shard_rows = lax.all_gather(weight, "fsdp", axis=0, tiled=True)
    picked = lax.slice_in_dim(grads, 0, shard_rows.shape[0], axis=1)
    return jnp.dot(picked, shard_rows, preferred_element_type=jnp.float32)


def weight_grad(grads, inputs, shard_size):
    picked = lax.slice_in_dim(grads, 0, shard_size * lax.axis_size("fsdp"), axis=1)
    summed = lax.psum_scatter(
        lax.dot_general(
            picked, inputs, (((0,), (0,)), ((), ())), preferred_element_type=jnp.float32
        ).astype(jnp.bfloat16),
        "fsdp",
        scatter_dimension=0,
        tiled=True,
    )
    return lax.psum(summed, "seq").astype(jnp.float32)


def backward_pair(grads, inputs, weight):
    wgrad = weight_grad(grads, inputs, weight.shape[0])
    return (project_back(grads, weight), wgrad)


def body(hidden, positions, gains, w_qkv, w_out, w_gate_up, w_down, cotangent):
    seq_count, part_len, model_width = hidden.shape
    row_count = seq_count * part_len
    group_count = lax.axis_size("seq")
    full_len = part_len * group_count
    heads_dev = H // group_count
    share = H // KVH
    kv_dev = max(1, heads_dev // share)
    first_kv = np.arange(group_count) * heads_dev // share
    slot_table = np.concatenate(
        [
            first_kv[:, None] + np.arange(kv_dev)[None, :],
            KVH + first_kv[:, None] + np.arange(kv_dev)[None, :],
        ],
        1,
    ).reshape(-1)
    slot_onehot = jnp.asarray(
        (slot_table[:, None] == np.arange(2 * KVH)[None, :]).astype(np.float32), jnp.bfloat16
    )
    cosines, sines = rope_tables(positions)
    layer_index = 0
    gain = gains[layer_index]
    normed, scale_one = normalize(hidden, gain[0])
    normed_flat = normed.reshape(row_count, model_width)
    joint = project(normed_flat, w_qkv[layer_index]).reshape(seq_count, part_len, -1)
    queries = joint[..., : H * HD].reshape(seq_count, part_len, H, HD)
    keys_in = joint[..., H * HD : (H + KVH) * HD].reshape(seq_count, part_len, KVH, HD)
    values_in = joint[..., (H + KVH) * HD :].reshape(seq_count, part_len, KVH, HD)
    q_rot = rotate(queries, cosines, sines).astype(jnp.bfloat16)
    kv_all = jnp.concatenate(
        [rotate(keys_in, cosines, sines).astype(jnp.bfloat16), values_in.astype(jnp.bfloat16)], 2
    )
    q_send = q_rot.reshape(seq_count, part_len, group_count, heads_dev * HD)
    kv_send = jnp.take(kv_all, slot_table, axis=2).reshape(
        seq_count, part_len, group_count, 2 * kv_dev * HD
    )
    q_heads = lax.all_to_all(q_send, "seq", split_axis=2, concat_axis=1, tiled=True)
    kv_heads = lax.all_to_all(kv_send, "seq", split_axis=2, concat_axis=1, tiled=True)
    q_heads = q_heads.reshape(seq_count, full_len, heads_dev, HD)
    kv_heads = kv_heads.reshape(seq_count, full_len, 2 * kv_dev, HD)
    k_heads = kv_heads[:, :, :kv_dev]
    v_heads = kv_heads[:, :, kv_dev:]
    o_heads, log_total = lax.map(local_attend, (q_heads, k_heads, v_heads))
    o_back = lax.all_to_all(
        o_heads.reshape(seq_count, full_len, 1, heads_dev * HD),
        "seq",
        split_axis=1,
        concat_axis=2,
        tiled=True,
    )
    attn_flat = o_back.reshape(row_count, model_width)
    middle = hidden + project(attn_flat, w_out[layer_index]).reshape(
        seq_count, part_len, model_width
    )
    normed_two, scale_two = normalize(middle, gain[1])
    normed_two_flat = normed_two.reshape(row_count, model_width)
    both = project(normed_two_flat, w_gate_up[layer_index])
    gate_part = both[:, :FF]
    up_part = both[:, FF:]
    activated = (jax.nn.silu(gate_part) * up_part).astype(jnp.bfloat16)
    result = middle + project(activated, w_down[layer_index]).reshape(
        seq_count, part_len, model_width
    )
    saved = [
        (
            hidden,
            normed_flat,
            scale_one,
            q_heads,
            k_heads,
            v_heads,
            o_heads,
            log_total,
            attn_flat,
            middle,
            normed_two_flat,
            scale_two,
            gate_part,
            up_part,
            activated,
        )
    ]
    flowing = cotangent
    grads_qkv = [None] * LAYERS
    grads_out = [None] * LAYERS
    grads_gate_up = [None] * LAYERS
    grads_down = [None] * LAYERS
    gain_terms = [None] * LAYERS
    for layer_index in reversed(range(LAYERS)):
        (
            layer_in,
            normed_flat,
            scale_one,
            q_heads,
            k_heads,
            v_heads,
            o_heads,
            log_total,
            attn_flat,
            middle,
            normed_two_flat,
            scale_two,
            gate_part,
            up_part,
            activated,
        ) = saved[layer_index]
        gain = gains[layer_index]
        dm_cast = flowing.reshape(row_count, model_width).astype(jnp.bfloat16)
        dact, grads_down[layer_index] = backward_pair(dm_cast, activated, w_down[layer_index])
        sigma = jax.nn.sigmoid(gate_part)
        dgate = dact * up_part * sigma * (1.0 + gate_part * (1.0 - sigma))
        dup = dact * gate_part * sigma
        dgu = jnp.concatenate([dgate, dup], 1).astype(jnp.bfloat16)
        dnormed_two, grads_gate_up[layer_index] = backward_pair(
            dgu, normed_two_flat, w_gate_up[layer_index]
        )
        dnormed_two = dnormed_two.reshape(seq_count, part_len, model_width)
        dmid_norm, gain_two = normalize_back(dnormed_two, middle, scale_two, gain[1])
        dmiddle = flowing + dmid_norm
        dy_cast = dmiddle.reshape(row_count, model_width).astype(jnp.bfloat16)
        dattn_wide, grads_out[layer_index] = backward_pair(dy_cast, attn_flat, w_out[layer_index])
        dattn = dattn_wide.astype(jnp.bfloat16)
        dattn_heads = lax.all_to_all(
            dattn.reshape(seq_count, part_len, group_count, heads_dev * HD),
            "seq",
            split_axis=2,
            concat_axis=1,
            tiled=True,
        )
        dattn_heads = dattn_heads.reshape(seq_count, full_len, heads_dev, HD)
        dq_heads, dk_heads, dv_heads = lax.map(
            local_attend_back, (q_heads, k_heads, v_heads, o_heads, log_total, dattn_heads)
        )
        dkv_heads = jnp.concatenate([dk_heads, dv_heads], 2).reshape(
            seq_count, full_len, 1, 2 * kv_dev * HD
        )
        dq_tok, dkv_tok = (
            lax.all_to_all(
                dq_heads.reshape(seq_count, full_len, 1, heads_dev * HD),
                "seq",
                split_axis=1,
                concat_axis=2,
                tiled=True,
            ),
            lax.all_to_all(dkv_heads, "seq", split_axis=1, concat_axis=2, tiled=True),
        )
        dqueries = dq_tok.reshape(seq_count, part_len, H, HD)
        dkv_sum = jnp.einsum(
            "stnd,nm->stmd",
            dkv_tok.reshape(seq_count, part_len, group_count * 2 * kv_dev, HD),
            slot_onehot,
            preferred_element_type=jnp.float32,
        )
        dq_pre = unrotate(dqueries, cosines, sines)
        dk_pre = unrotate(dkv_sum[:, :, :KVH], cosines, sines)
        dvalues = dkv_sum[:, :, KVH:]
        djoint = jnp.concatenate(
            [
                dq_pre.reshape(row_count, -1),
                dk_pre.reshape(row_count, -1),
                dvalues.reshape(row_count, -1),
            ],
            1,
        ).astype(jnp.bfloat16)
        dnormed, grads_qkv[layer_index] = backward_pair(djoint, normed_flat, w_qkv[layer_index])
        dnormed = dnormed.reshape(seq_count, part_len, model_width)
        dcur_norm, gain_one = normalize_back(dnormed, layer_in, scale_one, gain[0])
        gain_terms[layer_index] = jnp.stack([gain_one, gain_two])
        flowing = dmiddle + dcur_norm
    gain_total = lax.psum(jnp.stack(gain_terms), ("fsdp", "seq"))
    return (
        result,
        flowing,
        gain_total,
        jnp.stack(grads_qkv),
        jnp.stack(grads_out),
        jnp.stack(grads_gate_up),
        jnp.stack(grads_down),
    )


def neighbour(values, step):
    count = lax.axis_size("seq")
    return lax.ppermute(values, "seq", [(i, i ^ step) for i in range(count)])


def matmul(left, right, left_dim, right_dim):
    return lax.dot_general(
        left, right, (((left_dim,), (right_dim,)), ((), ())), preferred_element_type=jnp.float32
    )


ROOT = HD ** (-0.5)
LIMIT = 60 * 1024 * 1024


def swap_halves(values):
    width = values.shape[1]
    half = HD // 2
    column = lax.broadcasted_iota(jnp.int32, values.shape, 1)
    return jnp.where(
        column % HD < half, pltpu.roll(values, width - half, 1), pltpu.roll(values, half, 1)
    )


def spread_tables(table, pairs, last):
    half = HD // 2
    cosines, sines = table[:, :half], table[:, half:]
    ones, zeros = jnp.ones_like(table), jnp.zeros_like(table)
    tail = [[cosines, cosines, ones], [-sines, sines, zeros]] if last else [[], []]
    if not pairs:
        return jnp.concatenate(tail[0], 1), jnp.concatenate(tail[1], 1)
    cosines = [jnp.concatenate([cosines] * 4, 1)] * pairs
    sines = [jnp.concatenate([-sines, sines] * 2, 1)] * pairs
    if last:
        cosines.append(jnp.concatenate(tail[0], 1))
        sines.append(jnp.concatenate(tail[1], 1))
    return jnp.concatenate(cosines, 1), jnp.concatenate(sines, 1)


MESH = pl.DeviceIdType.MESH


def seq_peer(step):
    return {"seq": lax.axis_index("seq") ^ step}


def fsdp_peer(place):
    return {"fsdp": place}


def remote(source, target, sems, slot, peer):
    return pltpu.make_async_remote_copy(
        src_ref=source,
        dst_ref=target,
        send_sem=sems[0].at[slot],
        recv_sem=sems[1].at[slot],
        device_id=peer,
        device_id_type=MESH,
    )


def gather_copies(own, slots, half, sems, base=0):
    top, bottom = pl.ds(0, half), pl.ds(half, own.shape[0] - half)

    def slot(step, rows):
        return slots.at[step].at[rows]

    return [
        remote(own.at[top], slot(1, top), sems, base, seq_peer(1)),
        remote(own.at[bottom], slot(2, bottom), sems, base + 1, seq_peer(2)),
        remote(own.at[bottom], slot(1, bottom), sems, base + 2, seq_peer(1)),
        remote(own.at[top], slot(2, top), sems, base + 3, seq_peer(2)),
        remote(slot(1, top), slot(3, top), sems, base + 4, seq_peer(2)),
        remote(slot(2, bottom), slot(3, bottom), sems, base + 5, seq_peer(1)),
    ]


def greet(peers):
    barrier = pltpu.get_barrier_semaphore()
    for peer in peers:
        pl.semaphore_signal(barrier, inc=1, device_id=peer, device_id_type=MESH)
    pl.semaphore_wait(barrier, len(peers))


def sum_copies(sent, side, below, far, half, sems, passed=None):
    top, bottom = pl.ds(0, half), pl.ds(half, half)
    return [
        remote(sent.at[3].at[top], side.at[1], sems, 0, seq_peer(1)),
        remote(sent.at[3].at[bottom], below.at[1], sems, 1, seq_peer(2)),
        remote(sent.at[2].at[bottom], below.at[0], sems, 2, seq_peer(2)),
        remote(sent.at[1].at[top], side.at[0], sems, 3, seq_peer(1)),
        remote(passed.at[0] if passed is not None else sent.at[2].at[top], far.at[0], sems, 4, seq_peer(2)),
        remote(passed.at[1] if passed is not None else sent.at[1].at[bottom], far.at[1], sems, 5, seq_peer(1)),
    ]


def pass_sums(turn, step, partial, sums, sent_ref, side_ref, below_ref, own_ref, half):
    wide, narrow = jnp.float32, jnp.bfloat16
    last = len(sums) // 2

    @pl.when(turn == last)
    def _():
        own_ref[...] = partial

    @pl.when(turn < last)
    def _():
        sent_ref[step] = partial.astype(narrow)

    @pl.when(turn == 0)
    def _():
        sums[0].start()
        sums[1].start()

    @pl.when(turn == 1)
    def _():
        sums[2].start()

    @pl.when(turn == 2)
    def _():
        sums[3].start()
        sums[0].wait_recv()
        sent_ref[2, :half] = (sent_ref[2, :half].astype(wide) + side_ref[1].astype(wide)).astype(narrow)
        sums[4].start()
        sums[1].wait_recv()
        sent_ref[1, half:] = (sent_ref[1, half:].astype(wide) + below_ref[1].astype(wide)).astype(narrow)
        sums[5].start()


def end_sums(sums, side_ref, below_ref, far_ref, own_ref, half):
    wide = jnp.float32
    sums[2].wait_recv()
    sums[3].wait_recv()
    own_ref[:half] += side_ref[0].astype(wide)
    own_ref[half:] += below_ref[0].astype(wide)
    sums[4].wait_recv()
    own_ref[:half] += far_ref[0].astype(wide)
    sums[5].wait_recv()
    own_ref[half:] += far_ref[1].astype(wide)


def share_own(own_ref, all_ref, half, sems, before):
    copies = gather_copies(own_ref, all_ref, half, sems, len(before))
    for copy in copies[:4]:
        copy.start()
    copies[0].wait_recv()
    copies[4].start()
    copies[1].wait_recv()
    copies[5].start()
    for copy in copies[2:]:
        copy.wait_recv()
    for copy in before + copies:
        copy.wait_send()


def enter_kernel(
    count, current_in, gain_ref, positions_ref, shard_ref, out_shard_ref, gate_up_ref, down_ref,
    all_ref, rows_ref, out_ref, table_ref, gate_up_part_ref, down_part_ref, scale_ref,
    current_ref, normed_ref, spots_ref, held_ref, part_ref, held_down,
    send_sems, recv_sems, spot_send, spot_recv, item_up, item_down, item_side, item_recv, local_sem,
):
    part, _ = current_ref.shape
    heads = H // count
    pieces = heads + 2
    items = pieces + lax.axis_size("fsdp")
    per_shard = shard_ref.shape[0] // HD
    out_rows, columns = out_shard_ref.shape[0], heads * HD
    chips = lax.axis_size("fsdp") // 2
    index = lax.axis_index("seq")
    place = lax.axis_index("fsdp")
    chip, core = place // 2, place % 2
    sems = (send_sems, recv_sems)

    take_current = pltpu.make_async_copy(current_in, current_ref, local_sem.at[items + 4])
    take_current.start()
    barrier = pltpu.get_barrier_semaphore()
    for peer in [seq_peer(step) for step in range(1, count)] + [fsdp_peer(place ^ 1)]:
        pl.semaphore_signal(barrier, inc=1, device_id=peer, device_id_type=MESH)

    @pl.when(chip > 0)
    def _():
        pl.semaphore_signal(barrier, inc=1, device_id=fsdp_peer(place - 2), device_id_type=MESH)

    @pl.when(chip < chips - 1)
    def _():
        pl.semaphore_signal(barrier, inc=1, device_id=fsdp_peer(place + 2), device_id_type=MESH)

    greetings = count + (chip > 0).astype(jnp.int32) + (chip < chips - 1).astype(jnp.int32)
    pl.semaphore_wait(barrier, greetings)

    part_rows = part_ref.shape[0]
    take = pltpu.make_async_copy(
        gate_up_ref.at[pl.ds(pl.multiple_of(index * part_rows, part_rows), part_rows)], part_ref, local_sem.at[items + 1]
    )
    take.start()
    take_down = pltpu.make_async_copy(down_ref, held_down, local_sem.at[items + 3])
    take_down.start()

    def qkv_item(item):
        block = jnp.where(
            item < heads, index * heads + item, jnp.where(item == heads, H + index, H + KVH + index)
        )
        source = shard_ref.at[pl.ds(pl.multiple_of(block % per_shard * HD, HD), HD)]
        return block // per_shard, source, rows_ref.at[pl.ds(pl.multiple_of(item * HD, HD), HD)], item

    def out_item(item):
        source = out_shard_ref.at[:, pl.ds(pl.multiple_of(index * columns, columns), columns)]
        target = out_ref.at[pl.ds(pl.multiple_of(item * out_rows, out_rows), out_rows)]
        return item, source, target, item + pieces

    kinds = ((qkv_item, pieces), (out_item, items - pieces))

    def item_copy(source, target, slot, sem, peer):
        return pltpu.make_async_remote_copy(
            src_ref=source,
            dst_ref=target,
            send_sem=sem.at[slot],
            recv_sem=item_recv.at[slot],
            device_id=fsdp_peer(peer),
            device_id_type=MESH,
        )

    def pass_on(source, target, slot, owner_chip, act):
        @pl.when((chip >= owner_chip) & (chip < chips - 1))
        def _():
            act(item_copy(source, target, slot, item_up, place + 2))

        @pl.when((chip <= owner_chip) & (chip > 0))
        def _():
            act(item_copy(source, target, slot, item_down, place - 2))

        act(item_copy(source, target, slot, item_side, place ^ 1))

    def send_own(item_of):
        def body(item, carry):
            owner, source, target, slot = item_of(item)

            @pl.when(place == owner)
            def _():
                pass_on(source, target, slot, owner // 2, lambda copy: copy.start())
                pltpu.make_async_copy(source, target, local_sem.at[slot]).start()

            return carry

        return body

    def pass_far(item_of, distance):
        def body(item, carry):
            owner, _, target, slot = item_of(item)
            owner_chip = owner // 2
            apart = jnp.where(chip > owner_chip, chip - owner_chip, owner_chip - chip)

            @pl.when((apart == distance) & (core == owner % 2))
            def _():
                item_copy(target, target, slot, item_side, place ^ 1).wait_recv()
                pass_on(target, target, slot, owner_chip, lambda copy: copy.start())

            return carry

        return body

    for item_of, number in kinds:
        lax.fori_loop(0, number, send_own(item_of), 0)
    take_current.wait()
    current = current_ref[...]
    scale = lax.rsqrt(jnp.mean(current * current, 1, keepdims=True) + EPS)
    scale_ref[...] = jnp.broadcast_to(scale, scale_ref.shape)
    normed_ref[...] = (current * scale * gain_ref[...]).astype(jnp.bfloat16)
    copies = gather_copies(normed_ref, all_ref, part // 2, sems)
    for copy in copies[:4]:
        copy.start()
    spots_ref[...] = jnp.broadcast_to(positions_ref[...].astype(jnp.float32), spots_ref.shape)
    held_ref[0] = spots_ref[...]
    spot_copies = [
        remote(spots_ref, held_ref.at[step], (spot_send, spot_recv), step - 1, seq_peer(step))
        for step in range(1, count)
    ]
    for copy in spot_copies:
        copy.start()
    own = pltpu.make_async_copy(normed_ref, all_ref.at[0], local_sem.at[items])
    own.start()
    for distance in range(1, chips):
        for item_of, number in kinds:
            lax.fori_loop(0, number, pass_far(item_of, distance), 0)
            if distance == 1 and item_of is qkv_item:
                copies[0].wait_recv()
                copies[4].start()
                copies[1].wait_recv()
                copies[5].start()

    take.wait()
    put = pltpu.make_async_copy(part_ref, gate_up_part_ref, local_sem.at[items + 2])
    put.start()
    take_down.wait()
    columns_here = part_rows
    for device in range(count):

        @pl.when(index == device)
        def _():
            down_part_ref[...] = jnp.concatenate(
                [
                    held_down[:, start + device * columns_here : start + (device + 1) * columns_here]
                    for start in range(0, held_down.shape[1], count * columns_here)
                ],
                1,
            )

    for copy in spot_copies:
        copy.wait()
    half = HD // 2
    for step in range(count):
        spots = held_ref[step][:1]
        frequency = jnp.exp(
            lax.broadcasted_iota(jnp.int32, (half, 1), 0).astype(jnp.float32) * (-2.0 * math.log(10000.0) / HD)
        )
        angles = frequency * spots
        turned = jnp.concatenate([jnp.cos(angles), jnp.sin(angles)], 0)
        table_ref[pl.ds(step * part, part), :] = jnp.transpose(turned)

    def finish(item_of):
        def body(item, carry):
            owner, source, target, slot = item_of(item)

            @pl.when(core != owner % 2)
            def _():
                item_copy(target, target, slot, item_side, place ^ 1).wait_recv()

            @pl.when(place == owner)
            def _():
                pltpu.make_async_copy(source, target, local_sem.at[slot]).wait()

            @pl.when(core == owner % 2)
            def _():
                pass_on(target, target, slot, owner // 2, lambda copy: copy.wait_send())

            return carry

        return body

    for item_of, number in kinds:
        lax.fori_loop(0, number, finish(item_of), 0)
    own.wait()
    put.wait()
    for copy in copies[2:]:
        copy.wait_recv()
    for copy in copies:
        copy.wait_send()


def enter(current, gain, positions, shard, out_shard, gate_up, down, count):
    part, width = current.shape
    length = part * count
    heads = H // count
    pieces = heads + 2
    items = pieces + lax.axis_size("fsdp")
    vmem = pl.BlockSpec(memory_space=pltpu.VMEM)
    whole = pl.BlockSpec(memory_space=pl.ANY)
    part_shape = (gate_up.shape[0] // count, width)
    gathered, rows, out_cols, table, gate_up_part, down_part, scale = pl.pallas_call(
        lambda *refs: enter_kernel(count, *refs),
        out_shape=(
            jax.ShapeDtypeStruct((count, part, width), jnp.bfloat16),
            jax.ShapeDtypeStruct((pieces * HD, width), jnp.bfloat16),
            jax.ShapeDtypeStruct((out_shard.shape[0] * (items - pieces), heads * HD), jnp.bfloat16),
            jax.ShapeDtypeStruct((length, HD), jnp.float32),
            jax.ShapeDtypeStruct(part_shape, gate_up.dtype),
            jax.ShapeDtypeStruct((down.shape[0], down.shape[1] // count), down.dtype),
            jax.ShapeDtypeStruct((part, 128), jnp.float32),
        ),
        in_specs=[whole] + [vmem] * 2 + [whole] * 4,
        out_specs=[whole] + [vmem] * 3 + [whole] + [vmem] * 2,
        scratch_shapes=[
            pltpu.VMEM((part, width), jnp.float32),
            pltpu.VMEM((part, width), jnp.bfloat16),
            pltpu.VMEM((8, part), jnp.float32),
            pltpu.VMEM((count, 8, part), jnp.float32),
            pltpu.VMEM(part_shape, gate_up.dtype),
            pltpu.VMEM(down.shape, down.dtype),
            pltpu.SemaphoreType.DMA((6,)),
            pltpu.SemaphoreType.DMA((6,)),
            pltpu.SemaphoreType.DMA((count - 1,)),
            pltpu.SemaphoreType.DMA((count - 1,)),
            pltpu.SemaphoreType.DMA((items,)),
            pltpu.SemaphoreType.DMA((items,)),
            pltpu.SemaphoreType.DMA((items,)),
            pltpu.SemaphoreType.DMA((items,)),
            pltpu.SemaphoreType.DMA((items + 5,)),
        ],
        compiler_params=pltpu.CompilerParams(collective_id=1, has_side_effects=True, vmem_limit_bytes=LIMIT),
        name="enter",
    )(current, gain, positions, shard, out_shard, gate_up, down)
    return gathered.reshape(length, width), rows, out_cols, table, gate_up_part, down_part, scale


def qkv_kernel(index_ref, normed_ref, weight_ref, table_ref, q_ref, k_ref, v_ref):
    heads = q_ref.shape[0]
    joint = matmul(normed_ref[...], weight_ref[...], 1, 1)
    cosines, sines = spread_tables(table_ref[...], heads // 2, True)
    turned = joint * cosines + swap_halves(joint) * sines
    for head in range(heads):
        rounded = turned[:, head * HD : (head + 1) * HD].astype(jnp.bfloat16).astype(jnp.float32)
        q_ref[head] = (rounded * ROOT).astype(jnp.bfloat16)
    k_ref[...] = turned[:, heads * HD : (heads + 1) * HD].astype(jnp.bfloat16)
    v_ref[...] = turned[:, (heads + 1) * HD :].astype(jnp.bfloat16)


def project_qkv(index, normed, weight, table, count):
    length, width = normed.shape
    part = length // count
    heads = weight.shape[0] // HD - 2
    return pl.pallas_call(
        qkv_kernel,
        out_shape=(
            jax.ShapeDtypeStruct((heads, length, HD), jnp.bfloat16),
            jax.ShapeDtypeStruct((length, HD), jnp.bfloat16),
            jax.ShapeDtypeStruct((length, HD), jnp.bfloat16),
        ),
        grid_spec=pltpu.PrefetchScalarGridSpec(
            num_scalar_prefetch=1,
            grid=(count,),
            in_specs=[
                pl.BlockSpec((part, width), lambda i, s: (i, 0)),
                pl.BlockSpec(weight.shape, lambda i, s: (0, 0)),
                pl.BlockSpec((part, table.shape[1]), lambda i, s: (i, 0)),
            ],
            out_specs=[
                pl.BlockSpec((heads, part, HD), lambda i, s: (0, i ^ s[0], 0)),
                pl.BlockSpec((part, HD), lambda i, s: (i ^ s[0], 0)),
                pl.BlockSpec((part, HD), lambda i, s: (i ^ s[0], 0)),
            ],
        ),
        compiler_params=pltpu.CompilerParams(vmem_limit_bytes=LIMIT),
        name="project_qkv",
    )(index, normed, weight, table)


def attend_kernel(
    count, q_ref, k_ref, v_ref, weight_ref, current_ref, gain_ref,
    attn_ref, lse_ref, middle_ref, scale_ref, all_ref,
    held_ref, sent_ref, side_ref, below_ref, far_ref, two_ref, send_sems, recv_sems, own_sem,
):
    heads, _, _ = q_ref.shape
    part, _ = current_ref.shape
    half = part // 2
    index = lax.axis_index("seq")
    top, bottom = pl.ds(0, half), pl.ds(half, half)
    sems = (send_sems, recv_sems)
    greet([seq_peer(1), seq_peer(2)])
    sums = sum_copies(sent_ref, side_ref, below_ref, far_ref, half, sems)
    row = lax.broadcasted_iota(jnp.int32, (part, part), 0)
    column = lax.broadcasted_iota(jnp.int32, (part, part), 1)

    def one_part(turn, carry):
        step = count - 1 - turn
        here = step ^ index
        rows_here = pl.ds(pl.multiple_of(here * part, part), part)
        rows_step = pl.ds(pl.multiple_of(step * part, part), part)
        for block in range(count):

            @pl.when(here == block)
            def _():
                before = block * part
                seen = before + part
                keys_in, values_in = k_ref[:seen], v_ref[:seen]

                def one_head(head, carry):
                    scores = matmul(q_ref[head, before:seen, :], keys_in, 1, 1)
                    last = jnp.where(row >= column, scores[:, before:], -1e30)
                    scores = jnp.concatenate([scores[:, :before], last], 1) if block else last
                    peak = jnp.max(scores, 1, keepdims=True)
                    weights = jnp.exp(scores - peak)
                    total = jnp.sum(weights, 1, keepdims=True)
                    output = matmul(weights.astype(jnp.bfloat16), values_in, 1, 0) / total
                    held_ref[head] = output.astype(jnp.bfloat16)
                    log_total = jnp.broadcast_to(peak + jnp.log(total), (part, 128))
                    lse_ref[pl.ds(head, 1), before:seen] = jnp.transpose(log_total)[:1]
                    return carry

                lax.fori_loop(0, heads, one_head, 0, unroll=2)

        attn = jnp.concatenate([held_ref[head] for head in range(heads)], 1)
        attn_ref[rows_step, :] = attn
        partial = matmul(attn, weight_ref[...], 1, 1)

        pass_sums(turn, step, partial, sums, sent_ref, side_ref, below_ref, middle_ref, half)
        return carry

    lax.fori_loop(0, count, one_part, 0)
    end_sums(sums, side_ref, below_ref, far_ref, middle_ref, half)
    middle_ref[...] += current_ref[...]
    middle = middle_ref[...]
    scale = lax.rsqrt(jnp.mean(middle * middle, 1, keepdims=True) + EPS)
    scale_ref[...] = jnp.broadcast_to(scale, scale_ref.shape)
    two_ref[...] = (middle * scale * gain_ref[...]).astype(jnp.bfloat16)
    own = pltpu.make_async_copy(two_ref, all_ref.at[0], own_sem)
    share_own(two_ref, all_ref, half, sems, sums)
    own.start()
    own.wait()


def attend(queries, keys_in, values_in, weight, current, gain, count):
    heads, length, _ = queries.shape
    part, width = current.shape
    vmem = pl.BlockSpec(memory_space=pltpu.VMEM)
    attn, lse, middle, scale, gathered = pl.pallas_call(
        lambda *refs: attend_kernel(count, *refs),
        out_shape=(
            jax.ShapeDtypeStruct((length, heads * HD), jnp.bfloat16),
            jax.ShapeDtypeStruct((heads, length), jnp.float32),
            jax.ShapeDtypeStruct((part, width), jnp.float32),
            jax.ShapeDtypeStruct((part, 128), jnp.float32),
            jax.ShapeDtypeStruct((count, part, width), jnp.bfloat16),
        ),
        in_specs=[vmem] * 6,
        out_specs=[vmem] * 4 + [pl.BlockSpec(memory_space=pl.ANY)],
        scratch_shapes=[
            pltpu.VMEM((heads, part, HD), jnp.bfloat16),
            pltpu.VMEM((count, part, width), jnp.bfloat16),
            pltpu.VMEM((2, part // 2, width), jnp.bfloat16),
            pltpu.VMEM((2, part // 2, width), jnp.bfloat16),
            pltpu.VMEM((2, part // 2, width), jnp.bfloat16),
            pltpu.VMEM((part, width), jnp.bfloat16),
            pltpu.SemaphoreType.DMA((12,)),
            pltpu.SemaphoreType.DMA((12,)),
            pltpu.SemaphoreType.DMA,
        ],
        compiler_params=pltpu.CompilerParams(collective_id=2, has_side_effects=True, vmem_limit_bytes=LIMIT),
        name="attend",
    )(queries, keys_in, values_in, weight, current, gain)
    return attn, lse, middle, scale, gathered.reshape(length, width)


def share_start(copies):
    for group in copies:
        group[0].start()
        group[1].start()
    for group in copies:
        group[2].start()
        group[3].start()


def share_on(group):
    group[0].wait_recv()
    group[4].start()
    group[1].wait_recv()
    group[5].start()


def share_end(copies):
    for group in copies:
        for copy in group[2:]:
            copy.wait_recv()
    for group in copies:
        for copy in group:
            copy.wait_send()


def upper_half(rows):
    return -(-(rows // 2) // 16) * 16


def attend_back_kernel(
    count, q_in, k_in, v_in, attn_in, lse_in, dy_ref, weight_in, table_in, pick_ref, passed_ref, shard_ref,
    out_ref, turned_ref, term_ref, far_ref, slot_ref,
    q_ref, k_ref, v_ref, attn_ref, lse_ref, weight_ref, table_ref,
    do_ref, delta_ref, dq_ref, dk_ref, dv_ref, held_dy, held_pick,
    send_sems, recv_sems, load_sems,
):
    heads, length, _ = q_in.shape
    part = length // count
    wide = jnp.float32
    index = lax.axis_index("seq")
    load_weight = pltpu.make_async_copy(weight_in, weight_ref, load_sems.at[count + 1])
    load_weight.start()
    greet([seq_peer(1), seq_peer(2)])
    sems = (send_sems, recv_sems)
    sums = [
        remote(passed_ref.at[0], far_ref.at[0], sems, 6, seq_peer(2)),
        remote(passed_ref.at[1], far_ref.at[1], sems, 7, seq_peer(1)),
    ]
    group = gather_copies(shard_ref, slot_ref, upper_half(shard_ref.shape[0]), sems)
    share_start([group])
    for copy in sums:
        copy.start()

    def load_dy(step):
        rows = pl.ds(pl.multiple_of(step * part, part), part)
        return pltpu.make_async_copy(dy_ref.at[rows], held_dy.at[rows], load_sems.at[step])

    load = pltpu.make_async_copy(pick_ref, held_pick, load_sems.at[count])
    sources, targets = (attn_in, q_in, k_in, v_in, lse_in, table_in), (attn_ref, q_ref, k_ref, v_ref, lse_ref, table_ref)
    loads = [
        pltpu.make_async_copy(source, target, load_sems.at[count + 2 + number])
        for number, (source, target) in enumerate(zip(sources, targets))
    ]
    load_dy(index).start()
    for copy in loads:
        copy.start()
    for here in range(1, count):
        load_dy(here ^ index).start()
    load.start()
    load_weight.wait()
    for copy in loads:
        copy.wait()
    dk_ref[...] = jnp.zeros_like(dk_ref)
    dv_ref[...] = jnp.zeros_like(dv_ref)
    owner = lax.broadcasted_iota(jnp.int32, (heads, heads * HD), 1) // HD
    same = (owner == lax.broadcasted_iota(jnp.int32, (heads, heads * HD), 0)).astype(wide)
    row = lax.broadcasted_iota(jnp.int32, (part, part), 0)
    column = lax.broadcasted_iota(jnp.int32, (part, part), 1)

    def unturn(grads, cosines, sines):
        return grads * cosines + swap_halves(grads * sines)

    def one_part(here, carry):
        spot = here ^ index
        rows_here = pl.ds(pl.multiple_of(spot * part, part), part)
        load_dy(spot).wait()
        dattn = matmul(held_dy[rows_here, :], weight_ref[...], 1, 0).astype(jnp.bfloat16)
        product = dattn.astype(wide) * attn_ref[rows_here, :].astype(wide)
        delta_ref[...] = lax.dot_general(
            same, product, (((1,), (1,)), ((), ())), precision=lax.Precision.HIGHEST, preferred_element_type=wide
        )
        for head in range(heads):
            do_ref[head] = dattn[:, head * HD : (head + 1) * HD]
        for block in range(count):

            @pl.when(here == block)
            def _():
                before = block * part
                seen = before + part
                keys_in, values_in = k_ref[:seen], v_ref[:seen]

                def one_head(head, carry):
                    query, dout = q_ref[head, before:seen, :], do_ref[head]
                    scores = matmul(keys_in, query, 1, 1)
                    last = jnp.where(row <= column, scores[before:], -1e30)
                    scores = jnp.concatenate([scores[:before], last], 0) if block else last
                    probs = jnp.exp(scores - lse_ref[pl.ds(head, 1), before:seen])
                    dprob = matmul(values_in, dout, 1, 1)
                    dscore = (probs * (dprob - delta_ref[pl.ds(head, 1), :])).astype(jnp.bfloat16)
                    dv_ref[:seen] += matmul(probs.astype(jnp.bfloat16), dout, 1, 0)
                    dk_ref[:seen] += matmul(dscore, query, 1, 0)
                    dq_ref[head] = (matmul(dscore, keys_in, 0, 0) * ROOT).astype(jnp.bfloat16)
                    return carry

                lax.fori_loop(0, heads, one_head, 0, unroll=2)

        dq = jnp.concatenate([dq_ref[head] for head in range(heads)], 1).astype(wide)
        dq = unturn(dq, *spread_tables(table_ref[rows_here, :], heads // 2, False))
        out_ref[rows_here, : heads * HD] = dq.astype(jnp.bfloat16)

        @pl.when(here == 1)
        def _():
            share_on(group)

        return carry

    lax.fori_loop(0, count, one_part, 0)
    for block in range(count):
        rows_there = pl.ds(pl.multiple_of((block ^ index) * part, part), part)
        rows_block = slice(block * part, (block + 1) * part)
        both = jnp.concatenate([dk_ref[rows_block], dv_ref[rows_block]], 1).astype(jnp.bfloat16).astype(wide)
        both = unturn(both, *spread_tables(table_ref[rows_there, :], 0, True))
        out_ref[rows_there, heads * HD :] = both.astype(jnp.bfloat16)
    load.wait()
    chosen = matmul(held_pick[...], out_ref[...], 1, 1).astype(jnp.bfloat16)
    size = turned_ref.shape[1]
    for block in range(count):
        turned_ref[block] = chosen[block * size : (block + 1) * size]
    tile = 2 * 128

    def one_tile(number, carry):
        columns = pl.ds(pl.multiple_of(number * tile, tile), tile)
        term_ref[columns, :] = matmul(held_dy[:, columns], attn_ref[...], 0, 0).astype(jnp.bfloat16)
        return carry

    lax.fori_loop(0, held_dy.shape[1] // tile, one_tile, 0)
    for copy in sums:
        copy.wait_recv()
    share_end([group])
    for copy in sums:
        copy.wait_send()


def attend_back(queries, keys_in, values_in, attn, lse, dy, weight, table, pick, passed, shard, count):
    heads, length, _ = queries.shape
    part, width = length // count, dy.shape[1]
    columns = (heads + 2) * HD
    vmem, whole = pl.BlockSpec(memory_space=pltpu.VMEM), pl.BlockSpec(memory_space=pl.ANY)
    return pl.pallas_call(
        lambda *refs: attend_back_kernel(count, *refs),
        out_shape=[
            jax.ShapeDtypeStruct((length, columns), jnp.bfloat16),
            jax.ShapeDtypeStruct((count, columns // count, length), jnp.bfloat16),
            jax.ShapeDtypeStruct((width, heads * HD), jnp.bfloat16),
            jax.ShapeDtypeStruct((2, part // 2, width), jnp.bfloat16),
            jax.ShapeDtypeStruct((count,) + shard.shape, shard.dtype),
        ],
        in_specs=[whole] * 11,
        out_specs=[vmem] * 3 + [whole] * 2,
        scratch_shapes=[
            pltpu.VMEM(value.shape, value.dtype) for value in (queries, keys_in, values_in, attn, lse, weight, table)
        ]
        + [
            pltpu.VMEM((heads, part, HD), jnp.bfloat16),
            pltpu.VMEM((heads, part), jnp.float32),
            pltpu.VMEM((heads, part, HD), jnp.bfloat16),
            pltpu.VMEM((length, HD), jnp.float32),
            pltpu.VMEM((length, HD), jnp.float32),
        ]
        + [pltpu.VMEM(dy.shape, dy.dtype), pltpu.VMEM(pick.shape, pick.dtype)]
        + [pltpu.SemaphoreType.DMA((8,)), pltpu.SemaphoreType.DMA((8,)), pltpu.SemaphoreType.DMA((count + 8,))],
        compiler_params=pltpu.CompilerParams(collective_id=4, has_side_effects=True, vmem_limit_bytes=LIMIT),
        name="attend_back",
    )(queries, keys_in, values_in, attn, lse, dy, weight, table, pick, passed, shard)


def leave_kernel(
    count, grads_in, weight_in, first_in, scale_ref, gain_ref, other_ref, turned_ref, normed_in,
    own_ref, total_ref, term_ref,
    sent_ref, side_ref, below_ref, far_ref, slot_ref, whole_ref, normed_ref, first_ref, grads_ref, weight_ref,
    told_ref, heard_ref, send_sems, recv_sems, swap_send, swap_recv, load_sems, sum_send, sum_recv,
):
    part, _ = first_ref.shape
    half = part // 2
    size = turned_ref.shape[1]
    heads = H // count
    chunk = size // (heads + 2)
    index = lax.axis_index("seq")
    place = lax.axis_index("fsdp")
    peers = [seq_peer(step) for step in range(1, count)]
    fsdp_peers = [fsdp_peer(place ^ (1 << bit)) for bit in range(lax.axis_size("fsdp").bit_length() - 1)]
    greet(peers + fsdp_peers)
    swaps = [
        remote(turned_ref.at[index ^ step], slot_ref.at[step], (swap_send, swap_recv), step - 1, seq_peer(step))
        for step in range(1, count)
    ]
    for copy in swaps:
        copy.start()
    loads = [
        pltpu.make_async_copy(source, target, load_sems.at[number])
        for number, (source, target) in enumerate(
            (
                (turned_ref.at[index], slot_ref.at[0]),
                (normed_in, normed_ref),
                (first_in, first_ref),
                (grads_in, grads_ref),
                (weight_in, weight_ref),
            )
        )
    ]
    for number in (3, 4, 1, 0, 2):
        loads[number].start()
    total_ref[0:1] = jnp.zeros_like(other_ref)
    total_ref[1:2] = other_ref[...]
    for number in (3, 4, 1):
        loads[number].wait()
    sums = sum_copies(sent_ref, side_ref, below_ref, far_ref, half, (send_sems, recv_sems))

    def one_part(turn, carry):
        step = count - 1 - turn
        rows_step = pl.ds(pl.multiple_of(step * part, part), part)
        partial = matmul(grads_ref[rows_step, :], weight_ref[...], 1, 0)
        total_ref[0:1] += jnp.sum(partial * normed_ref[rows_step, :].astype(jnp.float32), 0, keepdims=True)
        pass_sums(turn, step, partial, sums, sent_ref, side_ref, below_ref, own_ref, half)
        return carry

    lax.fori_loop(0, count, one_part, 0)
    loads[0].wait()
    loads[2].wait()
    total_ref[0:1] = total_ref[0:1] / gain_ref[...]
    tells = []
    for step, peer in enumerate(fsdp_peers):
        told_ref[step] = total_ref[...]
        tell = remote(told_ref.at[step], heard_ref.at[step], (sum_send, sum_recv), step, peer)
        tell.start()
        tell.wait_recv()
        total_ref[...] += heard_ref[step]
        tells.append(tell)
    first = len(tells)
    told_ref[first] = total_ref[...]
    for step, peer in enumerate(peers):
        tells.append(
            remote(told_ref.at[first], heard_ref.at[first + step], (sum_send, sum_recv), first + step, peer)
        )
        tells[-1].start()
    for step in range(count):
        if step:
            swaps[step - 1].wait_recv()
        peer = index ^ step
        for block in range(count):
            piece = slot_ref[step, :, (step ^ block) * part : ((step ^ block) + 1) * part]
            tokens = slice(block * part, (block + 1) * part)
            for start, rows in ((0, heads * chunk), (H * chunk, chunk), ((H + KVH) * chunk, chunk)):
                begin = 0 if start == 0 else heads * chunk + (0 if start == H * chunk else chunk)
                spot = pl.multiple_of(start + peer * rows, chunk)
                whole_ref[pl.ds(spot, rows), tokens] = piece[begin : begin + rows]
    term_ref[...] = matmul(whole_ref[...], normed_ref[...], 1, 0).astype(jnp.bfloat16)
    end_sums(sums, side_ref, below_ref, far_ref, own_ref, half)
    unit = first_ref[...] * scale_ref[:, :1]
    grads = own_ref[...]
    inner = grads * gain_ref[...]
    own_ref[...] = scale_ref[:, :1] * (inner - unit * jnp.mean(inner * unit, 1, keepdims=True))
    for step in range(len(peers)):
        tells[first + step].wait_recv()
        total_ref[...] += heard_ref[first + step]
    for copy in sums + swaps + tells:
        copy.wait_send()


def leave(grads, weight, first, scale, gain, other, turned, normed, count):
    part, width = first.shape
    vmem, whole = pl.BlockSpec(memory_space=pltpu.VMEM), pl.BlockSpec(memory_space=pl.ANY)
    size, length = turned.shape[1:]
    steps = lax.axis_size("fsdp").bit_length() - 1 + count - 1
    own, total, term = pl.pallas_call(
        lambda *refs: leave_kernel(count, *refs),
        out_shape=(
            jax.ShapeDtypeStruct((part, width), jnp.float32),
            jax.ShapeDtypeStruct((2, width), jnp.float32),
            jax.ShapeDtypeStruct((size * count, width), jnp.bfloat16),
        ),
        in_specs=[whole] * 3 + [vmem] * 3 + [whole] * 2,
        out_specs=[vmem] * 3,
        scratch_shapes=[
            pltpu.VMEM((count, part, width), jnp.bfloat16),
            pltpu.VMEM((2, part // 2, width), jnp.bfloat16),
            pltpu.VMEM((2, part // 2, width), jnp.bfloat16),
            pltpu.VMEM((2, part // 2, width), jnp.bfloat16),
            pltpu.VMEM((count, size, length), jnp.bfloat16),
            pltpu.VMEM((count * size, length), jnp.bfloat16),
            pltpu.VMEM(normed.shape, jnp.bfloat16),
            pltpu.VMEM((part, width), jnp.float32),
            pltpu.VMEM(grads.shape, grads.dtype),
            pltpu.VMEM(weight.shape, weight.dtype),
            pltpu.VMEM((steps, 2, width), jnp.float32),
            pltpu.VMEM((steps, 2, width), jnp.float32),
            pltpu.SemaphoreType.DMA((6,)),
            pltpu.SemaphoreType.DMA((6,)),
            pltpu.SemaphoreType.DMA((count - 1,)),
            pltpu.SemaphoreType.DMA((count - 1,)),
            pltpu.SemaphoreType.DMA((5,)),
            pltpu.SemaphoreType.DMA((steps,)),
            pltpu.SemaphoreType.DMA((steps,)),
        ],
        compiler_params=pltpu.CompilerParams(collective_id=5, has_side_effects=True, vmem_limit_bytes=LIMIT),
        name="leave",
    )(grads, weight, first, scale, gain, other, turned, normed)
    return own, total, term


def join_rows_kernel(index_ref, own_ref, side_ref, below_ref, top_ref, bottom_ref, out_ref):
    step = pl.program_id(0) ^ index_ref[0]
    half = top_ref.shape[0]
    for number, ref in enumerate((own_ref, side_ref, below_ref)):

        @pl.when(step == number)
        def _():
            out_ref[...] = ref[...].astype(jnp.float32)

    @pl.when(step == 3)
    def _():
        out_ref[:half] = top_ref[...].astype(jnp.float32)
        out_ref[half:] = bottom_ref[...].astype(jnp.float32)


def join_rows(index, own, side, below, top, bottom, count):
    rows, width = own.shape
    parts = (own, side, below, top, bottom)
    return pl.pallas_call(
        join_rows_kernel,
        out_shape=jax.ShapeDtypeStruct((rows * count, width), jnp.float32),
        grid_spec=pltpu.PrefetchScalarGridSpec(
            num_scalar_prefetch=1,
            grid=(count,),
            in_specs=[pl.BlockSpec(part.shape, lambda i, s: (0, 0)) for part in parts],
            out_specs=pl.BlockSpec((rows, width), lambda i, s: (i, 0)),
        ),
        compiler_params=pltpu.CompilerParams(vmem_limit_bytes=LIMIT),
        name="join_rows",
    )(index, *parts)


def join_pieces_kernel(count, row_piece, column_piece, index_ref, own_ref, *refs):
    slot_refs, out_ref = refs[:-1], refs[-1]
    index = index_ref[0]
    rows, columns = own_ref.shape
    for device in range(count):
        if len(slot_refs) == 1:
            values = slot_refs[0][device ^ index]
        else:
            values = own_ref[...]
            for step, ref in enumerate(slot_refs):
                values = jnp.where(device ^ index == step + 1, ref[...], values)
        values = jnp.where(device == index, own_ref[...], values).astype(jnp.float32)
        for top in range(0, rows, row_piece):
            for left in range(0, columns, column_piece):
                down = top * count + device * row_piece if row_piece < rows else top
                across = left * count + device * column_piece if row_piece == rows else left
                out_ref[down : down + row_piece, across : across + column_piece] = values[
                    top : top + row_piece, left : left + column_piece
                ]


def join_pieces(index, own, slots, count, row_piece, column_piece):
    rows, columns = own.shape
    shape = (rows * count, columns) if row_piece < rows else (rows, columns * count)
    return pl.pallas_call(
        lambda *refs: join_pieces_kernel(count, row_piece, column_piece, *refs),
        out_shape=jax.ShapeDtypeStruct(shape, jnp.float32),
        grid_spec=pltpu.PrefetchScalarGridSpec(
            num_scalar_prefetch=1,
            grid=(1,),
            in_specs=[pl.BlockSpec(own.shape, lambda i, s: (0, 0))]
            + [pl.BlockSpec(slot.shape, lambda i, s, n=slot.ndim: (0,) * n) for slot in slots],
            out_specs=pl.BlockSpec(shape, lambda i, s: (0, 0)),
        ),
        compiler_params=pltpu.CompilerParams(vmem_limit_bytes=LIMIT),
        name="join_pieces",
    )(index, own, *slots)


def last_sums_kernel(base_ref, passed_ref, flowing_ref, piece_ref, result_ref, grad_ref):
    result_ref[...] = base_ref[...] + passed_ref[...].astype(jnp.float32)
    grad_ref[...] = flowing_ref[...] + piece_ref[...]


def last_sums(base, passed, flowing, piece):
    rows, width = base.shape
    tile = rows // 4
    block = pl.BlockSpec((tile, width), lambda i: (i, 0))
    return pl.pallas_call(
        last_sums_kernel,
        out_shape=[jax.ShapeDtypeStruct((rows, width), jnp.float32)] * 2,
        grid=(4,),
        in_specs=[block] * 4,
        out_specs=[block] * 2,
        compiler_params=pltpu.CompilerParams(vmem_limit_bytes=LIMIT),
        name="last_sums",
    )(base, passed, flowing, piece)


def norm_back_kernel(
    count, act_in, down_in, dm_in, gates_in, weight_in, flowing_in, middle_in, inputs_in, scale_ref, gain_ref,
    own_ref, gain_out_ref, dy_ref, term_ref, product_ref, from_side_ref, from_below_ref,
    act_ref, down_ref, dm_ref, gates_ref, grads_ref, weight_ref, flowing_ref, middle_ref, inputs_ref,
    held_ref, sent_ref, side_ref, below_ref, far_ref, stage_ref,
    send_sems, recv_sems, load_sems, part_sems, store_sems, product_sems,
):
    part, _ = flowing_in.shape
    half = part // 2
    wide, narrow = jnp.float32, jnp.bfloat16
    units = down_ref.shape[1]
    sems = (send_sems, recv_sems)

    def load(source, target, number):
        copy = pltpu.make_async_copy(source, target, load_sems.at[number])
        copy.start()
        return copy

    def load_parts(turn):
        rows = pl.ds(pl.multiple_of((count - 1 - turn) * part, part), part)
        slot = turn % 2
        return [
            pltpu.make_async_copy(dm_in.at[rows], dm_ref.at[slot], part_sems.at[0, slot]),
            pltpu.make_async_copy(gates_in.at[rows], gates_ref.at[slot], part_sems.at[1, slot]),
        ]

    firsts = [load(act_in, act_ref, 0), load(down_in, down_ref, 1)]
    for copy in load_parts(0):
        copy.start()
    load_weight = load(weight_in, weight_ref, 2)
    for copy in load_parts(1):
        copy.start()
    lasts = [load(inputs_in, inputs_ref, 3), load(flowing_in, flowing_ref, 4), load(middle_in, middle_ref, 5)]
    greet([seq_peer(1), seq_peer(2)])
    top, bottom = pl.ds(0, half), pl.ds(half, half)
    firsts_sums = [
        remote(held_ref.at[3].at[top], from_side_ref.at[1], sems, 6, seq_peer(1)),
        remote(held_ref.at[3].at[bottom], from_below_ref.at[1], sems, 7, seq_peer(2)),
        remote(held_ref.at[2].at[bottom], from_below_ref.at[0], sems, 8, seq_peer(2)),
        remote(held_ref.at[1].at[top], from_side_ref.at[0], sems, 9, seq_peer(1)),
    ]
    sums = sum_copies(sent_ref, side_ref, below_ref, far_ref, half, sems)
    for copy in firsts:
        copy.wait()

    def down_part(turn, carry):
        step = count - 1 - turn
        rows = pl.ds(pl.multiple_of(step * part, part), part)
        held_ref[step] = matmul(act_ref[rows, :], down_ref[...], 1, 1).astype(narrow)

        @pl.when(turn == 0)
        def _():
            firsts_sums[0].start()
            firsts_sums[1].start()

        @pl.when(turn == 1)
        def _():
            firsts_sums[2].start()

        @pl.when(turn == 2)
        def _():
            firsts_sums[3].start()

        return carry

    lax.fori_loop(0, count, down_part, 0)
    product = pltpu.make_async_copy(held_ref, product_ref, product_sems.at[0])
    product.start()
    load_weight.wait()

    def one_part(turn, carry):
        step = count - 1 - turn
        slot = turn % 2
        rows = pl.ds(pl.multiple_of(step * part, part), part)
        for copy in load_parts(turn):
            copy.wait()
        dact = matmul(dm_ref[slot], down_ref[...], 1, 0)
        gate = gates_ref[slot, :, :units].astype(wide)
        up = gates_ref[slot, :, units:].astype(wide)
        sigma = jax.nn.sigmoid(gate)
        grads_ref[rows, :units] = (dact * up * sigma * (1.0 + gate * (1.0 - sigma))).astype(narrow)
        grads_ref[rows, units:] = (dact * gate * sigma).astype(narrow)

        @pl.when(turn < count - 2)
        def _():
            for copy in load_parts(turn + 2):
                copy.start()

        partial = matmul(grads_ref[rows, :], weight_ref[...], 1, 0)

        @pl.when(turn == count - 1)
        def _():
            own_ref[...] = partial

        @pl.when(turn < count - 1)
        def _():
            sent_ref[step] = partial.astype(narrow)

        @pl.when(turn == 0)
        def _():
            sums[0].start()
            sums[1].start()

        @pl.when(turn == 1)
        def _():
            sums[2].start()

        @pl.when(turn == 2)
        def _():
            sums[3].start()

        return carry

    lax.fori_loop(0, count, one_part, 0)
    sums[0].wait_recv()
    sent_ref[2, :half] = (sent_ref[2, :half].astype(wide) + side_ref[1].astype(wide)).astype(narrow)
    sums[4].start()
    sums[1].wait_recv()
    sent_ref[1, half:] = (sent_ref[1, half:].astype(wide) + below_ref[1].astype(wide)).astype(narrow)
    sums[5].start()
    for copy in lasts:
        copy.wait()
    tile = stage_ref.shape[1]
    tiles = grads_ref.shape[1] // tile

    def store(number):
        rows = pl.ds(pl.multiple_of(number * tile, tile), tile)
        return pltpu.make_async_copy(stage_ref.at[number % 2], term_ref.at[rows], store_sems.at[number % 2])

    def one_tile(number, carry):
        @pl.when(number >= 2)
        def _():
            store(number - 2).wait()

        columns = pl.ds(pl.multiple_of(number * tile, tile), tile)
        stage_ref[number % 2] = matmul(grads_ref[:, columns], inputs_ref[...], 0, 0).astype(narrow)
        store(number).start()
        return carry

    lax.fori_loop(0, tiles, one_tile, 0)
    end_sums(sums, side_ref, below_ref, far_ref, own_ref, half)
    scale = scale_ref[:, :1]
    unit = middle_ref[...] * scale
    grads = own_ref[...]
    gain_out_ref[...] = jnp.sum(grads * unit, 0, keepdims=True)
    inner = grads * gain_ref[...]
    own_ref[...] = flowing_ref[...] + scale * (inner - unit * jnp.mean(inner * unit, 1, keepdims=True))
    dy_ref[...] = own_ref[...].astype(narrow)
    for number in range(tiles - 2, tiles):
        store(number).wait()
    product.wait()
    for copy in firsts_sums:
        copy.wait_recv()
    for copy in sums + firsts_sums:
        copy.wait_send()


def norm_back(act, down, dm, gates, weight, flowing, middle, inputs, scale, gain, count):
    part, width = flowing.shape
    units = gates.shape[1]
    tile = 2 * 128
    vmem, whole = pl.BlockSpec(memory_space=pltpu.VMEM), pl.BlockSpec(memory_space=pl.ANY)
    narrow, wide = jnp.bfloat16, jnp.float32
    pair = (2, part // 2, width)
    own, gain_term, dy, term, product, from_side, from_below = pl.pallas_call(
        lambda *refs: norm_back_kernel(count, *refs),
        out_shape=(
            jax.ShapeDtypeStruct((part, width), wide),
            jax.ShapeDtypeStruct((1, width), wide),
            jax.ShapeDtypeStruct((part, width), narrow),
            jax.ShapeDtypeStruct((units, width), narrow),
            jax.ShapeDtypeStruct((count, part, width), narrow),
            jax.ShapeDtypeStruct(pair, narrow),
            jax.ShapeDtypeStruct(pair, narrow),
        ),
        in_specs=[whole] * 8 + [vmem] * 2,
        out_specs=[vmem] * 3 + [whole] * 4,
        scratch_shapes=[
            pltpu.VMEM(act.shape, narrow),
            pltpu.VMEM(down.shape, narrow),
            pltpu.VMEM((2, part, width), narrow),
            pltpu.VMEM((2, part, units), narrow),
            pltpu.VMEM((part * count, units), narrow),
            pltpu.VMEM(weight.shape, narrow),
            pltpu.VMEM((part, width), wide),
            pltpu.VMEM((part, width), wide),
            pltpu.VMEM(inputs.shape, narrow),
            pltpu.VMEM((count, part, width), narrow),
            pltpu.VMEM((count, part, width), narrow),
            pltpu.VMEM(pair, narrow),
            pltpu.VMEM(pair, narrow),
            pltpu.VMEM(pair, narrow),
            pltpu.VMEM((2, tile, width), narrow),
            pltpu.SemaphoreType.DMA((10,)),
            pltpu.SemaphoreType.DMA((10,)),
            pltpu.SemaphoreType.DMA((6,)),
            pltpu.SemaphoreType.DMA((2, 2)),
            pltpu.SemaphoreType.DMA((2,)),
            pltpu.SemaphoreType.DMA((1,)),
        ],
        compiler_params=pltpu.CompilerParams(collective_id=3, has_side_effects=True, vmem_limit_bytes=67043328),
        name="norm_back",
    )(act, down, dm, gates, weight, flowing, middle, inputs, scale, gain)
    return own, gain_term[0], dy, term, product, from_side, from_below


def share_dy_kernel(
    dy_ref, down_ref, side_in, below_in, middle_in, all_ref, base_ref, passed_ref,
    piece_ref, side_ref, below_ref, send_sems, recv_sems, load_sems,
):
    part = dy_ref.shape[0]
    half = part // 2
    wide = jnp.float32
    top, bottom = pl.ds(0, half), pl.ds(half, half)
    loads = [
        pltpu.make_async_copy(down_ref.at[0], piece_ref.at[0], load_sems.at[0]),
        pltpu.make_async_copy(down_ref.at[2].at[top], piece_ref.at[1].at[top], load_sems.at[1]),
        pltpu.make_async_copy(down_ref.at[1].at[bottom], piece_ref.at[1].at[bottom], load_sems.at[2]),
        pltpu.make_async_copy(dy_ref, all_ref.at[0], load_sems.at[3]),
        pltpu.make_async_copy(side_in, side_ref, load_sems.at[4]),
        pltpu.make_async_copy(below_in, below_ref, load_sems.at[5]),
        pltpu.make_async_copy(middle_in, base_ref, load_sems.at[6]),
    ]
    greet([seq_peer(1), seq_peer(2)])
    group = gather_copies(dy_ref, all_ref, half, (send_sems, recv_sems))
    share_start([group])
    for load in loads:
        load.start()
    for load in loads:
        load.wait()
    base_ref[...] += piece_ref[0].astype(wide)
    base_ref[:half] += side_ref[0].astype(wide)
    base_ref[half:] += below_ref[0].astype(wide)
    passed_ref[0] = (piece_ref[1, :half].astype(wide) + side_ref[1].astype(wide)).astype(jnp.bfloat16)
    passed_ref[1] = (piece_ref[1, half:].astype(wide) + below_ref[1].astype(wide)).astype(jnp.bfloat16)
    share_on(group)
    share_end([group])


def share_dy(dy, down, side, below, middle, count):
    part, width = dy.shape
    vmem, whole = pl.BlockSpec(memory_space=pltpu.VMEM), pl.BlockSpec(memory_space=pl.ANY)
    gathered, base, passed = pl.pallas_call(
        lambda *refs: share_dy_kernel(*refs),
        out_shape=[
            jax.ShapeDtypeStruct((count, part, width), jnp.bfloat16),
            jax.ShapeDtypeStruct((part, width), jnp.float32),
            jax.ShapeDtypeStruct((2, part // 2, width), jnp.bfloat16),
        ],
        in_specs=[vmem] + [whole] * 4,
        out_specs=[whole, vmem, vmem],
        scratch_shapes=[
            pltpu.VMEM((2, part, width), jnp.bfloat16),
            pltpu.VMEM((2, part // 2, width), jnp.bfloat16),
            pltpu.VMEM((2, part // 2, width), jnp.bfloat16),
            pltpu.SemaphoreType.DMA((6,)),
            pltpu.SemaphoreType.DMA((6,)),
            pltpu.SemaphoreType.DMA((7,)),
        ],
        compiler_params=pltpu.CompilerParams(collective_id=8, has_side_effects=True, vmem_limit_bytes=LIMIT),
        name="share_dy",
    )(dy, down, side, below, middle)
    return gathered.reshape(part * count, width), base, passed


def fast_body(hidden, positions, gains, w_qkv, w_out, w_gate_up, w_down, cotangent):
    count = lax.axis_size("seq")
    index = lax.axis_index("seq")
    place = index.astype(jnp.int32).reshape(1)
    current = hidden[0]
    part_len, width = current.shape
    heads = H // count
    gain = gains[0]
    after = lax.optimization_barrier

    rows = w_qkv.shape[1]
    group = math.gcd(rows, HD)
    chunk = group // count
    per_head = HD // group
    normed_all, qkv_rows, out_cols, table, gate_up_part, down_part, scale_one = enter(
        current, gain[:1], positions, w_qkv[0], w_out[0], w_gate_up[0], w_down[0], count
    )
    gu_rows = w_gate_up.shape[1] // count
    gate_up = lax.all_gather(gate_up_part, "fsdp", axis=0, tiled=True)
    units = FF // count
    down_rows = w_down.shape[1]

    queries, keys_in, values_in = project_qkv(place, normed_all, qkv_rows, table, count)
    attn_flat, log_total, middle, scale_two, normed_two_all = attend(
        queries, keys_in, values_in, out_cols, current, gain[1:], count
    )
    flowing = cotangent[0]
    normed_two_all, dm_sent, down_part = after((normed_two_all, flowing.astype(jnp.bfloat16), down_part))
    down_cols = lax.all_gather(down_part, "fsdp", axis=0, tiled=True)
    dm_all = jnp.concatenate([dm_sent] + [neighbour(dm_sent, step) for step in range(1, count)], 0)
    both = matmul(normed_two_all, gate_up, 1, 1)
    gates = both.astype(jnp.bfloat16)
    activated = (jax.nn.silu(both[:, :units]) * both[:, units:]).astype(jnp.bfloat16)

    def owned(grad):
        return lax.psum_scatter(grad.astype(jnp.bfloat16), "fsdp", scatter_dimension=0, tiled=True)

    term_down = matmul(dm_all, activated, 0, 0).astype(jnp.bfloat16)
    dm_all, activated, term_down = after((dm_all, activated, term_down))
    grad_down = owned(term_down)
    dmiddle, gain_two, dy, term_gate_up, down_sent, from_side, from_below = norm_back(
        activated, down_cols, dm_all, gates, gate_up, flowing, middle, normed_two_all, scale_two, gain[1:], count
    )
    grad_gate_up = owned(term_gate_up)
    dy_all, base, passed = share_dy(dy, down_sent, from_side, from_below, middle, count)
    pieces = heads + 2
    picked = np.arange(pieces * HD).reshape(pieces * per_head, count, chunk).transpose(1, 0, 2).reshape(-1)
    pick = jnp.asarray(picked[:, None] == np.arange(pieces * HD)[None, :], jnp.bfloat16)
    djoint, djoint_turned, term_out, passed_on, down_slots = attend_back(
        queries, keys_in, values_in, attn_flat, log_total, dy_all, out_cols, table, pick, passed, grad_down, count
    )
    grad_out = owned(term_out)
    grad_piece, gain_total, term_qkv = leave(
        djoint, qkv_rows, current, scale_one, gain[:1], gain_two[None], djoint_turned, normed_all, count
    )
    grad_qkv = owned(term_qkv)
    grad_gate_up, grad_piece = after((grad_gate_up, grad_piece))
    half = upper_half(gu_rows)
    side = neighbour(grad_gate_up, 1)
    below = neighbour(grad_gate_up, 2)
    far_top = neighbour(side[:half], 2)
    far_bottom = neighbour(below[half:], 1)
    down_shard = join_pieces(place, grad_down, (down_slots,), count, down_rows, gu_rows)
    result, grad_hidden = last_sums(base, passed_on.reshape(part_len, width), dmiddle, grad_piece)
    out_slots = [neighbour(grad_out, step) for step in range(1, count)]
    grad_qkv, out_slots = after((grad_qkv, out_slots))
    qkv_slots = [neighbour(grad_qkv, step) for step in range(1, count)]
    gate_up_shard = join_rows(place, grad_gate_up, side, below, far_top, far_bottom, count)
    out_shard = join_pieces(place, grad_out, out_slots, count, down_rows, heads * HD)
    qkv_shard = join_pieces(place, grad_qkv, qkv_slots, count, chunk, width)
    gain_total = gain_total[None]
    return (
        result[None],
        grad_hidden[None],
        gain_total,
        qkv_shard[None],
        out_shard[None],
        gate_up_shard[None],
        down_shard[None],
    )


def fits(mesh):
    count, fsdp = mesh.shape["seq"], mesh.shape["fsdp"]
    rows = (H + 2 * KVH) * HD // fsdp
    return count == KVH == 4 and fsdp % 2 == 0 and fsdp & (fsdp - 1) == 0 and rows % HD == 0


def solution(mesh):
    placed = (
        P("fsdp", "seq", None),
        P("fsdp", "seq"),
        P(),
        P(None, "fsdp", None),
        P(None, "fsdp", None),
        P(None, "fsdp", None),
        P(None, "fsdp", None),
        P("fsdp", "seq", None),
    )
    fast = fits(mesh)
    return jax.shard_map(
        fast_body if fast else body,
        mesh=mesh,
        in_specs=placed,
        out_specs=(
            P("fsdp", "seq", None),
            P("fsdp", "seq", None),
            P(),
            P(None, "fsdp", None),
            P(None, "fsdp", None),
            P(None, "fsdp", None),
            P(None, "fsdp", None),
        ),
        check_vma=False,
    )
```

```python
import math

import jax
import jax.numpy as jnp
import numpy as np
from jax import lax
from jax.experimental import pallas as pl
from jax.experimental.pallas import tpu as pltpu
from jax.sharding import PartitionSpec as P


H = 32
KVH = 4
HD = 64
FF = 5632
LAYERS = 1


EPS = 1e-05


def rope_tables(position_ids):
    halfway = HD // 2
    frequency = jnp.exp(jnp.arange(halfway, dtype=jnp.float32) * (-2.0 * math.log(10000.0) / HD))
    angles = position_ids.astype(jnp.float32)[..., None] * frequency
    cosines = jnp.cos(angles)
    sines = jnp.sin(angles)
    return (
        jnp.concatenate([cosines, cosines], -1)[..., None, :],
        jnp.concatenate([sines, sines], -1)[..., None, :],
    )


def rotate(values, cosines, sines):
    halfway = values.shape[-1] // 2
    turned = jnp.concatenate([-values[..., halfway:], values[..., :halfway]], -1)
    return values * cosines + turned * sines


def unrotate(grads, cosines, sines):
    halfway = grads.shape[-1] // 2
    scaled = grads * sines
    return grads * cosines + jnp.concatenate([scaled[..., halfway:], -scaled[..., :halfway]], -1)


def normalize(values, gain):
    scale = lax.rsqrt(jnp.mean(values * values, -1, keepdims=True) + EPS)
    return ((values * scale * gain).astype(jnp.bfloat16), scale)


def normalize_back(grads, values, scale, gain):
    unit = values * scale
    gain_grad = jnp.sum((grads * unit).reshape(-1, unit.shape[-1]), 0)
    inner = grads * gain
    return (scale * (inner - unit * jnp.mean(inner * unit, -1, keepdims=True)), gain_grad)


def masked_scores(queries, keys_wide):
    scores = jnp.einsum(
        "qhd,khd->hqk", queries, keys_wide, preferred_element_type=jnp.float32
    ) * queries.shape[-1] ** (-0.5)
    length = queries.shape[0]
    causal = jnp.arange(length)[:, None] >= jnp.arange(length)[None, :]
    return jnp.where(causal[None], scores, -1e30)


def local_attend(operands):
    queries, keys_in, values_in = operands
    repeat_by = queries.shape[1] // keys_in.shape[1]
    keys_wide = jnp.repeat(keys_in, repeat_by, axis=1)
    values_wide = jnp.repeat(values_in, repeat_by, axis=1)
    scores = masked_scores(queries, keys_wide)
    peak = jnp.max(scores, -1, keepdims=True)
    log_total = peak[..., 0] + jnp.log(jnp.sum(jnp.exp(scores - peak), -1))
    weights = jnp.exp(scores - log_total[..., None]).astype(jnp.bfloat16)
    output = jnp.einsum("hqk,khd->qhd", weights, values_wide, preferred_element_type=jnp.float32)
    return (output.astype(jnp.bfloat16), log_total)


def local_attend_back(operands):
    queries, keys_in, values_in, output, log_total, dattn = operands
    length, kv_dev, head_dim = keys_in.shape
    repeat_by = queries.shape[1] // kv_dev
    keys_wide = jnp.repeat(keys_in, repeat_by, axis=1)
    values_wide = jnp.repeat(values_in, repeat_by, axis=1)
    scores = masked_scores(queries, keys_wide)
    probs = jnp.exp(scores - log_total[..., None])
    delta = jnp.sum(output.astype(jnp.float32) * dattn.astype(jnp.float32), -1).T
    dprob = jnp.einsum("qhd,khd->hqk", dattn, values_wide, preferred_element_type=jnp.float32)
    dscore = (probs * (dprob - delta[..., None])).astype(jnp.bfloat16)
    dqueries = jnp.einsum(
        "hqk,khd->qhd", dscore, keys_wide, preferred_element_type=jnp.float32
    ) * head_dim ** (-0.5)
    dkeys = jnp.einsum(
        "hqk,qhd->khd", dscore, queries, preferred_element_type=jnp.float32
    ) * head_dim ** (-0.5)
    dvalues = jnp.einsum(
        "hqk,qhd->khd", probs.astype(jnp.bfloat16), dattn, preferred_element_type=jnp.float32
    )

    def fold_heads(per_head):
        return jnp.sum(per_head.reshape(length, kv_dev, repeat_by, head_dim), 2).astype(
            jnp.bfloat16
        )

    return (dqueries.astype(jnp.bfloat16), fold_heads(dkeys), fold_heads(dvalues))


def project(inputs, weight):
    return lax.dot_general(
        inputs,
        lax.all_gather(weight, "fsdp", axis=0, tiled=True),
        (((1,), (1,)), ((), ())),
        preferred_element_type=jnp.float32,
    )


def project_back(grads, weight):
    shard_rows = lax.all_gather(weight, "fsdp", axis=0, tiled=True)
    picked = lax.slice_in_dim(grads, 0, shard_rows.shape[0], axis=1)
    return jnp.dot(picked, shard_rows, preferred_element_type=jnp.float32)


def weight_grad(grads, inputs, shard_size):
    picked = lax.slice_in_dim(grads, 0, shard_size * lax.axis_size("fsdp"), axis=1)
    summed = lax.psum_scatter(
        lax.dot_general(
            picked, inputs, (((0,), (0,)), ((), ())), preferred_element_type=jnp.float32
        ).astype(jnp.bfloat16),
        "fsdp",
        scatter_dimension=0,
        tiled=True,
    )
    return lax.psum(summed, "seq").astype(jnp.float32)


def backward_pair(grads, inputs, weight):
    wgrad = weight_grad(grads, inputs, weight.shape[0])
    return (project_back(grads, weight), wgrad)


def body(hidden, positions, gains, w_qkv, w_out, w_gate_up, w_down, cotangent):
    seq_count, part_len, model_width = hidden.shape
    row_count = seq_count * part_len
    group_count = lax.axis_size("seq")
    full_len = part_len * group_count
    heads_dev = H // group_count
    share = H // KVH
    kv_dev = max(1, heads_dev // share)
    first_kv = np.arange(group_count) * heads_dev // share
    slot_table = np.concatenate(
        [
            first_kv[:, None] + np.arange(kv_dev)[None, :],
            KVH + first_kv[:, None] + np.arange(kv_dev)[None, :],
        ],
        1,
    ).reshape(-1)
    slot_onehot = jnp.asarray(
        (slot_table[:, None] == np.arange(2 * KVH)[None, :]).astype(np.float32), jnp.bfloat16
    )
    cosines, sines = rope_tables(positions)
    layer_index = 0
    gain = gains[layer_index]
    normed, scale_one = normalize(hidden, gain[0])
    normed_flat = normed.reshape(row_count, model_width)
    joint = project(normed_flat, w_qkv[layer_index]).reshape(seq_count, part_len, -1)
    queries = joint[..., : H * HD].reshape(seq_count, part_len, H, HD)
    keys_in = joint[..., H * HD : (H + KVH) * HD].reshape(seq_count, part_len, KVH, HD)
    values_in = joint[..., (H + KVH) * HD :].reshape(seq_count, part_len, KVH, HD)
    q_rot = rotate(queries, cosines, sines).astype(jnp.bfloat16)
    kv_all = jnp.concatenate(
        [rotate(keys_in, cosines, sines).astype(jnp.bfloat16), values_in.astype(jnp.bfloat16)], 2
    )
    q_send = q_rot.reshape(seq_count, part_len, group_count, heads_dev * HD)
    kv_send = jnp.take(kv_all, slot_table, axis=2).reshape(
        seq_count, part_len, group_count, 2 * kv_dev * HD
    )
    q_heads = lax.all_to_all(q_send, "seq", split_axis=2, concat_axis=1, tiled=True)
    kv_heads = lax.all_to_all(kv_send, "seq", split_axis=2, concat_axis=1, tiled=True)
    q_heads = q_heads.reshape(seq_count, full_len, heads_dev, HD)
    kv_heads = kv_heads.reshape(seq_count, full_len, 2 * kv_dev, HD)
    k_heads = kv_heads[:, :, :kv_dev]
    v_heads = kv_heads[:, :, kv_dev:]
    o_heads, log_total = lax.map(local_attend, (q_heads, k_heads, v_heads))
    o_back = lax.all_to_all(
        o_heads.reshape(seq_count, full_len, 1, heads_dev * HD),
        "seq",
        split_axis=1,
        concat_axis=2,
        tiled=True,
    )
    attn_flat = o_back.reshape(row_count, model_width)
    middle = hidden + project(attn_flat, w_out[layer_index]).reshape(
        seq_count, part_len, model_width
    )
    normed_two, scale_two = normalize(middle, gain[1])
    normed_two_flat = normed_two.reshape(row_count, model_width)
    both = project(normed_two_flat, w_gate_up[layer_index])
    gate_part = both[:, :FF]
    up_part = both[:, FF:]
    activated = (jax.nn.silu(gate_part) * up_part).astype(jnp.bfloat16)
    result = middle + project(activated, w_down[layer_index]).reshape(
        seq_count, part_len, model_width
    )
    saved = [
        (
            hidden,
            normed_flat,
            scale_one,
            q_heads,
            k_heads,
            v_heads,
            o_heads,
            log_total,
            attn_flat,
            middle,
            normed_two_flat,
            scale_two,
            gate_part,
            up_part,
            activated,
        )
    ]
    flowing = cotangent
    grads_qkv = [None] * LAYERS
    grads_out = [None] * LAYERS
    grads_gate_up = [None] * LAYERS
    grads_down = [None] * LAYERS
    gain_terms = [None] * LAYERS
    for layer_index in reversed(range(LAYERS)):
        (
            layer_in,
            normed_flat,
            scale_one,
            q_heads,
            k_heads,
            v_heads,
            o_heads,
            log_total,
            attn_flat,
            middle,
            normed_two_flat,
            scale_two,
            gate_part,
            up_part,
            activated,
        ) = saved[layer_index]
        gain = gains[layer_index]
        dm_cast = flowing.reshape(row_count, model_width).astype(jnp.bfloat16)
        dact, grads_down[layer_index] = backward_pair(dm_cast, activated, w_down[layer_index])
        sigma = jax.nn.sigmoid(gate_part)
        dgate = dact * up_part * sigma * (1.0 + gate_part * (1.0 - sigma))
        dup = dact * gate_part * sigma
        dgu = jnp.concatenate([dgate, dup], 1).astype(jnp.bfloat16)
        dnormed_two, grads_gate_up[layer_index] = backward_pair(
            dgu, normed_two_flat, w_gate_up[layer_index]
        )
        dnormed_two = dnormed_two.reshape(seq_count, part_len, model_width)
        dmid_norm, gain_two = normalize_back(dnormed_two, middle, scale_two, gain[1])
        dmiddle = flowing + dmid_norm
        dy_cast = dmiddle.reshape(row_count, model_width).astype(jnp.bfloat16)
        dattn_wide, grads_out[layer_index] = backward_pair(dy_cast, attn_flat, w_out[layer_index])
        dattn = dattn_wide.astype(jnp.bfloat16)
        dattn_heads = lax.all_to_all(
            dattn.reshape(seq_count, part_len, group_count, heads_dev * HD),
            "seq",
            split_axis=2,
            concat_axis=1,
            tiled=True,
        )
        dattn_heads = dattn_heads.reshape(seq_count, full_len, heads_dev, HD)
        dq_heads, dk_heads, dv_heads = lax.map(
            local_attend_back, (q_heads, k_heads, v_heads, o_heads, log_total, dattn_heads)
        )
        dkv_heads = jnp.concatenate([dk_heads, dv_heads], 2).reshape(
            seq_count, full_len, 1, 2 * kv_dev * HD
        )
        dq_tok, dkv_tok = (
            lax.all_to_all(
                dq_heads.reshape(seq_count, full_len, 1, heads_dev * HD),
                "seq",
                split_axis=1,
                concat_axis=2,
                tiled=True,
            ),
            lax.all_to_all(dkv_heads, "seq", split_axis=1, concat_axis=2, tiled=True),
        )
        dqueries = dq_tok.reshape(seq_count, part_len, H, HD)
        dkv_sum = jnp.einsum(
            "stnd,nm->stmd",
            dkv_tok.reshape(seq_count, part_len, group_count * 2 * kv_dev, HD),
            slot_onehot,
            preferred_element_type=jnp.float32,
        )
        dq_pre = unrotate(dqueries, cosines, sines)
        dk_pre = unrotate(dkv_sum[:, :, :KVH], cosines, sines)
        dvalues = dkv_sum[:, :, KVH:]
        djoint = jnp.concatenate(
            [
                dq_pre.reshape(row_count, -1),
                dk_pre.reshape(row_count, -1),
                dvalues.reshape(row_count, -1),
            ],
            1,
        ).astype(jnp.bfloat16)
        dnormed, grads_qkv[layer_index] = backward_pair(djoint, normed_flat, w_qkv[layer_index])
        dnormed = dnormed.reshape(seq_count, part_len, model_width)
        dcur_norm, gain_one = normalize_back(dnormed, layer_in, scale_one, gain[0])
        gain_terms[layer_index] = jnp.stack([gain_one, gain_two])
        flowing = dmiddle + dcur_norm
    gain_total = lax.psum(jnp.stack(gain_terms), ("fsdp", "seq"))
    return (
        result,
        flowing,
        gain_total,
        jnp.stack(grads_qkv),
        jnp.stack(grads_out),
        jnp.stack(grads_gate_up),
        jnp.stack(grads_down),
    )


def neighbour(values, step):
    count = lax.axis_size("seq")
    return lax.ppermute(values, "seq", [(i, i ^ step) for i in range(count)])


def matmul(left, right, left_dim, right_dim):
    return lax.dot_general(
        left, right, (((left_dim,), (right_dim,)), ((), ())), preferred_element_type=jnp.float32
    )


ROOT = HD ** (-0.5)
LIMIT = 60 * 1024 * 1024


def swap_halves(values):
    width = values.shape[1]
    half = HD // 2
    column = lax.broadcasted_iota(jnp.int32, values.shape, 1)
    return jnp.where(
        column % HD < half, pltpu.roll(values, width - half, 1), pltpu.roll(values, half, 1)
    )


def spread_tables(table, pairs, last):
    half = HD // 2
    cosines, sines = table[:, :half], table[:, half:]
    ones, zeros = jnp.ones_like(table), jnp.zeros_like(table)
    tail = [[cosines, cosines, ones], [-sines, sines, zeros]] if last else [[], []]
    if not pairs:
        return jnp.concatenate(tail[0], 1), jnp.concatenate(tail[1], 1)
    cosines = [jnp.concatenate([cosines] * 4, 1)] * pairs
    sines = [jnp.concatenate([-sines, sines] * 2, 1)] * pairs
    if last:
        cosines.append(jnp.concatenate(tail[0], 1))
        sines.append(jnp.concatenate(tail[1], 1))
    return jnp.concatenate(cosines, 1), jnp.concatenate(sines, 1)


MESH = pl.DeviceIdType.MESH


def seq_peer(step):
    return {"seq": lax.axis_index("seq") ^ step}


def fsdp_peer(place):
    return {"fsdp": place}


def remote(source, target, sems, slot, peer):
    return pltpu.make_async_remote_copy(
        src_ref=source,
        dst_ref=target,
        send_sem=sems[0].at[slot],
        recv_sem=sems[1].at[slot],
        device_id=peer,
        device_id_type=MESH,
    )


def gather_copies(own, slots, half, sems, base=0):
    top, bottom = pl.ds(0, half), pl.ds(half, own.shape[0] - half)

    def slot(step, rows):
        return slots.at[step].at[rows]

    return [
        remote(own.at[top], slot(1, top), sems, base, seq_peer(1)),
        remote(own.at[bottom], slot(2, bottom), sems, base + 1, seq_peer(2)),
        remote(own.at[bottom], slot(1, bottom), sems, base + 2, seq_peer(1)),
        remote(own.at[top], slot(2, top), sems, base + 3, seq_peer(2)),
        remote(slot(1, top), slot(3, top), sems, base + 4, seq_peer(2)),
        remote(slot(2, bottom), slot(3, bottom), sems, base + 5, seq_peer(1)),
    ]


def greet(peers):
    barrier = pltpu.get_barrier_semaphore()
    for peer in peers:
        pl.semaphore_signal(barrier, inc=1, device_id=peer, device_id_type=MESH)
    pl.semaphore_wait(barrier, len(peers))


def sum_copies(sent, side, below, far, half, sems, passed=None):
    top, bottom = pl.ds(0, half), pl.ds(half, half)
    return [
        remote(sent.at[3].at[top], side.at[1], sems, 0, seq_peer(1)),
        remote(sent.at[3].at[bottom], below.at[1], sems, 1, seq_peer(2)),
        remote(sent.at[2].at[bottom], below.at[0], sems, 2, seq_peer(2)),
        remote(sent.at[1].at[top], side.at[0], sems, 3, seq_peer(1)),
        remote(passed.at[0] if passed is not None else sent.at[2].at[top], far.at[0], sems, 4, seq_peer(2)),
        remote(passed.at[1] if passed is not None else sent.at[1].at[bottom], far.at[1], sems, 5, seq_peer(1)),
    ]


def pass_sums(turn, step, partial, sums, sent_ref, side_ref, below_ref, own_ref, half):
    wide, narrow = jnp.float32, jnp.bfloat16
    last = len(sums) // 2

    @pl.when(turn == last)
    def _():
        own_ref[...] = partial

    @pl.when(turn < last)
    def _():
        sent_ref[step] = partial.astype(narrow)

    @pl.when(turn == 0)
    def _():
        sums[0].start()
        sums[1].start()

    @pl.when(turn == 1)
    def _():
        sums[2].start()

    @pl.when(turn == 2)
    def _():
        sums[3].start()
        sums[0].wait_recv()
        sent_ref[2, :half] = (sent_ref[2, :half].astype(wide) + side_ref[1].astype(wide)).astype(narrow)
        sums[4].start()
        sums[1].wait_recv()
        sent_ref[1, half:] = (sent_ref[1, half:].astype(wide) + below_ref[1].astype(wide)).astype(narrow)
        sums[5].start()


def end_sums(sums, side_ref, below_ref, far_ref, own_ref, half):
    wide = jnp.float32
    sums[2].wait_recv()
    sums[3].wait_recv()
    own_ref[:half] += side_ref[0].astype(wide)
    own_ref[half:] += below_ref[0].astype(wide)
    sums[4].wait_recv()
    own_ref[:half] += far_ref[0].astype(wide)
    sums[5].wait_recv()
    own_ref[half:] += far_ref[1].astype(wide)


def share_own(own_ref, all_ref, half, sems, before):
    copies = gather_copies(own_ref, all_ref, half, sems, len(before))
    for copy in copies[:4]:
        copy.start()
    copies[0].wait_recv()
    copies[4].start()
    copies[1].wait_recv()
    copies[5].start()
    for copy in copies[2:]:
        copy.wait_recv()
    for copy in before + copies:
        copy.wait_send()


def enter_kernel(
    count, current_in, gain_ref, positions_ref, shard_ref, out_shard_ref, gate_up_ref, down_ref,
    all_ref, rows_ref, out_ref, table_ref, gate_up_part_ref, down_part_ref, scale_ref,
    current_ref, normed_ref, spots_ref, held_ref, part_ref, held_down,
    send_sems, recv_sems, spot_send, spot_recv, item_up, item_down, item_side, item_recv, local_sem,
):
    part, _ = current_ref.shape
    heads = H // count
    pieces = heads + 2
    items = pieces + lax.axis_size("fsdp")
    per_shard = shard_ref.shape[0] // HD
    out_rows, columns = out_shard_ref.shape[0], heads * HD
    chips = lax.axis_size("fsdp") // 2
    index = lax.axis_index("seq")
    place = lax.axis_index("fsdp")
    chip, core = place // 2, place % 2
    sems = (send_sems, recv_sems)

    take_current = pltpu.make_async_copy(current_in, current_ref, local_sem.at[items + 4])
    take_current.start()
    barrier = pltpu.get_barrier_semaphore()
    for peer in [seq_peer(step) for step in range(1, count)] + [fsdp_peer(place ^ 1)]:
        pl.semaphore_signal(barrier, inc=1, device_id=peer, device_id_type=MESH)

    @pl.when(chip > 0)
    def _():
        pl.semaphore_signal(barrier, inc=1, device_id=fsdp_peer(place - 2), device_id_type=MESH)

    @pl.when(chip < chips - 1)
    def _():
        pl.semaphore_signal(barrier, inc=1, device_id=fsdp_peer(place + 2), device_id_type=MESH)

    greetings = count + (chip > 0).astype(jnp.int32) + (chip < chips - 1).astype(jnp.int32)
    pl.semaphore_wait(barrier, greetings)

    part_rows = part_ref.shape[0]
    take = pltpu.make_async_copy(
        gate_up_ref.at[pl.ds(pl.multiple_of(index * part_rows, part_rows), part_rows)], part_ref, local_sem.at[items + 1]
    )
    take.start()
    take_down = pltpu.make_async_copy(down_ref, held_down, local_sem.at[items + 3])
    take_down.start()

    def qkv_item(item):
        block = jnp.where(
            item < heads, index * heads + item, jnp.where(item == heads, H + index, H + KVH + index)
        )
        source = shard_ref.at[pl.ds(pl.multiple_of(block % per_shard * HD, HD), HD)]
        return block // per_shard, source, rows_ref.at[pl.ds(pl.multiple_of(item * HD, HD), HD)], item

    def out_item(item):
        source = out_shard_ref.at[:, pl.ds(pl.multiple_of(index * columns, columns), columns)]
        target = out_ref.at[pl.ds(pl.multiple_of(item * out_rows, out_rows), out_rows)]
        return item, source, target, item + pieces

    kinds = ((qkv_item, pieces), (out_item, items - pieces))

    def item_copy(source, target, slot, sem, peer):
        return pltpu.make_async_remote_copy(
            src_ref=source,
            dst_ref=target,
            send_sem=sem.at[slot],
            recv_sem=item_recv.at[slot],
            device_id=fsdp_peer(peer),
            device_id_type=MESH,
        )

    def pass_on(source, target, slot, owner_chip, act):
        @pl.when((chip >= owner_chip) & (chip < chips - 1))
        def _():
            act(item_copy(source, target, slot, item_up, place + 2))

        @pl.when((chip <= owner_chip) & (chip > 0))
        def _():
            act(item_copy(source, target, slot, item_down, place - 2))

        act(item_copy(source, target, slot, item_side, place ^ 1))

    def send_own(item_of):
        def body(item, carry):
            owner, source, target, slot = item_of(item)

            @pl.when(place == owner)
            def _():
                pass_on(source, target, slot, owner // 2, lambda copy: copy.start())
                pltpu.make_async_copy(source, target, local_sem.at[slot]).start()

            return carry

        return body

    def pass_far(item_of, distance):
        def body(item, carry):
            owner, _, target, slot = item_of(item)
            owner_chip = owner // 2
            apart = jnp.where(chip > owner_chip, chip - owner_chip, owner_chip - chip)

            @pl.when((apart == distance) & (core == owner % 2))
            def _():
                item_copy(target, target, slot, item_side, place ^ 1).wait_recv()
                pass_on(target, target, slot, owner_chip, lambda copy: copy.start())

            return carry

        return body

    for item_of, number in kinds:
        lax.fori_loop(0, number, send_own(item_of), 0)
    take_current.wait()
    current = current_ref[...]
    scale = lax.rsqrt(jnp.mean(current * current, 1, keepdims=True) + EPS)
    scale_ref[...] = jnp.broadcast_to(scale, scale_ref.shape)
    normed_ref[...] = (current * scale * gain_ref[...]).astype(jnp.bfloat16)
    copies = gather_copies(normed_ref, all_ref, part // 2, sems)
    for copy in copies[:4]:
        copy.start()
    spots_ref[...] = jnp.broadcast_to(positions_ref[...].astype(jnp.float32), spots_ref.shape)
    held_ref[0] = spots_ref[...]
    spot_copies = [
        remote(spots_ref, held_ref.at[step], (spot_send, spot_recv), step - 1, seq_peer(step))
        for step in range(1, count)
    ]
    for copy in spot_copies:
        copy.start()
    own = pltpu.make_async_copy(normed_ref, all_ref.at[0], local_sem.at[items])
    own.start()
    for distance in range(1, chips):
        for item_of, number in kinds:
            lax.fori_loop(0, number, pass_far(item_of, distance), 0)
            if distance == 1 and item_of is qkv_item:
                copies[0].wait_recv()
                copies[4].start()
                copies[1].wait_recv()
                copies[5].start()

    take.wait()
    put = pltpu.make_async_copy(part_ref, gate_up_part_ref, local_sem.at[items + 2])
    put.start()
    take_down.wait()
    columns_here = part_rows
    for device in range(count):

        @pl.when(index == device)
        def _():
            down_part_ref[...] = jnp.concatenate(
                [
                    held_down[:, start + device * columns_here : start + (device + 1) * columns_here]
                    for start in range(0, held_down.shape[1], count * columns_here)
                ],
                1,
            )

    for copy in spot_copies:
        copy.wait()
    half = HD // 2
    for step in range(count):
        spots = held_ref[step][:1]
        frequency = jnp.exp(
            lax.broadcasted_iota(jnp.int32, (half, 1), 0).astype(jnp.float32) * (-2.0 * math.log(10000.0) / HD)
        )
        angles = frequency * spots
        turned = jnp.concatenate([jnp.cos(angles), jnp.sin(angles)], 0)
        table_ref[pl.ds(step * part, part), :] = jnp.transpose(turned)

    def finish(item_of):
        def body(item, carry):
            owner, source, target, slot = item_of(item)

            @pl.when(core != owner % 2)
            def _():
                item_copy(target, target, slot, item_side, place ^ 1).wait_recv()

            @pl.when(place == owner)
            def _():
                pltpu.make_async_copy(source, target, local_sem.at[slot]).wait()

            @pl.when(core == owner % 2)
            def _():
                pass_on(target, target, slot, owner // 2, lambda copy: copy.wait_send())

            return carry

        return body

    for item_of, number in kinds:
        lax.fori_loop(0, number, finish(item_of), 0)
    own.wait()
    put.wait()
    for copy in copies[2:]:
        copy.wait_recv()
    for copy in copies:
        copy.wait_send()


def enter(current, gain, positions, shard, out_shard, gate_up, down, count):
    part, width = current.shape
    length = part * count
    heads = H // count
    pieces = heads + 2
    items = pieces + lax.axis_size("fsdp")
    vmem = pl.BlockSpec(memory_space=pltpu.VMEM)
    whole = pl.BlockSpec(memory_space=pl.ANY)
    part_shape = (gate_up.shape[0] // count, width)
    gathered, rows, out_cols, table, gate_up_part, down_part, scale = pl.pallas_call(
        lambda *refs: enter_kernel(count, *refs),
        out_shape=(
            jax.ShapeDtypeStruct((count, part, width), jnp.bfloat16),
            jax.ShapeDtypeStruct((pieces * HD, width), jnp.bfloat16),
            jax.ShapeDtypeStruct((out_shard.shape[0] * (items - pieces), heads * HD), jnp.bfloat16),
            jax.ShapeDtypeStruct((length, HD), jnp.float32),
            jax.ShapeDtypeStruct(part_shape, gate_up.dtype),
            jax.ShapeDtypeStruct((down.shape[0], down.shape[1] // count), down.dtype),
            jax.ShapeDtypeStruct((part, 128), jnp.float32),
        ),
        in_specs=[whole] + [vmem] * 2 + [whole] * 4,
        out_specs=[whole] + [vmem] * 3 + [whole] + [vmem] * 2,
        scratch_shapes=[
            pltpu.VMEM((part, width), jnp.float32),
            pltpu.VMEM((part, width), jnp.bfloat16),
            pltpu.VMEM((8, part), jnp.float32),
            pltpu.VMEM((count, 8, part), jnp.float32),
            pltpu.VMEM(part_shape, gate_up.dtype),
            pltpu.VMEM(down.shape, down.dtype),
            pltpu.SemaphoreType.DMA((6,)),
            pltpu.SemaphoreType.DMA((6,)),
            pltpu.SemaphoreType.DMA((count - 1,)),
            pltpu.SemaphoreType.DMA((count - 1,)),
            pltpu.SemaphoreType.DMA((items,)),
            pltpu.SemaphoreType.DMA((items,)),
            pltpu.SemaphoreType.DMA((items,)),
            pltpu.SemaphoreType.DMA((items,)),
            pltpu.SemaphoreType.DMA((items + 5,)),
        ],
        compiler_params=pltpu.CompilerParams(collective_id=1, has_side_effects=True, vmem_limit_bytes=LIMIT),
        name="enter",
    )(current, gain, positions, shard, out_shard, gate_up, down)
    return gathered.reshape(length, width), rows, out_cols, table, gate_up_part, down_part, scale


def qkv_kernel(index_ref, normed_ref, weight_ref, table_ref, q_ref, k_ref, v_ref):
    heads = q_ref.shape[0]
    joint = matmul(normed_ref[...], weight_ref[...], 1, 1)
    cosines, sines = spread_tables(table_ref[...], heads // 2, True)
    turned = joint * cosines + swap_halves(joint) * sines
    for head in range(heads):
        rounded = turned[:, head * HD : (head + 1) * HD].astype(jnp.bfloat16).astype(jnp.float32)
        q_ref[head] = (rounded * ROOT).astype(jnp.bfloat16)
    k_ref[...] = turned[:, heads * HD : (heads + 1) * HD].astype(jnp.bfloat16)
    v_ref[...] = turned[:, (heads + 1) * HD :].astype(jnp.bfloat16)


def project_qkv(index, normed, weight, table, count):
    length, width = normed.shape
    part = length // count
    heads = weight.shape[0] // HD - 2
    return pl.pallas_call(
        qkv_kernel,
        out_shape=(
            jax.ShapeDtypeStruct((heads, length, HD), jnp.bfloat16),
            jax.ShapeDtypeStruct((length, HD), jnp.bfloat16),
            jax.ShapeDtypeStruct((length, HD), jnp.bfloat16),
        ),
        grid_spec=pltpu.PrefetchScalarGridSpec(
            num_scalar_prefetch=1,
            grid=(count,),
            in_specs=[
                pl.BlockSpec((part, width), lambda i, s: (i, 0)),
                pl.BlockSpec(weight.shape, lambda i, s: (0, 0)),
                pl.BlockSpec((part, table.shape[1]), lambda i, s: (i, 0)),
            ],
            out_specs=[
                pl.BlockSpec((heads, part, HD), lambda i, s: (0, i ^ s[0], 0)),
                pl.BlockSpec((part, HD), lambda i, s: (i ^ s[0], 0)),
                pl.BlockSpec((part, HD), lambda i, s: (i ^ s[0], 0)),
            ],
        ),
        compiler_params=pltpu.CompilerParams(vmem_limit_bytes=LIMIT),
        name="project_qkv",
    )(index, normed, weight, table)


def attend_kernel(
    count, q_ref, k_ref, v_ref, weight_ref, current_ref, gain_ref,
    attn_ref, lse_ref, middle_ref, scale_ref, all_ref,
    held_ref, sent_ref, side_ref, below_ref, far_ref, two_ref, send_sems, recv_sems, own_sem,
):
    heads, _, _ = q_ref.shape
    part, _ = current_ref.shape
    half = part // 2
    index = lax.axis_index("seq")
    top, bottom = pl.ds(0, half), pl.ds(half, half)
    sems = (send_sems, recv_sems)
    greet([seq_peer(1), seq_peer(2)])
    sums = sum_copies(sent_ref, side_ref, below_ref, far_ref, half, sems)
    row = lax.broadcasted_iota(jnp.int32, (part, part), 0)
    column = lax.broadcasted_iota(jnp.int32, (part, part), 1)

    def one_part(turn, carry):
        step = count - 1 - turn
        here = step ^ index
        rows_here = pl.ds(pl.multiple_of(here * part, part), part)
        rows_step = pl.ds(pl.multiple_of(step * part, part), part)
        for block in range(count):

            @pl.when(here == block)
            def _():
                before = block * part
                seen = before + part
                keys_in, values_in = k_ref[:seen], v_ref[:seen]

                def one_head(head, carry):
                    scores = matmul(q_ref[head, before:seen, :], keys_in, 1, 1)
                    last = jnp.where(row >= column, scores[:, before:], -1e30)
                    scores = jnp.concatenate([scores[:, :before], last], 1) if block else last
                    peak = jnp.max(scores, 1, keepdims=True)
                    weights = jnp.exp(scores - peak)
                    total = jnp.sum(weights, 1, keepdims=True)
                    output = matmul(weights.astype(jnp.bfloat16), values_in, 1, 0) / total
                    held_ref[head] = output.astype(jnp.bfloat16)
                    log_total = jnp.broadcast_to(peak + jnp.log(total), (part, 128))
                    lse_ref[pl.ds(head, 1), before:seen] = jnp.transpose(log_total)[:1]
                    return carry

                lax.fori_loop(0, heads, one_head, 0, unroll=2)

        attn = jnp.concatenate([held_ref[head] for head in range(heads)], 1)
        attn_ref[rows_step, :] = attn
        partial = matmul(attn, weight_ref[...], 1, 1)

        pass_sums(turn, step, partial, sums, sent_ref, side_ref, below_ref, middle_ref, half)
        return carry

    lax.fori_loop(0, count, one_part, 0)
    end_sums(sums, side_ref, below_ref, far_ref, middle_ref, half)
    middle_ref[...] += current_ref[...]
    middle = middle_ref[...]
    scale = lax.rsqrt(jnp.mean(middle * middle, 1, keepdims=True) + EPS)
    scale_ref[...] = jnp.broadcast_to(scale, scale_ref.shape)
    two_ref[...] = (middle * scale * gain_ref[...]).astype(jnp.bfloat16)
    own = pltpu.make_async_copy(two_ref, all_ref.at[0], own_sem)
    share_own(two_ref, all_ref, half, sems, sums)
    own.start()
    own.wait()


def attend(queries, keys_in, values_in, weight, current, gain, count):
    heads, length, _ = queries.shape
    part, width = current.shape
    vmem = pl.BlockSpec(memory_space=pltpu.VMEM)
    attn, lse, middle, scale, gathered = pl.pallas_call(
        lambda *refs: attend_kernel(count, *refs),
        out_shape=(
            jax.ShapeDtypeStruct((length, heads * HD), jnp.bfloat16),
            jax.ShapeDtypeStruct((heads, length), jnp.float32),
            jax.ShapeDtypeStruct((part, width), jnp.float32),
            jax.ShapeDtypeStruct((part, 128), jnp.float32),
            jax.ShapeDtypeStruct((count, part, width), jnp.bfloat16),
        ),
        in_specs=[vmem] * 6,
        out_specs=[vmem] * 4 + [pl.BlockSpec(memory_space=pl.ANY)],
        scratch_shapes=[
            pltpu.VMEM((heads, part, HD), jnp.bfloat16),
            pltpu.VMEM((count, part, width), jnp.bfloat16),
            pltpu.VMEM((2, part // 2, width), jnp.bfloat16),
            pltpu.VMEM((2, part // 2, width), jnp.bfloat16),
            pltpu.VMEM((2, part // 2, width), jnp.bfloat16),
            pltpu.VMEM((part, width), jnp.bfloat16),
            pltpu.SemaphoreType.DMA((12,)),
            pltpu.SemaphoreType.DMA((12,)),
            pltpu.SemaphoreType.DMA,
        ],
        compiler_params=pltpu.CompilerParams(collective_id=2, has_side_effects=True, vmem_limit_bytes=LIMIT),
        name="attend",
    )(queries, keys_in, values_in, weight, current, gain)
    return attn, lse, middle, scale, gathered.reshape(length, width)


def share_start(copies):
    for group in copies:
        group[0].start()
        group[1].start()
    for group in copies:
        group[2].start()
        group[3].start()


def share_on(group):
    group[0].wait_recv()
    group[4].start()
    group[1].wait_recv()
    group[5].start()


def share_end(copies):
    for group in copies:
        for copy in group[2:]:
            copy.wait_recv()
    for group in copies:
        for copy in group:
            copy.wait_send()


def upper_half(rows):
    return -(-(rows // 2) // 16) * 16


def attend_back_kernel(
    count, q_in, k_in, v_in, attn_in, lse_in, dy_ref, weight_in, table_in, pick_ref, passed_ref, shard_ref,
    out_ref, turned_ref, term_ref, far_ref, slot_ref,
    q_ref, k_ref, v_ref, attn_ref, lse_ref, weight_ref, table_ref,
    do_ref, delta_ref, dq_ref, dk_ref, dv_ref, held_dy, held_pick,
    send_sems, recv_sems, load_sems,
):
    heads, length, _ = q_in.shape
    part = length // count
    wide = jnp.float32
    index = lax.axis_index("seq")
    load_weight = pltpu.make_async_copy(weight_in, weight_ref, load_sems.at[count + 1])
    load_weight.start()
    greet([seq_peer(1), seq_peer(2)])
    sems = (send_sems, recv_sems)
    sums = [
        remote(passed_ref.at[0], far_ref.at[0], sems, 6, seq_peer(2)),
        remote(passed_ref.at[1], far_ref.at[1], sems, 7, seq_peer(1)),
    ]
    group = gather_copies(shard_ref, slot_ref, upper_half(shard_ref.shape[0]), sems)
    share_start([group])
    for copy in sums:
        copy.start()

    def load_dy(step):
        rows = pl.ds(pl.multiple_of(step * part, part), part)
        return pltpu.make_async_copy(dy_ref.at[rows], held_dy.at[rows], load_sems.at[step])

    load = pltpu.make_async_copy(pick_ref, held_pick, load_sems.at[count])
    sources, targets = (attn_in, q_in, k_in, v_in, lse_in, table_in), (attn_ref, q_ref, k_ref, v_ref, lse_ref, table_ref)
    loads = [
        pltpu.make_async_copy(source, target, load_sems.at[count + 2 + number])
        for number, (source, target) in enumerate(zip(sources, targets))
    ]
    load_dy(index).start()
    for copy in loads:
        copy.start()
    for here in range(1, count):
        load_dy(here ^ index).start()
    load.start()
    load_weight.wait()
    for copy in loads:
        copy.wait()
    dk_ref[...] = jnp.zeros_like(dk_ref)
    dv_ref[...] = jnp.zeros_like(dv_ref)
    owner = lax.broadcasted_iota(jnp.int32, (heads, heads * HD), 1) // HD
    same = (owner == lax.broadcasted_iota(jnp.int32, (heads, heads * HD), 0)).astype(wide)
    row = lax.broadcasted_iota(jnp.int32, (part, part), 0)
    column = lax.broadcasted_iota(jnp.int32, (part, part), 1)

    def unturn(grads, cosines, sines):
        return grads * cosines + swap_halves(grads * sines)

    def one_part(here, carry):
        spot = here ^ index
        rows_here = pl.ds(pl.multiple_of(spot * part, part), part)
        load_dy(spot).wait()
        dattn = matmul(held_dy[rows_here, :], weight_ref[...], 1, 0).astype(jnp.bfloat16)
        product = dattn.astype(wide) * attn_ref[rows_here, :].astype(wide)
        delta_ref[...] = lax.dot_general(
            same, product, (((1,), (1,)), ((), ())), precision=lax.Precision.HIGHEST, preferred_element_type=wide
        )
        for head in range(heads):
            do_ref[head] = dattn[:, head * HD : (head + 1) * HD]
        for block in range(count):

            @pl.when(here == block)
            def _():
                before = block * part
                seen = before + part
                keys_in, values_in = k_ref[:seen], v_ref[:seen]

                def one_head(head, carry):
                    query, dout = q_ref[head, before:seen, :], do_ref[head]
                    scores = matmul(keys_in, query, 1, 1)
                    last = jnp.where(row <= column, scores[before:], -1e30)
                    scores = jnp.concatenate([scores[:before], last], 0) if block else last
                    probs = jnp.exp(scores - lse_ref[pl.ds(head, 1), before:seen])
                    dprob = matmul(values_in, dout, 1, 1)
                    dscore = (probs * (dprob - delta_ref[pl.ds(head, 1), :])).astype(jnp.bfloat16)
                    dv_ref[:seen] += matmul(probs.astype(jnp.bfloat16), dout, 1, 0)
                    dk_ref[:seen] += matmul(dscore, query, 1, 0)
                    dq_ref[head] = (matmul(dscore, keys_in, 0, 0) * ROOT).astype(jnp.bfloat16)
                    return carry

                lax.fori_loop(0, heads, one_head, 0, unroll=2)

        dq = jnp.concatenate([dq_ref[head] for head in range(heads)], 1).astype(wide)
        dq = unturn(dq, *spread_tables(table_ref[rows_here, :], heads // 2, False))
        out_ref[rows_here, : heads * HD] = dq.astype(jnp.bfloat16)

        @pl.when(here == 1)
        def _():
            share_on(group)

        return carry

    lax.fori_loop(0, count, one_part, 0)
    for block in range(count):
        rows_there = pl.ds(pl.multiple_of((block ^ index) * part, part), part)
        rows_block = slice(block * part, (block + 1) * part)
        both = jnp.concatenate([dk_ref[rows_block], dv_ref[rows_block]], 1).astype(jnp.bfloat16).astype(wide)
        both = unturn(both, *spread_tables(table_ref[rows_there, :], 0, True))
        out_ref[rows_there, heads * HD :] = both.astype(jnp.bfloat16)
    load.wait()
    chosen = matmul(held_pick[...], out_ref[...], 1, 1).astype(jnp.bfloat16)
    size = turned_ref.shape[1]
    for block in range(count):
        turned_ref[block] = chosen[block * size : (block + 1) * size]
    tile = 2 * 128

    def one_tile(number, carry):
        columns = pl.ds(pl.multiple_of(number * tile, tile), tile)
        term_ref[columns, :] = matmul(held_dy[:, columns], attn_ref[...], 0, 0).astype(jnp.bfloat16)
        return carry

    lax.fori_loop(0, held_dy.shape[1] // tile, one_tile, 0)
    for copy in sums:
        copy.wait_recv()
    share_end([group])
    for copy in sums:
        copy.wait_send()


def attend_back(queries, keys_in, values_in, attn, lse, dy, weight, table, pick, passed, shard, count):
    heads, length, _ = queries.shape
    part, width = length // count, dy.shape[1]
    columns = (heads + 2) * HD
    vmem, whole = pl.BlockSpec(memory_space=pltpu.VMEM), pl.BlockSpec(memory_space=pl.ANY)
    return pl.pallas_call(
        lambda *refs: attend_back_kernel(count, *refs),
        out_shape=[
            jax.ShapeDtypeStruct((length, columns), jnp.bfloat16),
            jax.ShapeDtypeStruct((count, columns // count, length), jnp.bfloat16),
            jax.ShapeDtypeStruct((width, heads * HD), jnp.bfloat16),
            jax.ShapeDtypeStruct((2, part // 2, width), jnp.bfloat16),
            jax.ShapeDtypeStruct((count,) + shard.shape, shard.dtype),
        ],
        in_specs=[whole] * 11,
        out_specs=[vmem] * 3 + [whole] * 2,
        scratch_shapes=[
            pltpu.VMEM(value.shape, value.dtype) for value in (queries, keys_in, values_in, attn, lse, weight, table)
        ]
        + [
            pltpu.VMEM((heads, part, HD), jnp.bfloat16),
            pltpu.VMEM((heads, part), jnp.float32),
            pltpu.VMEM((heads, part, HD), jnp.bfloat16),
            pltpu.VMEM((length, HD), jnp.float32),
            pltpu.VMEM((length, HD), jnp.float32),
        ]
        + [pltpu.VMEM(dy.shape, dy.dtype), pltpu.VMEM(pick.shape, pick.dtype)]
        + [pltpu.SemaphoreType.DMA((8,)), pltpu.SemaphoreType.DMA((8,)), pltpu.SemaphoreType.DMA((count + 8,))],
        compiler_params=pltpu.CompilerParams(collective_id=4, has_side_effects=True, vmem_limit_bytes=LIMIT),
        name="attend_back",
    )(queries, keys_in, values_in, attn, lse, dy, weight, table, pick, passed, shard)


def leave_kernel(
    count, grads_in, weight_in, first_in, scale_ref, gain_ref, other_ref, turned_ref, normed_in,
    own_ref, total_ref, term_ref,
    sent_ref, side_ref, below_ref, far_ref, slot_ref, whole_ref, normed_ref, first_ref, grads_ref, weight_ref,
    told_ref, heard_ref, send_sems, recv_sems, swap_send, swap_recv, load_sems, sum_send, sum_recv,
):
    part, _ = first_ref.shape
    half = part // 2
    size = turned_ref.shape[1]
    heads = H // count
    chunk = size // (heads + 2)
    index = lax.axis_index("seq")
    place = lax.axis_index("fsdp")
    peers = [seq_peer(step) for step in range(1, count)]
    fsdp_peers = [fsdp_peer(place ^ (1 << bit)) for bit in range(lax.axis_size("fsdp").bit_length() - 1)]
    greet(peers + fsdp_peers)
    swaps = [
        remote(turned_ref.at[index ^ step], slot_ref.at[step], (swap_send, swap_recv), step - 1, seq_peer(step))
        for step in range(1, count)
    ]
    for copy in swaps:
        copy.start()
    loads = [
        pltpu.make_async_copy(source, target, load_sems.at[number])
        for number, (source, target) in enumerate(
            (
                (turned_ref.at[index], slot_ref.at[0]),
                (normed_in, normed_ref),
                (first_in, first_ref),
                (grads_in, grads_ref),
                (weight_in, weight_ref),
            )
        )
    ]
    for number in (3, 4, 1, 0, 2):
        loads[number].start()
    total_ref[0:1] = jnp.zeros_like(other_ref)
    total_ref[1:2] = other_ref[...]
    for number in (3, 4, 1):
        loads[number].wait()
    sums = sum_copies(sent_ref, side_ref, below_ref, far_ref, half, (send_sems, recv_sems))

    def one_part(turn, carry):
        step = count - 1 - turn
        rows_step = pl.ds(pl.multiple_of(step * part, part), part)
        partial = matmul(grads_ref[rows_step, :], weight_ref[...], 1, 0)
        total_ref[0:1] += jnp.sum(partial * normed_ref[rows_step, :].astype(jnp.float32), 0, keepdims=True)
        pass_sums(turn, step, partial, sums, sent_ref, side_ref, below_ref, own_ref, half)
        return carry

    lax.fori_loop(0, count, one_part, 0)
    loads[0].wait()
    loads[2].wait()
    total_ref[0:1] = total_ref[0:1] / gain_ref[...]
    tells = []
    for step, peer in enumerate(fsdp_peers):
        told_ref[step] = total_ref[...]
        tell = remote(told_ref.at[step], heard_ref.at[step], (sum_send, sum_recv), step, peer)
        tell.start()
        tell.wait_recv()
        total_ref[...] += heard_ref[step]
        tells.append(tell)
    first = len(tells)
    told_ref[first] = total_ref[...]
    for step, peer in enumerate(peers):
        tells.append(
            remote(told_ref.at[first], heard_ref.at[first + step], (sum_send, sum_recv), first + step, peer)
        )
        tells[-1].start()
    for step in range(count):
        if step:
            swaps[step - 1].wait_recv()
        peer = index ^ step
        for block in range(count):
            piece = slot_ref[step, :, (step ^ block) * part : ((step ^ block) + 1) * part]
            tokens = slice(block * part, (block + 1) * part)
            for start, rows in ((0, heads * chunk), (H * chunk, chunk), ((H + KVH) * chunk, chunk)):
                begin = 0 if start == 0 else heads * chunk + (0 if start == H * chunk else chunk)
                spot = pl.multiple_of(start + peer * rows, chunk)
                whole_ref[pl.ds(spot, rows), tokens] = piece[begin : begin + rows]
    term_ref[...] = matmul(whole_ref[...], normed_ref[...], 1, 0).astype(jnp.bfloat16)
    end_sums(sums, side_ref, below_ref, far_ref, own_ref, half)
    unit = first_ref[...] * scale_ref[:, :1]
    grads = own_ref[...]
    inner = grads * gain_ref[...]
    own_ref[...] = scale_ref[:, :1] * (inner - unit * jnp.mean(inner * unit, 1, keepdims=True))
    for step in range(len(peers)):
        tells[first + step].wait_recv()
        total_ref[...] += heard_ref[first + step]
    for copy in sums + swaps + tells:
        copy.wait_send()


def leave(grads, weight, first, scale, gain, other, turned, normed, count):
    part, width = first.shape
    vmem, whole = pl.BlockSpec(memory_space=pltpu.VMEM), pl.BlockSpec(memory_space=pl.ANY)
    size, length = turned.shape[1:]
    steps = lax.axis_size("fsdp").bit_length() - 1 + count - 1
    own, total, term = pl.pallas_call(
        lambda *refs: leave_kernel(count, *refs),
        out_shape=(
            jax.ShapeDtypeStruct((part, width), jnp.float32),
            jax.ShapeDtypeStruct((2, width), jnp.float32),
            jax.ShapeDtypeStruct((size * count, width), jnp.bfloat16),
        ),
        in_specs=[whole] * 3 + [vmem] * 3 + [whole] * 2,
        out_specs=[vmem] * 3,
        scratch_shapes=[
            pltpu.VMEM((count, part, width), jnp.bfloat16),
            pltpu.VMEM((2, part // 2, width), jnp.bfloat16),
            pltpu.VMEM((2, part // 2, width), jnp.bfloat16),
            pltpu.VMEM((2, part // 2, width), jnp.bfloat16),
            pltpu.VMEM((count, size, length), jnp.bfloat16),
            pltpu.VMEM((count * size, length), jnp.bfloat16),
            pltpu.VMEM(normed.shape, jnp.bfloat16),
            pltpu.VMEM((part, width), jnp.float32),
            pltpu.VMEM(grads.shape, grads.dtype),
            pltpu.VMEM(weight.shape, weight.dtype),
            pltpu.VMEM((steps, 2, width), jnp.float32),
            pltpu.VMEM((steps, 2, width), jnp.float32),
            pltpu.SemaphoreType.DMA((6,)),
            pltpu.SemaphoreType.DMA((6,)),
            pltpu.SemaphoreType.DMA((count - 1,)),
            pltpu.SemaphoreType.DMA((count - 1,)),
            pltpu.SemaphoreType.DMA((5,)),
            pltpu.SemaphoreType.DMA((steps,)),
            pltpu.SemaphoreType.DMA((steps,)),
        ],
        compiler_params=pltpu.CompilerParams(collective_id=5, has_side_effects=True, vmem_limit_bytes=LIMIT),
        name="leave",
    )(grads, weight, first, scale, gain, other, turned, normed)
    return own, total, term


def join_rows_kernel(index_ref, own_ref, side_ref, below_ref, top_ref, bottom_ref, out_ref):
    step = pl.program_id(0) ^ index_ref[0]
    half = top_ref.shape[0]
    for number, ref in enumerate((own_ref, side_ref, below_ref)):

        @pl.when(step == number)
        def _():
            out_ref[...] = ref[...].astype(jnp.float32)

    @pl.when(step == 3)
    def _():
        out_ref[:half] = top_ref[...].astype(jnp.float32)
        out_ref[half:] = bottom_ref[...].astype(jnp.float32)


def join_rows(index, own, side, below, top, bottom, count):
    rows, width = own.shape
    parts = (own, side, below, top, bottom)
    return pl.pallas_call(
        join_rows_kernel,
        out_shape=jax.ShapeDtypeStruct((rows * count, width), jnp.float32),
        grid_spec=pltpu.PrefetchScalarGridSpec(
            num_scalar_prefetch=1,
            grid=(count,),
            in_specs=[pl.BlockSpec(part.shape, lambda i, s: (0, 0)) for part in parts],
            out_specs=pl.BlockSpec((rows, width), lambda i, s: (i, 0)),
        ),
        compiler_params=pltpu.CompilerParams(vmem_limit_bytes=LIMIT),
        name="join_rows",
    )(index, *parts)


def join_pieces_kernel(count, row_piece, column_piece, index_ref, own_ref, *refs):
    slot_refs, out_ref = refs[:-1], refs[-1]
    index = index_ref[0]
    rows, columns = own_ref.shape
    for device in range(count):
        if len(slot_refs) == 1:
            values = slot_refs[0][device ^ index]
        else:
            values = own_ref[...]
            for step, ref in enumerate(slot_refs):
                values = jnp.where(device ^ index == step + 1, ref[...], values)
        values = jnp.where(device == index, own_ref[...], values).astype(jnp.float32)
        for top in range(0, rows, row_piece):
            for left in range(0, columns, column_piece):
                down = top * count + device * row_piece if row_piece < rows else top
                across = left * count + device * column_piece if row_piece == rows else left
                out_ref[down : down + row_piece, across : across + column_piece] = values[
                    top : top + row_piece, left : left + column_piece
                ]


def join_pieces(index, own, slots, count, row_piece, column_piece):
    rows, columns = own.shape
    shape = (rows * count, columns) if row_piece < rows else (rows, columns * count)
    return pl.pallas_call(
        lambda *refs: join_pieces_kernel(count, row_piece, column_piece, *refs),
        out_shape=jax.ShapeDtypeStruct(shape, jnp.float32),
        grid_spec=pltpu.PrefetchScalarGridSpec(
            num_scalar_prefetch=1,
            grid=(1,),
            in_specs=[pl.BlockSpec(own.shape, lambda i, s: (0, 0))]
            + [pl.BlockSpec(slot.shape, lambda i, s, n=slot.ndim: (0,) * n) for slot in slots],
            out_specs=pl.BlockSpec(shape, lambda i, s: (0, 0)),
        ),
        compiler_params=pltpu.CompilerParams(vmem_limit_bytes=LIMIT),
        name="join_pieces",
    )(index, own, *slots)


def last_sums_kernel(base_ref, passed_ref, flowing_ref, piece_ref, result_ref, grad_ref):
    result_ref[...] = base_ref[...] + passed_ref[...].astype(jnp.float32)
    grad_ref[...] = flowing_ref[...] + piece_ref[...]


def last_sums(base, passed, flowing, piece):
    rows, width = base.shape
    tile = rows // 4
    block = pl.BlockSpec((tile, width), lambda i: (i, 0))
    return pl.pallas_call(
        last_sums_kernel,
        out_shape=[jax.ShapeDtypeStruct((rows, width), jnp.float32)] * 2,
        grid=(4,),
        in_specs=[block] * 4,
        out_specs=[block] * 2,
        compiler_params=pltpu.CompilerParams(vmem_limit_bytes=LIMIT),
        name="last_sums",
    )(base, passed, flowing, piece)


def greet_chain(count):
    place = lax.axis_index("fsdp")
    chips = lax.axis_size("fsdp") // 2
    chip = place // 2
    barrier = pltpu.get_barrier_semaphore()
    for peer in [seq_peer(step) for step in range(1, count)] + [fsdp_peer(place ^ 1)]:
        pl.semaphore_signal(barrier, inc=1, device_id=peer, device_id_type=MESH)

    @pl.when(chip > 0)
    def _():
        pl.semaphore_signal(barrier, inc=1, device_id=fsdp_peer(place - 2), device_id_type=MESH)

    @pl.when(chip < chips - 1)
    def _():
        pl.semaphore_signal(barrier, inc=1, device_id=fsdp_peer(place + 2), device_id_type=MESH)

    greetings = count + (chip > 0).astype(jnp.int32) + (chip < chips - 1).astype(jnp.int32)
    pl.semaphore_wait(barrier, greetings)


def weight_chain(item_of, number, sems):
    item_up, item_down, item_side, item_recv, local_sem = sems
    place = lax.axis_index("fsdp")
    chips = lax.axis_size("fsdp") // 2
    chip, core = place // 2, place % 2

    def item_copy(source, target, slot, sem, peer):
        return pltpu.make_async_remote_copy(
            src_ref=source,
            dst_ref=target,
            send_sem=sem.at[slot],
            recv_sem=item_recv.at[slot],
            device_id=fsdp_peer(peer),
            device_id_type=MESH,
        )

    def pass_on(source, target, slot, owner_chip, act):
        @pl.when((chip >= owner_chip) & (chip < chips - 1))
        def _():
            act(item_copy(source, target, slot, item_up, place + 2))

        @pl.when((chip <= owner_chip) & (chip > 0))
        def _():
            act(item_copy(source, target, slot, item_down, place - 2))

        act(item_copy(source, target, slot, item_side, place ^ 1))

    def send_own():
        def body(item, carry):
            owner, source, target, slot = item_of(item)

            @pl.when(place == owner)
            def _():
                pass_on(source, target, slot, owner // 2, lambda copy: copy.start())
                pltpu.make_async_copy(source, target, local_sem.at[slot]).start()

            return carry

        lax.fori_loop(0, number, body, 0)

    def pass_far(distance):
        def body(item, carry):
            owner, _, target, slot = item_of(item)
            owner_chip = owner // 2
            apart = jnp.where(chip > owner_chip, chip - owner_chip, owner_chip - chip)

            @pl.when((apart == distance) & (core == owner % 2))
            def _():
                item_copy(target, target, slot, item_side, place ^ 1).wait_recv()
                pass_on(target, target, slot, owner_chip, lambda copy: copy.start())

            return carry

        lax.fori_loop(0, number, body, 0)

    def finish():
        def body(item, carry):
            owner, source, target, slot = item_of(item)

            @pl.when(core != owner % 2)
            def _():
                item_copy(target, target, slot, item_side, place ^ 1).wait_recv()

            @pl.when(place == owner)
            def _():
                pltpu.make_async_copy(source, target, local_sem.at[slot]).wait()

            @pl.when(core == owner % 2)
            def _():
                pass_on(target, target, slot, owner // 2, lambda copy: copy.wait_send())

            return carry

        lax.fori_loop(0, number, body, 0)

    return send_own, pass_far, finish


def feed_kernel(
    count, normed_in, weight_in, dm_in, down_part_ref,
    gates_out, act_out, dm_out, term_out, down_ref,
    normed_ref, weight_ref, gates_ref, act_ref, dm_ref, term_ref,
    send_sems, recv_sems, load_sems, item_up, item_down, item_side, item_recv, local_sem,
    gates_sems, act_sems, dm_sem, term_sems,
):
    part, width = dm_in.shape
    units = act_ref.shape[1]
    chips = lax.axis_size("fsdp") // 2
    narrow = jnp.bfloat16
    load_weight = pltpu.make_async_copy(weight_in, weight_ref, load_sems.at[0])
    load_normed = pltpu.make_async_copy(normed_in, normed_ref, load_sems.at[1])
    load_weight.start()
    load_normed.start()
    greet_chain(count)
    down_rows = down_part_ref.shape[0]

    def down_item(item):
        target = down_ref.at[pl.ds(pl.multiple_of(item * down_rows, down_rows), down_rows)]
        return item, down_part_ref, target, item

    send_own, pass_far, finish = weight_chain(
        down_item, 2 * chips, (item_up, item_down, item_side, item_recv, local_sem)
    )
    send_own()
    group = gather_copies(dm_in, dm_ref, part // 2, (send_sems, recv_sems))
    share_start([group])
    dm_ref[0] = dm_in[...]
    load_normed.wait()
    load_weight.wait()

    def store_gates(step):
        rows = pl.ds(pl.multiple_of(step * part, part), part)
        return pltpu.make_async_copy(gates_ref.at[step % 2], gates_out.at[rows], gates_sems.at[step % 2])

    def store_act(step):
        rows = pl.ds(pl.multiple_of(step * part, part), part)
        return pltpu.make_async_copy(act_ref.at[rows], act_out.at[rows], act_sems.at[step])

    def one_part(step, carry):
        rows = pl.ds(pl.multiple_of(step * part, part), part)
        both = matmul(normed_ref[rows, :], weight_ref[...], 1, 1)

        @pl.when(step >= 2)
        def _():
            store_gates(step - 2).wait()

        gates_ref[step % 2] = both.astype(narrow)
        gate = both[:, :units]
        act_ref[rows, :] = (gate * jax.nn.sigmoid(gate) * both[:, units:]).astype(narrow)
        store_gates(step).start()
        store_act(step).start()

        @pl.when(step == count - 2)
        def _():
            share_on(group)
            pass_far(1)

        return carry

    lax.fori_loop(0, count, one_part, 0)
    pass_far(2)
    share_end([group])
    keep_dm = pltpu.make_async_copy(dm_ref, dm_out, dm_sem)
    keep_dm.start()
    tile = 2 * 128
    tiles = width // tile

    def store_term(number):
        rows = pl.ds(pl.multiple_of(number * tile, tile), tile)
        return pltpu.make_async_copy(term_ref.at[number % 2], term_out.at[rows], term_sems.at[number % 2])

    def one_tile(number, carry):
        @pl.when(number >= 2)
        def _():
            store_term(number - 2).wait()

        columns = pl.ds(pl.multiple_of(number * tile, tile), tile)
        upstream = dm_ref[:, :, columns].reshape(part * count, tile)
        term_ref[number % 2] = matmul(upstream, act_ref[...], 0, 0).astype(narrow)
        store_term(number).start()
        return carry

    lax.fori_loop(0, tiles, one_tile, 0)
    for distance in range(3, chips):
        pass_far(distance)
    for step in range(count - 2, count):
        store_gates(step).wait()
    for step in range(count):
        store_act(step).wait()
    keep_dm.wait()
    for number in range(tiles - 2, tiles):
        store_term(number).wait()
    finish()


def feed(normed, weight, dm, down_part, count):
    part, width = dm.shape
    length, units = part * count, down_part.shape[1]
    items = lax.axis_size("fsdp")
    vmem, whole = pl.BlockSpec(memory_space=pltpu.VMEM), pl.BlockSpec(memory_space=pl.ANY)
    gates, act, dm_all, term, down_cols = pl.pallas_call(
        lambda *refs: feed_kernel(count, *refs),
        out_shape=[
            jax.ShapeDtypeStruct((length, 2 * units), jnp.bfloat16),
            jax.ShapeDtypeStruct((length, units), jnp.bfloat16),
            jax.ShapeDtypeStruct((count, part, width), jnp.bfloat16),
            jax.ShapeDtypeStruct((width, units), jnp.bfloat16),
            jax.ShapeDtypeStruct((items * down_part.shape[0], units), jnp.bfloat16),
        ],
        in_specs=[whole] * 2 + [vmem] + [whole],
        out_specs=[whole] * 5,
        scratch_shapes=[
            pltpu.VMEM(normed.shape, normed.dtype),
            pltpu.VMEM(weight.shape, weight.dtype),
            pltpu.VMEM((2, part, 2 * units), jnp.bfloat16),
            pltpu.VMEM((length, units), jnp.bfloat16),
            pltpu.VMEM((count, part, width), jnp.bfloat16),
            pltpu.VMEM((2, 2 * 128, units), jnp.bfloat16),
            pltpu.SemaphoreType.DMA((6,)),
            pltpu.SemaphoreType.DMA((6,)),
            pltpu.SemaphoreType.DMA((2,)),
        ]
        + [pltpu.SemaphoreType.DMA((items,))] * 5
        + [
            pltpu.SemaphoreType.DMA((2,)),
            pltpu.SemaphoreType.DMA((count,)),
            pltpu.SemaphoreType.DMA,
            pltpu.SemaphoreType.DMA((2,)),
        ],
        compiler_params=pltpu.CompilerParams(collective_id=9, has_side_effects=True, vmem_limit_bytes=LIMIT),
        name="feed",
    )(normed, weight, dm, down_part)
    return gates, act, dm_all.reshape(length, width), term, down_cols


def norm_back_kernel(
    count, act_in, down_in, dm_in, gates_in, weight_in, flowing_in, middle_in, inputs_in, scale_ref, gain_ref,
    own_ref, gain_out_ref, dy_ref, term_ref, product_ref, from_side_ref, from_below_ref,
    act_ref, down_ref, dm_ref, gates_ref, grads_ref, weight_ref, flowing_ref, middle_ref, inputs_ref,
    held_ref, sent_ref, side_ref, below_ref, far_ref, stage_ref,
    send_sems, recv_sems, load_sems, part_sems, store_sems, product_sems,
):
    part, _ = flowing_in.shape
    half = part // 2
    wide, narrow = jnp.float32, jnp.bfloat16
    units = down_ref.shape[1]
    sems = (send_sems, recv_sems)

    def load(source, target, number):
        copy = pltpu.make_async_copy(source, target, load_sems.at[number])
        copy.start()
        return copy

    def load_parts(turn):
        rows = pl.ds(pl.multiple_of((count - 1 - turn) * part, part), part)
        slot = turn % 2
        return [
            pltpu.make_async_copy(dm_in.at[rows], dm_ref.at[slot], part_sems.at[0, slot]),
            pltpu.make_async_copy(gates_in.at[rows], gates_ref.at[slot], part_sems.at[1, slot]),
        ]

    firsts = [load(act_in, act_ref, 0), load(down_in, down_ref, 1)]
    for copy in load_parts(0):
        copy.start()
    load_weight = load(weight_in, weight_ref, 2)
    for copy in load_parts(1):
        copy.start()
    lasts = [load(inputs_in, inputs_ref, 3), load(flowing_in, flowing_ref, 4), load(middle_in, middle_ref, 5)]
    greet([seq_peer(1), seq_peer(2)])
    top, bottom = pl.ds(0, half), pl.ds(half, half)
    firsts_sums = [
        remote(held_ref.at[3].at[top], from_side_ref.at[1], sems, 6, seq_peer(1)),
        remote(held_ref.at[3].at[bottom], from_below_ref.at[1], sems, 7, seq_peer(2)),
        remote(held_ref.at[2].at[bottom], from_below_ref.at[0], sems, 8, seq_peer(2)),
        remote(held_ref.at[1].at[top], from_side_ref.at[0], sems, 9, seq_peer(1)),
    ]
    sums = sum_copies(sent_ref, side_ref, below_ref, far_ref, half, sems)
    for copy in firsts:
        copy.wait()

    def down_part(turn, carry):
        step = count - 1 - turn
        rows = pl.ds(pl.multiple_of(step * part, part), part)
        held_ref[step] = matmul(act_ref[rows, :], down_ref[...], 1, 1).astype(narrow)

        @pl.when(turn == 0)
        def _():
            firsts_sums[0].start()
            firsts_sums[1].start()

        @pl.when(turn == 1)
        def _():
            firsts_sums[2].start()

        @pl.when(turn == 2)
        def _():
            firsts_sums[3].start()

        return carry

    lax.fori_loop(0, count, down_part, 0)
    product = pltpu.make_async_copy(held_ref, product_ref, product_sems.at[0])
    product.start()
    load_weight.wait()

    def one_part(turn, carry):
        step = count - 1 - turn
        slot = turn % 2
        rows = pl.ds(pl.multiple_of(step * part, part), part)
        for copy in load_parts(turn):
            copy.wait()
        dact = matmul(dm_ref[slot], down_ref[...], 1, 0)
        gate = gates_ref[slot, :, :units].astype(wide)
        up = gates_ref[slot, :, units:].astype(wide)
        sigma = jax.nn.sigmoid(gate)
        grads_ref[rows, :units] = (dact * up * sigma * (1.0 + gate * (1.0 - sigma))).astype(narrow)
        grads_ref[rows, units:] = (dact * gate * sigma).astype(narrow)

        @pl.when(turn < count - 2)
        def _():
            for copy in load_parts(turn + 2):
                copy.start()

        partial = matmul(grads_ref[rows, :], weight_ref[...], 1, 0)

        @pl.when(turn == count - 1)
        def _():
            own_ref[...] = partial

        @pl.when(turn < count - 1)
        def _():
            sent_ref[step] = partial.astype(narrow)

        @pl.when(turn == 0)
        def _():
            sums[0].start()
            sums[1].start()

        @pl.when(turn == 1)
        def _():
            sums[2].start()

        @pl.when(turn == 2)
        def _():
            sums[3].start()

        return carry

    lax.fori_loop(0, count, one_part, 0)
    sums[0].wait_recv()
    sent_ref[2, :half] = (sent_ref[2, :half].astype(wide) + side_ref[1].astype(wide)).astype(narrow)
    sums[4].start()
    sums[1].wait_recv()
    sent_ref[1, half:] = (sent_ref[1, half:].astype(wide) + below_ref[1].astype(wide)).astype(narrow)
    sums[5].start()
    for copy in lasts:
        copy.wait()
    tile = stage_ref.shape[1]
    tiles = grads_ref.shape[1] // tile

    def store(number):
        rows = pl.ds(pl.multiple_of(number * tile, tile), tile)
        return pltpu.make_async_copy(stage_ref.at[number % 2], term_ref.at[rows], store_sems.at[number % 2])

    def one_tile(number, carry):
        @pl.when(number >= 2)
        def _():
            store(number - 2).wait()

        columns = pl.ds(pl.multiple_of(number * tile, tile), tile)
        stage_ref[number % 2] = matmul(grads_ref[:, columns], inputs_ref[...], 0, 0).astype(narrow)
        store(number).start()
        return carry

    lax.fori_loop(0, tiles, one_tile, 0)
    end_sums(sums, side_ref, below_ref, far_ref, own_ref, half)
    scale = scale_ref[:, :1]
    unit = middle_ref[...] * scale
    grads = own_ref[...]
    gain_out_ref[...] = jnp.sum(grads * unit, 0, keepdims=True)
    inner = grads * gain_ref[...]
    own_ref[...] = flowing_ref[...] + scale * (inner - unit * jnp.mean(inner * unit, 1, keepdims=True))
    dy_ref[...] = own_ref[...].astype(narrow)
    for number in range(tiles - 2, tiles):
        store(number).wait()
    product.wait()
    for copy in firsts_sums:
        copy.wait_recv()
    for copy in sums + firsts_sums:
        copy.wait_send()


def norm_back(act, down, dm, gates, weight, flowing, middle, inputs, scale, gain, count):
    part, width = flowing.shape
    units = gates.shape[1]
    tile = 2 * 128
    vmem, whole = pl.BlockSpec(memory_space=pltpu.VMEM), pl.BlockSpec(memory_space=pl.ANY)
    narrow, wide = jnp.bfloat16, jnp.float32
    pair = (2, part // 2, width)
    own, gain_term, dy, term, product, from_side, from_below = pl.pallas_call(
        lambda *refs: norm_back_kernel(count, *refs),
        out_shape=(
            jax.ShapeDtypeStruct((part, width), wide),
            jax.ShapeDtypeStruct((1, width), wide),
            jax.ShapeDtypeStruct((part, width), narrow),
            jax.ShapeDtypeStruct((units, width), narrow),
            jax.ShapeDtypeStruct((count, part, width), narrow),
            jax.ShapeDtypeStruct(pair, narrow),
            jax.ShapeDtypeStruct(pair, narrow),
        ),
        in_specs=[whole] * 8 + [vmem] * 2,
        out_specs=[vmem] * 3 + [whole] * 4,
        scratch_shapes=[
            pltpu.VMEM(act.shape, narrow),
            pltpu.VMEM(down.shape, narrow),
            pltpu.VMEM((2, part, width), narrow),
            pltpu.VMEM((2, part, units), narrow),
            pltpu.VMEM((part * count, units), narrow),
            pltpu.VMEM(weight.shape, narrow),
            pltpu.VMEM((part, width), wide),
            pltpu.VMEM((part, width), wide),
            pltpu.VMEM(inputs.shape, narrow),
            pltpu.VMEM((count, part, width), narrow),
            pltpu.VMEM((count, part, width), narrow),
            pltpu.VMEM(pair, narrow),
            pltpu.VMEM(pair, narrow),
            pltpu.VMEM(pair, narrow),
            pltpu.VMEM((2, tile, width), narrow),
            pltpu.SemaphoreType.DMA((10,)),
            pltpu.SemaphoreType.DMA((10,)),
            pltpu.SemaphoreType.DMA((6,)),
            pltpu.SemaphoreType.DMA((2, 2)),
            pltpu.SemaphoreType.DMA((2,)),
            pltpu.SemaphoreType.DMA((1,)),
        ],
        compiler_params=pltpu.CompilerParams(collective_id=3, has_side_effects=True, vmem_limit_bytes=67043328),
        name="norm_back",
    )(act, down, dm, gates, weight, flowing, middle, inputs, scale, gain)
    return own, gain_term[0], dy, term, product, from_side, from_below


def share_dy_kernel(
    dy_ref, down_ref, side_in, below_in, middle_in, all_ref, base_ref, passed_ref,
    piece_ref, side_ref, below_ref, send_sems, recv_sems, load_sems,
):
    part = dy_ref.shape[0]
    half = part // 2
    wide = jnp.float32
    top, bottom = pl.ds(0, half), pl.ds(half, half)
    loads = [
        pltpu.make_async_copy(down_ref.at[0], piece_ref.at[0], load_sems.at[0]),
        pltpu.make_async_copy(down_ref.at[2].at[top], piece_ref.at[1].at[top], load_sems.at[1]),
        pltpu.make_async_copy(down_ref.at[1].at[bottom], piece_ref.at[1].at[bottom], load_sems.at[2]),
        pltpu.make_async_copy(dy_ref, all_ref.at[0], load_sems.at[3]),
        pltpu.make_async_copy(side_in, side_ref, load_sems.at[4]),
        pltpu.make_async_copy(below_in, below_ref, load_sems.at[5]),
        pltpu.make_async_copy(middle_in, base_ref, load_sems.at[6]),
    ]
    greet([seq_peer(1), seq_peer(2)])
    group = gather_copies(dy_ref, all_ref, half, (send_sems, recv_sems))
    share_start([group])
    for load in loads:
        load.start()
    for load in loads:
        load.wait()
    base_ref[...] += piece_ref[0].astype(wide)
    base_ref[:half] += side_ref[0].astype(wide)
    base_ref[half:] += below_ref[0].astype(wide)
    passed_ref[0] = (piece_ref[1, :half].astype(wide) + side_ref[1].astype(wide)).astype(jnp.bfloat16)
    passed_ref[1] = (piece_ref[1, half:].astype(wide) + below_ref[1].astype(wide)).astype(jnp.bfloat16)
    share_on(group)
    share_end([group])


def share_dy(dy, down, side, below, middle, count):
    part, width = dy.shape
    vmem, whole = pl.BlockSpec(memory_space=pltpu.VMEM), pl.BlockSpec(memory_space=pl.ANY)
    gathered, base, passed = pl.pallas_call(
        lambda *refs: share_dy_kernel(*refs),
        out_shape=[
            jax.ShapeDtypeStruct((count, part, width), jnp.bfloat16),
            jax.ShapeDtypeStruct((part, width), jnp.float32),
            jax.ShapeDtypeStruct((2, part // 2, width), jnp.bfloat16),
        ],
        in_specs=[vmem] + [whole] * 4,
        out_specs=[whole, vmem, vmem],
        scratch_shapes=[
            pltpu.VMEM((2, part, width), jnp.bfloat16),
            pltpu.VMEM((2, part // 2, width), jnp.bfloat16),
            pltpu.VMEM((2, part // 2, width), jnp.bfloat16),
            pltpu.SemaphoreType.DMA((6,)),
            pltpu.SemaphoreType.DMA((6,)),
            pltpu.SemaphoreType.DMA((7,)),
        ],
        compiler_params=pltpu.CompilerParams(collective_id=8, has_side_effects=True, vmem_limit_bytes=LIMIT),
        name="share_dy",
    )(dy, down, side, below, middle)
    return gathered.reshape(part * count, width), base, passed


def fast_body(hidden, positions, gains, w_qkv, w_out, w_gate_up, w_down, cotangent):
    count = lax.axis_size("seq")
    index = lax.axis_index("seq")
    place = index.astype(jnp.int32).reshape(1)
    current = hidden[0]
    part_len, width = current.shape
    heads = H // count
    gain = gains[0]
    after = lax.optimization_barrier

    rows = w_qkv.shape[1]
    group = math.gcd(rows, HD)
    chunk = group // count
    per_head = HD // group
    normed_all, qkv_rows, out_cols, table, gate_up_part, down_part, scale_one = enter(
        current, gain[:1], positions, w_qkv[0], w_out[0], w_gate_up[0], w_down[0], count
    )
    gu_rows = w_gate_up.shape[1] // count
    gate_up = lax.all_gather(gate_up_part, "fsdp", axis=0, tiled=True)
    down_rows = w_down.shape[1]

    queries, keys_in, values_in = project_qkv(place, normed_all, qkv_rows, table, count)
    attn_flat, log_total, middle, scale_two, normed_two_all = attend(
        queries, keys_in, values_in, out_cols, current, gain[1:], count
    )
    flowing = cotangent[0]
    gates, activated, dm_all, term_down, down_cols = feed(
        normed_two_all, gate_up, flowing.astype(jnp.bfloat16), down_part, count
    )

    def owned(grad):
        return lax.psum_scatter(grad.astype(jnp.bfloat16), "fsdp", scatter_dimension=0, tiled=True)

    grad_down = owned(term_down)
    dmiddle, gain_two, dy, term_gate_up, down_sent, from_side, from_below = norm_back(
        activated, down_cols, dm_all, gates, gate_up, flowing, middle, normed_two_all, scale_two, gain[1:], count
    )
    grad_gate_up = owned(term_gate_up)
    dy_all, base, passed = share_dy(dy, down_sent, from_side, from_below, middle, count)
    pieces = heads + 2
    picked = np.arange(pieces * HD).reshape(pieces * per_head, count, chunk).transpose(1, 0, 2).reshape(-1)
    pick = jnp.asarray(picked[:, None] == np.arange(pieces * HD)[None, :], jnp.bfloat16)
    djoint, djoint_turned, term_out, passed_on, down_slots = attend_back(
        queries, keys_in, values_in, attn_flat, log_total, dy_all, out_cols, table, pick, passed, grad_down, count
    )
    grad_out = owned(term_out)
    grad_piece, gain_total, term_qkv = leave(
        djoint, qkv_rows, current, scale_one, gain[:1], gain_two[None], djoint_turned, normed_all, count
    )
    grad_qkv = owned(term_qkv)
    grad_gate_up, grad_piece = after((grad_gate_up, grad_piece))
    half = upper_half(gu_rows)
    side = neighbour(grad_gate_up, 1)
    below = neighbour(grad_gate_up, 2)
    far_top = neighbour(side[:half], 2)
    far_bottom = neighbour(below[half:], 1)
    down_shard = join_pieces(place, grad_down, (down_slots,), count, down_rows, gu_rows)
    result, grad_hidden = last_sums(base, passed_on.reshape(part_len, width), dmiddle, grad_piece)
    out_slots = [neighbour(grad_out, step) for step in range(1, count)]
    grad_qkv, out_slots = after((grad_qkv, out_slots))
    qkv_slots = [neighbour(grad_qkv, step) for step in range(1, count)]
    gate_up_shard = join_rows(place, grad_gate_up, side, below, far_top, far_bottom, count)
    out_shard = join_pieces(place, grad_out, out_slots, count, down_rows, heads * HD)
    qkv_shard = join_pieces(place, grad_qkv, qkv_slots, count, chunk, width)
    gain_total = gain_total[None]
    return (
        result[None],
        grad_hidden[None],
        gain_total,
        qkv_shard[None],
        out_shard[None],
        gate_up_shard[None],
        down_shard[None],
    )


def fits(mesh):
    count, fsdp = mesh.shape["seq"], mesh.shape["fsdp"]
    rows = (H + 2 * KVH) * HD // fsdp
    return count == KVH == 4 and fsdp % 2 == 0 and fsdp & (fsdp - 1) == 0 and rows % HD == 0


def solution(mesh):
    placed = (
        P("fsdp", "seq", None),
        P("fsdp", "seq"),
        P(),
        P(None, "fsdp", None),
        P(None, "fsdp", None),
        P(None, "fsdp", None),
        P(None, "fsdp", None),
        P("fsdp", "seq", None),
    )
    fast = fits(mesh)
    return jax.shard_map(
        fast_body if fast else body,
        mesh=mesh,
        in_specs=placed,
        out_specs=(
            P("fsdp", "seq", None),
            P("fsdp", "seq", None),
            P(),
            P(None, "fsdp", None),
            P(None, "fsdp", None),
            P(None, "fsdp", None),
            P(None, "fsdp", None),
        ),
        check_vma=False,
    )
```

```python
import math

import jax
import jax.numpy as jnp
import numpy as np
from jax import lax
from jax.experimental import pallas as pl
from jax.experimental.pallas import tpu as pltpu
from jax.sharding import PartitionSpec as P


H = 32
KVH = 4
HD = 64
FF = 5632
LAYERS = 1


EPS = 1e-05


def rope_tables(position_ids):
    halfway = HD // 2
    frequency = jnp.exp(jnp.arange(halfway, dtype=jnp.float32) * (-2.0 * math.log(10000.0) / HD))
    angles = position_ids.astype(jnp.float32)[..., None] * frequency
    cosines = jnp.cos(angles)
    sines = jnp.sin(angles)
    return (
        jnp.concatenate([cosines, cosines], -1)[..., None, :],
        jnp.concatenate([sines, sines], -1)[..., None, :],
    )


def rotate(values, cosines, sines):
    halfway = values.shape[-1] // 2
    turned = jnp.concatenate([-values[..., halfway:], values[..., :halfway]], -1)
    return values * cosines + turned * sines


def unrotate(grads, cosines, sines):
    halfway = grads.shape[-1] // 2
    scaled = grads * sines
    return grads * cosines + jnp.concatenate([scaled[..., halfway:], -scaled[..., :halfway]], -1)


def normalize(values, gain):
    scale = lax.rsqrt(jnp.mean(values * values, -1, keepdims=True) + EPS)
    return ((values * scale * gain).astype(jnp.bfloat16), scale)


def normalize_back(grads, values, scale, gain):
    unit = values * scale
    gain_grad = jnp.sum((grads * unit).reshape(-1, unit.shape[-1]), 0)
    inner = grads * gain
    return (scale * (inner - unit * jnp.mean(inner * unit, -1, keepdims=True)), gain_grad)


def masked_scores(queries, keys_wide):
    scores = jnp.einsum(
        "qhd,khd->hqk", queries, keys_wide, preferred_element_type=jnp.float32
    ) * queries.shape[-1] ** (-0.5)
    length = queries.shape[0]
    causal = jnp.arange(length)[:, None] >= jnp.arange(length)[None, :]
    return jnp.where(causal[None], scores, -1e30)


def local_attend(operands):
    queries, keys_in, values_in = operands
    repeat_by = queries.shape[1] // keys_in.shape[1]
    keys_wide = jnp.repeat(keys_in, repeat_by, axis=1)
    values_wide = jnp.repeat(values_in, repeat_by, axis=1)
    scores = masked_scores(queries, keys_wide)
    peak = jnp.max(scores, -1, keepdims=True)
    log_total = peak[..., 0] + jnp.log(jnp.sum(jnp.exp(scores - peak), -1))
    weights = jnp.exp(scores - log_total[..., None]).astype(jnp.bfloat16)
    output = jnp.einsum("hqk,khd->qhd", weights, values_wide, preferred_element_type=jnp.float32)
    return (output.astype(jnp.bfloat16), log_total)


def local_attend_back(operands):
    queries, keys_in, values_in, output, log_total, dattn = operands
    length, kv_dev, head_dim = keys_in.shape
    repeat_by = queries.shape[1] // kv_dev
    keys_wide = jnp.repeat(keys_in, repeat_by, axis=1)
    values_wide = jnp.repeat(values_in, repeat_by, axis=1)
    scores = masked_scores(queries, keys_wide)
    probs = jnp.exp(scores - log_total[..., None])
    delta = jnp.sum(output.astype(jnp.float32) * dattn.astype(jnp.float32), -1).T
    dprob = jnp.einsum("qhd,khd->hqk", dattn, values_wide, preferred_element_type=jnp.float32)
    dscore = (probs * (dprob - delta[..., None])).astype(jnp.bfloat16)
    dqueries = jnp.einsum(
        "hqk,khd->qhd", dscore, keys_wide, preferred_element_type=jnp.float32
    ) * head_dim ** (-0.5)
    dkeys = jnp.einsum(
        "hqk,qhd->khd", dscore, queries, preferred_element_type=jnp.float32
    ) * head_dim ** (-0.5)
    dvalues = jnp.einsum(
        "hqk,qhd->khd", probs.astype(jnp.bfloat16), dattn, preferred_element_type=jnp.float32
    )

    def fold_heads(per_head):
        return jnp.sum(per_head.reshape(length, kv_dev, repeat_by, head_dim), 2).astype(
            jnp.bfloat16
        )

    return (dqueries.astype(jnp.bfloat16), fold_heads(dkeys), fold_heads(dvalues))


def project(inputs, weight):
    return lax.dot_general(
        inputs,
        lax.all_gather(weight, "fsdp", axis=0, tiled=True),
        (((1,), (1,)), ((), ())),
        preferred_element_type=jnp.float32,
    )


def project_back(grads, weight):
    shard_rows = lax.all_gather(weight, "fsdp", axis=0, tiled=True)
    picked = lax.slice_in_dim(grads, 0, shard_rows.shape[0], axis=1)
    return jnp.dot(picked, shard_rows, preferred_element_type=jnp.float32)


def weight_grad(grads, inputs, shard_size):
    picked = lax.slice_in_dim(grads, 0, shard_size * lax.axis_size("fsdp"), axis=1)
    summed = lax.psum_scatter(
        lax.dot_general(
            picked, inputs, (((0,), (0,)), ((), ())), preferred_element_type=jnp.float32
        ).astype(jnp.bfloat16),
        "fsdp",
        scatter_dimension=0,
        tiled=True,
    )
    return lax.psum(summed, "seq").astype(jnp.float32)


def backward_pair(grads, inputs, weight):
    wgrad = weight_grad(grads, inputs, weight.shape[0])
    return (project_back(grads, weight), wgrad)


def body(hidden, positions, gains, w_qkv, w_out, w_gate_up, w_down, cotangent):
    seq_count, part_len, model_width = hidden.shape
    row_count = seq_count * part_len
    group_count = lax.axis_size("seq")
    full_len = part_len * group_count
    heads_dev = H // group_count
    share = H // KVH
    kv_dev = max(1, heads_dev // share)
    first_kv = np.arange(group_count) * heads_dev // share
    slot_table = np.concatenate(
        [
            first_kv[:, None] + np.arange(kv_dev)[None, :],
            KVH + first_kv[:, None] + np.arange(kv_dev)[None, :],
        ],
        1,
    ).reshape(-1)
    slot_onehot = jnp.asarray(
        (slot_table[:, None] == np.arange(2 * KVH)[None, :]).astype(np.float32), jnp.bfloat16
    )
    cosines, sines = rope_tables(positions)
    layer_index = 0
    gain = gains[layer_index]
    normed, scale_one = normalize(hidden, gain[0])
    normed_flat = normed.reshape(row_count, model_width)
    joint = project(normed_flat, w_qkv[layer_index]).reshape(seq_count, part_len, -1)
    queries = joint[..., : H * HD].reshape(seq_count, part_len, H, HD)
    keys_in = joint[..., H * HD : (H + KVH) * HD].reshape(seq_count, part_len, KVH, HD)
    values_in = joint[..., (H + KVH) * HD :].reshape(seq_count, part_len, KVH, HD)
    q_rot = rotate(queries, cosines, sines).astype(jnp.bfloat16)
    kv_all = jnp.concatenate(
        [rotate(keys_in, cosines, sines).astype(jnp.bfloat16), values_in.astype(jnp.bfloat16)], 2
    )
    q_send = q_rot.reshape(seq_count, part_len, group_count, heads_dev * HD)
    kv_send = jnp.take(kv_all, slot_table, axis=2).reshape(
        seq_count, part_len, group_count, 2 * kv_dev * HD
    )
    q_heads = lax.all_to_all(q_send, "seq", split_axis=2, concat_axis=1, tiled=True)
    kv_heads = lax.all_to_all(kv_send, "seq", split_axis=2, concat_axis=1, tiled=True)
    q_heads = q_heads.reshape(seq_count, full_len, heads_dev, HD)
    kv_heads = kv_heads.reshape(seq_count, full_len, 2 * kv_dev, HD)
    k_heads = kv_heads[:, :, :kv_dev]
    v_heads = kv_heads[:, :, kv_dev:]
    o_heads, log_total = lax.map(local_attend, (q_heads, k_heads, v_heads))
    o_back = lax.all_to_all(
        o_heads.reshape(seq_count, full_len, 1, heads_dev * HD),
        "seq",
        split_axis=1,
        concat_axis=2,
        tiled=True,
    )
    attn_flat = o_back.reshape(row_count, model_width)
    middle = hidden + project(attn_flat, w_out[layer_index]).reshape(
        seq_count, part_len, model_width
    )
    normed_two, scale_two = normalize(middle, gain[1])
    normed_two_flat = normed_two.reshape(row_count, model_width)
    both = project(normed_two_flat, w_gate_up[layer_index])
    gate_part = both[:, :FF]
    up_part = both[:, FF:]
    activated = (jax.nn.silu(gate_part) * up_part).astype(jnp.bfloat16)
    result = middle + project(activated, w_down[layer_index]).reshape(
        seq_count, part_len, model_width
    )
    saved = [
        (
            hidden,
            normed_flat,
            scale_one,
            q_heads,
            k_heads,
            v_heads,
            o_heads,
            log_total,
            attn_flat,
            middle,
            normed_two_flat,
            scale_two,
            gate_part,
            up_part,
            activated,
        )
    ]
    flowing = cotangent
    grads_qkv = [None] * LAYERS
    grads_out = [None] * LAYERS
    grads_gate_up = [None] * LAYERS
    grads_down = [None] * LAYERS
    gain_terms = [None] * LAYERS
    for layer_index in reversed(range(LAYERS)):
        (
            layer_in,
            normed_flat,
            scale_one,
            q_heads,
            k_heads,
            v_heads,
            o_heads,
            log_total,
            attn_flat,
            middle,
            normed_two_flat,
            scale_two,
            gate_part,
            up_part,
            activated,
        ) = saved[layer_index]
        gain = gains[layer_index]
        dm_cast = flowing.reshape(row_count, model_width).astype(jnp.bfloat16)
        dact, grads_down[layer_index] = backward_pair(dm_cast, activated, w_down[layer_index])
        sigma = jax.nn.sigmoid(gate_part)
        dgate = dact * up_part * sigma * (1.0 + gate_part * (1.0 - sigma))
        dup = dact * gate_part * sigma
        dgu = jnp.concatenate([dgate, dup], 1).astype(jnp.bfloat16)
        dnormed_two, grads_gate_up[layer_index] = backward_pair(
            dgu, normed_two_flat, w_gate_up[layer_index]
        )
        dnormed_two = dnormed_two.reshape(seq_count, part_len, model_width)
        dmid_norm, gain_two = normalize_back(dnormed_two, middle, scale_two, gain[1])
        dmiddle = flowing + dmid_norm
        dy_cast = dmiddle.reshape(row_count, model_width).astype(jnp.bfloat16)
        dattn_wide, grads_out[layer_index] = backward_pair(dy_cast, attn_flat, w_out[layer_index])
        dattn = dattn_wide.astype(jnp.bfloat16)
        dattn_heads = lax.all_to_all(
            dattn.reshape(seq_count, part_len, group_count, heads_dev * HD),
            "seq",
            split_axis=2,
            concat_axis=1,
            tiled=True,
        )
        dattn_heads = dattn_heads.reshape(seq_count, full_len, heads_dev, HD)
        dq_heads, dk_heads, dv_heads = lax.map(
            local_attend_back, (q_heads, k_heads, v_heads, o_heads, log_total, dattn_heads)
        )
        dkv_heads = jnp.concatenate([dk_heads, dv_heads], 2).reshape(
            seq_count, full_len, 1, 2 * kv_dev * HD
        )
        dq_tok, dkv_tok = (
            lax.all_to_all(
                dq_heads.reshape(seq_count, full_len, 1, heads_dev * HD),
                "seq",
                split_axis=1,
                concat_axis=2,
                tiled=True,
            ),
            lax.all_to_all(dkv_heads, "seq", split_axis=1, concat_axis=2, tiled=True),
        )
        dqueries = dq_tok.reshape(seq_count, part_len, H, HD)
        dkv_sum = jnp.einsum(
            "stnd,nm->stmd",
            dkv_tok.reshape(seq_count, part_len, group_count * 2 * kv_dev, HD),
            slot_onehot,
            preferred_element_type=jnp.float32,
        )
        dq_pre = unrotate(dqueries, cosines, sines)
        dk_pre = unrotate(dkv_sum[:, :, :KVH], cosines, sines)
        dvalues = dkv_sum[:, :, KVH:]
        djoint = jnp.concatenate(
            [
                dq_pre.reshape(row_count, -1),
                dk_pre.reshape(row_count, -1),
                dvalues.reshape(row_count, -1),
            ],
            1,
        ).astype(jnp.bfloat16)
        dnormed, grads_qkv[layer_index] = backward_pair(djoint, normed_flat, w_qkv[layer_index])
        dnormed = dnormed.reshape(seq_count, part_len, model_width)
        dcur_norm, gain_one = normalize_back(dnormed, layer_in, scale_one, gain[0])
        gain_terms[layer_index] = jnp.stack([gain_one, gain_two])
        flowing = dmiddle + dcur_norm
    gain_total = lax.psum(jnp.stack(gain_terms), ("fsdp", "seq"))
    return (
        result,
        flowing,
        gain_total,
        jnp.stack(grads_qkv),
        jnp.stack(grads_out),
        jnp.stack(grads_gate_up),
        jnp.stack(grads_down),
    )


def neighbour(values, step):
    count = lax.axis_size("seq")
    return lax.ppermute(values, "seq", [(i, i ^ step) for i in range(count)])


def matmul(left, right, left_dim, right_dim):
    return lax.dot_general(
        left, right, (((left_dim,), (right_dim,)), ((), ())), preferred_element_type=jnp.float32
    )


ROOT = HD ** (-0.5)
LIMIT = 60 * 1024 * 1024


def swap_halves(values):
    width = values.shape[1]
    half = HD // 2
    column = lax.broadcasted_iota(jnp.int32, values.shape, 1)
    return jnp.where(
        column % HD < half, pltpu.roll(values, width - half, 1), pltpu.roll(values, half, 1)
    )


def spread_tables(table, pairs, last):
    half = HD // 2
    cosines, sines = table[:, :half], table[:, half:]
    ones, zeros = jnp.ones_like(table), jnp.zeros_like(table)
    tail = [[cosines, cosines, ones], [-sines, sines, zeros]] if last else [[], []]
    if not pairs:
        return jnp.concatenate(tail[0], 1), jnp.concatenate(tail[1], 1)
    cosines = [jnp.concatenate([cosines] * 4, 1)] * pairs
    sines = [jnp.concatenate([-sines, sines] * 2, 1)] * pairs
    if last:
        cosines.append(jnp.concatenate(tail[0], 1))
        sines.append(jnp.concatenate(tail[1], 1))
    return jnp.concatenate(cosines, 1), jnp.concatenate(sines, 1)


MESH = pl.DeviceIdType.MESH


def seq_peer(step):
    return {"seq": lax.axis_index("seq") ^ step}


def fsdp_peer(place):
    return {"fsdp": place}


def remote(source, target, sems, slot, peer):
    return pltpu.make_async_remote_copy(
        src_ref=source,
        dst_ref=target,
        send_sem=sems[0].at[slot],
        recv_sem=sems[1].at[slot],
        device_id=peer,
        device_id_type=MESH,
    )


def gather_copies(own, slots, half, sems, base=0):
    top, bottom = pl.ds(0, half), pl.ds(half, own.shape[0] - half)

    def slot(step, rows):
        return slots.at[step].at[rows]

    return [
        remote(own.at[top], slot(1, top), sems, base, seq_peer(1)),
        remote(own.at[bottom], slot(2, bottom), sems, base + 1, seq_peer(2)),
        remote(own.at[bottom], slot(1, bottom), sems, base + 2, seq_peer(1)),
        remote(own.at[top], slot(2, top), sems, base + 3, seq_peer(2)),
        remote(slot(1, top), slot(3, top), sems, base + 4, seq_peer(2)),
        remote(slot(2, bottom), slot(3, bottom), sems, base + 5, seq_peer(1)),
    ]


def greet(peers):
    barrier = pltpu.get_barrier_semaphore()
    for peer in peers:
        pl.semaphore_signal(barrier, inc=1, device_id=peer, device_id_type=MESH)
    pl.semaphore_wait(barrier, len(peers))


def sum_copies(sent, side, below, far, half, sems, passed=None):
    top, bottom = pl.ds(0, half), pl.ds(half, half)
    return [
        remote(sent.at[3].at[top], side.at[1], sems, 0, seq_peer(1)),
        remote(sent.at[3].at[bottom], below.at[1], sems, 1, seq_peer(2)),
        remote(sent.at[2].at[bottom], below.at[0], sems, 2, seq_peer(2)),
        remote(sent.at[1].at[top], side.at[0], sems, 3, seq_peer(1)),
        remote(passed.at[0] if passed is not None else sent.at[2].at[top], far.at[0], sems, 4, seq_peer(2)),
        remote(passed.at[1] if passed is not None else sent.at[1].at[bottom], far.at[1], sems, 5, seq_peer(1)),
    ]


def pass_sums(turn, step, partial, sums, sent_ref, side_ref, below_ref, own_ref, half):
    wide, narrow = jnp.float32, jnp.bfloat16
    last = len(sums) // 2

    @pl.when(turn == last)
    def _():
        own_ref[...] = partial

    @pl.when(turn < last)
    def _():
        sent_ref[step] = partial.astype(narrow)

    @pl.when(turn == 0)
    def _():
        sums[0].start()
        sums[1].start()

    @pl.when(turn == 1)
    def _():
        sums[2].start()

    @pl.when(turn == 2)
    def _():
        sums[3].start()
        sums[0].wait_recv()
        sent_ref[2, :half] = (sent_ref[2, :half].astype(wide) + side_ref[1].astype(wide)).astype(narrow)
        sums[4].start()
        sums[1].wait_recv()
        sent_ref[1, half:] = (sent_ref[1, half:].astype(wide) + below_ref[1].astype(wide)).astype(narrow)
        sums[5].start()


def end_sums(sums, side_ref, below_ref, far_ref, own_ref, half):
    wide = jnp.float32
    sums[2].wait_recv()
    sums[3].wait_recv()
    own_ref[:half] += side_ref[0].astype(wide)
    own_ref[half:] += below_ref[0].astype(wide)
    sums[4].wait_recv()
    own_ref[:half] += far_ref[0].astype(wide)
    sums[5].wait_recv()
    own_ref[half:] += far_ref[1].astype(wide)


def share_own(own_ref, all_ref, half, sems, before):
    copies = gather_copies(own_ref, all_ref, half, sems, len(before))
    for copy in copies[:4]:
        copy.start()
    copies[0].wait_recv()
    copies[4].start()
    copies[1].wait_recv()
    copies[5].start()
    for copy in copies[2:]:
        copy.wait_recv()
    for copy in before + copies:
        copy.wait_send()


def enter_kernel(
    count, current_in, gain_ref, positions_ref, shard_ref, out_shard_ref, gate_up_ref, down_ref,
    all_ref, rows_ref, out_ref, table_ref, gate_up_part_ref, down_part_ref, scale_ref,
    current_ref, normed_ref, spots_ref, held_ref, part_ref, held_down,
    send_sems, recv_sems, spot_send, spot_recv, item_up, item_down, item_side, item_recv, local_sem,
):
    part, _ = current_ref.shape
    heads = H // count
    pieces = heads + 2
    items = pieces + lax.axis_size("fsdp")
    per_shard = shard_ref.shape[0] // HD
    out_rows, columns = out_shard_ref.shape[0], heads * HD
    chips = lax.axis_size("fsdp") // 2
    index = lax.axis_index("seq")
    place = lax.axis_index("fsdp")
    chip, core = place // 2, place % 2
    sems = (send_sems, recv_sems)

    take_current = pltpu.make_async_copy(current_in, current_ref, local_sem.at[items + 4])
    take_current.start()
    barrier = pltpu.get_barrier_semaphore()
    for peer in [seq_peer(step) for step in range(1, count)] + [fsdp_peer(place ^ 1)]:
        pl.semaphore_signal(barrier, inc=1, device_id=peer, device_id_type=MESH)

    @pl.when(chip > 0)
    def _():
        pl.semaphore_signal(barrier, inc=1, device_id=fsdp_peer(place - 2), device_id_type=MESH)

    @pl.when(chip < chips - 1)
    def _():
        pl.semaphore_signal(barrier, inc=1, device_id=fsdp_peer(place + 2), device_id_type=MESH)

    greetings = count + (chip > 0).astype(jnp.int32) + (chip < chips - 1).astype(jnp.int32)
    pl.semaphore_wait(barrier, greetings)

    part_rows = part_ref.shape[0]
    take = pltpu.make_async_copy(
        gate_up_ref.at[pl.ds(pl.multiple_of(index * part_rows, part_rows), part_rows)], part_ref, local_sem.at[items + 1]
    )
    take.start()
    take_down = pltpu.make_async_copy(down_ref, held_down, local_sem.at[items + 3])
    take_down.start()

    def qkv_item(item):
        block = jnp.where(
            item < heads, index * heads + item, jnp.where(item == heads, H + index, H + KVH + index)
        )
        source = shard_ref.at[pl.ds(pl.multiple_of(block % per_shard * HD, HD), HD)]
        return block // per_shard, source, rows_ref.at[pl.ds(pl.multiple_of(item * HD, HD), HD)], item

    def out_item(item):
        source = out_shard_ref.at[:, pl.ds(pl.multiple_of(index * columns, columns), columns)]
        target = out_ref.at[pl.ds(pl.multiple_of(item * out_rows, out_rows), out_rows)]
        return item, source, target, item + pieces

    kinds = ((qkv_item, pieces), (out_item, items - pieces))

    def item_copy(source, target, slot, sem, peer):
        return pltpu.make_async_remote_copy(
            src_ref=source,
            dst_ref=target,
            send_sem=sem.at[slot],
            recv_sem=item_recv.at[slot],
            device_id=fsdp_peer(peer),
            device_id_type=MESH,
        )

    def pass_on(source, target, slot, owner_chip, act):
        @pl.when((chip >= owner_chip) & (chip < chips - 1))
        def _():
            act(item_copy(source, target, slot, item_up, place + 2))

        @pl.when((chip <= owner_chip) & (chip > 0))
        def _():
            act(item_copy(source, target, slot, item_down, place - 2))

        act(item_copy(source, target, slot, item_side, place ^ 1))

    def send_own(item_of):
        def body(item, carry):
            owner, source, target, slot = item_of(item)

            @pl.when(place == owner)
            def _():
                pass_on(source, target, slot, owner // 2, lambda copy: copy.start())
                pltpu.make_async_copy(source, target, local_sem.at[slot]).start()

            return carry

        return body

    def pass_far(item_of, distance):
        def body(item, carry):
            owner, _, target, slot = item_of(item)
            owner_chip = owner // 2
            apart = jnp.where(chip > owner_chip, chip - owner_chip, owner_chip - chip)

            @pl.when((apart == distance) & (core == owner % 2))
            def _():
                item_copy(target, target, slot, item_side, place ^ 1).wait_recv()
                pass_on(target, target, slot, owner_chip, lambda copy: copy.start())

            return carry

        return body

    for item_of, number in kinds:
        lax.fori_loop(0, number, send_own(item_of), 0)
    take_current.wait()
    current = current_ref[...]
    scale = lax.rsqrt(jnp.mean(current * current, 1, keepdims=True) + EPS)
    scale_ref[...] = jnp.broadcast_to(scale, scale_ref.shape)
    normed_ref[...] = (current * scale * gain_ref[:1]).astype(jnp.bfloat16)
    copies = gather_copies(normed_ref, all_ref, part // 2, sems)
    for copy in copies[:4]:
        copy.start()
    spots_ref[...] = jnp.broadcast_to(positions_ref[...].astype(jnp.float32), spots_ref.shape)
    held_ref[0] = spots_ref[...]
    spot_copies = [
        remote(spots_ref, held_ref.at[step], (spot_send, spot_recv), step - 1, seq_peer(step))
        for step in range(1, count)
    ]
    for copy in spot_copies:
        copy.start()
    own = pltpu.make_async_copy(normed_ref, all_ref.at[0], local_sem.at[items])
    own.start()
    for distance in range(1, chips):
        for item_of, number in kinds:
            lax.fori_loop(0, number, pass_far(item_of, distance), 0)
            if distance == 1 and item_of is qkv_item:
                copies[0].wait_recv()
                copies[4].start()
                copies[1].wait_recv()
                copies[5].start()

    take.wait()
    put = pltpu.make_async_copy(part_ref, gate_up_part_ref, local_sem.at[items + 2])
    put.start()
    take_down.wait()
    columns_here = part_rows
    for device in range(count):

        @pl.when(index == device)
        def _():
            down_part_ref[...] = jnp.concatenate(
                [
                    held_down[:, start + device * columns_here : start + (device + 1) * columns_here]
                    for start in range(0, held_down.shape[1], count * columns_here)
                ],
                1,
            )

    for copy in spot_copies:
        copy.wait()
    half = HD // 2
    for step in range(count):
        spots = held_ref[step][:1]
        frequency = jnp.exp(
            lax.broadcasted_iota(jnp.int32, (half, 1), 0).astype(jnp.float32) * (-2.0 * math.log(10000.0) / HD)
        )
        angles = frequency * spots
        turned = jnp.concatenate([jnp.cos(angles), jnp.sin(angles)], 0)
        table_ref[pl.ds(step * part, part), :] = jnp.transpose(turned)

    def finish(item_of):
        def body(item, carry):
            owner, source, target, slot = item_of(item)

            @pl.when(core != owner % 2)
            def _():
                item_copy(target, target, slot, item_side, place ^ 1).wait_recv()

            @pl.when(place == owner)
            def _():
                pltpu.make_async_copy(source, target, local_sem.at[slot]).wait()

            @pl.when(core == owner % 2)
            def _():
                pass_on(target, target, slot, owner // 2, lambda copy: copy.wait_send())

            return carry

        return body

    for item_of, number in kinds:
        lax.fori_loop(0, number, finish(item_of), 0)
    own.wait()
    put.wait()
    for copy in copies[2:]:
        copy.wait_recv()
    for copy in copies:
        copy.wait_send()


def enter(current, gain, positions, shard, out_shard, gate_up, down, count):
    part, width = current.shape
    length = part * count
    heads = H // count
    pieces = heads + 2
    items = pieces + lax.axis_size("fsdp")
    vmem = pl.BlockSpec(memory_space=pltpu.VMEM)
    whole = pl.BlockSpec(memory_space=pl.ANY)
    part_shape = (gate_up.shape[0] // count, width)
    gathered, rows, out_cols, table, gate_up_part, down_part, scale = pl.pallas_call(
        lambda *refs: enter_kernel(count, *refs),
        out_shape=(
            jax.ShapeDtypeStruct((count, part, width), jnp.bfloat16),
            jax.ShapeDtypeStruct((pieces * HD, width), jnp.bfloat16),
            jax.ShapeDtypeStruct((out_shard.shape[0] * (items - pieces), heads * HD), jnp.bfloat16),
            jax.ShapeDtypeStruct((length, HD), jnp.float32),
            jax.ShapeDtypeStruct(part_shape, gate_up.dtype),
            jax.ShapeDtypeStruct((down.shape[0], down.shape[1] // count), down.dtype),
            jax.ShapeDtypeStruct((part, 128), jnp.float32),
        ),
        in_specs=[whole] + [vmem] * 2 + [whole] * 4,
        out_specs=[whole] * 3 + [vmem, whole] + [vmem] * 2,
        scratch_shapes=[
            pltpu.VMEM((part, width), jnp.float32),
            pltpu.VMEM((part, width), jnp.bfloat16),
            pltpu.VMEM((8, part), jnp.float32),
            pltpu.VMEM((count, 8, part), jnp.float32),
            pltpu.VMEM(part_shape, gate_up.dtype),
            pltpu.VMEM(down.shape, down.dtype),
            pltpu.SemaphoreType.DMA((6,)),
            pltpu.SemaphoreType.DMA((6,)),
            pltpu.SemaphoreType.DMA((count - 1,)),
            pltpu.SemaphoreType.DMA((count - 1,)),
            pltpu.SemaphoreType.DMA((items,)),
            pltpu.SemaphoreType.DMA((items,)),
            pltpu.SemaphoreType.DMA((items,)),
            pltpu.SemaphoreType.DMA((items,)),
            pltpu.SemaphoreType.DMA((items + 5,)),
        ],
        compiler_params=pltpu.CompilerParams(collective_id=1, has_side_effects=True, vmem_limit_bytes=LIMIT),
        name="enter",
    )(current, gain, positions, shard, out_shard, gate_up, down)
    return gathered.reshape(length, width), rows, out_cols, table, gate_up_part, down_part, scale


def qkv_kernel(index_ref, normed_ref, weight_ref, table_ref, q_ref, k_ref, v_ref):
    heads = q_ref.shape[0]
    joint = matmul(normed_ref[...], weight_ref[...], 1, 1)
    cosines, sines = spread_tables(table_ref[...], heads // 2, True)
    turned = joint * cosines + swap_halves(joint) * sines
    for head in range(heads):
        rounded = turned[:, head * HD : (head + 1) * HD].astype(jnp.bfloat16).astype(jnp.float32)
        q_ref[head] = (rounded * ROOT).astype(jnp.bfloat16)
    k_ref[...] = turned[:, heads * HD : (heads + 1) * HD].astype(jnp.bfloat16)
    v_ref[...] = turned[:, (heads + 1) * HD :].astype(jnp.bfloat16)


def project_qkv(index, normed, weight, table, count):
    length, width = normed.shape
    part = length // count
    heads = weight.shape[0] // HD - 2
    return pl.pallas_call(
        qkv_kernel,
        out_shape=(
            jax.ShapeDtypeStruct((heads, length, HD), jnp.bfloat16),
            jax.ShapeDtypeStruct((length, HD), jnp.bfloat16),
            jax.ShapeDtypeStruct((length, HD), jnp.bfloat16),
        ),
        grid_spec=pltpu.PrefetchScalarGridSpec(
            num_scalar_prefetch=1,
            grid=(count,),
            in_specs=[
                pl.BlockSpec((part, width), lambda i, s: (i, 0)),
                pl.BlockSpec(weight.shape, lambda i, s: (0, 0)),
                pl.BlockSpec((part, table.shape[1]), lambda i, s: (i, 0)),
            ],
            out_specs=[
                pl.BlockSpec((heads, part, HD), lambda i, s: (0, i ^ s[0], 0)),
                pl.BlockSpec((part, HD), lambda i, s: (i ^ s[0], 0)),
                pl.BlockSpec((part, HD), lambda i, s: (i ^ s[0], 0)),
            ],
        ),
        compiler_params=pltpu.CompilerParams(vmem_limit_bytes=LIMIT),
        name="project_qkv",
    )(index, normed, weight, table)


def attend_kernel(
    count, q_ref, k_ref, v_ref, weight_ref, current_ref, gain_ref,
    attn_ref, lse_ref, middle_ref, scale_ref, all_ref,
    held_ref, sent_ref, side_ref, below_ref, far_ref, two_ref, send_sems, recv_sems, own_sem,
):
    heads, _, _ = q_ref.shape
    part, _ = current_ref.shape
    half = part // 2
    index = lax.axis_index("seq")
    top, bottom = pl.ds(0, half), pl.ds(half, half)
    sems = (send_sems, recv_sems)
    greet([seq_peer(1), seq_peer(2)])
    sums = sum_copies(sent_ref, side_ref, below_ref, far_ref, half, sems)
    row = lax.broadcasted_iota(jnp.int32, (part, part), 0)
    column = lax.broadcasted_iota(jnp.int32, (part, part), 1)

    def one_part(turn, carry):
        step = count - 1 - turn
        here = step ^ index
        rows_here = pl.ds(pl.multiple_of(here * part, part), part)
        rows_step = pl.ds(pl.multiple_of(step * part, part), part)
        for block in range(count):

            @pl.when(here == block)
            def _():
                before = block * part
                seen = before + part
                keys_in, values_in = k_ref[:seen], v_ref[:seen]

                def one_head(head, carry):
                    scores = matmul(q_ref[head, before:seen, :], keys_in, 1, 1)
                    last = jnp.where(row >= column, scores[:, before:], -1e30)
                    scores = jnp.concatenate([scores[:, :before], last], 1) if block else last
                    peak = jnp.max(scores, 1, keepdims=True)
                    weights = jnp.exp(scores - peak)
                    total = jnp.sum(weights, 1, keepdims=True)
                    output = matmul(weights.astype(jnp.bfloat16), values_in, 1, 0) / total
                    held_ref[head] = output.astype(jnp.bfloat16)
                    log_total = jnp.broadcast_to(peak + jnp.log(total), (part, 128))
                    lse_ref[pl.ds(head, 1), before:seen] = jnp.transpose(log_total)[:1]
                    return carry

                lax.fori_loop(0, heads, one_head, 0, unroll=2)

        attn = jnp.concatenate([held_ref[head] for head in range(heads)], 1)
        attn_ref[rows_step, :] = attn
        partial = matmul(attn, weight_ref[...], 1, 1)

        pass_sums(turn, step, partial, sums, sent_ref, side_ref, below_ref, middle_ref, half)
        return carry

    lax.fori_loop(0, count, one_part, 0)
    end_sums(sums, side_ref, below_ref, far_ref, middle_ref, half)
    middle_ref[...] += current_ref[...]
    middle = middle_ref[...]
    scale = lax.rsqrt(jnp.mean(middle * middle, 1, keepdims=True) + EPS)
    scale_ref[...] = jnp.broadcast_to(scale, scale_ref.shape)
    two_ref[...] = (middle * scale * gain_ref[1:2]).astype(jnp.bfloat16)
    own = pltpu.make_async_copy(two_ref, all_ref.at[0], own_sem)
    share_own(two_ref, all_ref, half, sems, sums)
    own.start()
    own.wait()


def attend(queries, keys_in, values_in, weight, current, gain, count):
    heads, length, _ = queries.shape
    part, width = current.shape
    vmem = pl.BlockSpec(memory_space=pltpu.VMEM)
    attn, lse, middle, scale, gathered = pl.pallas_call(
        lambda *refs: attend_kernel(count, *refs),
        out_shape=(
            jax.ShapeDtypeStruct((length, heads * HD), jnp.bfloat16),
            jax.ShapeDtypeStruct((heads, length), jnp.float32),
            jax.ShapeDtypeStruct((part, width), jnp.float32),
            jax.ShapeDtypeStruct((part, 128), jnp.float32),
            jax.ShapeDtypeStruct((count, part, width), jnp.bfloat16),
        ),
        in_specs=[vmem] * 6,
        out_specs=[vmem] * 4 + [pl.BlockSpec(memory_space=pl.ANY)],
        scratch_shapes=[
            pltpu.VMEM((heads, part, HD), jnp.bfloat16),
            pltpu.VMEM((count, part, width), jnp.bfloat16),
            pltpu.VMEM((2, part // 2, width), jnp.bfloat16),
            pltpu.VMEM((2, part // 2, width), jnp.bfloat16),
            pltpu.VMEM((2, part // 2, width), jnp.bfloat16),
            pltpu.VMEM((part, width), jnp.bfloat16),
            pltpu.SemaphoreType.DMA((12,)),
            pltpu.SemaphoreType.DMA((12,)),
            pltpu.SemaphoreType.DMA,
        ],
        compiler_params=pltpu.CompilerParams(collective_id=2, has_side_effects=True, vmem_limit_bytes=LIMIT),
        name="attend",
    )(queries, keys_in, values_in, weight, current, gain)
    return attn, lse, middle, scale, gathered.reshape(length, width)


def share_start(copies):
    for group in copies:
        group[0].start()
        group[1].start()
    for group in copies:
        group[2].start()
        group[3].start()


def share_on(group):
    group[0].wait_recv()
    group[4].start()
    group[1].wait_recv()
    group[5].start()


def share_end(copies):
    for group in copies:
        for copy in group[2:]:
            copy.wait_recv()
    for group in copies:
        for copy in group:
            copy.wait_send()


def upper_half(rows):
    return -(-(rows // 2) // 16) * 16


def attend_back_kernel(
    count, q_in, k_in, v_in, attn_in, lse_in, dy_ref, weight_in, table_in, pick_ref, passed_ref, shard_ref,
    out_ref, turned_ref, term_ref, far_ref, slot_ref,
    q_ref, k_ref, v_ref, attn_ref, lse_ref, weight_ref, table_ref,
    do_ref, delta_ref, dq_ref, dk_ref, dv_ref, held_dy, held_pick,
    send_sems, recv_sems, load_sems,
):
    heads, length, _ = q_in.shape
    part = length // count
    wide = jnp.float32
    index = lax.axis_index("seq")
    load_weight = pltpu.make_async_copy(weight_in, weight_ref, load_sems.at[count + 1])
    load_weight.start()
    greet([seq_peer(1), seq_peer(2)])
    sems = (send_sems, recv_sems)
    sums = [
        remote(passed_ref.at[0], far_ref.at[0], sems, 6, seq_peer(2)),
        remote(passed_ref.at[1], far_ref.at[1], sems, 7, seq_peer(1)),
    ]
    group = gather_copies(shard_ref, slot_ref, upper_half(shard_ref.shape[0]), sems)
    share_start([group])
    for copy in sums:
        copy.start()

    def load_dy(step):
        rows = pl.ds(pl.multiple_of(step * part, part), part)
        return pltpu.make_async_copy(dy_ref.at[rows], held_dy.at[rows], load_sems.at[step])

    load = pltpu.make_async_copy(pick_ref, held_pick, load_sems.at[count])
    sources, targets = (attn_in, q_in, k_in, v_in, lse_in, table_in), (attn_ref, q_ref, k_ref, v_ref, lse_ref, table_ref)
    loads = [
        pltpu.make_async_copy(source, target, load_sems.at[count + 2 + number])
        for number, (source, target) in enumerate(zip(sources, targets))
    ]
    load_dy(index).start()
    for copy in loads:
        copy.start()
    for here in range(1, count):
        load_dy(here ^ index).start()
    load.start()
    load_weight.wait()
    for copy in loads:
        copy.wait()
    dk_ref[...] = jnp.zeros_like(dk_ref)
    dv_ref[...] = jnp.zeros_like(dv_ref)
    owner = lax.broadcasted_iota(jnp.int32, (heads, heads * HD), 1) // HD
    same = (owner == lax.broadcasted_iota(jnp.int32, (heads, heads * HD), 0)).astype(wide)
    row = lax.broadcasted_iota(jnp.int32, (part, part), 0)
    column = lax.broadcasted_iota(jnp.int32, (part, part), 1)

    def unturn(grads, cosines, sines):
        return grads * cosines + swap_halves(grads * sines)

    def one_part(here, carry):
        spot = here ^ index
        rows_here = pl.ds(pl.multiple_of(spot * part, part), part)
        load_dy(spot).wait()
        dattn = matmul(held_dy[rows_here, :], weight_ref[...], 1, 0).astype(jnp.bfloat16)
        product = dattn.astype(wide) * attn_ref[rows_here, :].astype(wide)
        delta_ref[...] = lax.dot_general(
            same, product, (((1,), (1,)), ((), ())), precision=lax.Precision.HIGHEST, preferred_element_type=wide
        )
        for head in range(heads):
            do_ref[head] = dattn[:, head * HD : (head + 1) * HD]
        for block in range(count):

            @pl.when(here == block)
            def _():
                before = block * part
                seen = before + part
                keys_in, values_in = k_ref[:seen], v_ref[:seen]

                def one_head(head, carry):
                    query, dout = q_ref[head, before:seen, :], do_ref[head]
                    scores = matmul(keys_in, query, 1, 1)
                    last = jnp.where(row <= column, scores[before:], -1e30)
                    scores = jnp.concatenate([scores[:before], last], 0) if block else last
                    probs = jnp.exp(scores - lse_ref[pl.ds(head, 1), before:seen])
                    dprob = matmul(values_in, dout, 1, 1)
                    dscore = (probs * (dprob - delta_ref[pl.ds(head, 1), :])).astype(jnp.bfloat16)
                    dv_ref[:seen] += matmul(probs.astype(jnp.bfloat16), dout, 1, 0)
                    dk_ref[:seen] += matmul(dscore, query, 1, 0)
                    dq_ref[head] = (matmul(dscore, keys_in, 0, 0) * ROOT).astype(jnp.bfloat16)
                    return carry

                lax.fori_loop(0, heads, one_head, 0, unroll=2)

        dq = jnp.concatenate([dq_ref[head] for head in range(heads)], 1).astype(wide)
        dq = unturn(dq, *spread_tables(table_ref[rows_here, :], heads // 2, False))
        out_ref[rows_here, : heads * HD] = dq.astype(jnp.bfloat16)

        @pl.when(here == 1)
        def _():
            share_on(group)

        return carry

    lax.fori_loop(0, count, one_part, 0)
    for block in range(count):
        rows_there = pl.ds(pl.multiple_of((block ^ index) * part, part), part)
        rows_block = slice(block * part, (block + 1) * part)
        both = jnp.concatenate([dk_ref[rows_block], dv_ref[rows_block]], 1).astype(jnp.bfloat16).astype(wide)
        both = unturn(both, *spread_tables(table_ref[rows_there, :], 0, True))
        out_ref[rows_there, heads * HD :] = both.astype(jnp.bfloat16)
    load.wait()
    chosen = matmul(held_pick[...], out_ref[...], 1, 1).astype(jnp.bfloat16)
    size = turned_ref.shape[1]
    for block in range(count):
        turned_ref[block] = chosen[block * size : (block + 1) * size]
    tile = 2 * 128

    def one_tile(number, carry):
        columns = pl.ds(pl.multiple_of(number * tile, tile), tile)
        term_ref[columns, :] = matmul(held_dy[:, columns], attn_ref[...], 0, 0).astype(jnp.bfloat16)
        return carry

    lax.fori_loop(0, held_dy.shape[1] // tile, one_tile, 0)
    for copy in sums:
        copy.wait_recv()
    share_end([group])
    for copy in sums:
        copy.wait_send()


def attend_back(queries, keys_in, values_in, attn, lse, dy, weight, table, pick, passed, shard, count):
    heads, length, _ = queries.shape
    part, width = length // count, dy.shape[1]
    columns = (heads + 2) * HD
    vmem, whole = pl.BlockSpec(memory_space=pltpu.VMEM), pl.BlockSpec(memory_space=pl.ANY)
    return pl.pallas_call(
        lambda *refs: attend_back_kernel(count, *refs),
        out_shape=[
            jax.ShapeDtypeStruct((length, columns), jnp.bfloat16),
            jax.ShapeDtypeStruct((count, columns // count, length), jnp.bfloat16),
            jax.ShapeDtypeStruct((width, heads * HD), jnp.bfloat16),
            jax.ShapeDtypeStruct((2, part // 2, width), jnp.bfloat16),
            jax.ShapeDtypeStruct((count,) + shard.shape, shard.dtype),
        ],
        in_specs=[whole] * 11,
        out_specs=[vmem] * 3 + [whole] * 2,
        scratch_shapes=[
            pltpu.VMEM(value.shape, value.dtype) for value in (queries, keys_in, values_in, attn, lse, weight, table)
        ]
        + [
            pltpu.VMEM((heads, part, HD), jnp.bfloat16),
            pltpu.VMEM((heads, part), jnp.float32),
            pltpu.VMEM((heads, part, HD), jnp.bfloat16),
            pltpu.VMEM((length, HD), jnp.float32),
            pltpu.VMEM((length, HD), jnp.float32),
        ]
        + [pltpu.VMEM(dy.shape, dy.dtype), pltpu.VMEM(pick.shape, pick.dtype)]
        + [pltpu.SemaphoreType.DMA((8,)), pltpu.SemaphoreType.DMA((8,)), pltpu.SemaphoreType.DMA((count + 8,))],
        compiler_params=pltpu.CompilerParams(collective_id=4, has_side_effects=True, vmem_limit_bytes=LIMIT),
        name="attend_back",
    )(queries, keys_in, values_in, attn, lse, dy, weight, table, pick, passed, shard)


def leave_kernel(
    count, grads_in, weight_in, first_in, scale_ref, gain_ref, other_ref, turned_ref, normed_in,
    own_ref, total_ref, term_ref,
    sent_ref, side_ref, below_ref, far_ref, slot_ref, whole_ref, normed_ref, first_ref, grads_ref, weight_ref,
    told_ref, heard_ref, send_sems, recv_sems, swap_send, swap_recv, load_sems, sum_send, sum_recv,
):
    part, _ = first_ref.shape
    half = part // 2
    size = turned_ref.shape[1]
    heads = H // count
    chunk = size // (heads + 2)
    index = lax.axis_index("seq")
    place = lax.axis_index("fsdp")
    peers = [seq_peer(step) for step in range(1, count)]
    fsdp_peers = [fsdp_peer(place ^ (1 << bit)) for bit in range(lax.axis_size("fsdp").bit_length() - 1)]
    greet(peers + fsdp_peers)
    swaps = [
        remote(turned_ref.at[index ^ step], slot_ref.at[step], (swap_send, swap_recv), step - 1, seq_peer(step))
        for step in range(1, count)
    ]
    for copy in swaps:
        copy.start()
    loads = [
        pltpu.make_async_copy(source, target, load_sems.at[number])
        for number, (source, target) in enumerate(
            (
                (turned_ref.at[index], slot_ref.at[0]),
                (normed_in, normed_ref),
                (first_in, first_ref),
                (grads_in, grads_ref),
                (weight_in, weight_ref),
            )
        )
    ]
    for number in (3, 4, 1, 0, 2):
        loads[number].start()
    total_ref[0:1] = jnp.zeros_like(other_ref)
    total_ref[1:2] = other_ref[...]
    for number in (3, 4, 1):
        loads[number].wait()
    sums = sum_copies(sent_ref, side_ref, below_ref, far_ref, half, (send_sems, recv_sems))

    def one_part(turn, carry):
        step = count - 1 - turn
        rows_step = pl.ds(pl.multiple_of(step * part, part), part)
        partial = matmul(grads_ref[rows_step, :], weight_ref[...], 1, 0)
        total_ref[0:1] += jnp.sum(partial * normed_ref[rows_step, :].astype(jnp.float32), 0, keepdims=True)
        pass_sums(turn, step, partial, sums, sent_ref, side_ref, below_ref, own_ref, half)
        return carry

    lax.fori_loop(0, count, one_part, 0)
    loads[0].wait()
    loads[2].wait()
    total_ref[0:1] = total_ref[0:1] / gain_ref[:1]
    tells = []
    for step, peer in enumerate(fsdp_peers):
        told_ref[step] = total_ref[...]
        tell = remote(told_ref.at[step], heard_ref.at[step], (sum_send, sum_recv), step, peer)
        tell.start()
        tell.wait_recv()
        total_ref[...] += heard_ref[step]
        tells.append(tell)
    first = len(tells)
    told_ref[first] = total_ref[...]
    for step, peer in enumerate(peers):
        tells.append(
            remote(told_ref.at[first], heard_ref.at[first + step], (sum_send, sum_recv), first + step, peer)
        )
        tells[-1].start()
    for step in range(count):
        if step:
            swaps[step - 1].wait_recv()
        peer = index ^ step
        for block in range(count):
            piece = slot_ref[step, :, (step ^ block) * part : ((step ^ block) + 1) * part]
            tokens = slice(block * part, (block + 1) * part)
            for start, rows in ((0, heads * chunk), (H * chunk, chunk), ((H + KVH) * chunk, chunk)):
                begin = 0 if start == 0 else heads * chunk + (0 if start == H * chunk else chunk)
                spot = pl.multiple_of(start + peer * rows, chunk)
                whole_ref[pl.ds(spot, rows), tokens] = piece[begin : begin + rows]
    term_ref[...] = matmul(whole_ref[...], normed_ref[...], 1, 0).astype(jnp.bfloat16)
    end_sums(sums, side_ref, below_ref, far_ref, own_ref, half)
    unit = first_ref[...] * scale_ref[:, :1]
    grads = own_ref[...]
    inner = grads * gain_ref[:1]
    own_ref[...] = scale_ref[:, :1] * (inner - unit * jnp.mean(inner * unit, 1, keepdims=True))
    for step in range(len(peers)):
        tells[first + step].wait_recv()
        total_ref[...] += heard_ref[first + step]
    for copy in sums + swaps + tells:
        copy.wait_send()


def leave(grads, weight, first, scale, gain, other, turned, normed, count):
    part, width = first.shape
    vmem, whole = pl.BlockSpec(memory_space=pltpu.VMEM), pl.BlockSpec(memory_space=pl.ANY)
    size, length = turned.shape[1:]
    steps = lax.axis_size("fsdp").bit_length() - 1 + count - 1
    own, total, term = pl.pallas_call(
        lambda *refs: leave_kernel(count, *refs),
        out_shape=(
            jax.ShapeDtypeStruct((part, width), jnp.float32),
            jax.ShapeDtypeStruct((2, width), jnp.float32),
            jax.ShapeDtypeStruct((size * count, width), jnp.bfloat16),
        ),
        in_specs=[whole] * 3 + [vmem] * 3 + [whole] * 2,
        out_specs=[vmem] * 3,
        scratch_shapes=[
            pltpu.VMEM((count, part, width), jnp.bfloat16),
            pltpu.VMEM((2, part // 2, width), jnp.bfloat16),
            pltpu.VMEM((2, part // 2, width), jnp.bfloat16),
            pltpu.VMEM((2, part // 2, width), jnp.bfloat16),
            pltpu.VMEM((count, size, length), jnp.bfloat16),
            pltpu.VMEM((count * size, length), jnp.bfloat16),
            pltpu.VMEM(normed.shape, jnp.bfloat16),
            pltpu.VMEM((part, width), jnp.float32),
            pltpu.VMEM(grads.shape, grads.dtype),
            pltpu.VMEM(weight.shape, weight.dtype),
            pltpu.VMEM((steps, 2, width), jnp.float32),
            pltpu.VMEM((steps, 2, width), jnp.float32),
            pltpu.SemaphoreType.DMA((6,)),
            pltpu.SemaphoreType.DMA((6,)),
            pltpu.SemaphoreType.DMA((count - 1,)),
            pltpu.SemaphoreType.DMA((count - 1,)),
            pltpu.SemaphoreType.DMA((5,)),
            pltpu.SemaphoreType.DMA((steps,)),
            pltpu.SemaphoreType.DMA((steps,)),
        ],
        compiler_params=pltpu.CompilerParams(collective_id=5, has_side_effects=True, vmem_limit_bytes=LIMIT),
        name="leave",
    )(grads, weight, first, scale, gain, other, turned, normed)
    return own, total, term


def join_rows_kernel(index_ref, own_ref, side_ref, below_ref, top_ref, bottom_ref, out_ref):
    step = pl.program_id(0) ^ index_ref[0]
    half = top_ref.shape[0]
    for number, ref in enumerate((own_ref, side_ref, below_ref)):

        @pl.when(step == number)
        def _():
            out_ref[...] = ref[...].astype(jnp.float32)

    @pl.when(step == 3)
    def _():
        out_ref[:half] = top_ref[...].astype(jnp.float32)
        out_ref[half:] = bottom_ref[...].astype(jnp.float32)


def join_rows(index, own, side, below, top, bottom, count):
    rows, width = own.shape
    parts = (own, side, below, top, bottom)
    return pl.pallas_call(
        join_rows_kernel,
        out_shape=jax.ShapeDtypeStruct((rows * count, width), jnp.float32),
        grid_spec=pltpu.PrefetchScalarGridSpec(
            num_scalar_prefetch=1,
            grid=(count,),
            in_specs=[pl.BlockSpec(part.shape, lambda i, s: (0, 0)) for part in parts],
            out_specs=pl.BlockSpec((rows, width), lambda i, s: (i, 0)),
        ),
        compiler_params=pltpu.CompilerParams(vmem_limit_bytes=LIMIT),
        name="join_rows",
    )(index, *parts)


def join_pieces_kernel(count, row_piece, column_piece, index_ref, own_ref, *refs):
    slot_refs, out_ref = refs[:-1], refs[-1]
    index = index_ref[0]
    rows, columns = own_ref.shape
    for device in range(count):
        if len(slot_refs) == 1:
            values = slot_refs[0][device ^ index]
        else:
            values = own_ref[...]
            for step, ref in enumerate(slot_refs):
                values = jnp.where(device ^ index == step + 1, ref[...], values)
        values = jnp.where(device == index, own_ref[...], values).astype(jnp.float32)
        for top in range(0, rows, row_piece):
            for left in range(0, columns, column_piece):
                down = top * count + device * row_piece if row_piece < rows else top
                across = left * count + device * column_piece if row_piece == rows else left
                out_ref[down : down + row_piece, across : across + column_piece] = values[
                    top : top + row_piece, left : left + column_piece
                ]


def join_pieces(index, own, slots, count, row_piece, column_piece):
    rows, columns = own.shape
    shape = (rows * count, columns) if row_piece < rows else (rows, columns * count)
    return pl.pallas_call(
        lambda *refs: join_pieces_kernel(count, row_piece, column_piece, *refs),
        out_shape=jax.ShapeDtypeStruct(shape, jnp.float32),
        grid_spec=pltpu.PrefetchScalarGridSpec(
            num_scalar_prefetch=1,
            grid=(1,),
            in_specs=[pl.BlockSpec(own.shape, lambda i, s: (0, 0))]
            + [pl.BlockSpec(slot.shape, lambda i, s, n=slot.ndim: (0,) * n) for slot in slots],
            out_specs=pl.BlockSpec(shape, lambda i, s: (0, 0)),
        ),
        compiler_params=pltpu.CompilerParams(vmem_limit_bytes=LIMIT),
        name="join_pieces",
    )(index, own, *slots)


def last_sums_kernel(base_ref, passed_ref, flowing_ref, piece_ref, result_ref, grad_ref):
    result_ref[...] = base_ref[...] + passed_ref[...].astype(jnp.float32)
    grad_ref[...] = flowing_ref[...] + piece_ref[...]


def last_sums(base, passed, flowing, piece):
    rows, width = base.shape
    tile = rows // 4
    block = pl.BlockSpec((tile, width), lambda i: (i, 0))
    return pl.pallas_call(
        last_sums_kernel,
        out_shape=[jax.ShapeDtypeStruct((rows, width), jnp.float32)] * 2,
        grid=(4,),
        in_specs=[block] * 4,
        out_specs=[block] * 2,
        compiler_params=pltpu.CompilerParams(vmem_limit_bytes=LIMIT),
        name="last_sums",
    )(base, passed, flowing, piece)


def greet_chain(count):
    place = lax.axis_index("fsdp")
    chips = lax.axis_size("fsdp") // 2
    chip = place // 2
    barrier = pltpu.get_barrier_semaphore()
    for peer in [seq_peer(step) for step in range(1, count)] + [fsdp_peer(place ^ 1)]:
        pl.semaphore_signal(barrier, inc=1, device_id=peer, device_id_type=MESH)

    @pl.when(chip > 0)
    def _():
        pl.semaphore_signal(barrier, inc=1, device_id=fsdp_peer(place - 2), device_id_type=MESH)

    @pl.when(chip < chips - 1)
    def _():
        pl.semaphore_signal(barrier, inc=1, device_id=fsdp_peer(place + 2), device_id_type=MESH)

    greetings = count + (chip > 0).astype(jnp.int32) + (chip < chips - 1).astype(jnp.int32)
    pl.semaphore_wait(barrier, greetings)


def weight_chain(item_of, number, sems):
    item_up, item_down, item_side, item_recv, local_sem = sems
    place = lax.axis_index("fsdp")
    chips = lax.axis_size("fsdp") // 2
    chip, core = place // 2, place % 2

    def item_copy(source, target, slot, sem, peer):
        return pltpu.make_async_remote_copy(
            src_ref=source,
            dst_ref=target,
            send_sem=sem.at[slot],
            recv_sem=item_recv.at[slot],
            device_id=fsdp_peer(peer),
            device_id_type=MESH,
        )

    def pass_on(source, target, slot, owner_chip, act):
        @pl.when((chip >= owner_chip) & (chip < chips - 1))
        def _():
            act(item_copy(source, target, slot, item_up, place + 2))

        @pl.when((chip <= owner_chip) & (chip > 0))
        def _():
            act(item_copy(source, target, slot, item_down, place - 2))

        act(item_copy(source, target, slot, item_side, place ^ 1))

    def send_own():
        def body(item, carry):
            owner, source, target, slot = item_of(item)

            @pl.when(place == owner)
            def _():
                pass_on(source, target, slot, owner // 2, lambda copy: copy.start())
                pltpu.make_async_copy(source, target, local_sem.at[slot]).start()

            return carry

        lax.fori_loop(0, number, body, 0)

    def pass_far(distance):
        def body(item, carry):
            owner, _, target, slot = item_of(item)
            owner_chip = owner // 2
            apart = jnp.where(chip > owner_chip, chip - owner_chip, owner_chip - chip)

            @pl.when((apart == distance) & (core == owner % 2))
            def _():
                item_copy(target, target, slot, item_side, place ^ 1).wait_recv()
                pass_on(target, target, slot, owner_chip, lambda copy: copy.start())

            return carry

        lax.fori_loop(0, number, body, 0)

    def finish():
        def body(item, carry):
            owner, source, target, slot = item_of(item)

            @pl.when(core != owner % 2)
            def _():
                item_copy(target, target, slot, item_side, place ^ 1).wait_recv()

            @pl.when(place == owner)
            def _():
                pltpu.make_async_copy(source, target, local_sem.at[slot]).wait()

            @pl.when(core == owner % 2)
            def _():
                pass_on(target, target, slot, owner // 2, lambda copy: copy.wait_send())

            return carry

        lax.fori_loop(0, number, body, 0)

    return send_own, pass_far, finish


def feed_kernel(
    count, normed_in, weight_in, dm_in, down_part_ref,
    gates_out, act_out, dm_out, term_out, down_ref,
    normed_ref, weight_ref, gates_ref, act_ref, dm_ref, term_ref,
    send_sems, recv_sems, load_sems, item_up, item_down, item_side, item_recv, local_sem,
    gates_sems, act_sems, dm_sem, term_sems,
):
    part, width = dm_in.shape
    units = act_ref.shape[1]
    chips = lax.axis_size("fsdp") // 2
    narrow = jnp.bfloat16
    load_weight = pltpu.make_async_copy(weight_in, weight_ref, load_sems.at[0])
    load_normed = pltpu.make_async_copy(normed_in, normed_ref, load_sems.at[1])
    load_weight.start()
    load_normed.start()
    greet_chain(count)
    down_rows = down_part_ref.shape[0]

    def down_item(item):
        target = down_ref.at[pl.ds(pl.multiple_of(item * down_rows, down_rows), down_rows)]
        return item, down_part_ref, target, item

    send_own, pass_far, finish = weight_chain(
        down_item, 2 * chips, (item_up, item_down, item_side, item_recv, local_sem)
    )
    send_own()
    group = gather_copies(dm_in, dm_ref, part // 2, (send_sems, recv_sems))
    share_start([group])
    dm_ref[0] = dm_in[...]
    load_normed.wait()
    load_weight.wait()

    def store_gates(step):
        rows = pl.ds(pl.multiple_of(step * part, part), part)
        return pltpu.make_async_copy(gates_ref.at[step % 2], gates_out.at[rows], gates_sems.at[step % 2])

    def store_act(step):
        rows = pl.ds(pl.multiple_of(step * part, part), part)
        return pltpu.make_async_copy(act_ref.at[rows], act_out.at[rows], act_sems.at[step])

    def one_part(step, carry):
        rows = pl.ds(pl.multiple_of(step * part, part), part)
        both = matmul(normed_ref[rows, :], weight_ref[...], 1, 1)

        @pl.when(step >= 2)
        def _():
            store_gates(step - 2).wait()

        gates_ref[step % 2] = both.astype(narrow)
        gate = both[:, :units]
        act_ref[rows, :] = (gate * jax.nn.sigmoid(gate) * both[:, units:]).astype(narrow)
        store_gates(step).start()
        store_act(step).start()

        @pl.when(step == count - 2)
        def _():
            share_on(group)
            pass_far(1)

        return carry

    lax.fori_loop(0, count, one_part, 0)
    pass_far(2)
    share_end([group])
    keep_dm = pltpu.make_async_copy(dm_ref, dm_out, dm_sem)
    keep_dm.start()
    tile = 2 * 128
    tiles = width // tile

    def store_term(number):
        rows = pl.ds(pl.multiple_of(number * tile, tile), tile)
        return pltpu.make_async_copy(term_ref.at[number % 2], term_out.at[rows], term_sems.at[number % 2])

    def one_tile(number, carry):
        @pl.when(number >= 2)
        def _():
            store_term(number - 2).wait()

        columns = pl.ds(pl.multiple_of(number * tile, tile), tile)
        upstream = dm_ref[:, :, columns].reshape(part * count, tile)
        term_ref[number % 2] = matmul(upstream, act_ref[...], 0, 0).astype(narrow)
        store_term(number).start()
        return carry

    lax.fori_loop(0, tiles, one_tile, 0)
    for distance in range(3, chips):
        pass_far(distance)
    for step in range(count - 2, count):
        store_gates(step).wait()
    for step in range(count):
        store_act(step).wait()
    keep_dm.wait()
    for number in range(tiles - 2, tiles):
        store_term(number).wait()
    finish()


def feed(normed, weight, dm, down_part, count):
    part, width = dm.shape
    length, units = part * count, down_part.shape[1]
    items = lax.axis_size("fsdp")
    vmem, whole = pl.BlockSpec(memory_space=pltpu.VMEM), pl.BlockSpec(memory_space=pl.ANY)
    gates, act, dm_all, term, down_cols = pl.pallas_call(
        lambda *refs: feed_kernel(count, *refs),
        out_shape=[
            jax.ShapeDtypeStruct((length, 2 * units), jnp.bfloat16),
            jax.ShapeDtypeStruct((length, units), jnp.bfloat16),
            jax.ShapeDtypeStruct((count, part, width), jnp.bfloat16),
            jax.ShapeDtypeStruct((width, units), jnp.bfloat16),
            jax.ShapeDtypeStruct((items * down_part.shape[0], units), jnp.bfloat16),
        ],
        in_specs=[whole] * 2 + [vmem] + [whole],
        out_specs=[whole] * 5,
        scratch_shapes=[
            pltpu.VMEM(normed.shape, normed.dtype),
            pltpu.VMEM(weight.shape, weight.dtype),
            pltpu.VMEM((2, part, 2 * units), jnp.bfloat16),
            pltpu.VMEM((length, units), jnp.bfloat16),
            pltpu.VMEM((count, part, width), jnp.bfloat16),
            pltpu.VMEM((2, 2 * 128, units), jnp.bfloat16),
            pltpu.SemaphoreType.DMA((6,)),
            pltpu.SemaphoreType.DMA((6,)),
            pltpu.SemaphoreType.DMA((2,)),
        ]
        + [pltpu.SemaphoreType.DMA((items,))] * 5
        + [
            pltpu.SemaphoreType.DMA((2,)),
            pltpu.SemaphoreType.DMA((count,)),
            pltpu.SemaphoreType.DMA,
            pltpu.SemaphoreType.DMA((2,)),
        ],
        compiler_params=pltpu.CompilerParams(collective_id=9, has_side_effects=True, vmem_limit_bytes=LIMIT),
        name="feed",
    )(normed, weight, dm, down_part)
    return gates, act, dm_all.reshape(length, width), term, down_cols


def norm_back_kernel(
    count, act_in, down_in, dm_in, gates_in, weight_in, flowing_in, middle_in, inputs_in, scale_ref, gain_ref,
    own_ref, gain_out_ref, dy_ref, term_ref, product_ref, from_side_ref, from_below_ref,
    act_ref, down_ref, dm_ref, gates_ref, grads_ref, weight_ref, flowing_ref, middle_ref, inputs_ref,
    held_ref, sent_ref, side_ref, below_ref, far_ref, stage_ref,
    send_sems, recv_sems, load_sems, part_sems, store_sems, product_sems,
):
    part, _ = flowing_in.shape
    half = part // 2
    wide, narrow = jnp.float32, jnp.bfloat16
    units = down_ref.shape[1]
    sems = (send_sems, recv_sems)

    def load(source, target, number):
        copy = pltpu.make_async_copy(source, target, load_sems.at[number])
        copy.start()
        return copy

    def load_parts(turn):
        rows = pl.ds(pl.multiple_of((count - 1 - turn) * part, part), part)
        slot = turn % 2
        return [
            pltpu.make_async_copy(dm_in.at[rows], dm_ref.at[slot], part_sems.at[0, slot]),
            pltpu.make_async_copy(gates_in.at[rows], gates_ref.at[slot], part_sems.at[1, slot]),
        ]

    firsts = [load(act_in, act_ref, 0), load(down_in, down_ref, 1)]
    for copy in load_parts(0):
        copy.start()
    load_weight = load(weight_in, weight_ref, 2)
    for copy in load_parts(1):
        copy.start()
    lasts = [load(inputs_in, inputs_ref, 3), load(flowing_in, flowing_ref, 4), load(middle_in, middle_ref, 5)]
    greet([seq_peer(1), seq_peer(2)])
    top, bottom = pl.ds(0, half), pl.ds(half, half)
    firsts_sums = [
        remote(held_ref.at[3].at[top], from_side_ref.at[1], sems, 6, seq_peer(1)),
        remote(held_ref.at[3].at[bottom], from_below_ref.at[1], sems, 7, seq_peer(2)),
        remote(held_ref.at[2].at[bottom], from_below_ref.at[0], sems, 8, seq_peer(2)),
        remote(held_ref.at[1].at[top], from_side_ref.at[0], sems, 9, seq_peer(1)),
    ]
    sums = sum_copies(sent_ref, side_ref, below_ref, far_ref, half, sems)
    for copy in firsts:
        copy.wait()

    def down_part(turn, carry):
        step = count - 1 - turn
        rows = pl.ds(pl.multiple_of(step * part, part), part)
        held_ref[step] = matmul(act_ref[rows, :], down_ref[...], 1, 1).astype(narrow)

        @pl.when(turn == 0)
        def _():
            firsts_sums[0].start()
            firsts_sums[1].start()

        @pl.when(turn == 1)
        def _():
            firsts_sums[2].start()

        @pl.when(turn == 2)
        def _():
            firsts_sums[3].start()

        return carry

    lax.fori_loop(0, count, down_part, 0)
    product = pltpu.make_async_copy(held_ref, product_ref, product_sems.at[0])
    product.start()
    load_weight.wait()

    def one_part(turn, carry):
        step = count - 1 - turn
        slot = turn % 2
        rows = pl.ds(pl.multiple_of(step * part, part), part)
        for copy in load_parts(turn):
            copy.wait()
        dact = matmul(dm_ref[slot], down_ref[...], 1, 0)
        gate = gates_ref[slot, :, :units].astype(wide)
        up = gates_ref[slot, :, units:].astype(wide)
        sigma = jax.nn.sigmoid(gate)
        grads_ref[rows, :units] = (dact * up * sigma * (1.0 + gate * (1.0 - sigma))).astype(narrow)
        grads_ref[rows, units:] = (dact * gate * sigma).astype(narrow)

        @pl.when(turn < count - 2)
        def _():
            for copy in load_parts(turn + 2):
                copy.start()

        partial = matmul(grads_ref[rows, :], weight_ref[...], 1, 0)

        @pl.when(turn == count - 1)
        def _():
            own_ref[...] = partial

        @pl.when(turn < count - 1)
        def _():
            sent_ref[step] = partial.astype(narrow)

        @pl.when(turn == 0)
        def _():
            sums[0].start()
            sums[1].start()

        @pl.when(turn == 1)
        def _():
            sums[2].start()

        @pl.when(turn == 2)
        def _():
            sums[3].start()

        return carry

    lax.fori_loop(0, count, one_part, 0)
    sums[0].wait_recv()
    sent_ref[2, :half] = (sent_ref[2, :half].astype(wide) + side_ref[1].astype(wide)).astype(narrow)
    sums[4].start()
    sums[1].wait_recv()
    sent_ref[1, half:] = (sent_ref[1, half:].astype(wide) + below_ref[1].astype(wide)).astype(narrow)
    sums[5].start()
    for copy in lasts:
        copy.wait()
    tile = stage_ref.shape[1]
    tiles = grads_ref.shape[1] // tile

    def store(number):
        rows = pl.ds(pl.multiple_of(number * tile, tile), tile)
        return pltpu.make_async_copy(stage_ref.at[number % 2], term_ref.at[rows], store_sems.at[number % 2])

    def one_tile(number, carry):
        @pl.when(number >= 2)
        def _():
            store(number - 2).wait()

        columns = pl.ds(pl.multiple_of(number * tile, tile), tile)
        stage_ref[number % 2] = matmul(grads_ref[:, columns], inputs_ref[...], 0, 0).astype(narrow)
        store(number).start()
        return carry

    lax.fori_loop(0, tiles, one_tile, 0)
    end_sums(sums, side_ref, below_ref, far_ref, own_ref, half)
    scale = scale_ref[:, :1]
    unit = middle_ref[...] * scale
    grads = own_ref[...]
    gain_out_ref[...] = jnp.sum(grads * unit, 0, keepdims=True)
    inner = grads * gain_ref[1:2]
    own_ref[...] = flowing_ref[...] + scale * (inner - unit * jnp.mean(inner * unit, 1, keepdims=True))
    dy_ref[...] = own_ref[...].astype(narrow)
    for number in range(tiles - 2, tiles):
        store(number).wait()
    product.wait()
    for copy in firsts_sums:
        copy.wait_recv()
    for copy in sums + firsts_sums:
        copy.wait_send()


def norm_back(act, down, dm, gates, weight, flowing, middle, inputs, scale, gain, count):
    part, width = flowing.shape
    units = gates.shape[1]
    tile = 2 * 128
    vmem, whole = pl.BlockSpec(memory_space=pltpu.VMEM), pl.BlockSpec(memory_space=pl.ANY)
    narrow, wide = jnp.bfloat16, jnp.float32
    pair = (2, part // 2, width)
    own, gain_term, dy, term, product, from_side, from_below = pl.pallas_call(
        lambda *refs: norm_back_kernel(count, *refs),
        out_shape=(
            jax.ShapeDtypeStruct((part, width), wide),
            jax.ShapeDtypeStruct((1, width), wide),
            jax.ShapeDtypeStruct((part, width), narrow),
            jax.ShapeDtypeStruct((units, width), narrow),
            jax.ShapeDtypeStruct((count, part, width), narrow),
            jax.ShapeDtypeStruct(pair, narrow),
            jax.ShapeDtypeStruct(pair, narrow),
        ),
        in_specs=[whole] * 8 + [vmem] * 2,
        out_specs=[vmem] * 3 + [whole] * 4,
        scratch_shapes=[
            pltpu.VMEM(act.shape, narrow),
            pltpu.VMEM(down.shape, narrow),
            pltpu.VMEM((2, part, width), narrow),
            pltpu.VMEM((2, part, units), narrow),
            pltpu.VMEM((part * count, units), narrow),
            pltpu.VMEM(weight.shape, narrow),
            pltpu.VMEM((part, width), wide),
            pltpu.VMEM((part, width), wide),
            pltpu.VMEM(inputs.shape, narrow),
            pltpu.VMEM((count, part, width), narrow),
            pltpu.VMEM((count, part, width), narrow),
            pltpu.VMEM(pair, narrow),
            pltpu.VMEM(pair, narrow),
            pltpu.VMEM(pair, narrow),
            pltpu.VMEM((2, tile, width), narrow),
            pltpu.SemaphoreType.DMA((10,)),
            pltpu.SemaphoreType.DMA((10,)),
            pltpu.SemaphoreType.DMA((6,)),
            pltpu.SemaphoreType.DMA((2, 2)),
            pltpu.SemaphoreType.DMA((2,)),
            pltpu.SemaphoreType.DMA((1,)),
        ],
        compiler_params=pltpu.CompilerParams(collective_id=3, has_side_effects=True, vmem_limit_bytes=67043328),
        name="norm_back",
    )(act, down, dm, gates, weight, flowing, middle, inputs, scale, gain)
    return own, gain_term[0], dy, term, product, from_side, from_below


def share_dy_kernel(
    dy_ref, down_ref, side_in, below_in, middle_in, all_ref, base_ref, passed_ref,
    piece_ref, side_ref, below_ref, send_sems, recv_sems, load_sems,
):
    part = dy_ref.shape[0]
    half = part // 2
    wide = jnp.float32
    top, bottom = pl.ds(0, half), pl.ds(half, half)
    loads = [
        pltpu.make_async_copy(down_ref.at[0], piece_ref.at[0], load_sems.at[0]),
        pltpu.make_async_copy(down_ref.at[2].at[top], piece_ref.at[1].at[top], load_sems.at[1]),
        pltpu.make_async_copy(down_ref.at[1].at[bottom], piece_ref.at[1].at[bottom], load_sems.at[2]),
        pltpu.make_async_copy(dy_ref, all_ref.at[0], load_sems.at[3]),
        pltpu.make_async_copy(side_in, side_ref, load_sems.at[4]),
        pltpu.make_async_copy(below_in, below_ref, load_sems.at[5]),
        pltpu.make_async_copy(middle_in, base_ref, load_sems.at[6]),
    ]
    greet([seq_peer(1), seq_peer(2)])
    group = gather_copies(dy_ref, all_ref, half, (send_sems, recv_sems))
    share_start([group])
    for load in loads:
        load.start()
    for load in loads:
        load.wait()
    base_ref[...] += piece_ref[0].astype(wide)
    base_ref[:half] += side_ref[0].astype(wide)
    base_ref[half:] += below_ref[0].astype(wide)
    passed_ref[0] = (piece_ref[1, :half].astype(wide) + side_ref[1].astype(wide)).astype(jnp.bfloat16)
    passed_ref[1] = (piece_ref[1, half:].astype(wide) + below_ref[1].astype(wide)).astype(jnp.bfloat16)
    share_on(group)
    share_end([group])


def share_dy(dy, down, side, below, middle, count):
    part, width = dy.shape
    vmem, whole = pl.BlockSpec(memory_space=pltpu.VMEM), pl.BlockSpec(memory_space=pl.ANY)
    gathered, base, passed = pl.pallas_call(
        lambda *refs: share_dy_kernel(*refs),
        out_shape=[
            jax.ShapeDtypeStruct((count, part, width), jnp.bfloat16),
            jax.ShapeDtypeStruct((part, width), jnp.float32),
            jax.ShapeDtypeStruct((2, part // 2, width), jnp.bfloat16),
        ],
        in_specs=[vmem] + [whole] * 4,
        out_specs=[whole, vmem, vmem],
        scratch_shapes=[
            pltpu.VMEM((2, part, width), jnp.bfloat16),
            pltpu.VMEM((2, part // 2, width), jnp.bfloat16),
            pltpu.VMEM((2, part // 2, width), jnp.bfloat16),
            pltpu.SemaphoreType.DMA((6,)),
            pltpu.SemaphoreType.DMA((6,)),
            pltpu.SemaphoreType.DMA((7,)),
        ],
        compiler_params=pltpu.CompilerParams(collective_id=8, has_side_effects=True, vmem_limit_bytes=LIMIT),
        name="share_dy",
    )(dy, down, side, below, middle)
    return gathered.reshape(part * count, width), base, passed


def fast_body(hidden, positions, gains, w_qkv, w_out, w_gate_up, w_down, cotangent):
    count = lax.axis_size("seq")
    index = lax.axis_index("seq")
    place = index.astype(jnp.int32).reshape(1)
    current = hidden[0]
    part_len, width = current.shape
    heads = H // count
    gain = gains[0]
    after = lax.optimization_barrier

    rows = w_qkv.shape[1]
    group = math.gcd(rows, HD)
    chunk = group // count
    per_head = HD // group
    normed_all, qkv_rows, out_cols, table, gate_up_part, down_part, scale_one = enter(
        current, gain, positions, w_qkv[0], w_out[0], w_gate_up[0], w_down[0], count
    )
    gu_rows = w_gate_up.shape[1] // count
    gate_up = lax.all_gather(gate_up_part, "fsdp", axis=0, tiled=True)
    down_rows = w_down.shape[1]

    queries, keys_in, values_in = project_qkv(place, normed_all, qkv_rows, table, count)
    attn_flat, log_total, middle, scale_two, normed_two_all = attend(
        queries, keys_in, values_in, out_cols, current, gain, count
    )
    flowing = cotangent[0]
    gates, activated, dm_all, term_down, down_cols = feed(
        normed_two_all, gate_up, flowing.astype(jnp.bfloat16), down_part, count
    )

    def owned(grad):
        return lax.psum_scatter(grad.astype(jnp.bfloat16), "fsdp", scatter_dimension=0, tiled=True)

    grad_down = owned(term_down)
    dmiddle, gain_two, dy, term_gate_up, down_sent, from_side, from_below = norm_back(
        activated, down_cols, dm_all, gates, gate_up, flowing, middle, normed_two_all, scale_two, gain, count
    )
    grad_gate_up = owned(term_gate_up)
    dy_all, base, passed = share_dy(dy, down_sent, from_side, from_below, middle, count)
    pieces = heads + 2
    picked = np.arange(pieces * HD).reshape(pieces * per_head, count, chunk).transpose(1, 0, 2).reshape(-1)
    pick = jnp.asarray(picked[:, None] == np.arange(pieces * HD)[None, :], jnp.bfloat16)
    djoint, djoint_turned, term_out, passed_on, down_slots = attend_back(
        queries, keys_in, values_in, attn_flat, log_total, dy_all, out_cols, table, pick, passed, grad_down, count
    )
    grad_out = owned(term_out)
    grad_piece, gain_total, term_qkv = leave(
        djoint, qkv_rows, current, scale_one, gain, gain_two[None], djoint_turned, normed_all, count
    )
    grad_qkv = owned(term_qkv)
    grad_gate_up, grad_piece = after((grad_gate_up, grad_piece))
    half = upper_half(gu_rows)
    side = neighbour(grad_gate_up, 1)
    below = neighbour(grad_gate_up, 2)
    far_top = neighbour(side[:half], 2)
    far_bottom = neighbour(below[half:], 1)
    down_shard = join_pieces(place, grad_down, (down_slots,), count, down_rows, gu_rows)
    result, grad_hidden = last_sums(base, passed_on.reshape(part_len, width), dmiddle, grad_piece)
    out_slots = [neighbour(grad_out, step) for step in range(1, count)]
    grad_qkv, out_slots = after((grad_qkv, out_slots))
    qkv_slots = [neighbour(grad_qkv, step) for step in range(1, count)]
    gate_up_shard = join_rows(place, grad_gate_up, side, below, far_top, far_bottom, count)
    out_shard = join_pieces(place, grad_out, out_slots, count, down_rows, heads * HD)
    qkv_shard = join_pieces(place, grad_qkv, qkv_slots, count, chunk, width)
    gain_total = gain_total[None]
    return (
        result[None],
        grad_hidden[None],
        gain_total,
        qkv_shard[None],
        out_shard[None],
        gate_up_shard[None],
        down_shard[None],
    )


def fits(mesh):
    count, fsdp = mesh.shape["seq"], mesh.shape["fsdp"]
    rows = (H + 2 * KVH) * HD // fsdp
    return count == KVH == 4 and fsdp % 2 == 0 and fsdp & (fsdp - 1) == 0 and rows % HD == 0


def solution(mesh):
    placed = (
        P("fsdp", "seq", None),
        P("fsdp", "seq"),
        P(),
        P(None, "fsdp", None),
        P(None, "fsdp", None),
        P(None, "fsdp", None),
        P(None, "fsdp", None),
        P("fsdp", "seq", None),
    )
    fast = fits(mesh)
    return jax.shard_map(
        fast_body if fast else body,
        mesh=mesh,
        in_specs=placed,
        out_specs=(
            P("fsdp", "seq", None),
            P("fsdp", "seq", None),
            P(),
            P(None, "fsdp", None),
            P(None, "fsdp", None),
            P(None, "fsdp", None),
            P(None, "fsdp", None),
        ),
        check_vma=False,
    )
```
